32 devices in a mesh: pipe: 2 (over core), fsdp: 4 (over z), tensor: 4 (over y, x).
Axes of the slice: x: 2, y: 2, z: 4, core: 2. Of those that a mesh axis runs over, the one named last changes fastest.
Arguments:
- layer_inputs: bfloat16 [4, 2048, 768], P(None, ('fsdp', 'tensor')), may hold values from -6 to 6
- cotangent: bfloat16 [4, 2048, 768], P(None, ('fsdp', 'tensor')), may hold values from -6 to 6
- input_master: float32 [2, 3, 768, 768], P('pipe', None, ('tensor', 'fsdp')), may hold values from -0.21875 to 0.21875
- output_master: float32 [2, 768, 768], P('pipe', ('tensor', 'fsdp')), may hold values from -1.75 to 1.75
- gate_master: float32 [2, 2, 3072, 768], P('pipe', None, ('tensor', 'fsdp')), may hold values from -0.21875 to 0.21875
- down_master: float32 [2, 3072, 768], P('pipe', ('tensor', 'fsdp')), may hold values from -0.109375 to 0.109375
- norm_tables: float32 [2, 4, 768], P('pipe'), may hold values from -2 to 2, as said below
- document_lengths: int32 [4, 4, 3], P(None, 'fsdp'), may hold values from 1 to 320, 512 in all within a row
Outputs:
- activations: float32 [2, 4, 2048, 768], P('pipe', None, ('fsdp', 'tensor'))
- input_gradient: float32 [2, 4, 2048, 768], P('pipe', None, ('fsdp', 'tensor'))
- input_master_gradient: float32 [2, 3, 768, 768], P('pipe', None, ('tensor', 'fsdp'))
- output_master_gradient: float32 [2, 768, 768], P('pipe', ('tensor', 'fsdp'))
- gate_master_gradient: float32 [2, 2, 3072, 768], P('pipe', None, ('tensor', 'fsdp'))
- down_master_gradient: float32 [2, 3072, 768], P('pipe', ('tensor', 'fsdp'))
- norm_tables_gradient: float32 [2, 4, 768], P('pipe')
The draws below stay inside these ranges and needn't reach their ends.
Inputs may be any that keep to these rules, and one draw needn't show every extreme that they name: `document_lengths`: the 3 lengths of each micro-batch of each group sum to 512. `norm_tables`: rows 0 and 2 of each section are gains, rows 1 and 3 shifts.
All inputs are finite; a program needn't handle non-finite values.
Results may differ from the reference program's by a relative error of at most 0.033.
Values may be sent and summed in bfloat16 or wider, within the bound.
A program may use at most 192 MiB of HBM per device.

```python
import math
import jax
import jax.numpy as jnp
import numpy as np
from jax import lax

D = 768
HEADS = 12
FF = 3072
HEAD_DIM = 64
MB_CAP = 512
MBS = 4
DOCS = 3
SECTIONS = 2
GROUPS = 4
TOKENS = 2048


def draw_norm_tables(key, part):
    noise = jnp.clip(jax.random.normal(key, (SECTIONS, 4, D), jnp.float32), -4.0, 4.0)
    parity = jnp.arange(4)[None, :, None] % 2
    return jnp.where(parity == 0, 1.0 + 0.2 * noise, 0.5 * noise)


def steps_of(key, extent, shards, low, high):
    def one(dim, parts):
        draws = jax.random.uniform(jax.random.fold_in(jax.random.fold_in(key, 6), dim), (parts,), jnp.float32, low / len(shards), high / len(shards))
        return jnp.repeat(jnp.exp(draws), extent[dim] // parts).reshape((-1,) + (1,) * (len(extent) - dim - 1))

    loudness = one(*shards[0])
    for cut in shards[1:]:
        loudness = loudness * one(*cut)
    return loudness


def profile(amount, total, most, slope):
    loads = [(1 << 20) // math.isqrt(grade ** slope) + 1 for grade in range(2, amount + 1)]
    surplus, given = total - most - (amount - 1), [1] * (amount - 1)
    while surplus > 0:
        candidates = [i for i in range(amount - 1) if given[i] < most]
        mass, budget = sum([loads[i] for i in candidates]), surplus
        for i in candidates:
            extra = min(most - given[i], max(1, budget * loads[i] // mass), surplus)
            given[i] = given[i] + extra
            surplus = surplus - extra
    return np.array([most] + given)


def uneven(key, amount, total, most, skew):
    if amount == 2:
        one = jax.random.randint(key, (), max(1, total - most), min(most, total - 1) + 1)
        return jnp.stack([one, total - one])
    tallies = jnp.asarray(profile(amount, total, most, skew), jnp.int32)
    twos = (amount - 1) // 2
    source_of, taker = tallies[1:1 + 2 * twos:2], tallies[2:2 + 2 * twos:2]
    room = jnp.minimum(source_of - 1, most - taker)
    shifted = jax.random.randint(jax.random.fold_in(key, 1), (twos,), 0, 1 << 20) % (room + 1)
    tallies = tallies.at[1:1 + 2 * twos:2].set(source_of - shifted).at[2:2 + 2 * twos:2].set(taker + shifted)
    return tallies[jax.random.permutation(jax.random.fold_in(key, 2), amount)]


def gaussian(stream_key, dims, deviation, reach, shards=(), held_as=jnp.bfloat16):
    drawn = deviation * jax.random.normal(stream_key, dims, jnp.float32)
    if shards:
        drawn = drawn * steps_of(stream_key, dims, shards, -0.22, 0.18)
    return jnp.clip(drawn, -reach, reach).astype(held_as)


def setup_inputs(seed: int = 0) -> dict:
    key_of = jax.random.split(jax.random.key(seed), 9)
    layer_inputs = gaussian(key_of[0], (MBS, TOKENS, D), 1.0, 6.0, ((1, 16),))
    cotangent = gaussian(key_of[1], (MBS, TOKENS, D), 1.0, 6.0, ((1, 16),))
    input_master = gaussian(key_of[2], (SECTIONS, 3, D, D), D ** -0.5, 0.21875, ((0, 2), (2, 16)), jnp.float32)
    output_master = gaussian(key_of[3], (SECTIONS, D, D), (D // 64) ** -0.5, 1.75, ((0, 2), (1, 16)), jnp.float32)
    gate_master = gaussian(key_of[4], (SECTIONS, 2, FF, D), D ** -0.5, 0.21875, ((0, 2), (2, 16)), jnp.float32)
    down_master = gaussian(key_of[5], (SECTIONS, FF, D), FF ** -0.5, 0.109375, ((0, 2), (1, 16)), jnp.float32)
    norm_tables = draw_norm_tables(jax.random.fold_in(key_of[8], 71), 0)
    document_lengths = jax.vmap(lambda own: uneven(own, DOCS, MB_CAP, MB_CAP * 5 // 8, 2))(jax.random.split(key_of[7], MBS * GROUPS)).reshape((MBS, GROUPS, DOCS)).astype(jnp.int32)
    return dict(layer_inputs=layer_inputs, cotangent=cotangent, input_master=input_master, output_master=output_master, gate_master=gate_master, down_master=down_master, norm_tables=norm_tables, document_lengths=document_lengths)


@jax.custom_vjp
def low(v):
    return lax.optimization_barrier(v.astype(jnp.bfloat16)).astype(jnp.float32)

@jax.custom_vjp
def low_back(v):
    return v

def low_keep(v):
    return (low(v), None)

def low_pass(kept, grad):
    return (grad,)

def back_keep(v):
    return (v, None)

def back_low(kept, grad):
    return (low(grad),)
low.defvjp(low_keep, low_pass)
low_back.defvjp(back_keep, back_low)
highest = lax.Precision.HIGHEST
epsilon = 1e-05
rope_base = 1000.0
masked_value = -1e+30

def segment_info(lengths):
    doc_ends = jnp.cumsum(lengths).astype(jnp.int32)
    starts = (doc_ends - lengths).astype(jnp.int32)
    places = jnp.arange(MB_CAP, dtype=jnp.int32)
    segment = lax.optimization_barrier(jnp.sum((places[:, None] >= doc_ends[None, :]).astype(jnp.int32), axis=1)).astype(jnp.int32)
    choose = segment[:, None] == jnp.arange(DOCS, dtype=jnp.int32)[None, :]
    offset = lax.optimization_barrier(jnp.sum(jnp.where(choose, starts[None, :], 0), axis=1)).astype(jnp.int32)
    return (segment, (places - offset).astype(jnp.int32))

def rotary_tables(position):
    half_dim = HEAD_DIM // 2
    frequency = rope_base ** (-2.0 * jnp.arange(half_dim, dtype=jnp.float32) / HEAD_DIM)
    angles = position.astype(jnp.float32)[:, None] * frequency[None, :]
    return (jnp.cos(angles)[:, None, :], jnp.sin(angles)[:, None, :])

def rotate(vectors, cosine, sines):
    half_dim = vectors.shape[-1] // 2
    first_half = vectors[..., :half_dim]
    second_half = vectors[..., half_dim:]
    return jnp.concatenate([first_half * cosine - second_half * sines, second_half * cosine + first_half * sines], axis=-1)

def layer_norm(summed, gain_row, shift_row):
    row_mean = lax.optimization_barrier(jnp.mean(summed, axis=-1, keepdims=True))
    centered = summed - row_mean
    inverse = lax.rsqrt(lax.optimization_barrier(jnp.mean(centered * centered, axis=-1, keepdims=True)) + epsilon)
    return centered * inverse * gain_row + shift_row

def layer_forward(token_rows, in_weight, out_weight, gate_weight, down_weight, norm_rows, segment, cosine, sines):
    tokens = token_rows.shape[0]
    shaped = (tokens, HEADS, HEAD_DIM)
    entries = low(token_rows)
    projected = low_back(jnp.einsum('td,chd->cth', entries, in_weight, precision=highest))
    queries = low(rotate(projected[0].reshape(shaped), cosine, sines))
    key_vecs = low(rotate(projected[1].reshape(shaped), cosine, sines))
    values = low(projected[2].reshape(shaped))
    block_rows = min(512, tokens)
    scaling = HEAD_DIM ** (-0.5)

    def attend(block_index):
        first_row = block_index * block_rows
        query_part = lax.dynamic_slice_in_dim(queries, first_row, block_rows, 0)
        segment_part = lax.dynamic_slice_in_dim(segment, first_row, block_rows, 0)
        scores = low_back(jnp.einsum('qhd,khd->hqk', query_part, key_vecs, precision=highest) * scaling)
        scores = jnp.where(segment_part[None, :, None] == segment[None, None, :], scores, masked_value)
        row_max = lax.optimization_barrier(jnp.max(scores, axis=-1, keepdims=True))
        weights_exp = jnp.exp(scores - row_max)
        chances = low(weights_exp / lax.optimization_barrier(jnp.sum(weights_exp, axis=-1, keepdims=True)))
        return jnp.einsum('hqk,khd->qhd', chances, values, precision=highest)
    context = lax.map(jax.checkpoint(attend), jnp.arange(tokens // block_rows, dtype=jnp.int32))
    context = low_back(low(context.reshape(tokens, D)))
    attended = low_back(jnp.dot(context, out_weight, precision=highest))
    middle = layer_norm(token_rows + attended, norm_rows[0], norm_rows[1])
    spread = low(middle)
    gate_up = low_back(jnp.einsum('td,chd->cth', spread, gate_weight, precision=highest))
    hidden = low(jax.nn.silu(gate_up[0]) * gate_up[1])
    feed_out = low_back(jnp.dot(hidden, down_weight, precision=highest))
    return layer_norm(middle + feed_out, norm_rows[2], norm_rows[3])

def reference(layer_inputs, cotangent, input_master, output_master, gate_master, down_master, norm_tables, document_lengths):
    item_count = MBS * GROUPS
    entering = layer_inputs.astype(jnp.float32).reshape(item_count, MB_CAP, D)
    upstream = cotangent.astype(jnp.float32).reshape(item_count, MB_CAP, D)
    segments, positions = jax.vmap(segment_info)(document_lengths.reshape(item_count, DOCS))
    cosines, sine_tables = jax.vmap(rotary_tables)(positions)

    def forward(first_input, in_master, out_master, gate_params, down_params, norm_params, extras):
        in_low = low(in_master)
        out_low = low(out_master)
        gate_low = low(gate_params)
        down_low = low(down_params)
        outputs = []
        current = first_input
        for section_num in range(SECTIONS):
            current = current + extras[section_num]

            def one_item(packed, section_num=section_num):
                token_rows, segment, cosine, sines = packed
                return layer_forward(token_rows, in_low[section_num], out_low[section_num], gate_low[section_num], down_low[section_num], norm_params[section_num], segment, cosine, sines)
            current = lax.map(jax.checkpoint(one_item), (current, segments, cosines, sine_tables))
            outputs.append(current)
        return jnp.stack(outputs)
    extras = jnp.zeros((SECTIONS, item_count, MB_CAP, D), jnp.float32)
    outputs, pullback = jax.vjp(forward, entering, input_master, output_master, gate_master, down_master, norm_tables, extras)
    seed_grad = jnp.zeros_like(outputs).at[SECTIONS - 1].set(upstream)
    gradients = pullback(seed_grad)
    shape_out = (SECTIONS, MBS, GROUPS * MB_CAP, D)
    return (outputs.reshape(shape_out), gradients[6].reshape(shape_out), gradients[1], gradients[2], gradients[3], gradients[4], gradients[5])
```

```python
import jax
import jax.numpy as jnp
from jax import lax
from jax.sharding import PartitionSpec as P

HEAD_DIM = 64
MB_CAP = 512
DOCS = 3

epsilon = 1e-05
rope_base = 1000.0
masked_value = -1e30

BF = jnp.bfloat16
F32 = jnp.float32


def segment_info(lengths):
    doc_ends = jnp.cumsum(lengths)
    starts = doc_ends - lengths
    places = jnp.arange(MB_CAP, dtype=jnp.int32)
    segment = jnp.sum((places[:, None] >= doc_ends[None, :]).astype(jnp.int32), axis=1)
    choose = segment[:, None] == jnp.arange(DOCS, dtype=jnp.int32)[None, :]
    offset = jnp.sum(jnp.where(choose, starts[None, :], 0), axis=1)
    return (segment, places - offset)


def rotary_tables(position):
    half_dim = HEAD_DIM // 2
    frequency = rope_base ** (-2.0 * jnp.arange(half_dim, dtype=F32) / HEAD_DIM)
    angles = position.astype(F32)[:, None] * frequency[None, :]
    return (jnp.cos(angles)[:, None, :], jnp.sin(angles)[:, None, :])


def rotate(vectors, cosine, sines):
    half_dim = vectors.shape[-1] // 2
    first_half = vectors[..., :half_dim]
    second_half = vectors[..., half_dim:]
    return jnp.concatenate(
        [first_half * cosine - second_half * sines, second_half * cosine + first_half * sines],
        axis=-1,
    )


def normed_parts(summed):
    row_mean = jnp.mean(summed, axis=-1, keepdims=True)
    centered = summed - row_mean
    inverse = lax.rsqrt(jnp.mean(centered * centered, axis=-1, keepdims=True) + epsilon)
    return (centered * inverse, inverse)


def norm_backward(normed, inverse, gain_row, upstream):
    scaled = upstream * gain_row
    through = inverse * (
        scaled
        - jnp.mean(scaled, axis=-1, keepdims=True)
        - normed * jnp.mean(scaled * normed, axis=-1, keepdims=True)
    )
    return (through, jnp.sum(upstream * normed, axis=0), jnp.sum(upstream, axis=0))


def flip(array, axis, bit):
    count = lax.axis_size(axis)
    return lax.ppermute(array, axis, [(i, i ^ bit) for i in range(count)])


def shifted(array, axis, by):
    count = lax.axis_size(axis)
    return lax.ppermute(array, axis, [(i, (i + by) % count) for i in range(count)])


def unxor(parts, index):
    parts = [jnp.where(index & 1, parts[m ^ 1], parts[m]) for m in range(4)]
    return [jnp.where(index & 2, parts[m ^ 2], parts[m]) for m in range(4)]


def pair_sum(partial):
    own = partial.astype(BF)
    other = flip(own, "pipe", 1)
    return own.astype(F32) + other.astype(F32)


def ring_gather(shard):
    count = lax.axis_size("fsdp")
    return [shard] + [shifted(shard, "fsdp", k) for k in range(1, count)]


def ring_reduce(parts):
    count = len(parts)
    total = parts[0].astype(F32)
    for k in range(1, count):
        total = total + shifted(parts[k].astype(BF), "fsdp", -k).astype(F32)
    return total


def plane_gather(column):
    half = column.shape[0] // 2
    across_x = flip(column, "tensor", 1)
    across_y = flip(column, "tensor", 2)
    first = flip(across_x[:half], "tensor", 2)
    second = flip(across_y[half:], "tensor", 1)
    return [column, across_x, across_y, jnp.concatenate([first, second], axis=0)]


def plane_reduce(columns):
    own, across_x, across_y, corner = columns
    half = own.shape[0] // 2
    first = flip(corner[:half], "tensor", 1)
    second = flip(corner[half:], "tensor", 2)
    to_y = jnp.concatenate(
        [(across_y[:half].astype(F32) + first.astype(F32)).astype(BF), across_y[half:]], axis=0
    )
    to_x = jnp.concatenate(
        [across_x[:half], (across_x[half:].astype(F32) + second.astype(F32)).astype(BF)], axis=0
    )
    from_y = flip(to_y, "tensor", 2)
    from_x = flip(to_x, "tensor", 1)
    return (own.astype(F32) + from_x.astype(F32) + from_y.astype(F32)).astype(BF)


def core_perms():
    both = ("pipe", "tensor")
    count = lax.axis_size("tensor")

    def at(core, place):
        return core * count + place

    one = [(at(0, t), at(1, t ^ 2)) for t in range(count)]
    one += [(at(1, t), at(0, t)) for t in range(count)]
    two = [(at(0, t), at(0, t ^ 1)) for t in range(count)]
    two += [(at(1, t), at(1, t ^ 2)) for t in range(count)]
    three = [(at(0, t), at(1, t ^ 3)) for t in range(count)]
    three += [(at(1, t), at(0, t ^ 1)) for t in range(count)]
    four = [(at(1, t), at(1, t ^ 3)) for t in range(count)]
    four += [(at(0, t), at(0, t)) for t in range(count)]
    return both, (one, two, three, four)


def back(pairs):
    return [(b, a) for a, b in pairs]


def gather_heads(column, core):
    both, perms = core_perms()
    got = [lax.ppermute(column, both, perm) for perm in perms]
    first = [column, got[0], got[1], got[2]]
    slots = [jnp.where(core == 0, a, b) for a, b in zip(first, got)]
    return ([slots[0], slots[2]], [slots[1], slots[3]])


def reduce_heads(layer_a, layer_b, core):
    both, perms = core_perms()
    slots = [layer_a[0], layer_b[0], layer_a[1], layer_b[1]]
    sent = [
        slots[0],
        jnp.where(core == 0, slots[1], slots[0]),
        jnp.where(core == 0, slots[2], slots[1]),
        jnp.where(core == 0, slots[3], slots[2]),
        jnp.where(core == 0, slots[0], slots[3]),
    ]
    got = [lax.ppermute(part, both, back(perm)) for part, perm in zip(sent[1:], perms)]
    total = got[0].astype(F32)
    for part in got[1:]:
        total = total + part.astype(F32)
    return total.astype(BF)


def layer_forward(x, weights, norm_rows, same, cosine, sines):
    in_weight, out_weight, gate_weight, down_weight = weights
    tokens = x.shape[0]
    shaped = (tokens, out_weight.shape[0] // HEAD_DIM, HEAD_DIM)
    xb = x.astype(BF)
    projected = jnp.einsum("td,chd->cth", xb, in_weight, preferred_element_type=F32)
    queries = rotate(projected[0].reshape(shaped), cosine, sines).astype(BF)
    key_vecs = rotate(projected[1].reshape(shaped), cosine, sines).astype(BF)
    values = projected[2].reshape(shaped).astype(BF)
    scores = jnp.einsum("qhd,khd->hqk", queries, key_vecs, preferred_element_type=F32)
    scores = jnp.where(same[None], scores * HEAD_DIM ** (-0.5), masked_value)
    row_max = jnp.max(scores, axis=-1, keepdims=True)
    weights_exp = jnp.exp(scores - row_max)
    chances = weights_exp / jnp.sum(weights_exp, axis=-1, keepdims=True)
    context = jnp.einsum(
        "hqk,khd->qhd", chances.astype(BF), values, preferred_element_type=F32
    ).astype(BF)
    context = context.reshape(tokens, shaped[1] * HEAD_DIM)
    pre_middle = x + pair_sum(jnp.dot(context, out_weight, preferred_element_type=F32))
    normed_one, inverse_one = normed_parts(pre_middle)
    middle = normed_one * norm_rows[0] + norm_rows[1]
    spread = middle.astype(BF)
    gate_up = jnp.einsum("td,chd->cth", spread, gate_weight, preferred_element_type=F32)
    hidden = (jax.nn.silu(gate_up[0]) * gate_up[1]).astype(BF)
    pre_output = middle + pair_sum(jnp.dot(hidden, down_weight, preferred_element_type=F32))
    normed_two, inverse_two = normed_parts(pre_output)
    output = normed_two * norm_rows[2] + norm_rows[3]
    kept = (xb, queries, key_vecs, values, chances, context, normed_one, inverse_one, spread,
            gate_up, hidden, normed_two, inverse_two)
    return (output, kept)


def layer_backward(weights, norm_rows, cosine, sines, upstream, kept):
    in_weight, out_weight, gate_weight, down_weight = weights
    (xb, queries, key_vecs, values, chances, context, normed_one, inverse_one, spread,
     gate_up, hidden, normed_two, inverse_two) = kept
    tokens = xb.shape[0]
    shaped = queries.shape
    grad_pre_output, gain_two, shift_two = norm_backward(
        normed_two, inverse_two, norm_rows[2], upstream
    )
    grad_feed = grad_pre_output.astype(BF)
    grad_hidden = jnp.einsum("td,hd->th", grad_feed, down_weight, preferred_element_type=F32)
    grad_down = jnp.einsum("th,td->hd", hidden, grad_feed, preferred_element_type=F32).astype(BF)
    sigmoid = jax.nn.sigmoid(gate_up[0])
    grad_gate = grad_hidden * gate_up[1] * sigmoid * (1.0 + gate_up[0] * (1.0 - sigmoid))
    grad_up = grad_hidden * gate_up[0] * sigmoid
    grad_gate_up = jnp.stack([grad_gate, grad_up]).astype(BF)
    grad_gate_weight = jnp.einsum(
        "cth,td->chd", grad_gate_up, spread, preferred_element_type=F32
    ).astype(BF)
    grad_middle = grad_pre_output + pair_sum(
        jnp.einsum("cth,chd->td", grad_gate_up, gate_weight, preferred_element_type=F32)
    )
    grad_pre_middle, gain_one, shift_one = norm_backward(
        normed_one, inverse_one, norm_rows[0], grad_middle
    )
    grad_attended = grad_pre_middle.astype(BF)
    grad_context = (
        jnp.einsum("td,hd->th", grad_attended, out_weight, preferred_element_type=F32)
        .astype(BF)
        .reshape(shaped)
    )
    grad_out_weight = jnp.einsum(
        "th,td->hd", context, grad_attended, preferred_element_type=F32
    ).astype(BF)
    scaling = HEAD_DIM ** (-0.5)
    grad_values = jnp.einsum(
        "hqk,qhd->khd", chances.astype(BF), grad_context, preferred_element_type=F32
    )
    grad_chances = jnp.einsum("qhd,khd->hqk", grad_context, values, preferred_element_type=F32)
    row_dot = jnp.sum(chances * grad_chances, axis=-1, keepdims=True)
    grad_scores = (chances * (grad_chances - row_dot)).astype(BF)
    grad_queries = scaling * jnp.einsum(
        "hqk,khd->qhd", grad_scores, key_vecs, preferred_element_type=F32
    )
    grad_keys = scaling * jnp.einsum(
        "hqk,qhd->khd", grad_scores, queries, preferred_element_type=F32
    )
    flat_shape = (tokens, shaped[1] * HEAD_DIM)
    grad_projected = jnp.stack(
        [
            rotate(grad_queries, cosine, -sines).reshape(flat_shape),
            rotate(grad_keys, cosine, -sines).reshape(flat_shape),
            grad_values.reshape(flat_shape),
        ]
    ).astype(BF)
    grad_in_weight = jnp.einsum(
        "cth,td->chd", grad_projected, xb, preferred_element_type=F32
    ).astype(BF)
    grad_rows = grad_pre_middle + pair_sum(
        jnp.einsum("cth,chd->td", grad_projected, in_weight, preferred_element_type=F32)
    )
    norm_grad = jnp.stack([gain_one, shift_one, gain_two, shift_two])
    return (grad_rows, (grad_in_weight, grad_out_weight, grad_gate_weight, grad_down), norm_grad)


def to_item(array, place):
    def piece(k):
        return lax.dynamic_index_in_dim(array, place ^ k, 0, keepdims=False)

    parts = [piece(0)] + [flip(piece(k), "tensor", k) for k in range(1, 4)]
    return jnp.concatenate(unxor(parts, place), axis=0)


def from_item(item, place):
    rows = item.shape[0] // 4

    def piece(k):
        return lax.dynamic_slice_in_dim(item, (place ^ k) * rows, rows, 0)

    parts = [piece(0)] + [flip(piece(k), "tensor", k) for k in range(1, 4)]
    return jnp.stack(unxor(parts, place))


def body(
    layer_inputs,
    cotangent,
    input_master,
    output_master,
    gate_master,
    down_master,
    norm_tables,
    document_lengths,
):
    core = lax.axis_index("pipe")
    place = lax.axis_index("tensor")
    group = lax.axis_index("fsdp")
    ring = lax.axis_size("fsdp")
    width = layer_inputs.shape[2]
    head_rows = input_master.shape[2]
    half_units = down_master.shape[1] // 2

    lengths = lax.dynamic_index_in_dim(document_lengths[:, 0, :], place, 0, keepdims=False)
    segment, position = segment_info(lengths)
    same = segment[:, None] == segment[None, :]
    cosine, sines = rotary_tables(position)

    x = to_item(layer_inputs, place).astype(F32)
    upstream = to_item(cotangent, place).astype(F32)
    norm_own = norm_tables[0]
    norm_other = flip(norm_own, "pipe", 1)
    norms = [
        jnp.where(core == 0, norm_own, norm_other),
        jnp.where(core == 0, norm_other, norm_own),
    ]

    head_shard = jnp.concatenate([input_master[0], output_master], axis=0).astype(BF)
    head_slots = ring_gather(head_shard.reshape(4 * head_rows, width))
    ascending = jnp.stack(head_slots[::-1] + head_slots[::-1])
    column = lax.dynamic_slice_in_dim(ascending, ring - 1 - group, ring, 0)
    column = column.reshape(ring, 4, head_rows, width).transpose(1, 0, 2, 3)
    column = column.reshape(4, ring * head_rows, width)
    heads = gather_heads(column, core)

    units = jnp.concatenate([gate_master[0], down_master], axis=0).astype(BF)
    units = units.reshape(3, 2, half_units, width)
    mine = lax.dynamic_index_in_dim(units, core, 1, keepdims=False)
    theirs = flip(lax.dynamic_index_in_dim(units, 1 - core, 1, keepdims=False), "pipe", 1)
    unit_shards = [jnp.where(core == 0, mine, theirs), jnp.where(core == 0, theirs, mine)]

    layers = []
    for s in range(2):
        blocks = jnp.concatenate(heads[s], axis=1)
        slots = ring_gather(unit_shards[s])
        planes = plane_gather(jnp.stack(slots))
        feed = jnp.concatenate(planes, axis=0).transpose(1, 0, 2, 3)
        feed = feed.reshape(3, -1, width)
        layers.append((blocks[:3], blocks[3], feed[:2], feed[2]))

    kept = []
    outputs = []
    current = x
    for s in range(2):
        current, saved = layer_forward(current, layers[s], norms[s], same, cosine, sines)
        outputs.append(current)
        kept.append(saved)
    activations = from_item(
        jnp.where(core == 0, outputs[0], outputs[1]).astype(BF), place
    ).astype(F32)

    grads = [None, None]
    input_grads = [None, None]
    norm_grads = [None, None]
    for s in (1, 0):
        upstream, grads[s], norm_grads[s] = layer_backward(
            layers[s], norms[s], cosine, sines, upstream, kept[s]
        )
        input_grads[s] = upstream
    gradients_in = from_item(
        jnp.where(core == 0, input_grads[0], input_grads[1]).astype(BF), place
    ).astype(F32)

    unit_totals = [None, None]
    head_parts = [None, None]
    for s in (1, 0):
        grad_in, grad_out, grad_gate, grad_down = grads[s]
        feed = jnp.concatenate([grad_gate, grad_down[None]], axis=0)
        feed = feed.reshape(3, 4, ring, half_units, width).transpose(1, 2, 0, 3, 4)
        owned = plane_reduce([feed[i] for i in range(4)])
        unit_totals[s] = ring_reduce([owned[k] for k in range(ring)]).astype(BF)
        blocks = jnp.concatenate([grad_in, grad_out[None]], axis=0)
        head_parts[s] = jnp.split(blocks, 2, axis=1)
    column = reduce_heads(head_parts[0], head_parts[1], core)
    column = column.reshape(4, ring, head_rows, width).transpose(1, 0, 2, 3)
    ascending = jnp.concatenate([column, column], axis=0)
    rolled = lax.dynamic_slice_in_dim(ascending, (group + 1) % ring, ring, 0)
    head_total = ring_reduce([rolled[ring - 1 - k] for k in range(ring)])

    mine = jnp.where(core == 0, unit_totals[0], unit_totals[1])
    theirs = flip(jnp.where(core == 0, unit_totals[1], unit_totals[0]), "pipe", 1)
    low = jnp.where(core == 0, mine, theirs)
    high = jnp.where(core == 0, theirs, mine)
    unit_total = jnp.concatenate([low, high], axis=1).astype(F32)

    norm_sum = jnp.where(core == 0, norm_grads[0], norm_grads[1])
    bit = 1
    while bit < ring:
        norm_sum = norm_sum + flip(norm_sum, "fsdp", bit)
        bit = bit * 2
    for bit in (1, 2):
        norm_sum = norm_sum + flip(norm_sum, "tensor", bit)
    return (
        activations[None],
        gradients_in[None],
        head_total[None, :3],
        head_total[None, 3],
        unit_total[None, :2],
        unit_total[None, 2],
        norm_sum[None],
    )


def solution(mesh):
    placed = (
        P(None, ("fsdp", "tensor"), None),
        P(None, ("fsdp", "tensor"), None),
        P("pipe", None, ("tensor", "fsdp"), None),
        P("pipe", ("tensor", "fsdp"), None),
        P("pipe", None, ("tensor", "fsdp"), None),
        P("pipe", ("tensor", "fsdp"), None),
        P("pipe", None, None),
        P(None, "fsdp", None),
    )
    return jax.shard_map(
        body,
        mesh=mesh,
        in_specs=placed,
        out_specs=(
            P("pipe", None, ("fsdp", "tensor"), None),
            P("pipe", None, ("fsdp", "tensor"), None),
            P("pipe", None, ("tensor", "fsdp"), None),
            P("pipe", ("tensor", "fsdp"), None),
            P("pipe", None, ("tensor", "fsdp"), None),
            P("pipe", ("tensor", "fsdp"), None),
            P("pipe", None, None),
        ),
        check_vma=False,
    )
```

```python
import jax
import jax.numpy as jnp
from jax import lax
from jax.experimental import pallas as pl
from jax.experimental.pallas import tpu as pltpu
from jax.sharding import PartitionSpec as P

HEAD_DIM = 64
MB_CAP = 512
DOCS = 3

epsilon = 1e-05
rope_base = 1000.0
masked_value = -1e30

BF = jnp.bfloat16
PIPE, FSDP, TENSOR = "pipe", "fsdp", "tensor"
F32 = jnp.float32


def segment_info(lengths):
    doc_ends = jnp.cumsum(lengths)
    starts = doc_ends - lengths
    places = jnp.arange(MB_CAP, dtype=jnp.int32)
    segment = jnp.sum((places[:, None] >= doc_ends[None, :]).astype(jnp.int32), axis=1)
    choose = segment[:, None] == jnp.arange(DOCS, dtype=jnp.int32)[None, :]
    offset = jnp.sum(jnp.where(choose, starts[None, :], 0), axis=1)
    return (segment, places - offset)


def rotary_tables(position):
    half_dim = HEAD_DIM // 2
    frequency = rope_base ** (-2.0 * jnp.arange(half_dim, dtype=F32) / HEAD_DIM)
    angles = position.astype(F32)[:, None] * frequency[None, :]
    cosine, sine = jnp.cos(angles), jnp.sin(angles)
    return jnp.tile(cosine, (1, 4)), jnp.tile(jnp.concatenate([-sine, sine], axis=1), (1, 2))


def flip(array, axis, bit):
    count = lax.axis_size(axis)
    return lax.ppermute(array, axis, [(i, i ^ bit) for i in range(count)])


def shifted(array, axis, by):
    count = lax.axis_size(axis)
    return lax.ppermute(array, axis, [(i, (i + by) % count) for i in range(count)])


def unxor(parts, index):
    parts = [jnp.where(index & 1, parts[m ^ 1], parts[m]) for m in range(4)]
    return [jnp.where(index & 2, parts[m ^ 2], parts[m]) for m in range(4)]


def mixed_flip(array, core_bit, place_bits):
    count = lax.axis_size(TENSOR)
    pairs = [
        (c * count + t, (c ^ core_bit) * count + (t ^ place_bits))
        for c in range(2)
        for t in range(count)
    ]
    return lax.ppermute(array, (PIPE, TENSOR), pairs)


def ring_gather(shard, tag):
    count = lax.axis_size(FSDP)
    slots = [shard]
    for k in range(1, count):
        with jax.named_scope(f"z{k}_{tag}"):
            slots.append(shifted(shard, FSDP, k))
    return slots


def ring_reduce(parts, tag):
    count = len(parts)
    total = parts[0].astype(F32)
    for k in range(1, count):
        with jax.named_scope(f"z{k}_{tag}"):
            part = shifted(parts[k].astype(BF), FSDP, -k)
        total = total + part.astype(F32)
    return total


def cross(array, axis, bit, tag):
    with jax.named_scope(tag):
        return flip(array, axis, bit)


def spread_out(column, tag):
    neighbour = cross(column, TENSOR, 2, "y_" + tag)
    return [
        column,
        neighbour,
        cross(column, PIPE, 1, "c_" + tag),
        cross(neighbour, PIPE, 1, "n_" + tag),
    ]


def added(a, b):
    return (a.astype(F32) + b.astype(F32)).astype(BF)


def row_norm(summed):
    centered = summed - jnp.mean(summed, axis=-1, keepdims=True)
    inverse = lax.rsqrt(jnp.mean(centered * centered, axis=-1, keepdims=True) + epsilon)
    return centered * inverse, inverse


def row_norm_back(normed, inverse, gain_row, upstream):
    scaled = upstream * gain_row
    through = inverse * (
        scaled
        - jnp.mean(scaled, axis=-1, keepdims=True)
        - normed * jnp.mean(scaled * normed, axis=-1, keepdims=True)
    )
    sums = [
        jnp.sum(upstream * normed, axis=0, keepdims=True),
        jnp.sum(upstream, axis=0, keepdims=True),
    ]
    return through, jnp.concatenate(sums + [jnp.zeros((6, sums[0].shape[1]), F32)], axis=0)


def nn(a, b):
    return lax.dot_general(a, b, (((1,), (0,)), ((), ())), preferred_element_type=F32)


def nt(a, b):
    return lax.dot_general(a, b, (((1,), (1,)), ((), ())), preferred_element_type=F32)


def tn(a, b):
    return lax.dot_general(a, b, (((0,), (0,)), ((), ())), preferred_element_type=F32)


def turned(slab, cosine, sines):
    lane = lax.broadcasted_iota(jnp.int32, slab.shape, 1)
    swapped = jnp.where(
        lane % HEAD_DIM < HEAD_DIM // 2, pltpu.roll(slab, 96, 1), pltpu.roll(slab, 32, 1)
    )
    return slab * cosine + swapped * sines


def head_masks(rows):
    lane = lax.broadcasted_iota(jnp.int32, (rows, 128), 1)
    low = (lane < HEAD_DIM).astype(F32)
    return low, 1.0 - low


def rows_of(half, columns, rows):
    return pl.BlockSpec((rows, columns), lambda i: (half, 0))


def whole(array):
    zeros = (0,) * array.ndim
    return pl.BlockSpec(array.shape, lambda i: zeros)


ANYWHERE = pl.BlockSpec(memory_space=pl.ANY)


def staged(tag, kernel, ins, outs, before, scratch=()):
    before = list(before or [])
    arrays = [array for array, _ in ins] + before
    specs = [spec for _, spec in ins] + [ANYWHERE] * len(before)
    first_out = len(outs) - len(before)
    first_in = len(ins)
    count = len(before)

    def run(*refs):
        kernel(*refs[:first_in], *refs[first_in + count:])

    call = pl.pallas_call(
        run,
        grid=(1,),
        in_specs=specs,
        out_specs=[spec for _, _, spec in outs],
        out_shape=[jax.ShapeDtypeStruct(shape, kind) for shape, kind, _ in outs],
        scratch_shapes=list(scratch),
        input_output_aliases={first_in + i: first_out + i for i in range(count)},
        compiler_params=pltpu.CompilerParams(vmem_limit_bytes=40 << 20),
        cost_estimate=pl.CostEstimate(flops=1024, bytes_accessed=1024, transcendentals=0),
        name=kernel.__name__,
    )
    with jax.named_scope("k_" + tag):
        return call(*arrays)


def project(tag, half, sources, norm_rows, weight, cosine, sines, before):
    given = len(sources) == 1
    total, width = sources[0].shape
    heads = weight.shape[1]
    rows = total // 2

    def project_kernel(*refs):
        if given:
            x_ref, w_ref, cos_ref, sin_ref, q_ref, k_ref, v_ref = refs
            low = x_ref[...]
        else:
            (mid_ref, own_ref, got_ref, norm_ref, w_ref, cos_ref, sin_ref,
             q_ref, k_ref, v_ref, x_ref, low_ref) = refs
            summed = mid_ref[...] + own_ref[...].astype(F32) + got_ref[...].astype(F32)
            x = row_norm(summed)[0] * norm_ref[2:3] + norm_ref[3:4]
            x_ref[...] = x
            low = x.astype(BF)
            low_ref[...] = low
        cosine, sines = cos_ref[...], sin_ref[...]
        for c, out in ((0, q_ref), (1, k_ref)):
            turning = nt(low, w_ref[c])
            for slab in range(heads // 128):
                at = slice(128 * slab, 128 * slab + 128)
                out[:, at] = turned(turning[:, at], cosine, sines).astype(BF)
        v_ref[...] = nt(low, w_ref[2]).astype(BF)

    here = rows_of(half, width, rows)
    ins = [(sources[0], here)]
    outs = [((total, heads), BF, rows_of(half, heads, rows)) for _ in range(3)]
    if not given:
        plain = pl.BlockSpec((rows, width), lambda i: (0, 0))
        ins += [(sources[1], plain), (sources[2], plain), (norm_rows, whole(norm_rows))]
        outs += [((total, width), F32, here), ((total, width), BF, here)]
    ins += [(weight, whole(weight))]
    ins += [(table, rows_of(half, 128, rows)) for table in (cosine, sines)]
    return staged(tag, project_kernel, ins, outs, before)


def attend(tag, half, queries, key_vecs, values, segment_column, segment_row, out_weight, before):
    total, heads = queries.shape
    width = out_weight.shape[1]
    rows = total // 2

    def attend_kernel(q_ref, k_ref, v_ref, col_ref, row_ref, w_ref, part_ref, ctx_ref, lse_ref):
        masks = head_masks(rows)
        lane = lax.broadcasted_iota(jnp.int32, (rows, 128), 1)
        same = col_ref[:, :1] == row_ref[:1, :]
        totals = jnp.zeros((rows, 128), F32)
        for slab in range(heads // 128):
            at = slice(128 * slab, 128 * slab + 128)
            q, k, v = q_ref[:, at], k_ref[:, at], v_ref[:, at]
            gathered = jnp.zeros((rows, 128), F32)
            for h in range(2):
                scores = nt(q * masks[h].astype(BF), k) * HEAD_DIM ** (-0.5)
                scores = jnp.where(same, scores, masked_value)
                top = jnp.max(scores, axis=-1, keepdims=True)
                powers = jnp.exp(scores - top)
                mass = jnp.sum(powers, axis=-1, keepdims=True)
                chances = (powers * (1.0 / mass)).astype(BF)
                gathered = gathered + nn(chances, v) * masks[h]
                totals = jnp.where(lane == 2 * slab + h, top + jnp.log(mass), totals)
            ctx_ref[:, at] = gathered.astype(BF)
        lse_ref[...] = totals.T[:8]
        part_ref[...] = nn(ctx_ref[...], w_ref[...]).astype(BF)

    ins = [
        (queries, rows_of(half, heads, rows)),
        (key_vecs, whole(key_vecs)),
        (values, whole(values)),
        (segment_column, rows_of(half, 128, rows)),
        (segment_row, whole(segment_row)),
        (out_weight, whole(out_weight)),
    ]
    outs = [
        ((rows, width), BF, pl.BlockSpec((rows, width), lambda i: (0, 0))),
        ((total, heads), BF, rows_of(half, heads, rows)),
        ((8, total), F32, pl.BlockSpec((8, rows), lambda i: (0, half))),
    ]
    return staged(tag, attend_kernel, ins, outs, before)


def feed_scratch(blocks, rows, width):
    return [
        pltpu.VMEM((len(blocks),) + blocks[0].shape, BF),
        pltpu.VMEM((rows, width), F32),
        pltpu.SemaphoreType.DMA((len(blocks),)),
    ]


def fetch_blocks(block_refs, buffer, sems):
    for j, ref in enumerate(block_refs):
        pltpu.make_async_copy(ref, buffer.at[j], sems.at[j]).start()


def share_blocks(p, block_refs, buffer, sems):
    each = len(block_refs) // 2
    for j in range(p * each, p * each + each):
        pltpu.make_async_copy(block_refs[j], buffer.at[j], sems.at[j]).wait()

    def joined(c):
        return jnp.concatenate([buffer[p * each + j, c] for j in range(each)], axis=0)

    return joined(0), joined(1), joined(2)


def feed(tag, half, x, own, got, norm_rows, blocks, before):
    total, width = x.shape
    rows = total // 2
    step = len(blocks) // 2 * blocks[0].shape[1]
    units = len(blocks) * blocks[0].shape[1]
    count = len(blocks)

    def feed_kernel(*refs):
        x_ref, own_ref, got_ref, norm_ref = refs[:4]
        block_refs = refs[4:4 + count]
        (part_ref, mid_ref, low_ref, gate_ref, up_ref, own_hid, other_hid,
         buffer, acc_ref, sems) = refs[4 + count:]
        fetch_blocks(block_refs, buffer, sems)
        summed = x_ref[...] + own_ref[...].astype(F32) + got_ref[...].astype(F32)
        middle = row_norm(summed)[0] * norm_ref[0:1] + norm_ref[1:2]
        mid_ref[...] = middle
        low = middle.astype(BF)
        low_ref[...] = low
        for p in range(2):
            gate_w, up_w, down_w = share_blocks(p, block_refs, buffer, sems)
            at = slice(p * step, p * step + step)
            gate = nt(low, gate_w)
            up = nt(low, up_w)
            gate_ref[:, at] = gate.astype(BF)
            up_ref[:, at] = up.astype(BF)
            hidden = (gate * jax.nn.sigmoid(gate) * up).astype(BF)
            (own_hid, other_hid)[p][...] = hidden
            fed = nn(hidden, down_w)
            acc_ref[...] = fed if p == 0 else acc_ref[...] + fed
        part_ref[...] = acc_ref[...].astype(BF)

    plain = pl.BlockSpec((rows, width), lambda i: (0, 0))
    here = rows_of(half, width, rows)
    wide = rows_of(half, units, rows)
    ins = [(x, here), (own, plain), (got, plain), (norm_rows, whole(norm_rows))]
    ins += [(block, ANYWHERE) for block in blocks]
    outs = [((rows, width), BF, plain), ((total, width), F32, here), ((total, width), BF, here)]
    outs += [((total, units), BF, wide) for _ in range(2)]
    outs += [((total, step), BF, rows_of(half, step, rows)) for _ in range(2)]
    return staged(tag, feed_kernel, ins, outs, before, feed_scratch(blocks, rows, width))


def feed_back(tag, half, sources, middle, own, got, norm_rows, gate, up, blocks, before):
    top = len(sources) == 1
    total, width = middle.shape
    rows = total // 2
    step = len(blocks) // 2 * blocks[0].shape[1]
    units = len(blocks) * blocks[0].shape[1]
    count = len(blocks)

    def feed_back_kernel(*refs):
        taken = len(sources)
        mid_ref, own_ref, got_ref, norm_ref, gate_ref, up_ref = refs[taken:taken + 6]
        block_refs = refs[taken + 6:taken + 6 + count]
        (part_ref, sums_ref, edge_ref, pre_ref, feed_ref, own_grads, other_grads,
         buffer, acc_ref, sems) = refs[taken + 6 + count:]
        fetch_blocks(block_refs, buffer, sems)
        summed = mid_ref[...] + own_ref[...].astype(F32) + got_ref[...].astype(F32)
        normed, inverse = row_norm(summed)
        if top:
            upstream = refs[0][...].astype(F32)
            edge_ref[...] = (normed * norm_ref[2:3] + norm_ref[3:4]).astype(BF)
        else:
            upstream = refs[0][...] + refs[1][...].astype(F32) + refs[2][...].astype(F32)
            edge_ref[...] = upstream.astype(BF)
        through, sums_ref[...] = row_norm_back(normed, inverse, norm_ref[2:3], upstream)
        pre_ref[...] = through
        low = through.astype(BF)
        feed_ref[...] = low
        for p in range(2):
            gate_w, up_w, down_w = share_blocks(p, block_refs, buffer, sems)
            at = slice(p * step, p * step + step)
            gate, up = gate_ref[:, at].astype(F32), up_ref[:, at].astype(F32)
            grad_hidden = nt(low, down_w)
            sigmoid = jax.nn.sigmoid(gate)
            grad_gate = (grad_hidden * up * sigmoid * (1.0 + gate * (1.0 - sigmoid))).astype(BF)
            grad_up = (grad_hidden * gate * sigmoid).astype(BF)
            share_ref = (own_grads, other_grads)[p]
            share_ref[:, :step] = grad_gate
            share_ref[:, step:] = grad_up
            back_through = nn(grad_gate, gate_w) + nn(grad_up, up_w)
            acc_ref[...] = back_through if p == 0 else acc_ref[...] + back_through
        part_ref[...] = acc_ref[...].astype(BF)

    plain = pl.BlockSpec((rows, width), lambda i: (0, 0))
    here = rows_of(half, width, rows)
    wide = rows_of(half, units, rows)
    ins = [(sources[0], here)] + [(source, plain) for source in sources[1:]]
    ins += [(middle, here), (own, plain), (got, plain), (norm_rows, whole(norm_rows))]
    ins += [(gate, wide), (up, wide)] + [(block, ANYWHERE) for block in blocks]
    outs = [((rows, width), BF, plain), ((8, width), F32, pl.BlockSpec((8, width), lambda i: (0, 0)))]
    outs += [((total, width), BF, here), ((total, width), F32, here), ((total, width), BF, here)]
    outs += [((total, units), BF, wide) for _ in range(2)]
    return staged(tag, feed_back_kernel, ins, outs, before, feed_scratch(blocks, rows, width))


def attend_back(tag, half, grad_middle, x, own, got, norm_rows, queries, key_vecs, values, totals,
                segment_column, segment_row, out_weight, cosine, sines, partial, before):
    total, heads = queries.shape
    width = out_weight.shape[1]
    rows = total // 2
    last = partial is not None

    def attend_back_kernel(*refs):
        (pre_ref, fed_ref, fed_got_ref, x_ref, own_ref, got_ref, norm_ref, q_ref, k_ref, v_ref,
         lse_ref, col_ref, row_ref, w_ref, cos_ref, sin_ref) = refs[:16]
        if last:
            dk_in, dv_in = refs[16:18]
        sums_ref, dk_ref, dv_ref, mid_ref, att_ref, dq_ref, dctx_ref = refs[18 if last else 16:]
        upstream = pre_ref[...] + fed_ref[...].astype(F32) + fed_got_ref[...].astype(F32)
        summed = x_ref[...] + own_ref[...].astype(F32) + got_ref[...].astype(F32)
        normed, inverse = row_norm(summed)
        through, sums_ref[...] = row_norm_back(normed, inverse, norm_ref[0:1], upstream)
        mid_ref[...] = through
        low = through.astype(BF)
        att_ref[...] = low
        dctx_ref[...] = nt(low, w_ref[...]).astype(BF)
        masks = head_masks(rows)
        wide_masks = head_masks(total)
        same = col_ref[:, :1] == row_ref[:1, :]
        scaling = HEAD_DIM ** (-0.5)
        here = pl.ds(half * rows, rows)
        cosine, sines = cos_ref[...], sin_ref[...]
        for slab in range(heads // 128):
            at = slice(128 * slab, 128 * slab + 128)
            q, k, v, grad_ctx = q_ref[:, at], k_ref[:, at], v_ref[:, at], dctx_ref[:, at]
            dq = jnp.zeros((rows, 128), F32)
            dk = jnp.zeros((total, 128), F32)
            dv = jnp.zeros((total, 128), F32)
            for h in range(2):
                mask = masks[h].astype(BF)
                scores = nt(k, q * mask) * scaling
                scores = jnp.where(same, scores, masked_value)
                chances = jnp.exp(scores - lse_ref[2 * slab + h:2 * slab + h + 1, :])
                grad_chances = nt(v, grad_ctx * mask)
                row_dot = jnp.sum(chances * grad_chances, axis=0, keepdims=True)
                grad_scores = (chances * (grad_chances - row_dot)).astype(BF)
                dv = dv + nn(chances.astype(BF), grad_ctx) * wide_masks[h]
                dk = dk + nn(grad_scores, q) * wide_masks[h]
                dq = dq + tn(grad_scores, k) * masks[h]
            dq_ref[:, at] = turned(dq * scaling, cos_ref[here, :], -sin_ref[here, :]).astype(BF)
            if last:
                dk = dk_in[:, at] + dk
                dv = dv_in[:, at] + dv
                dk_ref[:, at] = turned(dk * scaling, cosine, -sines).astype(BF)
                dv_ref[:, at] = dv.astype(BF)
            else:
                dk_ref[:, at] = dk
                dv_ref[:, at] = dv

    plain = pl.BlockSpec((rows, width), lambda i: (0, 0))
    here = rows_of(half, width, rows)
    ins = [(grad_middle[0], here), (grad_middle[1], plain), (grad_middle[2], plain)]
    ins += [(x, here), (own, plain), (got, plain), (norm_rows, whole(norm_rows))]
    ins += [(queries, rows_of(half, heads, rows)), (key_vecs, whole(key_vecs)),
            (values, whole(values)), (totals, pl.BlockSpec((8, rows), lambda i: (0, half))),
            (segment_column, whole(segment_column)),
            (segment_row, pl.BlockSpec((8, rows), lambda i: (0, half))),
            (out_weight, whole(out_weight)), (cosine, whole(cosine)), (sines, whole(sines))]
    if last:
        ins += [(part, whole(part)) for part in partial]
    kind = BF if last else F32
    all_rows = pl.BlockSpec((total, heads), lambda i: (0, 0))
    outs = [((8, width), F32, pl.BlockSpec((8, width), lambda i: (0, 0))),
            ((total, heads), kind, all_rows), ((total, heads), kind, all_rows),
            ((total, width), F32, here), ((total, width), BF, here),
            ((total, heads), BF, rows_of(half, heads, rows))]
    return staged(tag, attend_back_kernel, ins, outs, before, [pltpu.VMEM((rows, heads), BF)])


def inputs_back(tag, half, grads, weight):
    total, heads = grads[0].shape
    width = weight.shape[2]
    rows = total // 2

    def inputs_back_kernel(dq_ref, dk_ref, dv_ref, w_ref, part_ref):
        acc = nn(dq_ref[...], w_ref[0]) + nn(dk_ref[...], w_ref[1]) + nn(dv_ref[...], w_ref[2])
        part_ref[...] = acc.astype(BF)

    ins = [(grad, rows_of(half, heads, rows)) for grad in grads] + [(weight, whole(weight))]
    outs = [((rows, width), BF, pl.BlockSpec((rows, width), lambda i: (0, 0)))]
    return staged(tag, inputs_back_kernel, ins, outs, None)[0]


def across(part, tag):
    with jax.named_scope("x_" + tag):
        return flip(part, TENSOR, 1)


def tied(value, *others):
    return lax.optimization_barrier((value, *others))[0]


def weight_grad(left, right, tag):
    with jax.named_scope("w_" + tag):
        return jnp.einsum("th,td->hd", left, right, preferred_element_type=F32).astype(BF)


def attention_forward(tag, sources, weights, norm_before, tables, wait=()):
    in_weight, out_weight = weights[:2]
    segment_column, segment_row, cosine, sines = tables
    projected = None
    for half in range(2):
        projected = project(f"p{tag}{half}", half, sources[half], norm_before, in_weight, cosine, sines, projected)
    queries, key_vecs, values = projected[:3]
    if len(projected) == 5:
        x, low = projected[3:]
    else:
        low = sources[0][0]
        x = low.astype(F32)
    kept = None
    attended = []
    for half in range(2):
        taken = tied(queries, *wait) if half == 1 else queries
        part, *kept = attend(f"t{tag}{half}", half, taken, key_vecs, values, segment_column, segment_row,
                             out_weight, kept)
        attended.append((part, across(part, f"t{tag}{half}")))
    context, totals = kept
    return (x, low, queries, key_vecs, values, context, totals), attended


def feed_forward(tag, halves, weights, norm_rows, first_wait, second_wait):
    before, attended = halves
    blocks = weights[2]
    x = before[0]
    saved = None
    fed = []
    for half in range(2):
        taken = tied(x, *(second_wait if half else first_wait))
        part, *saved = feed(f"f{tag}{half}", half, taken, *attended[half], norm_rows, blocks, saved)
        fed.append((part, across(part, f"f{tag}{half}")))
    middle, spread, gate, up, *hidden = saved
    ends = [(middle, *fed[half]) for half in range(2)]
    return ends, (*before, attended, middle, spread, gate, up, hidden, fed)


def layer_backward(tag, sources, weights, norm_rows, tables, kept, pull_units, pull_heads, waits):
    in_weight, out_weight, blocks = weights
    segment_column, segment_row, cosine, sines = tables
    (x, low, queries, key_vecs, values, context, totals, attended, middle, spread,
     gate, up, hidden, fed) = kept
    saved = None
    through = []
    sums = []
    for half in range(2):
        part, total, *saved = feed_back(f"g{tag}{half}", half, sources[half], middle, *fed[half], norm_rows,
                                        gate, up, blocks, saved)
        through.append((part, across(part, f"g{tag}{half}")))
        sums.append(total)
    edge, grad_pre_output, grad_feed, *grad_shares = saved
    down = [weight_grad(hidden[i], grad_feed, f"d{tag}{i}") for i in (1, 0)]
    gate_up = [weight_grad(grad_shares[i], spread, f"u{tag}{i}") for i in (1, 0)]
    down, gate_up = down[::-1], gate_up[::-1]
    units = pull_units(tag, gate_up, down)
    partial = None
    saved = None
    first_sums = []
    for half in range(2):
        wait = waits if half == 0 else units[:2]
        total, dk, dv, *saved = attend_back(
            f"h{tag}{half}", half, (tied(grad_pre_output, *wait), *through[half]), x, *attended[half], norm_rows,
            queries, key_vecs, values, totals, segment_column, segment_row,
            out_weight, cosine, sines, partial, saved)
        partial = (dk, dv)
        first_sums.append(total)
    grad_pre_middle, grad_attended, dq = saved
    ends = []
    for half in range(2):
        part = inputs_back(f"i{tag}{half}", half, (dq, dk, dv), in_weight)
        ends.append((grad_pre_middle, part, across(part, f"i{tag}{half}")))
    grad_in = [weight_grad(grad, low, f"n{tag}") for grad in (dq, dk, dv)]
    grad_out = weight_grad(context, grad_attended, f"o{tag}")
    heads = pull_heads(tag, grad_in, grad_out)
    first = first_sums[0] + first_sums[1]
    second = sums[0] + sums[1]
    norm_grad = jnp.concatenate([first[:2], second[:2]], axis=0)
    return ends, edge, units, heads, norm_grad


MESH = pl.DeviceIdType.MESH


def forward_all(layer_inputs, heads_in, units_in, norm_in, tables):
    segment_column, segment_row, cosine, sines = tables
    ring = lax.axis_size(FSDP)
    count, own_rows, width = layer_inputs.shape
    total = count * own_rows
    rows = total // 2
    head_rows = heads_in.shape[1]
    half_units = units_in.shape[2]
    heads = 2 * ring * head_rows
    step = 2 * ring * half_units
    order = sorted(range(1, ring), key=lambda k: min(k, ring - k))

    saved = {}
    for l in range(2):
        saved.update({
            f"q{l}": ((total, heads), BF), f"k{l}": ((total, heads), BF),
            f"v{l}": ((total, heads), BF), f"ctx{l}": ((total, heads), BF),
            f"lse{l}": ((8, total), F32), f"pre1{l}": ((total, width), F32),
            f"pre2{l}": ((total, width), F32),
            f"spread{l}": ((total, width), BF), f"gate{l}": ((total, 2 * step), BF),
            f"up{l}": ((total, 2 * step), BF), f"hid{l}": ((total, 2 * step), BF),
        })
    saved.update({"low0": ((total, width), BF), "acts": ((2, total, width), BF)})
    inner = {"x1": ((total, width), F32), "mid": ((total, width), F32)}
    for l in range(2):
        for h in range(2):
            for stage in "tf":
                inner[f"own_{stage}{l}{h}"] = ((rows, width), BF)
                inner[f"got_{stage}{l}{h}"] = ((rows, width), BF)
    weights = {}
    for l in range(2):
        weights[f"heads{l}"] = ((4, 2, ring * head_rows, width), BF)
        weights[f"units{l}"] = ((3, 2, 2, ring * half_units, width), BF)
    outs = {**saved, **weights, "norms": ((2, 4, width), F32)}
    held = {**saved, **inner}
    stages = [f"{stage}{l}{h}" for l in range(2) for stage in "tf" for h in range(2)]

    def forward_kernel(inp, heads_ref, units_ref, norm_ref, col_ref, row_ref, cos_ref, sin_ref,
                       *refs):
        out = dict(zip(outs, refs[:len(outs)]))
        rest = refs[len(outs):]
        keep = dict(zip(held, rest[:len(held)]))
        (hbuf, ubuf, nbuf, acc_ref, z_s, z_r, y_s, y_r, k_s, k_r, e_s, e_r, x_s, x_r, i_s, i_r,
         l_s, f_s) = rest[len(held):]
        core = lax.axis_index(PIPE)
        place = lax.axis_index(TENSOR)
        group = lax.axis_index(FSDP)
        other = 1 - core
        item = (place // 2) * 2 + core

        def peer(k):
            low, high = place % 2, place // 2
            low = 1 - low if k & 1 else low
            high = 1 - high if k & 2 else high
            return high * 2 + low

        def near(k):
            return lax.rem(group + k, ring)

        sent = []

        def send(src, dst, send_sem, recv_sem, **to):
            copy = pltpu.make_async_remote_copy(
                src_ref=src, dst_ref=dst, send_sem=send_sem, recv_sem=recv_sem,
                device_id=to, device_id_type=MESH)
            copy.start()
            sent.append(copy)

        def arrived(dst, send_sem, recv_sem, **to):
            pltpu.make_async_remote_copy(
                src_ref=dst, dst_ref=dst, send_sem=send_sem, recv_sem=recv_sem,
                device_id=to, device_id_type=MESH).wait_recv()

        flushes = []
        done = set()

        def flush(src, name):
            done.add(name)
            copy = pltpu.make_async_copy(src, out[name], f_s.at[len(flushes)])
            copy.start()
            flushes.append(copy)

        def slot(piece, share, col, g):
            l, kind = piece // 2, piece % 2
            if kind == 0:
                at = pl.ds(pl.multiple_of(g * head_rows, 16), head_rows)
                return hbuf.at[l, pl.ds(2 * share, 2), col, at]
            at = pl.ds(pl.multiple_of(g * half_units, 16), half_units)
            return ubuf.at[l, :, share, col, at]

        barrier = pltpu.get_barrier_semaphore()
        peers = [dict(tensor=peer(k)) for k in (1, 2, 3)] + [dict(pipe=other)]
        peers += [dict(fsdp=near(k)) for k in range(1, ring)]
        for to in peers:
            pl.semaphore_signal(barrier, inc=1, device_id=to, device_id_type=MESH)
        pl.semaphore_wait(barrier, len(peers))

        mine = pl.ds(pl.multiple_of(group * head_rows, 16), head_rows)
        mine_units = pl.ds(pl.multiple_of(group * half_units, 16), half_units)
        local = [
            pltpu.make_async_copy(heads_ref.at[pl.ds(2 * core, 2)],
                                  hbuf.at[core, pl.ds(2 * core, 2), 0, mine], l_s.at[0]),
            pltpu.make_async_copy(units_ref.at[:, core],
                                  ubuf.at[core, :, core, 0, mine_units], l_s.at[1]),
            pltpu.make_async_copy(inp.at[item],
                                  keep["low0"].at[pl.ds(pl.multiple_of(place * own_rows, 16),
                                                        own_rows)], l_s.at[2]),
            pltpu.make_async_copy(norm_ref, nbuf.at[core], l_s.at[3]),
        ]
        send(heads_ref.at[pl.ds(2 * other, 2)], hbuf.at[core, pl.ds(2 * other, 2), 0, mine],
             e_s.at[0], e_r.at[0], pipe=other)
        for copy in local:
            copy.start()
        send(units_ref.at[:, other], ubuf.at[core, :, other, 0, mine_units],
             e_s.at[1], e_r.at[1], pipe=other)
        send(norm_ref, nbuf.at[core], e_s.at[2], e_r.at[2], pipe=other)
        for k in range(1, count):
            send(inp.at[(peer(k) // 2) * 2 + core],
                 keep["low0"].at[pl.ds(pl.multiple_of(place * own_rows, 16), own_rows)],
                 i_s.at[k], i_r.at[k], tensor=peer(k))

        def along_fsdp(piece):
            for k in order:
                here = slot(piece, core, 0, group)
                send(here, here, z_s.at[piece, k], z_r.at[piece, (ring - k) % ring],
                     fsdp=near(k))

        def pass_on(piece, k):
            g = near(k)
            here = slot(piece, core, 0, g)
            if k:
                arrived(here, z_s.at[piece, k], z_r.at[piece, k], fsdp=g)
            send(here, slot(piece, core, 1, g), y_s.at[piece, k], y_r.at[piece, k],
                 tensor=peer(2))
            send(here, here, k_s.at[piece, 0, k], k_r.at[piece, 0, k], pipe=other)

        def pass_second(piece):
            for k in [0] + order:
                here = slot(piece, core, 1, near(k))
                arrived(here, y_s.at[piece, k], y_r.at[piece, k], tensor=peer(2))
                send(here, here, k_s.at[piece, 1, k], k_r.at[piece, 1, k], pipe=other)

        def complete(piece):
            for col in range(2):
                for k in [0] + order:
                    arrived(slot(piece, other, col, near(k)), k_s.at[piece, col, k],
                            k_r.at[piece, col, k], pipe=other)
            l = piece // 2
            if piece % 2 == 0:
                flush(hbuf.at[l], f"heads{l}")
            else:
                flush(ubuf.at[l], f"units{l}")

        local[0].wait()
        arrived(hbuf.at[other, pl.ds(2 * core, 2), 0, mine],
                e_s.at[0], e_r.at[0], pipe=other)
        along_fsdp(0)
        pass_on(0, 0)
        local[1].wait()
        arrived(ubuf.at[other, :, core, 0, mine_units], e_s.at[1], e_r.at[1], pipe=other)
        along_fsdp(1)
        pass_on(1, 0)
        along_fsdp(2)
        along_fsdp(3)

        def part_of(name, l):
            return nbuf[l, name:name + 1, :]

        def exchange(tag):
            index = stages.index(tag)
            send(keep["own_" + tag], keep["got_" + tag], x_s.at[index], x_r.at[index],
                 tensor=peer(1))

        def taken(tag):
            index = stages.index(tag)
            arrived(keep["got_" + tag], x_s.at[index], x_r.at[index], tensor=peer(1))
            return keep["own_" + tag][...].astype(F32) + keep["got_" + tag][...].astype(F32)

        def do_project(l, half):
            at_rows = slice(half * rows, half * rows + rows)
            if l == 0:
                low = keep["low0"][at_rows]
            else:
                summed = keep["mid"][at_rows] + taken(f"f0{half}")
                keep["pre20"][at_rows] = summed
                x = row_norm(summed)[0] * part_of(2, 0) + part_of(3, 0)
                keep["x1"][at_rows] = x
                low = x.astype(BF)
                keep["acts"][0, at_rows] = low
            cosine, sines = cos_ref[at_rows], sin_ref[at_rows]
            for c, name in ((0, "q"), (1, "k")):
                turning = nt(low, hbuf[l, c].reshape(heads, width))
                for slab in range(heads // 128):
                    at = slice(128 * slab, 128 * slab + 128)
                    keep[f"{name}{l}"][at_rows, at] = turned(
                        turning[:, at], cosine, sines).astype(BF)
            keep[f"v{l}"][at_rows] = nt(low, hbuf[l, 2].reshape(heads, width)).astype(BF)

        def do_attend(l, half):
            at_rows = slice(half * rows, half * rows + rows)
            masks = head_masks(rows)
            lane = lax.broadcasted_iota(jnp.int32, (rows, 128), 1)
            same = col_ref[at_rows, :1] == row_ref[:1, :]
            totals = jnp.zeros((rows, 128), F32)
            for slab in range(heads // 128):
                at = slice(128 * slab, 128 * slab + 128)
                q, k, v = keep[f"q{l}"][at_rows, at], keep[f"k{l}"][:, at], keep[f"v{l}"][:, at]
                gathered = jnp.zeros((rows, 128), F32)
                for h in range(2):
                    scores = nt(q * masks[h].astype(BF), k) * HEAD_DIM ** (-0.5)
                    scores = jnp.where(same, scores, masked_value)
                    top = jnp.max(scores, axis=-1, keepdims=True)
                    powers = jnp.exp(scores - top)
                    mass = jnp.sum(powers, axis=-1, keepdims=True)
                    chances = (powers * (1.0 / mass)).astype(BF)
                    gathered = gathered + nn(chances, v) * masks[h]
                    totals = jnp.where(lane == 2 * slab + h, top + jnp.log(mass), totals)
                keep[f"ctx{l}"][at_rows, at] = gathered.astype(BF)
            keep[f"lse{l}"][:, at_rows] = totals.T[:8]
            part = nn(keep[f"ctx{l}"][at_rows], hbuf[l, 3].reshape(heads, width))
            keep[f"own_t{l}{half}"][...] = part.astype(BF)
            exchange(f"t{l}{half}")

        def do_feed(l, half):
            at_rows = slice(half * rows, half * rows + rows)
            x = keep["low0"][at_rows].astype(F32) if l == 0 else keep["x1"][at_rows]
            summed = x + taken(f"t{l}{half}")
            keep[f"pre1{l}"][at_rows] = summed
            middle = row_norm(summed)[0] * part_of(0, l) + part_of(1, l)
            keep["mid"][at_rows] = middle
            low = middle.astype(BF)
            keep[f"spread{l}"][at_rows] = low
            for share in range(2):
                at = slice(share * step, share * step + step)
                gate = nt(low, ubuf[l, 0, share].reshape(step, width))
                up = nt(low, ubuf[l, 1, share].reshape(step, width))
                keep[f"gate{l}"][at_rows, at] = gate.astype(BF)
                keep[f"up{l}"][at_rows, at] = up.astype(BF)
                hidden = (gate * jax.nn.sigmoid(gate) * up).astype(BF)
                keep[f"hid{l}"][at_rows, at] = hidden
                fed = nn(hidden, ubuf[l, 2, share].reshape(step, width))
                if share == 0:
                    acc_ref[...] = fed
                else:
                    keep[f"own_f{l}{half}"][...] = (acc_ref[...] + fed).astype(BF)
            exchange(f"f{l}{half}")

        for k in order:
            pass_on(0, k)
        pass_second(0)
        for k in range(1, count):
            arrived(keep["low0"].at[pl.ds(pl.multiple_of(peer(k) * own_rows, 16), own_rows)],
                    i_s.at[k], i_r.at[k], tensor=peer(k))
        local[2].wait()
        local[3].wait()
        arrived(nbuf.at[other], e_s.at[2], e_r.at[2], pipe=other)
        complete(0)
        do_project(0, 0)
        do_project(0, 1)
        do_attend(0, 0)
        do_attend(0, 1)
        for k in order:
            pass_on(1, k)
        pass_on(2, 0)
        pass_second(1)
        complete(1)
        do_feed(0, 0)
        for k in order:
            pass_on(2, k)
        pass_on(3, 0)
        do_feed(0, 1)
        for name in saved:
            if name[-1] == "0" and name != "pre20":
                flush(keep[name], name)
        pass_second(2)
        pass_on(3, order[0])
        complete(2)
        do_project(1, 0)
        do_project(1, 1)
        pass_on(3, order[1])
        do_attend(1, 0)
        for k in order[2:]:
            pass_on(3, k)
        do_attend(1, 1)
        pass_second(3)
        complete(3)
        do_feed(1, 0)
        do_feed(1, 1)
        flush(nbuf, "norms")
        for half in range(2):
            at_rows = slice(half * rows, half * rows + rows)
            summed = keep["mid"][at_rows] + taken(f"f1{half}")
            keep["pre21"][at_rows] = summed
            keep["acts"][1, at_rows] = (
                row_norm(summed)[0] * part_of(2, 1) + part_of(3, 1)).astype(BF)
        for name in saved:
            if name not in done:
                flush(keep[name], name)
        for copy in sent:
            copy.wait_send()
        for copy in flushes:
            copy.wait()

    anywhere = pl.BlockSpec(memory_space=pl.ANY)
    inside = pl.BlockSpec(memory_space=pltpu.VMEM)
    dma = pltpu.SemaphoreType.DMA
    scratch = [pltpu.VMEM(shape, kind) for shape, kind in held.values()]
    scratch += [
        pltpu.VMEM((2, 4, 2, ring * head_rows, width), BF),
        pltpu.VMEM((2, 3, 2, 2, ring * half_units, width), BF),
        pltpu.VMEM((2, 4, width), F32),
        pltpu.VMEM((rows, width), F32),
        dma((4, ring)), dma((4, ring)), dma((4, ring)), dma((4, ring)),
        dma((4, 2, ring)), dma((4, 2, ring)), dma((3,)), dma((3,)),
        dma((len(stages),)), dma((len(stages),)), dma((count,)), dma((count,)),
        dma((4,)), dma((len(outs),)),
    ]
    results = pl.pallas_call(
        forward_kernel,
        in_specs=[anywhere] * 3 + [inside] * 5,
        out_specs=[anywhere] * len(outs),
        out_shape=[jax.ShapeDtypeStruct(shape, kind) for shape, kind in outs.values()],
        scratch_shapes=scratch,
        compiler_params=pltpu.CompilerParams(
            collective_id=0, has_side_effects=True, vmem_limit_bytes=62 << 20),
        name="forward_kernel",
    )(layer_inputs, heads_in, units_in, norm_in, segment_column, segment_row, cosine, sines)
    return dict(zip(outs, results))


def backward_all(cotangent, saved, tables):
    segment_column, segment_row, cosine, sines = tables
    ring = lax.axis_size(FSDP)
    count, own_rows, width = cotangent.shape
    total = count * own_rows
    rows = total // 2
    heads = saved["q0"].shape[1]
    step = saved["hid0"].shape[1] // 2
    head_rows = heads // (2 * ring)
    half_units = step // (2 * ring)
    order = sorted(range(1, ring), key=lambda k: min(k, ring - k))
    loaded = ("q", "k", "v", "lse", "pre1", "pre2", "spread", "gate", "up", "hid", "heads",
              "units")
    arrays = [saved[f"{name}{l}"] for l in range(2) for name in loaded]
    arrays += [saved["ctx0"], saved["ctx1"], saved["low0"], saved["acts"]]
    stages = [f"{stage}{l}{h}" for l in range(2) for stage in "gi" for h in range(2)]
    pieces = ("d", "u", "h")
    scaling = HEAD_DIM ** (-0.5)

    def backward_kernel(cot_ref, norm_ref, col_ref, row_ref, cos_ref, sin_ref, *refs):
        n = len(arrays)
        from_hbm = {}
        for l in range(2):
            for i, name in enumerate(loaded):
                from_hbm[f"{name}{l}"] = refs[l * len(loaded) + i]
        from_hbm["ctx0"], from_hbm["ctx1"], from_hbm["low0"], acts_ref = refs[n - 4:n]
        from_hbm["low1"] = acts_ref.at[0]
        (act_out, grad_out, units_out, heads_out, norm_out) = refs[n:n + 5]
        rest = refs[n + 5:]
        here = dict(zip(loaded, rest[:len(loaded)]))
        (lefts, rights, dpre, dfeed, dctx, dkv, cot, grads, own, got, nsum, nred, nget, acc,
         keep_u, keep_h, give_u, give_h, core_u, core_h, side_u, side_h, line_u, line_h,
         fin_u, fin_h, x_s, x_r, i_s, i_r, a_s, a_r, b_s, b_r, c_s, c_r, y_s, y_r, z_s, z_r,
         n_s, n_r, j_s, j_r, l_s, m_s, credit_c, credit_y) = rest[len(loaded):]
        core = lax.axis_index(PIPE)
        place = lax.axis_index(TENSOR)
        group = lax.axis_index(FSDP)
        other = 1 - core
        item = (place // 2) * 2 + core

        def peer(k):
            low, high = place % 2, place // 2
            low = 1 - low if k & 1 else low
            high = 1 - high if k & 2 else high
            return high * 2 + low

        def near(k):
            return lax.rem(group + k, ring)

        pending = []

        def send(src, dst, send_sem, recv_sem, **to):
            copy = pltpu.make_async_remote_copy(
                src_ref=src, dst_ref=dst, send_sem=send_sem, recv_sem=recv_sem,
                device_id=to, device_id_type=MESH)
            copy.start()
            pending.append(copy)
            return copy

        def arrived(dst, send_sem, recv_sem, **to):
            pltpu.make_async_remote_copy(
                src_ref=dst, dst_ref=dst, send_sem=send_sem, recv_sem=recv_sem,
                device_id=to, device_id_type=MESH).wait_recv()

        def sent(copy):
            copy.wait_send()
            pending[:] = [held for held in pending if held is not copy]

        names = loaded + ("ctx", "low")
        loads = {}

        def load(l, *which):
            for name in which:
                to = {"ctx": lefts.at[3], "low": rights.at[0]}.get(name)
                to = here[name] if to is None else to
                copy = pltpu.make_async_copy(from_hbm[f"{name}{l}"], to,
                                             l_s.at[l * len(names) + names.index(name)])
                copy.start()
                loads[name, l] = copy

        def ready(l, *which):
            for name in which:
                loads.pop((name, l)).wait()

        def rows_at(index):
            return pl.ds(pl.multiple_of(index * own_rows, 16), own_rows)

        barrier = pltpu.get_barrier_semaphore()
        peers = [dict(tensor=peer(k)) for k in (1, 2, 3)]
        peers += [dict(pipe=other), dict(pipe=other, tensor=peer(2))]
        peers += [dict(fsdp=near(k)) for k in range(1, ring)]
        for to in peers:
            pl.semaphore_signal(barrier, inc=1, device_id=to, device_id_type=MESH)
        pl.semaphore_wait(barrier, len(peers))

        for k in range(1, count):
            send(cot_ref.at[(peer(k) // 2) * 2 + core], cot.at[rows_at(place)],
                 i_s.at[k], i_r.at[k], tensor=peer(k))
        own_cot = pltpu.make_async_copy(cot_ref.at[item], cot.at[rows_at(place)], m_s.at[0])
        own_cot.start()
        load(1, "pre2", "units", "gate", "up", "spread", "hid", "pre1", "heads", "q", "k", "v",
             "lse", "ctx", "low")

        def home(source, result, sems, index):
            copy = pltpu.make_async_copy(source.at[core, rows_at(place)], result.at[item],
                                         m_s.at[index])
            copy.start()
            for k in range(1, 4):
                layer = other if k & 1 else core
                to = dict(pipe=layer, tensor=peer(k & 2))
                send(source.at[layer, rows_at(peer(k & 2))], result.at[item],
                     sems[0].at[k], sems[1].at[k], **to)
            return copy

        def home_arrived(result, sems):
            for k in range(1, 4):
                to = dict(pipe=other if k & 1 else core, tensor=peer(k & 2))
                index = (peer(k & 2) // 2) * 2 + (other if k & 1 else core)
                arrived(result.at[index], sems[0].at[k], sems[1].at[k], **to)

        own_act = home(acts_ref, act_out, (a_s, a_r), 1)
        for k in range(1, count):
            arrived(cot.at[rows_at(peer(k))], i_s.at[k], i_r.at[k], tensor=peer(k))
        own_cot.wait()
        last_use = {}

        def exchange(tag, value):
            place_of = "gi".index(tag[0]) * 2 + int(tag[2])
            if place_of in last_use:
                sent(last_use[place_of])
            own[place_of] = value
            index = stages.index(tag)
            last_use[place_of] = send(own.at[place_of], got.at[index], x_s.at[index],
                                      x_r.at[index], tensor=peer(1))

        def taken(tag):
            index = stages.index(tag)
            place_of = "gi".index(tag[0]) * 2 + int(tag[2])
            arrived(got.at[index], x_s.at[index], x_r.at[index], tensor=peer(1))
            return own[place_of].astype(F32) + got[index].astype(F32)

        def part_of(name, l):
            return norm_ref[l, name:name + 1, :]

        def note_sums(l, half, first, sums):
            if half == 0:
                nsum[l, first:first + 2] = sums[:2]
            else:
                nsum[l, first:first + 2] = nsum[l, first:first + 2] + sums[:2]

        def do_feed_back(l, half):
            at_rows = slice(half * rows, half * rows + rows)
            if l == 1:
                upstream = cot[at_rows].astype(F32)
            else:
                upstream = dpre[at_rows] + taken(f"i1{half}")
                grads[1, at_rows] = upstream.astype(BF)
            if half == 0:
                ready(l, "pre2")
            normed, inverse = row_norm(here["pre2"][at_rows])
            through, sums = row_norm_back(normed, inverse, part_of(2, l), upstream)
            note_sums(l, half, 2, sums)
            dpre[at_rows] = through
            low = through.astype(BF)
            dfeed[at_rows] = low
            if half == 0:
                ready(l, "units", "gate", "up")
            units = here["units"]
            for share in range(2):
                at = slice(share * step, share * step + step)
                gate = here["gate"][at_rows, at].astype(F32)
                up = here["up"][at_rows, at].astype(F32)
                grad_hidden = nt(low, units[2, share].reshape(step, width))
                sigmoid = jax.nn.sigmoid(gate)
                grad_gate = (
                    grad_hidden * up * sigmoid * (1.0 + gate * (1.0 - sigmoid))).astype(BF)
                grad_up = (grad_hidden * gate * sigmoid).astype(BF)
                here["gate"][at_rows, at] = grad_gate
                here["up"][at_rows, at] = grad_up
                back = nn(grad_gate, units[0, share].reshape(step, width))
                back = back + nn(grad_up, units[1, share].reshape(step, width))
                if share == 0:
                    acc[...] = back
                else:
                    exchange(f"g{l}{half}", (acc[...] + back).astype(BF))

        def unit_grad(l, c, share, target):
            left = here[("gate", "up", "hid")[c]]
            right = dfeed if c == 2 else here["spread"]
            size = step // 2
            for col in range(2):
                at = pl.ds(pl.multiple_of(share * step + col * size, 128), size)
                target[col] = tn(left[:, at], right[...]).astype(BF)

        def head_grad(share, target):
            for i in range(2):
                j = 2 * share + i
                full = tn(lefts[j], rights[j // 3]).astype(BF)
                for col in range(2):
                    target[i, col] = full[col * (heads // 2):(col + 1) * (heads // 2)]

        def do_attend_back(l, half):
            at_rows = slice(half * rows, half * rows + rows)
            if half == 0:
                ready(l, "pre1", "heads", "q", "k", "v", "lse")
            upstream = dpre[at_rows] + taken(f"g{l}{half}")
            normed, inverse = row_norm(here["pre1"][at_rows])
            through, sums = row_norm_back(normed, inverse, part_of(0, l), upstream)
            note_sums(l, half, 0, sums)
            dpre[at_rows] = through
            low = through.astype(BF)
            rights[1, at_rows] = low
            dctx[...] = nt(low, here["heads"][3].reshape(heads, width)).astype(BF)
            masks = head_masks(rows)
            wide_masks = head_masks(total)
            same = col_ref[:, :1] == row_ref[:1, at_rows]
            for slab in range(heads // 128):
                at = slice(slab * 128, slab * 128 + 128)
                q, k = here["q"][at_rows, at], here["k"][:, at]
                v, grad_ctx = here["v"][:, at], dctx[:, at]
                dq = jnp.zeros((rows, 128), F32)
                dk = jnp.zeros((total, 128), F32)
                dv = jnp.zeros((total, 128), F32)
                for h in range(2):
                    mask = masks[h].astype(BF)
                    scores = nt(k, q * mask) * scaling
                    scores = jnp.where(same, scores, masked_value)
                    lse = here["lse"][2 * slab + h:2 * slab + h + 1, at_rows]
                    chances = jnp.exp(scores - lse)
                    grad_chances = nt(v, grad_ctx * mask)
                    row_dot = jnp.sum(chances * grad_chances, axis=0, keepdims=True)
                    grad_scores = (chances * (grad_chances - row_dot)).astype(BF)
                    dv = dv + nn(chances.astype(BF), grad_ctx) * wide_masks[h]
                    dk = dk + nn(grad_scores, q) * wide_masks[h]
                    dq = dq + tn(grad_scores, k) * masks[h]
                lefts[0, at_rows, at] = turned(
                    dq * scaling, cos_ref[at_rows], -sin_ref[at_rows]).astype(BF)
                if half == 0:
                    dkv[0, :, at] = dk
                    dkv[1, :, at] = dv
                else:
                    dk = dkv[0, :, at] + dk
                    dv = dkv[1, :, at] + dv
                    lefts[1, :, at] = turned(dk * scaling, cos_ref[...], -sin_ref[...]).astype(BF)
                    lefts[2, :, at] = dv.astype(BF)

        def do_inputs_back(l, half):
            at_rows = slice(half * rows, half * rows + rows)
            back = jnp.zeros((rows, width), F32)
            for c in range(3):
                back = back + nn(lefts[c, at_rows], here["heads"][c].reshape(heads, width))
            exchange(f"i{l}{half}", back.astype(BF))

        def parts(piece, units_ref, heads_ref):
            return {"d": units_ref.at[2:3], "u": units_ref.at[0:2], "h": heads_ref}[piece]

        def cell(piece, l):
            return l * 3 + pieces.index(piece)

        gave = {}

        def give(l, piece):
            if l == 0:
                pl.semaphore_wait(credit_c.at[pieces.index(piece)], 1)
            index = cell(piece, l)
            gave[piece] = send(parts(piece, give_u, give_h), parts(piece, core_u, core_h),
                               c_s.at[index], c_r.at[index], pipe=other)

        def add_core(l, piece):
            index = cell(piece, l)
            come = parts(piece, core_u, core_h)
            arrived(come, c_s.at[index], c_r.at[index], pipe=other)
            mine = parts(piece, keep_u.at[l], keep_h.at[l])
            mine[...] = (mine[...].astype(F32) + come[...].astype(F32)).astype(BF)
            if l == 1:
                pl.semaphore_signal(credit_c.at[pieces.index(piece)], inc=1,
                                    device_id=dict(pipe=other), device_id_type=MESH)
            else:
                pl.semaphore_wait(credit_y.at[pieces.index(piece)], 1)
            send(mine.at[:, 1], parts(piece, side_u, side_h), y_s.at[index], y_r.at[index],
                 tensor=peer(2))

        def slot_of(piece, ref, g):
            size = head_rows if piece == "h" else half_units
            return ref.at[:, pl.ds(pl.multiple_of(g * size, 16), size)]

        def add_side(l, piece):
            index = cell(piece, l)
            come = parts(piece, side_u, side_h)
            arrived(come, y_s.at[index], y_r.at[index], tensor=peer(2))
            mine = parts(piece, keep_u.at[l], keep_h.at[l]).at[:, 0]
            mine[...] = (mine[...].astype(F32) + come[...].astype(F32)).astype(BF)
            if l == 1:
                pl.semaphore_signal(credit_y.at[pieces.index(piece)], inc=1,
                                    device_id=dict(tensor=peer(2)), device_id_type=MESH)
            for k in order:
                send(slot_of(piece, mine, near(k)),
                     parts(piece, line_u.at[l, (ring - k) % ring], line_h.at[l, (ring - k) % ring]),
                     z_s.at[index, k], z_r.at[index, (ring - k) % ring], fsdp=near(k))

        def add_line(l, piece):
            index = cell(piece, l)
            mine = parts(piece, keep_u.at[l], keep_h.at[l]).at[:, 0]
            summed = slot_of(piece, mine, group)[...].astype(F32)
            for k in order:
                come = parts(piece, line_u.at[l, k], line_h.at[l, k])
                arrived(come, z_s.at[index, k], z_r.at[index, k], fsdp=near(k))
                summed = summed + come[...].astype(F32)
            parts(piece, fin_u.at[l], fin_h.at[l])[...] = summed.astype(BF)

        for half in range(2):
            do_feed_back(1, half)
        ready(1, "hid", "spread")
        unit_grad(1, 2, other, give_u.at[2])
        give(1, "d")
        unit_grad(1, 0, other, give_u.at[0])
        unit_grad(1, 1, other, give_u.at[1])
        give(1, "u")
        unit_grad(1, 2, core, keep_u.at[1, 2])
        add_core(1, "d")
        unit_grad(1, 0, core, keep_u.at[1, 0])
        unit_grad(1, 1, core, keep_u.at[1, 1])
        load(0, "pre2", "units", "gate", "up", "spread", "hid")
        do_attend_back(1, 0)
        add_core(1, "u")
        do_attend_back(1, 1)
        for half in range(2):
            do_inputs_back(1, half)
        add_side(1, "d")
        ready(1, "ctx", "low")
        head_grad(other, give_h)
        give(1, "h")
        head_grad(core, keep_h.at[1])
        load(0, "pre1", "heads", "q", "k", "v", "lse", "ctx", "low")

        do_feed_back(0, 0)
        add_core(1, "h")
        do_feed_back(0, 1)
        ready(0, "hid", "spread")
        sent(gave["d"])
        unit_grad(0, 2, other, give_u.at[2])
        give(0, "d")
        sent(gave["u"])
        unit_grad(0, 0, other, give_u.at[0])
        unit_grad(0, 1, other, give_u.at[1])
        give(0, "u")
        add_side(1, "u")
        unit_grad(0, 2, core, keep_u.at[0, 2])
        add_core(0, "d")
        unit_grad(0, 0, core, keep_u.at[0, 0])
        unit_grad(0, 1, core, keep_u.at[0, 1])
        do_attend_back(0, 0)
        add_side(1, "h")
        add_core(0, "u")
        do_attend_back(0, 1)
        for half in range(2):
            do_inputs_back(0, half)
        send(nsum.at[other], nget.at[0], n_s.at[0], n_r.at[0], pipe=other)
        ready(0, "ctx", "low")
        sent(gave["h"])
        head_grad(other, give_h)
        give(0, "h")
        add_side(0, "d")
        head_grad(core, keep_h.at[0])
        add_core(0, "h")
        arrived(nget.at[0], n_s.at[0], n_r.at[0], pipe=other)
        nred[0] = nsum[core] + nget[0]
        for half in range(2):
            at_rows = slice(half * rows, half * rows + rows)
            grads[0, at_rows] = (dpre[at_rows] + taken(f"i0{half}")).astype(BF)
        send(nred.at[0], nget.at[1], n_s.at[1], n_r.at[1], tensor=peer(2))
        own_grad = home(grads, grad_out, (b_s, b_r), 2)
        add_side(0, "u")
        arrived(nget.at[1], n_s.at[1], n_r.at[1], tensor=peer(2))
        nred[1] = nred[0] + nget[1]
        for k in order:
            send(nred.at[1], nget.at[1 + (ring - k) % ring], n_s.at[1 + k],
                 n_r.at[1 + (ring - k) % ring], fsdp=near(k))
        add_side(0, "h")
        for piece in pieces:
            add_line(1, piece)
        add_line(0, "d")
        norms = nred[1]
        for k in order:
            arrived(nget.at[1 + k], n_s.at[1 + k], n_r.at[1 + k], fsdp=near(k))
            norms = norms + nget[1 + k]
        norm_out[...] = norms
        add_line(0, "u")
        add_line(0, "h")
        joins = []
        for i, (fin, result) in enumerate(((fin_u, units_out), (fin_h, heads_out))):
            send(fin.at[other], result.at[core], j_s.at[i], j_r.at[i], pipe=other)
            copy = pltpu.make_async_copy(fin.at[core], result.at[core], m_s.at[3 + i])
            copy.start()
            joins.append(copy)
        for i, result in enumerate((units_out, heads_out)):
            arrived(result.at[other], j_s.at[i], j_r.at[i], pipe=other)
        home_arrived(act_out, (a_s, a_r))
        home_arrived(grad_out, (b_s, b_r))
        for copy in [own_act, own_grad] + joins:
            copy.wait()
        for copy in pending:
            copy.wait_send()

    anywhere = pl.BlockSpec(memory_space=pl.ANY)
    inside = pl.BlockSpec(memory_space=pltpu.VMEM)
    dma = pltpu.SemaphoreType.DMA
    scratch = [pltpu.VMEM(saved[f"{name}0"].shape, saved[f"{name}0"].dtype) for name in loaded]
    scratch += [
        pltpu.VMEM((4, total, heads), BF), pltpu.VMEM((2, total, width), BF),
        pltpu.VMEM((total, width), F32), pltpu.VMEM((total, width), BF),
        pltpu.VMEM((rows, heads), BF), pltpu.VMEM((2, total, heads), F32),
        pltpu.VMEM((total, width), BF), pltpu.VMEM((2, total, width), BF),
        pltpu.VMEM((4, rows, width), BF), pltpu.VMEM((8, rows, width), BF),
        pltpu.VMEM((2, 4, width), F32), pltpu.VMEM((2, 4, width), F32),
        pltpu.VMEM((1 + ring, 4, width), F32), pltpu.VMEM((rows, width), F32),
        pltpu.VMEM((2, 3, 2, ring * half_units, width), BF),
        pltpu.VMEM((2, 2, 2, ring * head_rows, width), BF),
        pltpu.VMEM((3, 2, ring * half_units, width), BF),
        pltpu.VMEM((2, 2, ring * head_rows, width), BF),
        pltpu.VMEM((3, 2, ring * half_units, width), BF),
        pltpu.VMEM((2, 2, ring * head_rows, width), BF),
        pltpu.VMEM((3, ring * half_units, width), BF),
        pltpu.VMEM((2, ring * head_rows, width), BF),
        pltpu.VMEM((2, ring, 3, half_units, width), BF),
        pltpu.VMEM((2, ring, 2, head_rows, width), BF),
        pltpu.VMEM((2, 3, half_units, width), BF),
        pltpu.VMEM((2, 2, head_rows, width), BF),
        dma((8,)), dma((8,)), dma((4,)), dma((4,)), dma((4,)), dma((4,)), dma((4,)), dma((4,)),
        dma((6,)), dma((6,)), dma((6,)), dma((6,)), dma((6, ring)), dma((6, ring)),
        dma((1 + ring,)), dma((1 + ring,)), dma((2,)), dma((2,)),
        dma((2 * (len(loaded) + 2),)), dma((5,)),
        pltpu.SemaphoreType.REGULAR((3,)), pltpu.SemaphoreType.REGULAR((3,)),
    ]
    return pl.pallas_call(
        backward_kernel,
        in_specs=[anywhere] + [inside] * 5 + [anywhere] * len(arrays),
        out_specs=[anywhere] * 4 + [inside],
        out_shape=[
            jax.ShapeDtypeStruct((count, own_rows, width), BF),
            jax.ShapeDtypeStruct((count, own_rows, width), BF),
            jax.ShapeDtypeStruct((2, 3, half_units, width), BF),
            jax.ShapeDtypeStruct((2, 2, head_rows, width), BF),
            jax.ShapeDtypeStruct((4, width), F32),
        ],
        scratch_shapes=scratch,
        compiler_params=pltpu.CompilerParams(
            collective_id=1, has_side_effects=True, vmem_limit_bytes=63 << 20),
        name="backward_kernel",
    )(cotangent, saved["norms"], segment_column, segment_row, cosine, sines, *arrays)


def to_item(array, core, place):
    def piece(k):
        return lax.dynamic_index_in_dim(array, ((place ^ k) & 2) | core, 0, keepdims=False)

    parts = [piece(0)] + [flip(piece(k), TENSOR, k) for k in range(1, 4)]
    return jnp.concatenate(unxor(parts, place), axis=0)


def from_item(by_layer, core, place):
    rows = by_layer[0].shape[0] // 4
    mine = jnp.where(core == 0, by_layer[0], by_layer[1])
    other = jnp.where(core == 0, by_layer[1], by_layer[0])

    def piece(k):
        target = place ^ (k & 2)
        return lax.dynamic_slice_in_dim(other if k & 1 else mine, target * rows, rows, 0)

    parts = [piece(0)] + [mixed_flip(piece(k), k & 1, k & 2) for k in range(1, 4)]
    return jnp.stack(unxor(parts, (place & 2) | core)).astype(F32)


def whole_step(
    layer_inputs,
    cotangent,
    input_master,
    output_master,
    gate_master,
    down_master,
    norm_tables,
    document_lengths,
):
    core = lax.axis_index(PIPE)
    place = lax.axis_index(TENSOR)
    group = lax.axis_index(FSDP)
    ring = lax.axis_size(FSDP)
    width = layer_inputs.shape[2]
    head_rows = input_master.shape[2]
    units = down_master.shape[1]
    half = units // 2
    first_core = core == 0

    item = (place & 2) | core
    lengths = lax.dynamic_index_in_dim(document_lengths[:, 0, :], item, 0, keepdims=False)
    segment, position = segment_info(lengths)
    segment_column = jnp.broadcast_to(segment[:, None], (MB_CAP, 128))
    segment_row = jnp.broadcast_to(segment[None, :], (8, MB_CAP))
    tables = (segment_column, segment_row) + rotary_tables(position)

    def split_by_core(for_first, for_second):
        keep = jnp.where(first_core, for_first, for_second)
        got = flip(jnp.where(first_core, for_second, for_first), PIPE, 1)
        return [jnp.where(first_core, keep, got), jnp.where(first_core, got, keep)]

    def joined_by_core(share_zero, share_one):
        keep = jnp.where(first_core, share_zero, share_one)
        got = flip(jnp.where(first_core, share_one, share_zero), PIPE, 1)
        return jnp.where(first_core, keep, got), jnp.where(first_core, got, keep)

    if head_rows % 16 == 0 and half % 16 == 0:
        heads_in = jnp.concatenate([input_master[0], output_master], axis=0).astype(BF)
        units_in = jnp.concatenate([gate_master[0], down_master], axis=0).astype(BF)
        saved = forward_all(layer_inputs, heads_in, units_in.reshape(3, 2, half, width),
                            norm_tables[0], tables)
        results = backward_all(cotangent, saved, tables)
        activations, gradients_in, unit_grad, head_grad, norm_sum = results
        head_grad = head_grad.reshape(4, head_rows, width).astype(F32)
        unit_grad = unit_grad.transpose(1, 0, 2, 3).reshape(3, units, width).astype(F32)
        return (
            activations[None].astype(F32),
            gradients_in[None].astype(F32),
            head_grad[None, :3],
            head_grad[None, 3],
            unit_grad[None, :2],
            unit_grad[None, 2],
            norm_sum[None],
        )

    in_low = input_master[0].astype(BF)
    out_low = output_master.astype(BF)
    head_shares = split_by_core(in_low[:2], jnp.concatenate([in_low[2:], out_low], axis=0))
    unit_low = jnp.concatenate([gate_master[0], down_master], axis=0).astype(BF)
    unit_shares = split_by_core(unit_low[:, :half], unit_low[:, half:])

    x = to_item(layer_inputs, core, place)
    norm_own = norm_tables[0]
    norm_other = flip(norm_own, PIPE, 1)
    norms = [
        jnp.where(first_core, norm_own, norm_other),
        jnp.where(first_core, norm_other, norm_own),
    ]

    quarter = half // 2
    rows = ring * head_rows

    def gather_heads(s, *waits):
        slots = ring_gather(tied(head_shares[s], *waits), f"h{s}")
        ascending = jnp.stack(slots[::-1] + slots[::-1])
        column = lax.dynamic_slice_in_dim(ascending, ring - 1 - group, ring, 0)
        return column.transpose(1, 0, 2, 3).reshape(2, rows, width)

    def head_weights(parts):
        mine = jnp.concatenate(parts[:2], axis=1)
        theirs = jnp.concatenate(parts[2:], axis=1)
        low = jnp.where(first_core, mine, theirs)
        high = jnp.where(first_core, theirs, mine)
        return jnp.concatenate([low, high[:1]], axis=0), high[1]

    def gather_units(s, i, *waits):
        piece = unit_shares[s][:, i * quarter:i * quarter + quarter]
        return jnp.concatenate(ring_gather(tied(piece, *waits), f"u{s}{i}"), axis=1)

    def in_order(pieces):
        return [pieces[i][j] for j in range(4) for i in range(2)]

    column = gather_heads(0)
    heads = spread_out(column, "h0")
    unit_a = gather_units(0, 0, column)
    pieces = [spread_out(unit_a, "u00")]
    unit_b = gather_units(0, 1, unit_a, heads[1])
    pieces.append(spread_out(unit_b, "u01"))
    weights = head_weights(heads) + (in_order(pieces),)
    layers = [weights]
    halves = attention_forward("0", [(tied(x, unit_a),), (x,)], weights, None, tables)
    column = gather_heads(1, unit_b, halves[1][1][0], pieces[0][1])
    heads = spread_out(column, "h1")
    next_a = gather_units(1, 0, column)
    next_pieces = [spread_out(next_a, "u10")]
    next_b = gather_units(1, 1, next_a, heads[1])
    next_pieces.append(spread_out(next_b, "u11"))
    layers.append(head_weights(heads) + (in_order(next_pieces),))
    ends, saved = feed_forward("0", halves, weights, norms[0], (column,), ())
    kept = [saved]
    ends[0] = (tied(ends[0][0], next_a),) + ends[0][1:]
    halves = attention_forward("1", ends, layers[1], norms[0], tables, (next_b,))
    ends, saved = feed_forward("1", halves, layers[1], norms[1], (), ())
    kept.append(saved)
    upstream = to_item(cotangent, core, place)

    def pull_units(tag, gate_up, down):
        parts = []
        for name, grad, count in (("u", gate_up, 2), ("d", down, 1)):
            own = grad[0].reshape(count, 2, ring * half, width)
            got = cross(grad[1], PIPE, 1, f"c_g{name}{tag}").reshape(count, 2, ring * half, width)
            parts.append([added(own[:, 1], got[:, 1]), (own[:, 0], got[:, 0])])
        return parts[0][0], parts[1][0], parts[0][1], parts[1][1]

    def cross_units(tag, units):
        columns = []
        for name, neighbour, (own, got) in (("u", units[0], units[2]), ("d", units[1], units[3])):
            other = cross(neighbour, TENSOR, 2, f"y_g{name}{tag}")
            column = own.astype(F32) + got.astype(F32) + other.astype(F32)
            columns.append(column.astype(BF))
        return columns

    def ring_units(tag, columns):
        totals = []
        for name, column in zip("ud", columns):
            count = column.shape[0]
            column = column.reshape(count, 2, ring, quarter, width)
            total = ring_reduce([column[:, :, k] for k in range(ring)], f"g{name}{tag}")
            totals.append(total.reshape(count, half, width).astype(BF))
        return jnp.concatenate(totals, axis=0)

    def pull_heads(tag, grad_in, grad_out):
        low = jnp.stack(grad_in[:2])
        high = jnp.stack([grad_in[2], grad_out])
        mine = jnp.where(first_core, low, high)
        theirs = cross(jnp.where(first_core, high, low), PIPE, 1, "c_gh" + tag)
        return added(mine[:, rows:], theirs[:, rows:]), mine[:, :rows], theirs[:, :rows]

    def cross_heads(tag, heads):
        neighbour, own, got = heads
        column = own.astype(F32) + got.astype(F32)
        column = column + cross(neighbour, TENSOR, 2, "y_gh" + tag).astype(F32)
        return column.astype(BF)

    def ring_heads(tag, column):
        column = column.reshape(2, ring, head_rows, width).transpose(1, 0, 2, 3)
        ascending = jnp.concatenate([column, column], axis=0)
        rolled = lax.dynamic_slice_in_dim(ascending, (group + 1) % ring, ring, 0)
        return ring_reduce([rolled[ring - 1 - k] for k in range(ring)], "gh" + tag).astype(BF)

    head_totals = [None, None]
    unit_totals = [None, None]
    edges = [None, None]
    norm_grads = [None, None]
    ends = [(upstream,), (upstream,)]
    waits = ()
    for s in (1, 0):
        tag = str(s)
        ends, edges[s], units, heads, norm_grads[s] = layer_backward(
            tag, ends, layers[s], norms[s], tables, kept[s], pull_units, pull_heads, waits
        )
        crossed = cross_units(tag, units)
        unit_totals[s] = ring_units(tag, crossed)
        head_columns = cross_heads(tag, heads)
        head_totals[s] = ring_heads(tag, head_columns)
        waits = crossed
    first_grad = jnp.concatenate(
        [
            (grad[half * MB_CAP // 2:(half + 1) * MB_CAP // 2] + own.astype(F32) + got.astype(F32))
            for half, (grad, own, got) in enumerate(ends)
        ],
        axis=0,
    ).astype(BF)
    activations = from_item([kept[1][1], edges[1]], core, place)
    gradients_in = from_item([first_grad, edges[0]], core, place)

    low, high = joined_by_core(head_totals[0], head_totals[1])
    unit_low, unit_high = joined_by_core(unit_totals[0], unit_totals[1])
    unit_grad = jnp.concatenate([unit_low, unit_high], axis=1).astype(F32)
    head_grad = jnp.concatenate([low, high], axis=0).astype(F32)
    norm_grads[0] = tied(norm_grads[0], heads[0])
    norm_own = jnp.where(first_core, norm_grads[0], norm_grads[1])
    norm_other = jnp.where(first_core, norm_grads[1], norm_grads[0])
    norm_sum = norm_own + flip(norm_other, PIPE, 1)
    norm_sum = norm_sum + flip(norm_sum, TENSOR, 2)
    bit = 1
    while bit < ring:
        norm_sum = norm_sum + flip(norm_sum, FSDP, bit)
        bit = bit * 2
    return (
        activations[None],
        gradients_in[None],
        head_grad[None, :3],
        head_grad[None, 3],
        unit_grad[None, :2],
        unit_grad[None, 2],
        norm_sum[None],
    )


def solution(mesh):
    placed = (
        P(None, (FSDP, TENSOR), None),
        P(None, (FSDP, TENSOR), None),
        P(PIPE, None, (TENSOR, FSDP), None),
        P(PIPE, (TENSOR, FSDP), None),
        P(PIPE, None, (TENSOR, FSDP), None),
        P(PIPE, (TENSOR, FSDP), None),
        P(PIPE, None, None),
        P(None, FSDP, None),
    )
    return jax.shard_map(
        whole_step,
        mesh=mesh,
        in_specs=placed,
        out_specs=(
            P(PIPE, None, (FSDP, TENSOR), None),
            P(PIPE, None, (FSDP, TENSOR), None),
            P(PIPE, None, (TENSOR, FSDP), None),
            P(PIPE, (TENSOR, FSDP), None),
            P(PIPE, None, (TENSOR, FSDP), None),
            P(PIPE, (TENSOR, FSDP), None),
            P(PIPE, None, None),
        ),
        check_vma=False,
    )
```

```python
import jax
import jax.numpy as jnp
from jax import lax
from jax.experimental import pallas as pl
from jax.experimental.pallas import tpu as pltpu
from jax.sharding import PartitionSpec as P

HEAD_DIM = 64
MB_CAP = 512
DOCS = 3

epsilon = 1e-05
rope_base = 1000.0
masked_value = -1e30

BF = jnp.bfloat16
PIPE, FSDP, TENSOR = "pipe", "fsdp", "tensor"
F32 = jnp.float32


def segment_info(lengths):
    doc_ends = jnp.cumsum(lengths)
    starts = doc_ends - lengths
    places = jnp.arange(MB_CAP, dtype=jnp.int32)
    segment = jnp.sum((places[:, None] >= doc_ends[None, :]).astype(jnp.int32), axis=1)
    choose = segment[:, None] == jnp.arange(DOCS, dtype=jnp.int32)[None, :]
    offset = jnp.sum(jnp.where(choose, starts[None, :], 0), axis=1)
    return (segment, places - offset)


def rotary_tables(position):
    half_dim = HEAD_DIM // 2
    frequency = rope_base ** (-2.0 * jnp.arange(half_dim, dtype=F32) / HEAD_DIM)
    angles = position.astype(F32)[:, None] * frequency[None, :]
    cosine, sine = jnp.cos(angles), jnp.sin(angles)
    return jnp.tile(cosine, (1, 4)), jnp.tile(jnp.concatenate([-sine, sine], axis=1), (1, 2))


def flip(array, axis, bit):
    count = lax.axis_size(axis)
    return lax.ppermute(array, axis, [(i, i ^ bit) for i in range(count)])


def shifted(array, axis, by):
    count = lax.axis_size(axis)
    return lax.ppermute(array, axis, [(i, (i + by) % count) for i in range(count)])


def unxor(parts, index):
    parts = [jnp.where(index & 1, parts[m ^ 1], parts[m]) for m in range(4)]
    return [jnp.where(index & 2, parts[m ^ 2], parts[m]) for m in range(4)]


def mixed_flip(array, core_bit, place_bits):
    count = lax.axis_size(TENSOR)
    pairs = [
        (c * count + t, (c ^ core_bit) * count + (t ^ place_bits))
        for c in range(2)
        for t in range(count)
    ]
    return lax.ppermute(array, (PIPE, TENSOR), pairs)


def ring_gather(shard, tag):
    count = lax.axis_size(FSDP)
    slots = [shard]
    for k in range(1, count):
        with jax.named_scope(f"z{k}_{tag}"):
            slots.append(shifted(shard, FSDP, k))
    return slots


def ring_reduce(parts, tag):
    count = len(parts)
    total = parts[0].astype(F32)
    for k in range(1, count):
        with jax.named_scope(f"z{k}_{tag}"):
            part = shifted(parts[k].astype(BF), FSDP, -k)
        total = total + part.astype(F32)
    return total


def cross(array, axis, bit, tag):
    with jax.named_scope(tag):
        return flip(array, axis, bit)


def spread_out(column, tag):
    neighbour = cross(column, TENSOR, 2, "y_" + tag)
    return [
        column,
        neighbour,
        cross(column, PIPE, 1, "c_" + tag),
        cross(neighbour, PIPE, 1, "n_" + tag),
    ]


def added(a, b):
    return (a.astype(F32) + b.astype(F32)).astype(BF)


def row_norm(summed):
    centered = summed - jnp.mean(summed, axis=-1, keepdims=True)
    inverse = lax.rsqrt(jnp.mean(centered * centered, axis=-1, keepdims=True) + epsilon)
    return centered * inverse, inverse


def row_norm_back(normed, inverse, gain_row, upstream):
    scaled = upstream * gain_row
    through = inverse * (
        scaled
        - jnp.mean(scaled, axis=-1, keepdims=True)
        - normed * jnp.mean(scaled * normed, axis=-1, keepdims=True)
    )
    sums = [
        jnp.sum(upstream * normed, axis=0, keepdims=True),
        jnp.sum(upstream, axis=0, keepdims=True),
    ]
    return through, jnp.concatenate(sums + [jnp.zeros((6, sums[0].shape[1]), F32)], axis=0)


def nn(a, b):
    return lax.dot_general(a, b, (((1,), (0,)), ((), ())), preferred_element_type=F32)


def nt(a, b):
    return lax.dot_general(a, b, (((1,), (1,)), ((), ())), preferred_element_type=F32)


def tn(a, b):
    return lax.dot_general(a, b, (((0,), (0,)), ((), ())), preferred_element_type=F32)


def turned(slab, cosine, sines):
    lane = lax.broadcasted_iota(jnp.int32, slab.shape, 1)
    swapped = jnp.where(
        lane % HEAD_DIM < HEAD_DIM // 2, pltpu.roll(slab, 96, 1), pltpu.roll(slab, 32, 1)
    )
    return slab * cosine + swapped * sines


def head_masks(rows):
    lane = lax.broadcasted_iota(jnp.int32, (rows, 128), 1)
    low = (lane < HEAD_DIM).astype(F32)
    return low, 1.0 - low


def rows_of(half, columns, rows):
    return pl.BlockSpec((rows, columns), lambda i: (half, 0))


def whole(array):
    zeros = (0,) * array.ndim
    return pl.BlockSpec(array.shape, lambda i: zeros)


ANYWHERE = pl.BlockSpec(memory_space=pl.ANY)


def staged(tag, kernel, ins, outs, before, scratch=()):
    before = list(before or [])
    arrays = [array for array, _ in ins] + before
    specs = [spec for _, spec in ins] + [ANYWHERE] * len(before)
    first_out = len(outs) - len(before)
    first_in = len(ins)
    count = len(before)

    def run(*refs):
        kernel(*refs[:first_in], *refs[first_in + count:])

    call = pl.pallas_call(
        run,
        grid=(1,),
        in_specs=specs,
        out_specs=[spec for _, _, spec in outs],
        out_shape=[jax.ShapeDtypeStruct(shape, kind) for shape, kind, _ in outs],
        scratch_shapes=list(scratch),
        input_output_aliases={first_in + i: first_out + i for i in range(count)},
        compiler_params=pltpu.CompilerParams(vmem_limit_bytes=40 << 20),
        cost_estimate=pl.CostEstimate(flops=1024, bytes_accessed=1024, transcendentals=0),
        name=kernel.__name__,
    )
    with jax.named_scope("k_" + tag):
        return call(*arrays)


def project(tag, half, sources, norm_rows, weight, cosine, sines, before):
    given = len(sources) == 1
    total, width = sources[0].shape
    heads = weight.shape[1]
    rows = total // 2

    def project_kernel(*refs):
        if given:
            x_ref, w_ref, cos_ref, sin_ref, q_ref, k_ref, v_ref = refs
            low = x_ref[...]
        else:
            (mid_ref, own_ref, got_ref, norm_ref, w_ref, cos_ref, sin_ref,
             q_ref, k_ref, v_ref, x_ref, low_ref) = refs
            summed = mid_ref[...] + own_ref[...].astype(F32) + got_ref[...].astype(F32)
            x = row_norm(summed)[0] * norm_ref[2:3] + norm_ref[3:4]
            x_ref[...] = x
            low = x.astype(BF)
            low_ref[...] = low
        cosine, sines = cos_ref[...], sin_ref[...]
        for c, out in ((0, q_ref), (1, k_ref)):
            turning = nt(low, w_ref[c])
            for slab in range(heads // 128):
                at = slice(128 * slab, 128 * slab + 128)
                out[:, at] = turned(turning[:, at], cosine, sines).astype(BF)
        v_ref[...] = nt(low, w_ref[2]).astype(BF)

    here = rows_of(half, width, rows)
    ins = [(sources[0], here)]
    outs = [((total, heads), BF, rows_of(half, heads, rows)) for _ in range(3)]
    if not given:
        plain = pl.BlockSpec((rows, width), lambda i: (0, 0))
        ins += [(sources[1], plain), (sources[2], plain), (norm_rows, whole(norm_rows))]
        outs += [((total, width), F32, here), ((total, width), BF, here)]
    ins += [(weight, whole(weight))]
    ins += [(table, rows_of(half, 128, rows)) for table in (cosine, sines)]
    return staged(tag, project_kernel, ins, outs, before)


def attend(tag, half, queries, key_vecs, values, segment_column, segment_row, out_weight, before):
    total, heads = queries.shape
    width = out_weight.shape[1]
    rows = total // 2

    def attend_kernel(q_ref, k_ref, v_ref, col_ref, row_ref, w_ref, part_ref, ctx_ref, lse_ref):
        masks = head_masks(rows)
        lane = lax.broadcasted_iota(jnp.int32, (rows, 128), 1)
        same = col_ref[:, :1] == row_ref[:1, :]
        totals = jnp.zeros((rows, 128), F32)
        for slab in range(heads // 128):
            at = slice(128 * slab, 128 * slab + 128)
            q, k, v = q_ref[:, at], k_ref[:, at], v_ref[:, at]
            gathered = jnp.zeros((rows, 128), F32)
            for h in range(2):
                scores = nt(q * masks[h].astype(BF), k) * HEAD_DIM ** (-0.5)
                scores = jnp.where(same, scores, masked_value)
                top = jnp.max(scores, axis=-1, keepdims=True)
                powers = jnp.exp(scores - top)
                mass = jnp.sum(powers, axis=-1, keepdims=True)
                chances = (powers * (1.0 / mass)).astype(BF)
                gathered = gathered + nn(chances, v) * masks[h]
                totals = jnp.where(lane == 2 * slab + h, top + jnp.log(mass), totals)
            ctx_ref[:, at] = gathered.astype(BF)
        lse_ref[...] = totals.T[:8]
        part_ref[...] = nn(ctx_ref[...], w_ref[...]).astype(BF)

    ins = [
        (queries, rows_of(half, heads, rows)),
        (key_vecs, whole(key_vecs)),
        (values, whole(values)),
        (segment_column, rows_of(half, 128, rows)),
        (segment_row, whole(segment_row)),
        (out_weight, whole(out_weight)),
    ]
    outs = [
        ((rows, width), BF, pl.BlockSpec((rows, width), lambda i: (0, 0))),
        ((total, heads), BF, rows_of(half, heads, rows)),
        ((8, total), F32, pl.BlockSpec((8, rows), lambda i: (0, half))),
    ]
    return staged(tag, attend_kernel, ins, outs, before)


def feed_scratch(blocks, rows, width):
    return [
        pltpu.VMEM((len(blocks),) + blocks[0].shape, BF),
        pltpu.VMEM((rows, width), F32),
        pltpu.SemaphoreType.DMA((len(blocks),)),
    ]


def fetch_blocks(block_refs, buffer, sems):
    for j, ref in enumerate(block_refs):
        pltpu.make_async_copy(ref, buffer.at[j], sems.at[j]).start()


def share_blocks(p, block_refs, buffer, sems):
    each = len(block_refs) // 2
    for j in range(p * each, p * each + each):
        pltpu.make_async_copy(block_refs[j], buffer.at[j], sems.at[j]).wait()

    def joined(c):
        return jnp.concatenate([buffer[p * each + j, c] for j in range(each)], axis=0)

    return joined(0), joined(1), joined(2)


def feed(tag, half, x, own, got, norm_rows, blocks, before):
    total, width = x.shape
    rows = total // 2
    step = len(blocks) // 2 * blocks[0].shape[1]
    units = len(blocks) * blocks[0].shape[1]
    count = len(blocks)

    def feed_kernel(*refs):
        x_ref, own_ref, got_ref, norm_ref = refs[:4]
        block_refs = refs[4:4 + count]
        (part_ref, mid_ref, low_ref, gate_ref, up_ref, own_hid, other_hid,
         buffer, acc_ref, sems) = refs[4 + count:]
        fetch_blocks(block_refs, buffer, sems)
        summed = x_ref[...] + own_ref[...].astype(F32) + got_ref[...].astype(F32)
        middle = row_norm(summed)[0] * norm_ref[0:1] + norm_ref[1:2]
        mid_ref[...] = middle
        low = middle.astype(BF)
        low_ref[...] = low
        for p in range(2):
            gate_w, up_w, down_w = share_blocks(p, block_refs, buffer, sems)
            at = slice(p * step, p * step + step)
            gate = nt(low, gate_w)
            up = nt(low, up_w)
            gate_ref[:, at] = gate.astype(BF)
            up_ref[:, at] = up.astype(BF)
            hidden = (gate * jax.nn.sigmoid(gate) * up).astype(BF)
            (own_hid, other_hid)[p][...] = hidden
            fed = nn(hidden, down_w)
            acc_ref[...] = fed if p == 0 else acc_ref[...] + fed
        part_ref[...] = acc_ref[...].astype(BF)

    plain = pl.BlockSpec((rows, width), lambda i: (0, 0))
    here = rows_of(half, width, rows)
    wide = rows_of(half, units, rows)
    ins = [(x, here), (own, plain), (got, plain), (norm_rows, whole(norm_rows))]
    ins += [(block, ANYWHERE) for block in blocks]
    outs = [((rows, width), BF, plain), ((total, width), F32, here), ((total, width), BF, here)]
    outs += [((total, units), BF, wide) for _ in range(2)]
    outs += [((total, step), BF, rows_of(half, step, rows)) for _ in range(2)]
    return staged(tag, feed_kernel, ins, outs, before, feed_scratch(blocks, rows, width))


def feed_back(tag, half, sources, middle, own, got, norm_rows, gate, up, blocks, before):
    top = len(sources) == 1
    total, width = middle.shape
    rows = total // 2
    step = len(blocks) // 2 * blocks[0].shape[1]
    units = len(blocks) * blocks[0].shape[1]
    count = len(blocks)

    def feed_back_kernel(*refs):
        taken = len(sources)
        mid_ref, own_ref, got_ref, norm_ref, gate_ref, up_ref = refs[taken:taken + 6]
        block_refs = refs[taken + 6:taken + 6 + count]
        (part_ref, sums_ref, edge_ref, pre_ref, feed_ref, own_grads, other_grads,
         buffer, acc_ref, sems) = refs[taken + 6 + count:]
        fetch_blocks(block_refs, buffer, sems)
        summed = mid_ref[...] + own_ref[...].astype(F32) + got_ref[...].astype(F32)
        normed, inverse = row_norm(summed)
        if top:
            upstream = refs[0][...].astype(F32)
            edge_ref[...] = (normed * norm_ref[2:3] + norm_ref[3:4]).astype(BF)
        else:
            upstream = refs[0][...] + refs[1][...].astype(F32) + refs[2][...].astype(F32)
            edge_ref[...] = upstream.astype(BF)
        through, sums_ref[...] = row_norm_back(normed, inverse, norm_ref[2:3], upstream)
        pre_ref[...] = through
        low = through.astype(BF)
        feed_ref[...] = low
        for p in range(2):
            gate_w, up_w, down_w = share_blocks(p, block_refs, buffer, sems)
            at = slice(p * step, p * step + step)
            gate, up = gate_ref[:, at].astype(F32), up_ref[:, at].astype(F32)
            grad_hidden = nt(low, down_w)
            sigmoid = jax.nn.sigmoid(gate)
            grad_gate = (grad_hidden * up * sigmoid * (1.0 + gate * (1.0 - sigmoid))).astype(BF)
            grad_up = (grad_hidden * gate * sigmoid).astype(BF)
            share_ref = (own_grads, other_grads)[p]
            share_ref[:, :step] = grad_gate
            share_ref[:, step:] = grad_up
            back_through = nn(grad_gate, gate_w) + nn(grad_up, up_w)
            acc_ref[...] = back_through if p == 0 else acc_ref[...] + back_through
        part_ref[...] = acc_ref[...].astype(BF)

    plain = pl.BlockSpec((rows, width), lambda i: (0, 0))
    here = rows_of(half, width, rows)
    wide = rows_of(half, units, rows)
    ins = [(sources[0], here)] + [(source, plain) for source in sources[1:]]
    ins += [(middle, here), (own, plain), (got, plain), (norm_rows, whole(norm_rows))]
    ins += [(gate, wide), (up, wide)] + [(block, ANYWHERE) for block in blocks]
    outs = [((rows, width), BF, plain), ((8, width), F32, pl.BlockSpec((8, width), lambda i: (0, 0)))]
    outs += [((total, width), BF, here), ((total, width), F32, here), ((total, width), BF, here)]
    outs += [((total, units), BF, wide) for _ in range(2)]
    return staged(tag, feed_back_kernel, ins, outs, before, feed_scratch(blocks, rows, width))


def attend_back(tag, half, grad_middle, x, own, got, norm_rows, queries, key_vecs, values, totals,
                segment_column, segment_row, out_weight, cosine, sines, partial, before):
    total, heads = queries.shape
    width = out_weight.shape[1]
    rows = total // 2
    last = partial is not None

    def attend_back_kernel(*refs):
        (pre_ref, fed_ref, fed_got_ref, x_ref, own_ref, got_ref, norm_ref, q_ref, k_ref, v_ref,
         lse_ref, col_ref, row_ref, w_ref, cos_ref, sin_ref) = refs[:16]
        if last:
            dk_in, dv_in = refs[16:18]
        sums_ref, dk_ref, dv_ref, mid_ref, att_ref, dq_ref, dctx_ref = refs[18 if last else 16:]
        upstream = pre_ref[...] + fed_ref[...].astype(F32) + fed_got_ref[...].astype(F32)
        summed = x_ref[...] + own_ref[...].astype(F32) + got_ref[...].astype(F32)
        normed, inverse = row_norm(summed)
        through, sums_ref[...] = row_norm_back(normed, inverse, norm_ref[0:1], upstream)
        mid_ref[...] = through
        low = through.astype(BF)
        att_ref[...] = low
        dctx_ref[...] = nt(low, w_ref[...]).astype(BF)
        masks = head_masks(rows)
        wide_masks = head_masks(total)
        same = col_ref[:, :1] == row_ref[:1, :]
        scaling = HEAD_DIM ** (-0.5)
        here = pl.ds(half * rows, rows)
        cosine, sines = cos_ref[...], sin_ref[...]
        for slab in range(heads // 128):
            at = slice(128 * slab, 128 * slab + 128)
            q, k, v, grad_ctx = q_ref[:, at], k_ref[:, at], v_ref[:, at], dctx_ref[:, at]
            dq = jnp.zeros((rows, 128), F32)
            dk = jnp.zeros((total, 128), F32)
            dv = jnp.zeros((total, 128), F32)
            for h in range(2):
                mask = masks[h].astype(BF)
                scores = nt(k, q * mask) * scaling
                scores = jnp.where(same, scores, masked_value)
                chances = jnp.exp(scores - lse_ref[2 * slab + h:2 * slab + h + 1, :])
                grad_chances = nt(v, grad_ctx * mask)
                row_dot = jnp.sum(chances * grad_chances, axis=0, keepdims=True)
                grad_scores = (chances * (grad_chances - row_dot)).astype(BF)
                dv = dv + nn(chances.astype(BF), grad_ctx) * wide_masks[h]
                dk = dk + nn(grad_scores, q) * wide_masks[h]
                dq = dq + tn(grad_scores, k) * masks[h]
            dq_ref[:, at] = turned(dq * scaling, cos_ref[here, :], -sin_ref[here, :]).astype(BF)
            if last:
                dk = dk_in[:, at] + dk
                dv = dv_in[:, at] + dv
                dk_ref[:, at] = turned(dk * scaling, cosine, -sines).astype(BF)
                dv_ref[:, at] = dv.astype(BF)
            else:
                dk_ref[:, at] = dk
                dv_ref[:, at] = dv

    plain = pl.BlockSpec((rows, width), lambda i: (0, 0))
    here = rows_of(half, width, rows)
    ins = [(grad_middle[0], here), (grad_middle[1], plain), (grad_middle[2], plain)]
    ins += [(x, here), (own, plain), (got, plain), (norm_rows, whole(norm_rows))]
    ins += [(queries, rows_of(half, heads, rows)), (key_vecs, whole(key_vecs)),
            (values, whole(values)), (totals, pl.BlockSpec((8, rows), lambda i: (0, half))),
            (segment_column, whole(segment_column)),
            (segment_row, pl.BlockSpec((8, rows), lambda i: (0, half))),
            (out_weight, whole(out_weight)), (cosine, whole(cosine)), (sines, whole(sines))]
    if last:
        ins += [(part, whole(part)) for part in partial]
    kind = BF if last else F32
    all_rows = pl.BlockSpec((total, heads), lambda i: (0, 0))
    outs = [((8, width), F32, pl.BlockSpec((8, width), lambda i: (0, 0))),
            ((total, heads), kind, all_rows), ((total, heads), kind, all_rows),
            ((total, width), F32, here), ((total, width), BF, here),
            ((total, heads), BF, rows_of(half, heads, rows))]
    return staged(tag, attend_back_kernel, ins, outs, before, [pltpu.VMEM((rows, heads), BF)])


def inputs_back(tag, half, grads, weight):
    total, heads = grads[0].shape
    width = weight.shape[2]
    rows = total // 2

    def inputs_back_kernel(dq_ref, dk_ref, dv_ref, w_ref, part_ref):
        acc = nn(dq_ref[...], w_ref[0]) + nn(dk_ref[...], w_ref[1]) + nn(dv_ref[...], w_ref[2])
        part_ref[...] = acc.astype(BF)

    ins = [(grad, rows_of(half, heads, rows)) for grad in grads] + [(weight, whole(weight))]
    outs = [((rows, width), BF, pl.BlockSpec((rows, width), lambda i: (0, 0)))]
    return staged(tag, inputs_back_kernel, ins, outs, None)[0]


def across(part, tag):
    with jax.named_scope("x_" + tag):
        return flip(part, TENSOR, 1)


def tied(value, *others):
    return lax.optimization_barrier((value, *others))[0]


def weight_grad(left, right, tag):
    with jax.named_scope("w_" + tag):
        return jnp.einsum("th,td->hd", left, right, preferred_element_type=F32).astype(BF)


def attention_forward(tag, sources, weights, norm_before, tables, wait=()):
    in_weight, out_weight = weights[:2]
    segment_column, segment_row, cosine, sines = tables
    projected = None
    for half in range(2):
        projected = project(f"p{tag}{half}", half, sources[half], norm_before, in_weight, cosine, sines, projected)
    queries, key_vecs, values = projected[:3]
    if len(projected) == 5:
        x, low = projected[3:]
    else:
        low = sources[0][0]
        x = low.astype(F32)
    kept = None
    attended = []
    for half in range(2):
        taken = tied(queries, *wait) if half == 1 else queries
        part, *kept = attend(f"t{tag}{half}", half, taken, key_vecs, values, segment_column, segment_row,
                             out_weight, kept)
        attended.append((part, across(part, f"t{tag}{half}")))
    context, totals = kept
    return (x, low, queries, key_vecs, values, context, totals), attended


def feed_forward(tag, halves, weights, norm_rows, first_wait, second_wait):
    before, attended = halves
    blocks = weights[2]
    x = before[0]
    saved = None
    fed = []
    for half in range(2):
        taken = tied(x, *(second_wait if half else first_wait))
        part, *saved = feed(f"f{tag}{half}", half, taken, *attended[half], norm_rows, blocks, saved)
        fed.append((part, across(part, f"f{tag}{half}")))
    middle, spread, gate, up, *hidden = saved
    ends = [(middle, *fed[half]) for half in range(2)]
    return ends, (*before, attended, middle, spread, gate, up, hidden, fed)


def layer_backward(tag, sources, weights, norm_rows, tables, kept, pull_units, pull_heads, waits):
    in_weight, out_weight, blocks = weights
    segment_column, segment_row, cosine, sines = tables
    (x, low, queries, key_vecs, values, context, totals, attended, middle, spread,
     gate, up, hidden, fed) = kept
    saved = None
    through = []
    sums = []
    for half in range(2):
        part, total, *saved = feed_back(f"g{tag}{half}", half, sources[half], middle, *fed[half], norm_rows,
                                        gate, up, blocks, saved)
        through.append((part, across(part, f"g{tag}{half}")))
        sums.append(total)
    edge, grad_pre_output, grad_feed, *grad_shares = saved
    down = [weight_grad(hidden[i], grad_feed, f"d{tag}{i}") for i in (1, 0)]
    gate_up = [weight_grad(grad_shares[i], spread, f"u{tag}{i}") for i in (1, 0)]
    down, gate_up = down[::-1], gate_up[::-1]
    units = pull_units(tag, gate_up, down)
    partial = None
    saved = None
    first_sums = []
    for half in range(2):
        wait = waits if half == 0 else units[:2]
        total, dk, dv, *saved = attend_back(
            f"h{tag}{half}", half, (tied(grad_pre_output, *wait), *through[half]), x, *attended[half], norm_rows,
            queries, key_vecs, values, totals, segment_column, segment_row,
            out_weight, cosine, sines, partial, saved)
        partial = (dk, dv)
        first_sums.append(total)
    grad_pre_middle, grad_attended, dq = saved
    ends = []
    for half in range(2):
        part = inputs_back(f"i{tag}{half}", half, (dq, dk, dv), in_weight)
        ends.append((grad_pre_middle, part, across(part, f"i{tag}{half}")))
    grad_in = [weight_grad(grad, low, f"n{tag}") for grad in (dq, dk, dv)]
    grad_out = weight_grad(context, grad_attended, f"o{tag}")
    heads = pull_heads(tag, grad_in, grad_out)
    first = first_sums[0] + first_sums[1]
    second = sums[0] + sums[1]
    norm_grad = jnp.concatenate([first[:2], second[:2]], axis=0)
    return ends, edge, units, heads, norm_grad


MESH = pl.DeviceIdType.MESH


def forward_all(layer_inputs, cotangent, heads_in, units_in, norm_in, tables):
    segment_column, segment_row, cosine, sines = tables
    ring = lax.axis_size(FSDP)
    count, own_rows, width = layer_inputs.shape
    total = count * own_rows
    rows = total // 2
    head_rows = heads_in.shape[1]
    half_units = units_in.shape[2]
    heads = 2 * ring * head_rows
    step = 2 * ring * half_units
    order = sorted(range(1, ring), key=lambda k: min(k, ring - k))

    saved = {}
    for l in range(2):
        saved.update({
            f"q{l}": ((total, heads), BF), f"k{l}": ((total, heads), BF),
            f"v{l}": ((total, heads), BF), f"ctx{l}": ((total, heads), BF),
            f"lse{l}": ((8, total), F32), f"pre1{l}": ((total, width), F32),
            f"pre2{l}": ((total, width), F32),
            f"spread{l}": ((total, width), BF), f"feed{l}": ((3, total, 2 * step), BF),
        })
    saved.update({"low0": ((total, width), BF), "acts": ((2, total, width), BF),
                  "cot": ((total, width), BF)})
    inner = {"x1": ((total, width), F32), "mid": ((total, width), F32)}
    for l in range(2):
        for h in range(2):
            for stage in "tf":
                inner[f"own_{stage}{l}{h}"] = ((rows, width), BF)
                inner[f"got_{stage}{l}{h}"] = ((rows, width), BF)
    weights = {}
    for l in range(2):
        weights[f"heads{l}"] = ((4, 2, ring * head_rows, width), BF)
        weights[f"units{l}"] = ((3, 2, 2, ring * half_units, width), BF)
    outs = {**saved, **weights, "norms": ((2, 4, width), F32)}
    held = {**saved, **inner}
    stages = [f"{stage}{l}{h}" for l in range(2) for stage in "tf" for h in range(2)]

    def forward_kernel(inp, cot_ref, heads_ref, units_ref, norm_ref, col_ref, row_ref, cos_ref, sin_ref,
                       *refs):
        out = dict(zip(outs, refs[:len(outs)]))
        rest = refs[len(outs):]
        keep = dict(zip(held, rest[:len(held)]))
        (hbuf, ubuf, nbuf, acc_ref, z_s, z_r, y_s, y_r, k_s, k_r, e_s, e_r, x_s, x_r, i_s, i_r,
         l_s, f_s) = rest[len(held):]
        core = lax.axis_index(PIPE)
        place = lax.axis_index(TENSOR)
        group = lax.axis_index(FSDP)
        other = 1 - core
        item = (place // 2) * 2 + core

        def peer(k):
            low, high = place % 2, place // 2
            low = 1 - low if k & 1 else low
            high = 1 - high if k & 2 else high
            return high * 2 + low

        def near(k):
            return lax.rem(group + k, ring)

        sent = []
        conditional = []

        def send(src, dst, send_sem, recv_sem, **to):
            copy = pltpu.make_async_remote_copy(
                src_ref=src, dst_ref=dst, send_sem=send_sem, recv_sem=recv_sem,
                device_id=to, device_id_type=MESH)
            copy.start()
            sent.append(copy)

        def arrived(dst, send_sem, recv_sem, **to):
            pltpu.make_async_remote_copy(
                src_ref=dst, dst_ref=dst, send_sem=send_sem, recv_sem=recv_sem,
                device_id=to, device_id_type=MESH).wait_recv()

        flushes = []
        done = set()

        def flush(src, name):
            done.add(name)
            copy = pltpu.make_async_copy(src, out[name], f_s.at[len(flushes)])
            copy.start()
            flushes.append(copy)

        def slot(piece, share, col, g):
            l, kind = piece // 2, piece % 2
            if kind == 0:
                at = pl.ds(pl.multiple_of(g * head_rows, 16), head_rows)
                return hbuf.at[l, pl.ds(2 * share, 2), col, at]
            at = pl.ds(pl.multiple_of(g * half_units, 16), half_units)
            return ubuf.at[l, :, share, col, at]

        barrier = pltpu.get_barrier_semaphore()
        peers = [dict(tensor=peer(k)) for k in (1, 2, 3)] + [dict(pipe=other)]
        peers += [dict(fsdp=near(k)) for k in range(1, ring)]
        for to in peers:
            pl.semaphore_signal(barrier, inc=1, device_id=to, device_id_type=MESH)
        pl.semaphore_wait(barrier, len(peers))

        mine = pl.ds(pl.multiple_of(group * head_rows, 16), head_rows)
        mine_units = pl.ds(pl.multiple_of(group * half_units, 16), half_units)
        local = [
            pltpu.make_async_copy(heads_ref.at[pl.ds(2 * core, 2)],
                                  hbuf.at[core, pl.ds(2 * core, 2), 0, mine], l_s.at[0]),
            pltpu.make_async_copy(units_ref.at[:, core],
                                  ubuf.at[core, :, core, 0, mine_units], l_s.at[1]),
            pltpu.make_async_copy(inp.at[item],
                                  keep["low0"].at[pl.ds(pl.multiple_of(place * own_rows, 16),
                                                        own_rows)], l_s.at[2]),
            pltpu.make_async_copy(norm_ref, nbuf.at[core], l_s.at[3]),
            pltpu.make_async_copy(cot_ref.at[item],
                                  keep["cot"].at[pl.ds(pl.multiple_of(place * own_rows, 16),
                                                       own_rows)], l_s.at[4]),
        ]
        send(heads_ref.at[pl.ds(2 * other, 2)], hbuf.at[core, pl.ds(2 * other, 2), 0, mine],
             e_s.at[0], e_r.at[0], pipe=other)
        for copy in local:
            copy.start()
        send(units_ref.at[:, other], ubuf.at[core, :, other, 0, mine_units],
             e_s.at[1], e_r.at[1], pipe=other)
        send(norm_ref, nbuf.at[core], e_s.at[2], e_r.at[2], pipe=other)
        for k in range(1, count):
            send(inp.at[(peer(k) // 2) * 2 + core],
                 keep["low0"].at[pl.ds(pl.multiple_of(place * own_rows, 16), own_rows)],
                 i_s.at[k], i_r.at[k], tensor=peer(k))

        reach = [(sign, d) for d in range(1, ring) for sign in (1, -1)]

        def number(sign, d):
            return d if sign > 0 else ring - 1 + d

        def exists(sign, d):
            return group + d < ring if sign > 0 else group >= d

        def when(condition, action):
            @pl.when(condition)
            def _():
                action().start()

            conditional.append((condition, action))

        def hop_on(piece, sign, d):
            here = slot(piece, core, 0, group + sign * d)
            onward = group >= 1 if sign > 0 else group + 1 < ring
            index = number(sign, d)

            def action():
                return pltpu.make_async_remote_copy(
                    src_ref=here, dst_ref=here, send_sem=z_s.at[piece, index],
                    recv_sem=z_r.at[piece, number(sign, d + 1)],
                    device_id={FSDP: group - sign}, device_id_type=MESH)

            return onward, action

        def own_along(piece):
            for sign in (1, -1):
                here = slot(piece, core, 0, group)
                onward = group >= 1 if sign > 0 else group + 1 < ring

                def action(sign=sign):
                    return pltpu.make_async_remote_copy(
                        src_ref=here, dst_ref=here,
                        send_sem=z_s.at[piece, 0 if sign > 0 else 2 * ring - 1],
                        recv_sem=z_r.at[piece, number(sign, 1)],
                        device_id={FSDP: group - sign}, device_id_type=MESH)

                when(onward, action)

        def across(piece, g, index):
            here = slot(piece, core, 0, g)
            to_side = pltpu.make_async_remote_copy(
                src_ref=here, dst_ref=slot(piece, core, 1, g), send_sem=y_s.at[piece, index],
                recv_sem=y_r.at[piece, index], device_id={TENSOR: peer(2)}, device_id_type=MESH)
            to_core = pltpu.make_async_remote_copy(
                src_ref=here, dst_ref=here, send_sem=k_s.at[piece, 0, index],
                recv_sem=k_r.at[piece, 0, index], device_id={PIPE: other}, device_id_type=MESH)
            return to_side, to_core

        def own_across(piece):
            for copy in across(piece, group, 0):
                copy.start()
                sent.append(copy)

        def hop(piece, d):
            for sign in (1, -1):
                index = number(sign, d)
                g = group + sign * d
                condition = exists(sign, d)

                @pl.when(condition)
                def _():
                    arrived(slot(piece, core, 0, g), z_s.at[piece, index], z_r.at[piece, index],
                            fsdp=group + sign)
                    for copy in across(piece, g, index):
                        copy.start()

                if d + 1 < ring:
                    onward, action = hop_on(piece, sign, d)
                    when(jnp.logical_and(condition, onward), action)
                for i in range(2):
                    conditional.append(
                        (condition, lambda i=i, g=g, index=index: across(piece, g, index)[i]))

        def own_second(piece):
            here = slot(piece, core, 1, group)
            arrived(here, y_s.at[piece, 0], y_r.at[piece, 0], tensor=peer(2))
            send(here, here, k_s.at[piece, 1, 0], k_r.at[piece, 1, 0], pipe=other)

        def second(piece, d):
            for sign in (1, -1):
                index = number(sign, d)
                here = slot(piece, core, 1, group + sign * d)
                condition = exists(sign, d)

                def action(here=here, index=index):
                    return pltpu.make_async_remote_copy(
                        src_ref=here, dst_ref=here, send_sem=k_s.at[piece, 1, index],
                        recv_sem=k_r.at[piece, 1, index], device_id={PIPE: other},
                        device_id_type=MESH)

                @pl.when(condition)
                def _():
                    arrived(here, y_s.at[piece, index], y_r.at[piece, index], tensor=peer(2))

                when(condition, action)

        def pass_second(piece):
            own_second(piece)
            for d in range(1, ring):
                second(piece, d)

        def complete(piece):
            for col in range(2):
                arrived(slot(piece, other, col, group), k_s.at[piece, col, 0],
                        k_r.at[piece, col, 0], pipe=other)
                for sign, d in reach:
                    index = number(sign, d)

                    @pl.when(exists(sign, d))
                    def _():
                        arrived(slot(piece, other, col, group + sign * d),
                                k_s.at[piece, col, index], k_r.at[piece, col, index], pipe=other)
            l = piece // 2
            if piece % 2 == 0:
                flush(hbuf.at[l], f"heads{l}")
            else:
                flush(ubuf.at[l], f"units{l}")

        local[0].wait()
        arrived(hbuf.at[other, pl.ds(2 * core, 2), 0, mine],
                e_s.at[0], e_r.at[0], pipe=other)
        own_along(0)
        own_across(0)
        local[1].wait()
        arrived(ubuf.at[other, :, core, 0, mine_units], e_s.at[1], e_r.at[1], pipe=other)

        def part_of(name, l):
            return nbuf[l, name:name + 1, :]

        def exchange(tag):
            index = stages.index(tag)
            send(keep["own_" + tag], keep["got_" + tag], x_s.at[index], x_r.at[index],
                 tensor=peer(1))

        def taken(tag):
            index = stages.index(tag)
            arrived(keep["got_" + tag], x_s.at[index], x_r.at[index], tensor=peer(1))
            return keep["own_" + tag][...].astype(F32) + keep["got_" + tag][...].astype(F32)

        def do_project(l, half):
            at_rows = slice(half * rows, half * rows + rows)
            if l == 0:
                low = keep["low0"][at_rows]
            else:
                summed = keep["mid"][at_rows] + taken(f"f0{half}")
                keep["pre20"][at_rows] = summed
                x = row_norm(summed)[0] * part_of(2, 0) + part_of(3, 0)
                keep["x1"][at_rows] = x
                low = x.astype(BF)
                keep["acts"][0, at_rows] = low
            cosine, sines = cos_ref[at_rows], sin_ref[at_rows]
            for c, name in ((0, "q"), (1, "k")):
                turning = nt(low, hbuf[l, c].reshape(heads, width))
                for slab in range(heads // 128):
                    at = slice(128 * slab, 128 * slab + 128)
                    keep[f"{name}{l}"][at_rows, at] = turned(
                        turning[:, at], cosine, sines).astype(BF)
            keep[f"v{l}"][at_rows] = nt(low, hbuf[l, 2].reshape(heads, width)).astype(BF)

        def do_attend(l, half):
            at_rows = slice(half * rows, half * rows + rows)
            masks = head_masks(rows)
            lane = lax.broadcasted_iota(jnp.int32, (rows, 128), 1)
            same = col_ref[at_rows, :1] == row_ref[:1, :]
            totals = jnp.zeros((rows, 128), F32)
            for slab in range(heads // 128):
                at = slice(128 * slab, 128 * slab + 128)
                q, k, v = keep[f"q{l}"][at_rows, at], keep[f"k{l}"][:, at], keep[f"v{l}"][:, at]
                gathered = jnp.zeros((rows, 128), F32)
                for h in range(2):
                    scores = nt(q * masks[h].astype(BF), k) * HEAD_DIM ** (-0.5)
                    scores = jnp.where(same, scores, masked_value)
                    top = jnp.max(scores, axis=-1, keepdims=True)
                    powers = jnp.exp(scores - top)
                    mass = jnp.sum(powers, axis=-1, keepdims=True)
                    chances = (powers * (1.0 / mass)).astype(BF)
                    gathered = gathered + nn(chances, v) * masks[h]
                    totals = jnp.where(lane == 2 * slab + h, top + jnp.log(mass), totals)
                keep[f"ctx{l}"][at_rows, at] = gathered.astype(BF)
            keep[f"lse{l}"][:, at_rows] = totals.T[:8]
            part = nn(keep[f"ctx{l}"][at_rows], hbuf[l, 3].reshape(heads, width))
            keep[f"own_t{l}{half}"][...] = part.astype(BF)
            exchange(f"t{l}{half}")

        def do_feed(l, half):
            at_rows = slice(half * rows, half * rows + rows)
            x = keep["low0"][at_rows].astype(F32) if l == 0 else keep["x1"][at_rows]
            summed = x + taken(f"t{l}{half}")
            keep[f"pre1{l}"][at_rows] = summed
            middle = row_norm(summed)[0] * part_of(0, l) + part_of(1, l)
            keep["mid"][at_rows] = middle
            low = middle.astype(BF)
            keep[f"spread{l}"][at_rows] = low
            for share in range(2):
                at = slice(share * step, share * step + step)
                gate = nt(low, ubuf[l, 0, share].reshape(step, width))
                up = nt(low, ubuf[l, 1, share].reshape(step, width))
                keep[f"feed{l}"][0, at_rows, at] = gate.astype(BF)
                keep[f"feed{l}"][1, at_rows, at] = up.astype(BF)
                hidden = (gate * jax.nn.sigmoid(gate) * up).astype(BF)
                keep[f"feed{l}"][2, at_rows, at] = hidden
                fed = nn(hidden, ubuf[l, 2, share].reshape(step, width))
                if share == 0:
                    acc_ref[...] = fed
                else:
                    keep[f"own_f{l}{half}"][...] = (acc_ref[...] + fed).astype(BF)
            exchange(f"f{l}{half}")

        hop(0, 1)
        for d in range(2, ring):
            if d == 3:
                own_along(1)
                own_across(1)
            hop(0, d)
        if ring < 4:
            own_along(1)
            own_across(1)
        pass_second(0)
        for k in range(1, count):
            arrived(keep["low0"].at[pl.ds(pl.multiple_of(peer(k) * own_rows, 16), own_rows)],
                    i_s.at[k], i_r.at[k], tensor=peer(k))
        local[2].wait()
        local[3].wait()
        arrived(nbuf.at[other], e_s.at[2], e_r.at[2], pipe=other)
        complete(0)
        do_project(0, 0)
        do_project(0, 1)
        hop(1, 1)
        own_along(2)
        do_attend(0, 0)
        do_attend(0, 1)
        hop(1, 2)
        own_across(2)
        hop(2, 1)
        own_along(3)
        for d in range(3, ring):
            hop(1, d)
        for d in range(2, ring):
            hop(2, d)
        own_across(3)
        pass_second(1)
        complete(1)
        do_feed(0, 0)
        hop(3, 1)
        do_feed(0, 1)
        hop(3, 2)
        pass_second(2)
        complete(2)
        do_project(1, 0)
        do_project(1, 1)
        for d in range(3, ring):
            hop(3, d)
        do_attend(1, 0)
        do_attend(1, 1)
        for k in range(1, count):
            send(cot_ref.at[(peer(k) // 2) * 2 + core],
                 keep["cot"].at[pl.ds(pl.multiple_of(place * own_rows, 16), own_rows)],
                 i_s.at[count + k], i_r.at[count + k], tensor=peer(k))
        pass_second(3)
        complete(3)
        do_feed(1, 0)
        do_feed(1, 1)
        flush(nbuf, "norms")
        local[4].wait()
        for k in range(1, count):
            arrived(keep["cot"].at[pl.ds(pl.multiple_of(peer(k) * own_rows, 16), own_rows)],
                    i_s.at[count + k], i_r.at[count + k], tensor=peer(k))
        for half in range(2):
            at_rows = slice(half * rows, half * rows + rows)
            summed = keep["mid"][at_rows] + taken(f"f1{half}")
            keep["pre21"][at_rows] = summed
            keep["acts"][1, at_rows] = (
                row_norm(summed)[0] * part_of(2, 1) + part_of(3, 1)).astype(BF)
        for name in saved:
            if name not in done:
                flush(keep[name], name)
        for copy in sent:
            copy.wait_send()
        for condition, action in conditional:
            @pl.when(condition)
            def _():
                action().wait_send()

        for copy in flushes:
            copy.wait()

    anywhere = pl.BlockSpec(memory_space=pl.ANY)
    inside = pl.BlockSpec(memory_space=pltpu.VMEM)
    dma = pltpu.SemaphoreType.DMA
    scratch = [pltpu.VMEM(shape, kind) for shape, kind in held.values()]
    scratch += [
        pltpu.VMEM((2, 4, 2, ring * head_rows, width), BF),
        pltpu.VMEM((2, 3, 2, 2, ring * half_units, width), BF),
        pltpu.VMEM((2, 4, width), F32),
        pltpu.VMEM((rows, width), F32),
        dma((4, 2 * ring)), dma((4, 2 * ring)), dma((4, 2 * ring)), dma((4, 2 * ring)),
        dma((4, 2, 2 * ring)), dma((4, 2, 2 * ring)), dma((3,)), dma((3,)),
        dma((len(stages),)), dma((len(stages),)), dma((2 * count,)), dma((2 * count,)),
        dma((5,)), dma((len(outs),)),
    ]
    results = pl.pallas_call(
        forward_kernel,
        in_specs=[anywhere] * 4 + [inside] * 5,
        out_specs=[anywhere] * len(outs),
        out_shape=[jax.ShapeDtypeStruct(shape, kind) for shape, kind in outs.values()],
        scratch_shapes=scratch,
        compiler_params=pltpu.CompilerParams(
            collective_id=0, has_side_effects=True, vmem_limit_bytes=62 << 20),
        name="forward_kernel",
    )(layer_inputs, cotangent, heads_in, units_in, norm_in, segment_column, segment_row, cosine, sines)
    return dict(zip(outs, results))


def backward_all(saved, count, tables):
    segment_column, segment_row, cosine, sines = tables
    ring = lax.axis_size(FSDP)
    total, width = saved["cot"].shape
    own_rows = total // count
    rows = total // 2
    heads = saved["q0"].shape[1]
    step = saved["feed0"].shape[2] // 2
    head_rows = heads // (2 * ring)
    half_units = step // (2 * ring)
    order = sorted(range(1, ring), key=lambda k: min(k, ring - k))
    loaded = ("q", "k", "v", "lse", "pre1", "pre2", "spread", "feed", "heads", "units")
    arrays = [saved[f"{name}{l}"] for l in range(2) for name in loaded]
    arrays += [saved["ctx0"], saved["ctx1"], saved["low0"], saved["acts"], saved["cot"]]
    stages = [f"{stage}{l}{h}" for l in range(2) for stage in "gi" for h in range(2)]
    pieces = ("d", "g", "u", "h")
    scaling = HEAD_DIM ** (-0.5)

    def backward_kernel(norm_ref, col_ref, row_ref, cos_ref, sin_ref, *refs):
        n = len(arrays)
        from_hbm = {}
        for l in range(2):
            for i, name in enumerate(loaded):
                from_hbm[f"{name}{l}"] = refs[l * len(loaded) + i]
        from_hbm["ctx0"], from_hbm["ctx1"], from_hbm["low0"], acts_ref, cot_ref = refs[n - 5:n]
        from_hbm["low1"] = acts_ref.at[0]
        (act_out, grad_out, units_out, heads_out, norm_out) = refs[n:n + 5]
        rest = refs[n + 5:]
        buffers = [name for name in loaded if name != "spread"]
        here = dict(zip(buffers, rest[:len(buffers)]))
        (lefts, rights, dpre, wide_rights, dctx, grads, own, got, nsum, nred, nget,
         acc, keep_u, keep_h, give_u, give_h, core_u, core_h, side_u, side_h, line_u, line_h,
         fin_u, fin_h, x_s, x_r, a_s, a_r, b_s, b_r, c_s, c_r, y_s, y_r, z_s, z_r,
         n_s, n_r, j_s, j_r, l_s, m_s, credit_c, credit_y) = rest[len(buffers):]
        dfeed = wide_rights.at[1]
        cot = grads.at[0]
        core = lax.axis_index(PIPE)
        place = lax.axis_index(TENSOR)
        group = lax.axis_index(FSDP)
        other = 1 - core
        item = (place // 2) * 2 + core

        def peer(k):
            low, high = place % 2, place // 2
            low = 1 - low if k & 1 else low
            high = 1 - high if k & 2 else high
            return high * 2 + low

        def near(k):
            return lax.rem(group + k, ring)

        pending = []

        def send(src, dst, send_sem, recv_sem, **to):
            copy = pltpu.make_async_remote_copy(
                src_ref=src, dst_ref=dst, send_sem=send_sem, recv_sem=recv_sem,
                device_id=to, device_id_type=MESH)
            copy.start()
            pending.append(copy)
            return copy

        def arrived(dst, send_sem, recv_sem, **to):
            pltpu.make_async_remote_copy(
                src_ref=dst, dst_ref=dst, send_sem=send_sem, recv_sem=recv_sem,
                device_id=to, device_id_type=MESH).wait_recv()

        def sent(copy):
            copy.wait_send()
            pending[:] = [held for held in pending if held is not copy]

        names = loaded + ("ctx", "low")
        loads = {}

        def load(l, *which):
            for name in which:
                to = {"ctx": lefts.at[3], "low": rights.at[0],
                      "spread": wide_rights.at[0]}.get(name)
                to = here[name] if to is None else to
                copy = pltpu.make_async_copy(from_hbm[f"{name}{l}"], to,
                                             l_s.at[l * len(names) + names.index(name)])
                copy.start()
                loads[name, l] = copy

        def ready(l, *which):
            for name in which:
                loads.pop((name, l)).wait()

        def rows_at(index):
            return pl.ds(pl.multiple_of(index * own_rows, 16), own_rows)

        barrier = pltpu.get_barrier_semaphore()
        peers = [dict(tensor=peer(k)) for k in (1, 2, 3)]
        peers += [dict(pipe=other), dict(pipe=other, tensor=peer(2))]
        peers += [dict(fsdp=near(k)) for k in range(1, ring)]
        for to in peers:
            pl.semaphore_signal(barrier, inc=1, device_id=to, device_id_type=MESH)
        pl.semaphore_wait(barrier, len(peers))

        own_cot = pltpu.make_async_copy(cot_ref, cot, m_s.at[0])
        own_cot.start()
        load(1, "pre2", "feed", "spread", "units", "pre1", "heads", "q", "k", "v", "lse", "ctx",
             "low")

        def home(source, result, sems, index):
            copy = pltpu.make_async_copy(source.at[core, rows_at(place)], result.at[item],
                                         m_s.at[index])
            copy.start()
            for k in range(1, 4):
                layer = other if k & 1 else core
                to = dict(pipe=layer, tensor=peer(k & 2))
                send(source.at[layer, rows_at(peer(k & 2))], result.at[item],
                     sems[0].at[k], sems[1].at[k], **to)
            return copy

        def home_arrived(result, sems):
            for k in range(1, 4):
                to = dict(pipe=other if k & 1 else core, tensor=peer(k & 2))
                index = (peer(k & 2) // 2) * 2 + (other if k & 1 else core)
                arrived(result.at[index], sems[0].at[k], sems[1].at[k], **to)

        own_act = home(acts_ref, act_out, (a_s, a_r), 1)
        own_cot.wait()
        last_use = {}

        def exchange(tag, value):
            place_of = "gi".index(tag[0]) * 2 + int(tag[2])
            if place_of in last_use:
                sent(last_use[place_of])
            own[place_of] = value
            index = stages.index(tag)
            last_use[place_of] = send(own.at[place_of], got.at[index], x_s.at[index],
                                      x_r.at[index], tensor=peer(1))

        def taken(tag):
            index = stages.index(tag)
            place_of = "gi".index(tag[0]) * 2 + int(tag[2])
            arrived(got.at[index], x_s.at[index], x_r.at[index], tensor=peer(1))
            return own[place_of].astype(F32) + got[index].astype(F32)

        def part_of(name, l):
            return norm_ref[l, name:name + 1, :]

        def note_sums(l, half, first, sums):
            if half == 0:
                nsum[l, first:first + 2] = sums[:2]
            else:
                nsum[l, first:first + 2] = nsum[l, first:first + 2] + sums[:2]

        def do_norm_back(l, half):
            at_rows = slice(half * rows, half * rows + rows)
            if l == 1:
                upstream = cot[at_rows].astype(F32)
            else:
                upstream = dpre[at_rows] + taken(f"i1{half}")
                grads[1, at_rows] = upstream.astype(BF)
            if half == 0:
                ready(l, "pre2")
            normed, inverse = row_norm(here["pre2"][at_rows])
            through, sums = row_norm_back(normed, inverse, part_of(2, l), upstream)
            note_sums(l, half, 2, sums)
            dpre[at_rows] = through
            dfeed[at_rows] = through.astype(BF)

        def do_feed_back(l, half):
            at_rows = slice(half * rows, half * rows + rows)
            low = dfeed[at_rows]
            if half == 0:
                ready(l, "units")
            units, feed_ref = here["units"], here["feed"]
            for share in range(2):
                at = slice(share * step, share * step + step)
                gate = feed_ref[0, at_rows, at].astype(F32)
                up = feed_ref[1, at_rows, at].astype(F32)
                grad_hidden = nt(low, units[2, share].reshape(step, width))
                sigmoid = jax.nn.sigmoid(gate)
                grad_gate = (
                    grad_hidden * up * sigmoid * (1.0 + gate * (1.0 - sigmoid))).astype(BF)
                grad_up = (grad_hidden * gate * sigmoid).astype(BF)
                feed_ref[0, at_rows, at] = grad_gate
                feed_ref[1, at_rows, at] = grad_up
                back = nn(grad_gate, units[0, share].reshape(step, width))
                back = back + nn(grad_up, units[1, share].reshape(step, width))
                if share == 0:
                    acc[...] = back
                else:
                    exchange(f"g{l}{half}", (acc[...] + back).astype(BF))

        def unit_grads(first, end, share, target):
            size = step // 2

            def one(i, _):
                c, col = i // 2, i % 2
                at = pl.ds(pl.multiple_of(share * step + col * size, 128), size)
                target[c, col] = tn(here["feed"][c, :, at], wide_rights[c // 2]).astype(BF)
                return 0

            lax.fori_loop(2 * first, 2 * end, one, 0)

        def head_grad(share, target):
            for i in range(2):
                j = 2 * share + i
                full = tn(lefts[j], rights[j // 3]).astype(BF)
                for col in range(2):
                    target[i, col] = full[col * (heads // 2):(col + 1) * (heads // 2)]

        def do_attend_back(l, half):
            at_rows = slice(half * rows, half * rows + rows)
            if half == 0:
                ready(l, "pre1", "heads", "q", "k", "v", "lse")
            upstream = dpre[at_rows] + taken(f"g{l}{half}")
            normed, inverse = row_norm(here["pre1"][at_rows])
            through, sums = row_norm_back(normed, inverse, part_of(0, l), upstream)
            note_sums(l, half, 0, sums)
            dpre[at_rows] = through
            low = through.astype(BF)
            rights[1, at_rows] = low
            dctx[...] = nt(low, here["heads"][3].reshape(heads, width)).astype(BF)
            masks = head_masks(rows)
            wide_masks = head_masks(total)
            same = col_ref[:, :1] == row_ref[:1, at_rows]
            for slab in range(heads // 128):
                at = slice(slab * 128, slab * 128 + 128)
                second_at = slice(heads + slab * 128, heads + slab * 128 + 128)
                q, k = here["q"][at_rows, at], here["k"][:, at]
                v, grad_ctx = here["v"][:, at], dctx[:, at]
                dq = jnp.zeros((rows, 128), F32)
                dk = jnp.zeros((total, 128), F32)
                dv = jnp.zeros((total, 128), F32)
                for h in range(2):
                    mask = masks[h].astype(BF)
                    scores = nt(k, q * mask) * scaling
                    scores = jnp.where(same, scores, masked_value)
                    lse = here["lse"][2 * slab + h:2 * slab + h + 1, at_rows]
                    chances = jnp.exp(scores - lse)
                    grad_chances = nt(v, grad_ctx * mask)
                    row_dot = jnp.sum(chances * grad_chances, axis=0, keepdims=True)
                    grad_scores = (chances * (grad_chances - row_dot)).astype(BF)
                    dv = dv + nn(chances.astype(BF), grad_ctx) * wide_masks[h]
                    dk = dk + nn(grad_scores, q) * wide_masks[h]
                    dq = dq + tn(grad_scores, k) * masks[h]
                lefts[0, at_rows, at] = turned(
                    dq * scaling, cos_ref[at_rows], -sin_ref[at_rows]).astype(BF)
                if half == 0:
                    here["pre2"][:, at] = dk
                    here["pre2"][:, second_at] = dv
                else:
                    dk = here["pre2"][:, at] + dk
                    dv = here["pre2"][:, second_at] + dv
                    lefts[1, :, at] = turned(dk * scaling, cos_ref[...], -sin_ref[...]).astype(BF)
                    lefts[2, :, at] = dv.astype(BF)

        def do_inputs_back(l, half):
            at_rows = slice(half * rows, half * rows + rows)
            back = jnp.zeros((rows, width), F32)
            for c in range(3):
                back = back + nn(lefts[c, at_rows], here["heads"][c].reshape(heads, width))
            exchange(f"i{l}{half}", back.astype(BF))

        def parts(piece, units_ref, heads_ref):
            index = pieces.index(piece)
            return heads_ref if index == 3 else units_ref.at[(2, 0, 1)[index]:(3, 1, 2)[index]]

        def cell(piece, l):
            return l * 4 + pieces.index(piece)

        gave = {}

        def give(l, piece):
            if l == 0:
                pl.semaphore_wait(credit_c.at[pieces.index(piece)], 1)
            index = cell(piece, l)
            gave[piece] = send(parts(piece, give_u, give_h), parts(piece, core_u, core_h),
                               c_s.at[index], c_r.at[index], pipe=other)

        def add_core(l, piece):
            index = cell(piece, l)
            come = parts(piece, core_u, core_h)
            arrived(come, c_s.at[index], c_r.at[index], pipe=other)
            mine = parts(piece, keep_u.at[l], keep_h.at[l])
            mine[...] = (mine[...].astype(F32) + come[...].astype(F32)).astype(BF)
            if l == 1:
                pl.semaphore_signal(credit_c.at[pieces.index(piece)], inc=1,
                                    device_id=dict(pipe=other), device_id_type=MESH)
            else:
                pl.semaphore_wait(credit_y.at[pieces.index(piece)], 1)
            send(mine.at[:, 1], parts(piece, side_u, side_h), y_s.at[index], y_r.at[index],
                 tensor=peer(2))

        def slot_of(piece, ref, g):
            size = head_rows if piece == "h" else half_units
            return ref.at[:, pl.ds(pl.multiple_of(g * size, 16), size)]

        def add_side(l, piece):
            index = cell(piece, l)
            come = parts(piece, side_u, side_h)
            arrived(come, y_s.at[index], y_r.at[index], tensor=peer(2))
            mine = parts(piece, keep_u.at[l], keep_h.at[l]).at[:, 0]
            mine[...] = (mine[...].astype(F32) + come[...].astype(F32)).astype(BF)
            if l == 1:
                pl.semaphore_signal(credit_y.at[pieces.index(piece)], inc=1,
                                    device_id=dict(tensor=peer(2)), device_id_type=MESH)
            for sign in (1, -1):
                @pl.when(inner(sign))
                def _():
                    next_one(l, piece, sign).start()

            @pl.when(at_end)
            def _():
                to_far(l, piece).start()
                to_relay(l, piece).start()

        at_end = jnp.logical_or(group == 0, group == ring - 1)

        def inner(sign):
            return group + 1 < ring if sign > 0 else group >= 1

        def line_send(l, piece, g, kind, to):
            index = cell(piece, l)
            mine = parts(piece, keep_u.at[l], keep_h.at[l]).at[:, 0]
            return pltpu.make_async_remote_copy(
                src_ref=slot_of(piece, mine, g),
                dst_ref=parts(piece, line_u.at[l, kind], line_h.at[l, kind]),
                send_sem=z_s.at[index, kind], recv_sem=z_r.at[index, kind],
                device_id={FSDP: to}, device_id_type=MESH)

        def next_one(l, piece, sign):
            return line_send(l, piece, group + sign, 0 if sign > 0 else 1, group + sign)

        def far():
            return lax.rem(group + 2, 4)

        def to_far(l, piece):
            return line_send(l, piece, far(), 2, far())

        def to_relay(l, piece):
            opposite = ring - 1 - group
            return line_send(l, piece, opposite, 3, jnp.where(group == 0, 1, 2))

        def relay(l, piece):
            @pl.when(jnp.logical_not(at_end))
            def _():
                index = cell(piece, l)
                come = parts(piece, line_u.at[l, 3], line_h.at[l, 3])
                arrived(come, z_s.at[index, 3], z_r.at[index, 3],
                        fsdp=jnp.where(group == 1, 0, 3))
                mine = slot_of(piece, parts(piece, keep_u.at[l], keep_h.at[l]).at[:, 0], far())
                mine[...] = (mine[...].astype(F32) + come[...].astype(F32)).astype(BF)
                to_far(l, piece).start()

        def add_line(l, piece):
            index = cell(piece, l)
            mine = parts(piece, keep_u.at[l], keep_h.at[l]).at[:, 0]
            result = parts(piece, fin_u.at[l], fin_h.at[l])
            come = [parts(piece, line_u.at[l, kind], line_h.at[l, kind]) for kind in range(3)]
            arrived(come[2], z_s.at[index, 2], z_r.at[index, 2], fsdp=far())
            result[...] = (slot_of(piece, mine, group)[...].astype(F32)
                           + come[2][...].astype(F32)).astype(BF)
            for sign in (1, -1):
                kind = 0 if sign > 0 else 1

                @pl.when(inner(-sign))
                def _():
                    arrived(come[kind], z_s.at[index, kind], z_r.at[index, kind],
                            fsdp=group - sign)
                    result[...] = (result[...].astype(F32)
                                   + come[kind][...].astype(F32)).astype(BF)

        def line_sent(l, piece):
            for sign in (1, -1):
                @pl.when(inner(sign))
                def _():
                    next_one(l, piece, sign).wait_send()

            to_far(l, piece).wait_send()

            @pl.when(at_end)
            def _():
                to_relay(l, piece).wait_send()

        do_norm_back(1, 0)
        do_norm_back(1, 1)
        ready(1, "feed", "spread")
        unit_grads(2, 3, other, give_u)
        give(1, "d")
        do_feed_back(1, 0)
        do_feed_back(1, 1)
        unit_grads(0, 2, other, give_u)
        give(1, "g")
        give(1, "u")
        unit_grads(2, 3, core, keep_u.at[1])
        add_core(1, "d")
        unit_grads(0, 2, core, keep_u.at[1])
        load(0, "feed", "spread", "units")
        do_attend_back(1, 0)
        add_core(1, "g")
        add_core(1, "u")
        do_attend_back(1, 1)
        load(0, "pre2")
        for half in range(2):
            do_inputs_back(1, half)
        add_side(1, "d")
        ready(1, "ctx", "low")
        head_grad(other, give_h)
        give(1, "h")
        relay(1, "d")
        head_grad(core, keep_h.at[1])
        load(0, "pre1", "heads", "q", "k", "v", "lse", "ctx", "low")
        add_side(1, "g")

        do_norm_back(0, 0)
        ready(0, "feed", "spread")
        do_feed_back(0, 0)
        add_core(1, "h")
        relay(1, "g")
        do_norm_back(0, 1)
        sent(gave["d"])
        unit_grads(2, 3, other, give_u)
        give(0, "d")
        do_feed_back(0, 1)
        add_side(1, "u")
        sent(gave["g"])
        sent(gave["u"])
        unit_grads(0, 2, other, give_u)
        give(0, "g")
        give(0, "u")
        unit_grads(2, 3, core, keep_u.at[0])
        add_core(0, "d")
        relay(1, "u")
        unit_grads(0, 2, core, keep_u.at[0])
        do_attend_back(0, 0)
        add_side(1, "h")
        add_core(0, "g")
        add_core(0, "u")
        relay(1, "h")
        do_attend_back(0, 1)
        send(nsum.at[other], nget.at[0], n_s.at[0], n_r.at[0], pipe=other)
        ready(0, "ctx", "low")
        sent(gave["h"])
        head_grad(other, give_h)
        give(0, "h")
        for half in range(2):
            do_inputs_back(0, half)
        head_grad(core, keep_h.at[0])
        add_core(0, "h")
        add_side(0, "d")
        relay(0, "d")
        add_side(0, "g")
        arrived(nget.at[0], n_s.at[0], n_r.at[0], pipe=other)
        nred[0] = nsum[core] + nget[0]
        send(nred.at[0], nget.at[1], n_s.at[1], n_r.at[1], tensor=peer(2))
        for half in range(2):
            at_rows = slice(half * rows, half * rows + rows)
            grads[0, at_rows] = (dpre[at_rows] + taken(f"i0{half}")).astype(BF)
        own_grad = home(grads, grad_out, (b_s, b_r), 2)
        relay(0, "g")
        add_side(0, "u")
        arrived(nget.at[1], n_s.at[1], n_r.at[1], tensor=peer(2))
        nred[1] = nred[0] + nget[1]
        for k in order:
            send(nred.at[1], nget.at[1 + (ring - k) % ring], n_s.at[1 + k],
                 n_r.at[1 + (ring - k) % ring], fsdp=near(k))
        relay(0, "u")
        add_side(0, "h")
        for piece in pieces:
            add_line(1, piece)
        relay(0, "h")
        add_line(0, "d")
        add_line(0, "g")
        norms = nred[1]
        for k in order:
            arrived(nget.at[1 + k], n_s.at[1 + k], n_r.at[1 + k], fsdp=near(k))
            norms = norms + nget[1 + k]
        norm_out[...] = norms
        add_line(0, "u")
        add_line(0, "h")
        joins = []
        for i, (fin, result) in enumerate(((fin_u, units_out), (fin_h, heads_out))):
            send(fin.at[other], result.at[core], j_s.at[i], j_r.at[i], pipe=other)
            copy = pltpu.make_async_copy(fin.at[core], result.at[core], m_s.at[3 + i])
            copy.start()
            joins.append(copy)
        for i, result in enumerate((units_out, heads_out)):
            arrived(result.at[other], j_s.at[i], j_r.at[i], pipe=other)
        home_arrived(act_out, (a_s, a_r))
        home_arrived(grad_out, (b_s, b_r))
        for copy in [own_act, own_grad] + joins:
            copy.wait()
        for copy in pending:
            copy.wait_send()
        for l in range(2):
            for piece in pieces:
                line_sent(l, piece)

    anywhere = pl.BlockSpec(memory_space=pl.ANY)
    inside = pl.BlockSpec(memory_space=pltpu.VMEM)
    dma = pltpu.SemaphoreType.DMA
    scratch = [pltpu.VMEM(saved[f"{name}0"].shape, saved[f"{name}0"].dtype) for name in loaded
               if name != "spread"]
    scratch += [
        pltpu.VMEM((4, total, heads), BF), pltpu.VMEM((2, total, width), BF),
        pltpu.VMEM((total, width), F32), pltpu.VMEM((2, total, width), BF),
        pltpu.VMEM((rows, heads), BF),
        pltpu.VMEM((2, total, width), BF),
        pltpu.VMEM((4, rows, width), BF), pltpu.VMEM((8, rows, width), BF),
        pltpu.VMEM((2, 4, width), F32), pltpu.VMEM((2, 4, width), F32),
        pltpu.VMEM((1 + ring, 4, width), F32), pltpu.VMEM((rows, width), F32),
        pltpu.VMEM((2, 3, 2, ring * half_units, width), BF),
        pltpu.VMEM((2, 2, 2, ring * head_rows, width), BF),
        pltpu.VMEM((3, 2, ring * half_units, width), BF),
        pltpu.VMEM((2, 2, ring * head_rows, width), BF),
        pltpu.VMEM((3, 2, ring * half_units, width), BF),
        pltpu.VMEM((2, 2, ring * head_rows, width), BF),
        pltpu.VMEM((3, ring * half_units, width), BF),
        pltpu.VMEM((2, ring * head_rows, width), BF),
        pltpu.VMEM((2, ring, 3, half_units, width), BF),
        pltpu.VMEM((2, ring, 2, head_rows, width), BF),
        pltpu.VMEM((2, 3, half_units, width), BF),
        pltpu.VMEM((2, 2, head_rows, width), BF),
        dma((8,)), dma((8,)), dma((4,)), dma((4,)), dma((4,)), dma((4,)),
        dma((8,)), dma((8,)), dma((8,)), dma((8,)), dma((8, 4)), dma((8, 4)),
        dma((1 + ring,)), dma((1 + ring,)), dma((2,)), dma((2,)),
        dma((2 * (len(loaded) + 2),)), dma((5,)),
        pltpu.SemaphoreType.REGULAR((4,)), pltpu.SemaphoreType.REGULAR((4,)),
    ]
    return pl.pallas_call(
        backward_kernel,
        in_specs=[inside] * 5 + [anywhere] * len(arrays),
        out_specs=[anywhere] * 4 + [inside],
        out_shape=[
            jax.ShapeDtypeStruct((count, own_rows, width), BF),
            jax.ShapeDtypeStruct((count, own_rows, width), BF),
            jax.ShapeDtypeStruct((2, 3, half_units, width), BF),
            jax.ShapeDtypeStruct((2, 2, head_rows, width), BF),
            jax.ShapeDtypeStruct((4, width), F32),
        ],
        scratch_shapes=scratch,
        compiler_params=pltpu.CompilerParams(
            collective_id=1, has_side_effects=True, vmem_limit_bytes=67043328),
        name="backward_kernel",
    )(saved["norms"], segment_column, segment_row, cosine, sines, *arrays)


def to_item(array, core, place):
    def piece(k):
        return lax.dynamic_index_in_dim(array, ((place ^ k) & 2) | core, 0, keepdims=False)

    parts = [piece(0)] + [flip(piece(k), TENSOR, k) for k in range(1, 4)]
    return jnp.concatenate(unxor(parts, place), axis=0)


def from_item(by_layer, core, place):
    rows = by_layer[0].shape[0] // 4
    mine = jnp.where(core == 0, by_layer[0], by_layer[1])
    other = jnp.where(core == 0, by_layer[1], by_layer[0])

    def piece(k):
        target = place ^ (k & 2)
        return lax.dynamic_slice_in_dim(other if k & 1 else mine, target * rows, rows, 0)

    parts = [piece(0)] + [mixed_flip(piece(k), k & 1, k & 2) for k in range(1, 4)]
    return jnp.stack(unxor(parts, (place & 2) | core)).astype(F32)


def whole_step(
    layer_inputs,
    cotangent,
    input_master,
    output_master,
    gate_master,
    down_master,
    norm_tables,
    document_lengths,
):
    core = lax.axis_index(PIPE)
    place = lax.axis_index(TENSOR)
    group = lax.axis_index(FSDP)
    ring = lax.axis_size(FSDP)
    width = layer_inputs.shape[2]
    head_rows = input_master.shape[2]
    units = down_master.shape[1]
    half = units // 2
    first_core = core == 0

    item = (place & 2) | core
    lengths = lax.dynamic_index_in_dim(document_lengths[:, 0, :], item, 0, keepdims=False)
    segment, position = segment_info(lengths)
    segment_column = jnp.broadcast_to(segment[:, None], (MB_CAP, 128))
    segment_row = jnp.broadcast_to(segment[None, :], (8, MB_CAP))
    tables = (segment_column, segment_row) + rotary_tables(position)

    def split_by_core(for_first, for_second):
        keep = jnp.where(first_core, for_first, for_second)
        got = flip(jnp.where(first_core, for_second, for_first), PIPE, 1)
        return [jnp.where(first_core, keep, got), jnp.where(first_core, got, keep)]

    def joined_by_core(share_zero, share_one):
        keep = jnp.where(first_core, share_zero, share_one)
        got = flip(jnp.where(first_core, share_one, share_zero), PIPE, 1)
        return jnp.where(first_core, keep, got), jnp.where(first_core, got, keep)

    if head_rows % 16 == 0 and half % 16 == 0 and ring == 4:
        heads_in = jnp.concatenate([input_master[0], output_master], axis=0).astype(BF)
        units_in = jnp.concatenate([gate_master[0], down_master], axis=0).astype(BF)
        saved = forward_all(layer_inputs, cotangent, heads_in, units_in.reshape(3, 2, half, width),
                            norm_tables[0], tables)
        results = backward_all(saved, cotangent.shape[0], tables)
        activations, gradients_in, unit_grad, head_grad, norm_sum = results
        head_grad = head_grad.reshape(4, head_rows, width).astype(F32)
        unit_grad = unit_grad.transpose(1, 0, 2, 3).reshape(3, units, width).astype(F32)
        return (
            activations[None].astype(F32),
            gradients_in[None].astype(F32),
            head_grad[None, :3],
            head_grad[None, 3],
            unit_grad[None, :2],
            unit_grad[None, 2],
            norm_sum[None],
        )

    in_low = input_master[0].astype(BF)
    out_low = output_master.astype(BF)
    head_shares = split_by_core(in_low[:2], jnp.concatenate([in_low[2:], out_low], axis=0))
    unit_low = jnp.concatenate([gate_master[0], down_master], axis=0).astype(BF)
    unit_shares = split_by_core(unit_low[:, :half], unit_low[:, half:])

    x = to_item(layer_inputs, core, place)
    norm_own = norm_tables[0]
    norm_other = flip(norm_own, PIPE, 1)
    norms = [
        jnp.where(first_core, norm_own, norm_other),
        jnp.where(first_core, norm_other, norm_own),
    ]

    quarter = half // 2
    rows = ring * head_rows

    def gather_heads(s, *waits):
        slots = ring_gather(tied(head_shares[s], *waits), f"h{s}")
        ascending = jnp.stack(slots[::-1] + slots[::-1])
        column = lax.dynamic_slice_in_dim(ascending, ring - 1 - group, ring, 0)
        return column.transpose(1, 0, 2, 3).reshape(2, rows, width)

    def head_weights(parts):
        mine = jnp.concatenate(parts[:2], axis=1)
        theirs = jnp.concatenate(parts[2:], axis=1)
        low = jnp.where(first_core, mine, theirs)
        high = jnp.where(first_core, theirs, mine)
        return jnp.concatenate([low, high[:1]], axis=0), high[1]

    def gather_units(s, i, *waits):
        piece = unit_shares[s][:, i * quarter:i * quarter + quarter]
        return jnp.concatenate(ring_gather(tied(piece, *waits), f"u{s}{i}"), axis=1)

    def in_order(pieces):
        return [pieces[i][j] for j in range(4) for i in range(2)]

    column = gather_heads(0)
    heads = spread_out(column, "h0")
    unit_a = gather_units(0, 0, column)
    pieces = [spread_out(unit_a, "u00")]
    unit_b = gather_units(0, 1, unit_a, heads[1])
    pieces.append(spread_out(unit_b, "u01"))
    weights = head_weights(heads) + (in_order(pieces),)
    layers = [weights]
    halves = attention_forward("0", [(tied(x, unit_a),), (x,)], weights, None, tables)
    column = gather_heads(1, unit_b, halves[1][1][0], pieces[0][1])
    heads = spread_out(column, "h1")
    next_a = gather_units(1, 0, column)
    next_pieces = [spread_out(next_a, "u10")]
    next_b = gather_units(1, 1, next_a, heads[1])
    next_pieces.append(spread_out(next_b, "u11"))
    layers.append(head_weights(heads) + (in_order(next_pieces),))
    ends, saved = feed_forward("0", halves, weights, norms[0], (column,), ())
    kept = [saved]
    ends[0] = (tied(ends[0][0], next_a),) + ends[0][1:]
    halves = attention_forward("1", ends, layers[1], norms[0], tables, (next_b,))
    ends, saved = feed_forward("1", halves, layers[1], norms[1], (), ())
    kept.append(saved)
    upstream = to_item(cotangent, core, place)

    def pull_units(tag, gate_up, down):
        parts = []
        for name, grad, count in (("u", gate_up, 2), ("d", down, 1)):
            own = grad[0].reshape(count, 2, ring * half, width)
            got = cross(grad[1], PIPE, 1, f"c_g{name}{tag}").reshape(count, 2, ring * half, width)
            parts.append([added(own[:, 1], got[:, 1]), (own[:, 0], got[:, 0])])
        return parts[0][0], parts[1][0], parts[0][1], parts[1][1]

    def cross_units(tag, units):
        columns = []
        for name, neighbour, (own, got) in (("u", units[0], units[2]), ("d", units[1], units[3])):
            other = cross(neighbour, TENSOR, 2, f"y_g{name}{tag}")
            column = own.astype(F32) + got.astype(F32) + other.astype(F32)
            columns.append(column.astype(BF))
        return columns

    def ring_units(tag, columns):
        totals = []
        for name, column in zip("ud", columns):
            count = column.shape[0]
            column = column.reshape(count, 2, ring, quarter, width)
            total = ring_reduce([column[:, :, k] for k in range(ring)], f"g{name}{tag}")
            totals.append(total.reshape(count, half, width).astype(BF))
        return jnp.concatenate(totals, axis=0)

    def pull_heads(tag, grad_in, grad_out):
        low = jnp.stack(grad_in[:2])
        high = jnp.stack([grad_in[2], grad_out])
        mine = jnp.where(first_core, low, high)
        theirs = cross(jnp.where(first_core, high, low), PIPE, 1, "c_gh" + tag)
        return added(mine[:, rows:], theirs[:, rows:]), mine[:, :rows], theirs[:, :rows]

    def cross_heads(tag, heads):
        neighbour, own, got = heads
        column = own.astype(F32) + got.astype(F32)
        column = column + cross(neighbour, TENSOR, 2, "y_gh" + tag).astype(F32)
        return column.astype(BF)

    def ring_heads(tag, column):
        column = column.reshape(2, ring, head_rows, width).transpose(1, 0, 2, 3)
        ascending = jnp.concatenate([column, column], axis=0)
        rolled = lax.dynamic_slice_in_dim(ascending, (group + 1) % ring, ring, 0)
        return ring_reduce([rolled[ring - 1 - k] for k in range(ring)], "gh" + tag).astype(BF)

    head_totals = [None, None]
    unit_totals = [None, None]
    edges = [None, None]
    norm_grads = [None, None]
    ends = [(upstream,), (upstream,)]
    waits = ()
    for s in (1, 0):
        tag = str(s)
        ends, edges[s], units, heads, norm_grads[s] = layer_backward(
            tag, ends, layers[s], norms[s], tables, kept[s], pull_units, pull_heads, waits
        )
        crossed = cross_units(tag, units)
        unit_totals[s] = ring_units(tag, crossed)
        head_columns = cross_heads(tag, heads)
        head_totals[s] = ring_heads(tag, head_columns)
        waits = crossed
    first_grad = jnp.concatenate(
        [
            (grad[half * MB_CAP // 2:(half + 1) * MB_CAP // 2] + own.astype(F32) + got.astype(F32))
            for half, (grad, own, got) in enumerate(ends)
        ],
        axis=0,
    ).astype(BF)
    activations = from_item([kept[1][1], edges[1]], core, place)
    gradients_in = from_item([first_grad, edges[0]], core, place)

    low, high = joined_by_core(head_totals[0], head_totals[1])
    unit_low, unit_high = joined_by_core(unit_totals[0], unit_totals[1])
    unit_grad = jnp.concatenate([unit_low, unit_high], axis=1).astype(F32)
    head_grad = jnp.concatenate([low, high], axis=0).astype(F32)
    norm_grads[0] = tied(norm_grads[0], heads[0])
    norm_own = jnp.where(first_core, norm_grads[0], norm_grads[1])
    norm_other = jnp.where(first_core, norm_grads[1], norm_grads[0])
    norm_sum = norm_own + flip(norm_other, PIPE, 1)
    norm_sum = norm_sum + flip(norm_sum, TENSOR, 2)
    bit = 1
    while bit < ring:
        norm_sum = norm_sum + flip(norm_sum, FSDP, bit)
        bit = bit * 2
    return (
        activations[None],
        gradients_in[None],
        head_grad[None, :3],
        head_grad[None, 3],
        unit_grad[None, :2],
        unit_grad[None, 2],
        norm_sum[None],
    )


def solution(mesh):
    placed = (
        P(None, (FSDP, TENSOR), None),
        P(None, (FSDP, TENSOR), None),
        P(PIPE, None, (TENSOR, FSDP), None),
        P(PIPE, (TENSOR, FSDP), None),
        P(PIPE, None, (TENSOR, FSDP), None),
        P(PIPE, (TENSOR, FSDP), None),
        P(PIPE, None, None),
        P(None, FSDP, None),
    )
    return jax.shard_map(
        whole_step,
        mesh=mesh,
        in_specs=placed,
        out_specs=(
            P(PIPE, None, (FSDP, TENSOR), None),
            P(PIPE, None, (FSDP, TENSOR), None),
            P(PIPE, None, (TENSOR, FSDP), None),
            P(PIPE, (TENSOR, FSDP), None),
            P(PIPE, None, (TENSOR, FSDP), None),
            P(PIPE, (TENSOR, FSDP), None),
            P(PIPE, None, None),
        ),
        check_vma=False,
    )
```

```python
import jax
import jax.numpy as jnp
from jax import lax
from jax.experimental import pallas as pl
from jax.experimental.pallas import tpu as pltpu
from jax.sharding import PartitionSpec as P

HEAD_DIM = 64
MB_CAP = 512
DOCS = 3

epsilon = 1e-05
rope_base = 1000.0
masked_value = -1e30

BF = jnp.bfloat16
PIPE, FSDP, TENSOR = "pipe", "fsdp", "tensor"
F32 = jnp.float32


def segment_info(lengths):
    doc_ends = jnp.cumsum(lengths)
    starts = doc_ends - lengths
    places = jnp.arange(MB_CAP, dtype=jnp.int32)
    segment = jnp.sum((places[:, None] >= doc_ends[None, :]).astype(jnp.int32), axis=1)
    choose = segment[:, None] == jnp.arange(DOCS, dtype=jnp.int32)[None, :]
    offset = jnp.sum(jnp.where(choose, starts[None, :], 0), axis=1)
    return (segment, places - offset)


def rotary_tables(position):
    half_dim = HEAD_DIM // 2
    lane = jnp.arange(2 * HEAD_DIM, dtype=jnp.int32)
    frequency = rope_base ** (-2.0 * (lane % half_dim).astype(F32) / HEAD_DIM)
    angles = position.astype(F32)[:, None] * frequency[None, :]
    sines = jnp.sin(angles)
    return jnp.cos(angles), jnp.where(lane[None, :] % HEAD_DIM < half_dim, -sines, sines)


def flip(array, axis, bit):
    count = lax.axis_size(axis)
    return lax.ppermute(array, axis, [(i, i ^ bit) for i in range(count)])


def shifted(array, axis, by):
    count = lax.axis_size(axis)
    return lax.ppermute(array, axis, [(i, (i + by) % count) for i in range(count)])


def unxor(parts, index):
    parts = [jnp.where(index & 1, parts[m ^ 1], parts[m]) for m in range(4)]
    return [jnp.where(index & 2, parts[m ^ 2], parts[m]) for m in range(4)]


def mixed_flip(array, core_bit, place_bits):
    count = lax.axis_size(TENSOR)
    pairs = [
        (c * count + t, (c ^ core_bit) * count + (t ^ place_bits))
        for c in range(2)
        for t in range(count)
    ]
    return lax.ppermute(array, (PIPE, TENSOR), pairs)


def ring_gather(shard, tag):
    count = lax.axis_size(FSDP)
    slots = [shard]
    for k in range(1, count):
        with jax.named_scope(f"z{k}_{tag}"):
            slots.append(shifted(shard, FSDP, k))
    return slots


def ring_reduce(parts, tag):
    count = len(parts)
    total = parts[0].astype(F32)
    for k in range(1, count):
        with jax.named_scope(f"z{k}_{tag}"):
            part = shifted(parts[k].astype(BF), FSDP, -k)
        total = total + part.astype(F32)
    return total


def cross(array, axis, bit, tag):
    with jax.named_scope(tag):
        return flip(array, axis, bit)


def spread_out(column, tag):
    neighbour = cross(column, TENSOR, 2, "y_" + tag)
    return [
        column,
        neighbour,
        cross(column, PIPE, 1, "c_" + tag),
        cross(neighbour, PIPE, 1, "n_" + tag),
    ]


def added(a, b):
    return (a.astype(F32) + b.astype(F32)).astype(BF)


def row_norm(summed):
    centered = summed - jnp.mean(summed, axis=-1, keepdims=True)
    inverse = lax.rsqrt(jnp.mean(centered * centered, axis=-1, keepdims=True) + epsilon)
    return centered * inverse, inverse


def row_norm_back(normed, inverse, gain_row, upstream):
    scaled = upstream * gain_row
    through = inverse * (
        scaled
        - jnp.mean(scaled, axis=-1, keepdims=True)
        - normed * jnp.mean(scaled * normed, axis=-1, keepdims=True)
    )
    sums = [
        jnp.sum(upstream * normed, axis=0, keepdims=True),
        jnp.sum(upstream, axis=0, keepdims=True),
    ]
    return through, jnp.concatenate(sums + [jnp.zeros((6, sums[0].shape[1]), F32)], axis=0)


def nn(a, b):
    return lax.dot_general(a, b, (((1,), (0,)), ((), ())), preferred_element_type=F32)


def nt(a, b):
    return lax.dot_general(a, b, (((1,), (1,)), ((), ())), preferred_element_type=F32)


def tn(a, b):
    return lax.dot_general(a, b, (((0,), (0,)), ((), ())), preferred_element_type=F32)


def turned(slab, cosine, sines):
    lane = lax.broadcasted_iota(jnp.int32, slab.shape, 1)
    swapped = jnp.where(
        lane % HEAD_DIM < HEAD_DIM // 2, pltpu.roll(slab, 96, 1), pltpu.roll(slab, 32, 1)
    )
    return slab * cosine + swapped * sines


def head_masks(rows):
    lane = lax.broadcasted_iota(jnp.int32, (rows, 128), 1)
    low = (lane < HEAD_DIM).astype(F32)
    return low, 1.0 - low


def rows_of(half, columns, rows):
    return pl.BlockSpec((rows, columns), lambda i: (half, 0))


def whole(array):
    zeros = (0,) * array.ndim
    return pl.BlockSpec(array.shape, lambda i: zeros)


ANYWHERE = pl.BlockSpec(memory_space=pl.ANY)


def staged(tag, kernel, ins, outs, before, scratch=()):
    before = list(before or [])
    arrays = [array for array, _ in ins] + before
    specs = [spec for _, spec in ins] + [ANYWHERE] * len(before)
    first_out = len(outs) - len(before)
    first_in = len(ins)
    count = len(before)

    def run(*refs):
        kernel(*refs[:first_in], *refs[first_in + count:])

    call = pl.pallas_call(
        run,
        grid=(1,),
        in_specs=specs,
        out_specs=[spec for _, _, spec in outs],
        out_shape=[jax.ShapeDtypeStruct(shape, kind) for shape, kind, _ in outs],
        scratch_shapes=list(scratch),
        input_output_aliases={first_in + i: first_out + i for i in range(count)},
        compiler_params=pltpu.CompilerParams(vmem_limit_bytes=40 << 20),
        cost_estimate=pl.CostEstimate(flops=1024, bytes_accessed=1024, transcendentals=0),
        name=kernel.__name__,
    )
    with jax.named_scope("k_" + tag):
        return call(*arrays)


def project(tag, half, sources, norm_rows, weight, cosine, sines, before):
    given = len(sources) == 1
    total, width = sources[0].shape
    heads = weight.shape[1]
    rows = total // 2

    def project_kernel(*refs):
        if given:
            x_ref, w_ref, cos_ref, sin_ref, q_ref, k_ref, v_ref = refs
            low = x_ref[...]
        else:
            (mid_ref, own_ref, got_ref, norm_ref, w_ref, cos_ref, sin_ref,
             q_ref, k_ref, v_ref, x_ref, low_ref) = refs
            summed = mid_ref[...] + own_ref[...].astype(F32) + got_ref[...].astype(F32)
            x = row_norm(summed)[0] * norm_ref[2:3] + norm_ref[3:4]
            x_ref[...] = x
            low = x.astype(BF)
            low_ref[...] = low
        cosine, sines = cos_ref[...], sin_ref[...]
        for c, out in ((0, q_ref), (1, k_ref)):
            turning = nt(low, w_ref[c])
            for slab in range(heads // 128):
                at = slice(128 * slab, 128 * slab + 128)
                out[:, at] = turned(turning[:, at], cosine, sines).astype(BF)
        v_ref[...] = nt(low, w_ref[2]).astype(BF)

    here = rows_of(half, width, rows)
    ins = [(sources[0], here)]
    outs = [((total, heads), BF, rows_of(half, heads, rows)) for _ in range(3)]
    if not given:
        plain = pl.BlockSpec((rows, width), lambda i: (0, 0))
        ins += [(sources[1], plain), (sources[2], plain), (norm_rows, whole(norm_rows))]
        outs += [((total, width), F32, here), ((total, width), BF, here)]
    ins += [(weight, whole(weight))]
    ins += [(table, rows_of(half, 128, rows)) for table in (cosine, sines)]
    return staged(tag, project_kernel, ins, outs, before)


def attend(tag, half, queries, key_vecs, values, segment_column, segment_row, out_weight, before):
    total, heads = queries.shape
    width = out_weight.shape[1]
    rows = total // 2

    def attend_kernel(q_ref, k_ref, v_ref, col_ref, row_ref, w_ref, part_ref, ctx_ref, lse_ref):
        masks = head_masks(rows)
        lane = lax.broadcasted_iota(jnp.int32, (rows, 128), 1)
        same = col_ref[:, :1] == row_ref[:1, :]
        totals = jnp.zeros((rows, 128), F32)
        for slab in range(heads // 128):
            at = slice(128 * slab, 128 * slab + 128)
            q, k, v = q_ref[:, at], k_ref[:, at], v_ref[:, at]
            gathered = jnp.zeros((rows, 128), F32)
            for h in range(2):
                scores = nt(q * masks[h].astype(BF), k) * HEAD_DIM ** (-0.5)
                scores = jnp.where(same, scores, masked_value)
                top = jnp.max(scores, axis=-1, keepdims=True)
                powers = jnp.exp(scores - top)
                mass = jnp.sum(powers, axis=-1, keepdims=True)
                chances = (powers * (1.0 / mass)).astype(BF)
                gathered = gathered + nn(chances, v) * masks[h]
                totals = jnp.where(lane == 2 * slab + h, top + jnp.log(mass), totals)
            ctx_ref[:, at] = gathered.astype(BF)
        lse_ref[...] = totals.T[:8]
        part_ref[...] = nn(ctx_ref[...], w_ref[...]).astype(BF)

    ins = [
        (queries, rows_of(half, heads, rows)),
        (key_vecs, whole(key_vecs)),
        (values, whole(values)),
        (segment_column, rows_of(half, 128, rows)),
        (segment_row, whole(segment_row)),
        (out_weight, whole(out_weight)),
    ]
    outs = [
        ((rows, width), BF, pl.BlockSpec((rows, width), lambda i: (0, 0))),
        ((total, heads), BF, rows_of(half, heads, rows)),
        ((8, total), F32, pl.BlockSpec((8, rows), lambda i: (0, half))),
    ]
    return staged(tag, attend_kernel, ins, outs, before)


def feed_scratch(blocks, rows, width):
    return [
        pltpu.VMEM((len(blocks),) + blocks[0].shape, BF),
        pltpu.VMEM((rows, width), F32),
        pltpu.SemaphoreType.DMA((len(blocks),)),
    ]


def fetch_blocks(block_refs, buffer, sems):
    for j, ref in enumerate(block_refs):
        pltpu.make_async_copy(ref, buffer.at[j], sems.at[j]).start()


def share_blocks(p, block_refs, buffer, sems):
    each = len(block_refs) // 2
    for j in range(p * each, p * each + each):
        pltpu.make_async_copy(block_refs[j], buffer.at[j], sems.at[j]).wait()

    def joined(c):
        return jnp.concatenate([buffer[p * each + j, c] for j in range(each)], axis=0)

    return joined(0), joined(1), joined(2)


def feed(tag, half, x, own, got, norm_rows, blocks, before):
    total, width = x.shape
    rows = total // 2
    step = len(blocks) // 2 * blocks[0].shape[1]
    units = len(blocks) * blocks[0].shape[1]
    count = len(blocks)

    def feed_kernel(*refs):
        x_ref, own_ref, got_ref, norm_ref = refs[:4]
        block_refs = refs[4:4 + count]
        (part_ref, mid_ref, low_ref, gate_ref, up_ref, own_hid, other_hid,
         buffer, acc_ref, sems) = refs[4 + count:]
        fetch_blocks(block_refs, buffer, sems)
        summed = x_ref[...] + own_ref[...].astype(F32) + got_ref[...].astype(F32)
        middle = row_norm(summed)[0] * norm_ref[0:1] + norm_ref[1:2]
        mid_ref[...] = middle
        low = middle.astype(BF)
        low_ref[...] = low
        for p in range(2):
            gate_w, up_w, down_w = share_blocks(p, block_refs, buffer, sems)
            at = slice(p * step, p * step + step)
            gate = nt(low, gate_w)
            up = nt(low, up_w)
            gate_ref[:, at] = gate.astype(BF)
            up_ref[:, at] = up.astype(BF)
            hidden = (gate * jax.nn.sigmoid(gate) * up).astype(BF)
            (own_hid, other_hid)[p][...] = hidden
            fed = nn(hidden, down_w)
            acc_ref[...] = fed if p == 0 else acc_ref[...] + fed
        part_ref[...] = acc_ref[...].astype(BF)

    plain = pl.BlockSpec((rows, width), lambda i: (0, 0))
    here = rows_of(half, width, rows)
    wide = rows_of(half, units, rows)
    ins = [(x, here), (own, plain), (got, plain), (norm_rows, whole(norm_rows))]
    ins += [(block, ANYWHERE) for block in blocks]
    outs = [((rows, width), BF, plain), ((total, width), F32, here), ((total, width), BF, here)]
    outs += [((total, units), BF, wide) for _ in range(2)]
    outs += [((total, step), BF, rows_of(half, step, rows)) for _ in range(2)]
    return staged(tag, feed_kernel, ins, outs, before, feed_scratch(blocks, rows, width))


def feed_back(tag, half, sources, middle, own, got, norm_rows, gate, up, blocks, before):
    top = len(sources) == 1
    total, width = middle.shape
    rows = total // 2
    step = len(blocks) // 2 * blocks[0].shape[1]
    units = len(blocks) * blocks[0].shape[1]
    count = len(blocks)

    def feed_back_kernel(*refs):
        taken = len(sources)
        mid_ref, own_ref, got_ref, norm_ref, gate_ref, up_ref = refs[taken:taken + 6]
        block_refs = refs[taken + 6:taken + 6 + count]
        (part_ref, sums_ref, edge_ref, pre_ref, feed_ref, own_grads, other_grads,
         buffer, acc_ref, sems) = refs[taken + 6 + count:]
        fetch_blocks(block_refs, buffer, sems)
        summed = mid_ref[...] + own_ref[...].astype(F32) + got_ref[...].astype(F32)
        normed, inverse = row_norm(summed)
        if top:
            upstream = refs[0][...].astype(F32)
            edge_ref[...] = (normed * norm_ref[2:3] + norm_ref[3:4]).astype(BF)
        else:
            upstream = refs[0][...] + refs[1][...].astype(F32) + refs[2][...].astype(F32)
            edge_ref[...] = upstream.astype(BF)
        through, sums_ref[...] = row_norm_back(normed, inverse, norm_ref[2:3], upstream)
        pre_ref[...] = through
        low = through.astype(BF)
        feed_ref[...] = low
        for p in range(2):
            gate_w, up_w, down_w = share_blocks(p, block_refs, buffer, sems)
            at = slice(p * step, p * step + step)
            gate, up = gate_ref[:, at].astype(F32), up_ref[:, at].astype(F32)
            grad_hidden = nt(low, down_w)
            sigmoid = jax.nn.sigmoid(gate)
            grad_gate = (grad_hidden * up * sigmoid * (1.0 + gate * (1.0 - sigmoid))).astype(BF)
            grad_up = (grad_hidden * gate * sigmoid).astype(BF)
            share_ref = (own_grads, other_grads)[p]
            share_ref[:, :step] = grad_gate
            share_ref[:, step:] = grad_up
            back_through = nn(grad_gate, gate_w) + nn(grad_up, up_w)
            acc_ref[...] = back_through if p == 0 else acc_ref[...] + back_through
        part_ref[...] = acc_ref[...].astype(BF)

    plain = pl.BlockSpec((rows, width), lambda i: (0, 0))
    here = rows_of(half, width, rows)
    wide = rows_of(half, units, rows)
    ins = [(sources[0], here)] + [(source, plain) for source in sources[1:]]
    ins += [(middle, here), (own, plain), (got, plain), (norm_rows, whole(norm_rows))]
    ins += [(gate, wide), (up, wide)] + [(block, ANYWHERE) for block in blocks]
    outs = [((rows, width), BF, plain), ((8, width), F32, pl.BlockSpec((8, width), lambda i: (0, 0)))]
    outs += [((total, width), BF, here), ((total, width), F32, here), ((total, width), BF, here)]
    outs += [((total, units), BF, wide) for _ in range(2)]
    return staged(tag, feed_back_kernel, ins, outs, before, feed_scratch(blocks, rows, width))


def attend_back(tag, half, grad_middle, x, own, got, norm_rows, queries, key_vecs, values, totals,
                segment_column, segment_row, out_weight, cosine, sines, partial, before):
    total, heads = queries.shape
    width = out_weight.shape[1]
    rows = total // 2
    last = partial is not None

    def attend_back_kernel(*refs):
        (pre_ref, fed_ref, fed_got_ref, x_ref, own_ref, got_ref, norm_ref, q_ref, k_ref, v_ref,
         lse_ref, col_ref, row_ref, w_ref, cos_ref, sin_ref) = refs[:16]
        if last:
            dk_in, dv_in = refs[16:18]
        sums_ref, dk_ref, dv_ref, mid_ref, att_ref, dq_ref, dctx_ref = refs[18 if last else 16:]
        upstream = pre_ref[...] + fed_ref[...].astype(F32) + fed_got_ref[...].astype(F32)
        summed = x_ref[...] + own_ref[...].astype(F32) + got_ref[...].astype(F32)
        normed, inverse = row_norm(summed)
        through, sums_ref[...] = row_norm_back(normed, inverse, norm_ref[0:1], upstream)
        mid_ref[...] = through
        low = through.astype(BF)
        att_ref[...] = low
        dctx_ref[...] = nt(low, w_ref[...]).astype(BF)
        masks = head_masks(rows)
        wide_masks = head_masks(total)
        same = col_ref[:, :1] == row_ref[:1, :]
        scaling = HEAD_DIM ** (-0.5)
        here = pl.ds(half * rows, rows)
        cosine, sines = cos_ref[...], sin_ref[...]
        for slab in range(heads // 128):
            at = slice(128 * slab, 128 * slab + 128)
            q, k, v, grad_ctx = q_ref[:, at], k_ref[:, at], v_ref[:, at], dctx_ref[:, at]
            dq = jnp.zeros((rows, 128), F32)
            dk = jnp.zeros((total, 128), F32)
            dv = jnp.zeros((total, 128), F32)
            for h in range(2):
                mask = masks[h].astype(BF)
                scores = nt(k, q * mask) * scaling
                scores = jnp.where(same, scores, masked_value)
                chances = jnp.exp(scores - lse_ref[2 * slab + h:2 * slab + h + 1, :])
                grad_chances = nt(v, grad_ctx * mask)
                row_dot = jnp.sum(chances * grad_chances, axis=0, keepdims=True)
                grad_scores = (chances * (grad_chances - row_dot)).astype(BF)
                dv = dv + nn(chances.astype(BF), grad_ctx) * wide_masks[h]
                dk = dk + nn(grad_scores, q) * wide_masks[h]
                dq = dq + tn(grad_scores, k) * masks[h]
            dq_ref[:, at] = turned(dq * scaling, cos_ref[here, :], -sin_ref[here, :]).astype(BF)
            if last:
                dk = dk_in[:, at] + dk
                dv = dv_in[:, at] + dv
                dk_ref[:, at] = turned(dk * scaling, cosine, -sines).astype(BF)
                dv_ref[:, at] = dv.astype(BF)
            else:
                dk_ref[:, at] = dk
                dv_ref[:, at] = dv

    plain = pl.BlockSpec((rows, width), lambda i: (0, 0))
    here = rows_of(half, width, rows)
    ins = [(grad_middle[0], here), (grad_middle[1], plain), (grad_middle[2], plain)]
    ins += [(x, here), (own, plain), (got, plain), (norm_rows, whole(norm_rows))]
    ins += [(queries, rows_of(half, heads, rows)), (key_vecs, whole(key_vecs)),
            (values, whole(values)), (totals, pl.BlockSpec((8, rows), lambda i: (0, half))),
            (segment_column, whole(segment_column)),
            (segment_row, pl.BlockSpec((8, rows), lambda i: (0, half))),
            (out_weight, whole(out_weight)), (cosine, whole(cosine)), (sines, whole(sines))]
    if last:
        ins += [(part, whole(part)) for part in partial]
    kind = BF if last else F32
    all_rows = pl.BlockSpec((total, heads), lambda i: (0, 0))
    outs = [((8, width), F32, pl.BlockSpec((8, width), lambda i: (0, 0))),
            ((total, heads), kind, all_rows), ((total, heads), kind, all_rows),
            ((total, width), F32, here), ((total, width), BF, here),
            ((total, heads), BF, rows_of(half, heads, rows))]
    return staged(tag, attend_back_kernel, ins, outs, before, [pltpu.VMEM((rows, heads), BF)])


def inputs_back(tag, half, grads, weight):
    total, heads = grads[0].shape
    width = weight.shape[2]
    rows = total // 2

    def inputs_back_kernel(dq_ref, dk_ref, dv_ref, w_ref, part_ref):
        acc = nn(dq_ref[...], w_ref[0]) + nn(dk_ref[...], w_ref[1]) + nn(dv_ref[...], w_ref[2])
        part_ref[...] = acc.astype(BF)

    ins = [(grad, rows_of(half, heads, rows)) for grad in grads] + [(weight, whole(weight))]
    outs = [((rows, width), BF, pl.BlockSpec((rows, width), lambda i: (0, 0)))]
    return staged(tag, inputs_back_kernel, ins, outs, None)[0]


def across(part, tag):
    with jax.named_scope("x_" + tag):
        return flip(part, TENSOR, 1)


def tied(value, *others):
    return lax.optimization_barrier((value, *others))[0]


def weight_grad(left, right, tag):
    with jax.named_scope("w_" + tag):
        return jnp.einsum("th,td->hd", left, right, preferred_element_type=F32).astype(BF)


def attention_forward(tag, sources, weights, norm_before, tables, wait=()):
    in_weight, out_weight = weights[:2]
    segment_column, segment_row, cosine, sines = tables
    projected = None
    for half in range(2):
        projected = project(f"p{tag}{half}", half, sources[half], norm_before, in_weight, cosine, sines, projected)
    queries, key_vecs, values = projected[:3]
    if len(projected) == 5:
        x, low = projected[3:]
    else:
        low = sources[0][0]
        x = low.astype(F32)
    kept = None
    attended = []
    for half in range(2):
        taken = tied(queries, *wait) if half == 1 else queries
        part, *kept = attend(f"t{tag}{half}", half, taken, key_vecs, values, segment_column, segment_row,
                             out_weight, kept)
        attended.append((part, across(part, f"t{tag}{half}")))
    context, totals = kept
    return (x, low, queries, key_vecs, values, context, totals), attended


def feed_forward(tag, halves, weights, norm_rows, first_wait, second_wait):
    before, attended = halves
    blocks = weights[2]
    x = before[0]
    saved = None
    fed = []
    for half in range(2):
        taken = tied(x, *(second_wait if half else first_wait))
        part, *saved = feed(f"f{tag}{half}", half, taken, *attended[half], norm_rows, blocks, saved)
        fed.append((part, across(part, f"f{tag}{half}")))
    middle, spread, gate, up, *hidden = saved
    ends = [(middle, *fed[half]) for half in range(2)]
    return ends, (*before, attended, middle, spread, gate, up, hidden, fed)


def layer_backward(tag, sources, weights, norm_rows, tables, kept, pull_units, pull_heads, waits):
    in_weight, out_weight, blocks = weights
    segment_column, segment_row, cosine, sines = tables
    (x, low, queries, key_vecs, values, context, totals, attended, middle, spread,
     gate, up, hidden, fed) = kept
    saved = None
    through = []
    sums = []
    for half in range(2):
        part, total, *saved = feed_back(f"g{tag}{half}", half, sources[half], middle, *fed[half], norm_rows,
                                        gate, up, blocks, saved)
        through.append((part, across(part, f"g{tag}{half}")))
        sums.append(total)
    edge, grad_pre_output, grad_feed, *grad_shares = saved
    down = [weight_grad(hidden[i], grad_feed, f"d{tag}{i}") for i in (1, 0)]
    gate_up = [weight_grad(grad_shares[i], spread, f"u{tag}{i}") for i in (1, 0)]
    down, gate_up = down[::-1], gate_up[::-1]
    units = pull_units(tag, gate_up, down)
    partial = None
    saved = None
    first_sums = []
    for half in range(2):
        wait = waits if half == 0 else units[:2]
        total, dk, dv, *saved = attend_back(
            f"h{tag}{half}", half, (tied(grad_pre_output, *wait), *through[half]), x, *attended[half], norm_rows,
            queries, key_vecs, values, totals, segment_column, segment_row,
            out_weight, cosine, sines, partial, saved)
        partial = (dk, dv)
        first_sums.append(total)
    grad_pre_middle, grad_attended, dq = saved
    ends = []
    for half in range(2):
        part = inputs_back(f"i{tag}{half}", half, (dq, dk, dv), in_weight)
        ends.append((grad_pre_middle, part, across(part, f"i{tag}{half}")))
    grad_in = [weight_grad(grad, low, f"n{tag}") for grad in (dq, dk, dv)]
    grad_out = weight_grad(context, grad_attended, f"o{tag}")
    heads = pull_heads(tag, grad_in, grad_out)
    first = first_sums[0] + first_sums[1]
    second = sums[0] + sums[1]
    norm_grad = jnp.concatenate([first[:2], second[:2]], axis=0)
    return ends, edge, units, heads, norm_grad


MESH = pl.DeviceIdType.MESH


def forward_all(layer_inputs, cotangent, heads_in, units_in, norm_in, tables):
    segment_column, segment_row, cosine, sines = tables
    ring = lax.axis_size(FSDP)
    count, own_rows, width = layer_inputs.shape
    total = count * own_rows
    rows = total // 2
    head_rows = heads_in.shape[1]
    half_units = units_in.shape[2]
    heads = 2 * ring * head_rows
    step = 2 * ring * half_units
    order = sorted(range(1, ring), key=lambda k: min(k, ring - k))

    saved = {}
    for l in range(2):
        saved.update({
            f"q{l}": ((total, heads), BF), f"k{l}": ((total, heads), BF),
            f"v{l}": ((total, heads), BF), f"ctx{l}": ((total, heads), BF),
            f"lse{l}": ((8, total), F32), f"pre1{l}": ((total, width), F32),
            f"pre2{l}": ((total, width), F32),
            f"spread{l}": ((total, width), BF), f"feed{l}": ((3, total, 2 * step), BF),
        })
    saved.update({"low0": ((total, width), BF), "acts": ((2, total, width), BF),
                  "cot": ((total, width), BF)})
    inner = {"x1": ((total, width), F32), "mid": ((total, width), F32)}
    for l in range(2):
        for h in range(2):
            for stage in "tf":
                inner[f"own_{stage}{l}{h}"] = ((rows, width), BF)
                inner[f"got_{stage}{l}{h}"] = ((rows, width), BF)
    weights = {}
    for l in range(2):
        weights[f"heads{l}"] = ((4, 2, ring * head_rows, width), BF)
        weights[f"units{l}"] = ((3, 2, 2, ring * half_units, width), BF)
    outs = {**saved, **weights, "norms": ((2, 4, width), F32)}
    held = {**saved, **inner}
    stages = [f"{stage}{l}{h}" for l in range(2) for stage in "tf" for h in range(2)]

    def forward_kernel(inp, cot_ref, heads_ref, units_ref, norm_ref, col_ref, row_ref, cos_ref, sin_ref,
                       *refs):
        out = dict(zip(outs, refs[:len(outs)]))
        rest = refs[len(outs):]
        keep = dict(zip(held, rest[:len(held)]))
        (hbuf, ubuf, nbuf, acc_ref, z_s, z_r, y_s, y_r, k_s, k_r, e_s, e_r, x_s, x_r, i_s, i_r,
         l_s, f_s) = rest[len(held):]
        core = lax.axis_index(PIPE)
        place = lax.axis_index(TENSOR)
        group = lax.axis_index(FSDP)
        other = 1 - core
        item = (place // 2) * 2 + core

        def peer(k):
            low, high = place % 2, place // 2
            low = 1 - low if k & 1 else low
            high = 1 - high if k & 2 else high
            return high * 2 + low

        def near(k):
            return lax.rem(group + k, ring)

        sent = []
        conditional = []

        def send(src, dst, send_sem, recv_sem, **to):
            copy = pltpu.make_async_remote_copy(
                src_ref=src, dst_ref=dst, send_sem=send_sem, recv_sem=recv_sem,
                device_id=to, device_id_type=MESH)
            copy.start()
            sent.append(copy)

        def arrived(dst, send_sem, recv_sem, **to):
            pltpu.make_async_remote_copy(
                src_ref=dst, dst_ref=dst, send_sem=send_sem, recv_sem=recv_sem,
                device_id=to, device_id_type=MESH).wait_recv()

        flushes = []
        done = set()

        def flush(src, name):
            done.add(name)
            copy = pltpu.make_async_copy(src, out[name], f_s.at[len(flushes)])
            copy.start()
            flushes.append(copy)

        def slot(piece, share, col, g):
            l, kind = piece // 2, piece % 2
            if kind == 0:
                at = pl.ds(pl.multiple_of(g * head_rows, 16), head_rows)
                return hbuf.at[l, pl.ds(2 * share, 2), col, at]
            at = pl.ds(pl.multiple_of(g * half_units, 16), half_units)
            return ubuf.at[l, :, share, col, at]

        barrier = pltpu.get_barrier_semaphore()
        peers = [dict(tensor=peer(k)) for k in (1, 2, 3)] + [dict(pipe=other)]
        peers += [dict(fsdp=near(k)) for k in range(1, ring)]
        for to in peers:
            pl.semaphore_signal(barrier, inc=1, device_id=to, device_id_type=MESH)
        pl.semaphore_wait(barrier, len(peers))

        mine = pl.ds(pl.multiple_of(group * head_rows, 16), head_rows)
        mine_units = pl.ds(pl.multiple_of(group * half_units, 16), half_units)
        local = [
            pltpu.make_async_copy(heads_ref.at[pl.ds(2 * core, 2)],
                                  hbuf.at[core, pl.ds(2 * core, 2), 0, mine], l_s.at[0]),
            pltpu.make_async_copy(units_ref.at[:, core],
                                  ubuf.at[core, :, core, 0, mine_units], l_s.at[1]),
            pltpu.make_async_copy(inp.at[item],
                                  keep["low0"].at[pl.ds(pl.multiple_of(place * own_rows, 16),
                                                        own_rows)], l_s.at[2]),
            pltpu.make_async_copy(norm_ref, nbuf.at[core], l_s.at[3]),
            pltpu.make_async_copy(cot_ref.at[item],
                                  keep["cot"].at[pl.ds(pl.multiple_of(place * own_rows, 16),
                                                       own_rows)], l_s.at[4]),
        ]
        send(heads_ref.at[pl.ds(2 * other, 2)], hbuf.at[core, pl.ds(2 * other, 2), 0, mine],
             e_s.at[0], e_r.at[0], pipe=other)
        for copy in local:
            copy.start()
        send(units_ref.at[:, other], ubuf.at[core, :, other, 0, mine_units],
             e_s.at[1], e_r.at[1], pipe=other)
        send(norm_ref, nbuf.at[core], e_s.at[2], e_r.at[2], pipe=other)
        for k in (1, 2):
            send(inp.at[(peer(k) // 2) * 2 + core],
                 keep["low0"].at[pl.ds(pl.multiple_of(place * own_rows, 16), own_rows)],
                 i_s.at[k], i_r.at[k], tensor=peer(k))

        reach = [(sign, d) for d in range(1, ring) for sign in (1, -1)]

        def number(sign, d):
            return d if sign > 0 else ring - 1 + d

        def exists(sign, d):
            return group + d < ring if sign > 0 else group >= d

        def when(condition, action):
            @pl.when(condition)
            def _():
                action().start()

            conditional.append((condition, action))

        def hop_on(piece, sign, d):
            here = slot(piece, core, 0, group + sign * d)
            onward = group >= 1 if sign > 0 else group + 1 < ring
            index = number(sign, d)

            def action():
                return pltpu.make_async_remote_copy(
                    src_ref=here, dst_ref=here, send_sem=z_s.at[piece, index],
                    recv_sem=z_r.at[piece, number(sign, d + 1)],
                    device_id={FSDP: group - sign}, device_id_type=MESH)

            return onward, action

        def own_along(piece):
            for sign in (1, -1):
                here = slot(piece, core, 0, group)
                onward = group >= 1 if sign > 0 else group + 1 < ring

                def action(sign=sign):
                    return pltpu.make_async_remote_copy(
                        src_ref=here, dst_ref=here,
                        send_sem=z_s.at[piece, 0 if sign > 0 else 2 * ring - 1],
                        recv_sem=z_r.at[piece, number(sign, 1)],
                        device_id={FSDP: group - sign}, device_id_type=MESH)

                when(onward, action)

        def across(piece, g, index):
            here = slot(piece, core, 0, g)
            to_side = pltpu.make_async_remote_copy(
                src_ref=here, dst_ref=slot(piece, core, 1, g), send_sem=y_s.at[piece, index],
                recv_sem=y_r.at[piece, index], device_id={TENSOR: peer(2)}, device_id_type=MESH)
            to_core = pltpu.make_async_remote_copy(
                src_ref=here, dst_ref=here, send_sem=k_s.at[piece, 0, index],
                recv_sem=k_r.at[piece, 0, index], device_id={PIPE: other}, device_id_type=MESH)
            return to_side, to_core

        def own_across(piece):
            for copy in across(piece, group, 0):
                copy.start()
                sent.append(copy)

        def hop(piece, d):
            for sign in (1, -1):
                index = number(sign, d)
                g = group + sign * d
                condition = exists(sign, d)

                @pl.when(condition)
                def _():
                    arrived(slot(piece, core, 0, g), z_s.at[piece, index], z_r.at[piece, index],
                            fsdp=group + sign)
                    for copy in across(piece, g, index):
                        copy.start()

                if d + 1 < ring:
                    onward, action = hop_on(piece, sign, d)
                    when(jnp.logical_and(condition, onward), action)
                for i in range(2):
                    conditional.append(
                        (condition, lambda i=i, g=g, index=index: across(piece, g, index)[i]))

        def own_second(piece):
            here = slot(piece, core, 1, group)
            arrived(here, y_s.at[piece, 0], y_r.at[piece, 0], tensor=peer(2))
            send(here, here, k_s.at[piece, 1, 0], k_r.at[piece, 1, 0], pipe=other)

        def second(piece, d):
            for sign in (1, -1):
                index = number(sign, d)
                here = slot(piece, core, 1, group + sign * d)
                condition = exists(sign, d)

                def action(here=here, index=index):
                    return pltpu.make_async_remote_copy(
                        src_ref=here, dst_ref=here, send_sem=k_s.at[piece, 1, index],
                        recv_sem=k_r.at[piece, 1, index], device_id={PIPE: other},
                        device_id_type=MESH)

                @pl.when(condition)
                def _():
                    arrived(here, y_s.at[piece, index], y_r.at[piece, index], tensor=peer(2))

                when(condition, action)

        def pass_second(piece):
            own_second(piece)
            for d in range(1, ring):
                second(piece, d)

        def complete(piece):
            for col in range(2):
                arrived(slot(piece, other, col, group), k_s.at[piece, col, 0],
                        k_r.at[piece, col, 0], pipe=other)
                for sign, d in reach:
                    index = number(sign, d)

                    @pl.when(exists(sign, d))
                    def _():
                        arrived(slot(piece, other, col, group + sign * d),
                                k_s.at[piece, col, index], k_r.at[piece, col, index], pipe=other)
            l = piece // 2
            if piece % 2 == 0:
                flush(hbuf.at[l], f"heads{l}")
            else:
                flush(ubuf.at[l], f"units{l}")

        local[0].wait()
        arrived(hbuf.at[other, pl.ds(2 * core, 2), 0, mine],
                e_s.at[0], e_r.at[0], pipe=other)
        own_along(0)
        own_across(0)
        local[1].wait()
        arrived(ubuf.at[other, :, core, 0, mine_units], e_s.at[1], e_r.at[1], pipe=other)

        def part_of(name, l):
            return nbuf[l, name:name + 1, :]

        def exchange(tag):
            index = stages.index(tag)
            send(keep["own_" + tag], keep["got_" + tag], x_s.at[index], x_r.at[index],
                 tensor=peer(1))

        def taken(tag):
            index = stages.index(tag)
            arrived(keep["got_" + tag], x_s.at[index], x_r.at[index], tensor=peer(1))
            return keep["own_" + tag][...].astype(F32) + keep["got_" + tag][...].astype(F32)

        def do_project(l, half):
            at_rows = slice(half * rows, half * rows + rows)
            if l == 0:
                low = keep["low0"][at_rows]
            else:
                summed = keep["mid"][at_rows] + taken(f"f0{half}")
                keep["pre20"][at_rows] = summed
                x = row_norm(summed)[0] * part_of(2, 0) + part_of(3, 0)
                keep["x1"][at_rows] = x
                low = x.astype(BF)
                keep["acts"][0, at_rows] = low
            cosine, sines = cos_ref[at_rows], sin_ref[at_rows]
            for c, name in ((0, "q"), (1, "k")):
                turning = nt(low, hbuf[l, c].reshape(heads, width))
                for slab in range(heads // 128):
                    at = slice(128 * slab, 128 * slab + 128)
                    keep[f"{name}{l}"][at_rows, at] = turned(
                        turning[:, at], cosine, sines).astype(BF)
            keep[f"v{l}"][at_rows] = nt(low, hbuf[l, 2].reshape(heads, width)).astype(BF)

        def do_attend(l, half):
            at_rows = slice(half * rows, half * rows + rows)
            masks = head_masks(rows)
            lane = lax.broadcasted_iota(jnp.int32, (rows, 128), 1)
            same = col_ref[at_rows, :1] == row_ref[:1, :]
            totals = jnp.zeros((rows, 128), F32)
            for slab in range(heads // 128):
                at = slice(128 * slab, 128 * slab + 128)
                q, k, v = keep[f"q{l}"][at_rows, at], keep[f"k{l}"][:, at], keep[f"v{l}"][:, at]
                gathered = jnp.zeros((rows, 128), F32)
                for h in range(2):
                    scores = nt(q * masks[h].astype(BF), k) * HEAD_DIM ** (-0.5)
                    scores = jnp.where(same, scores, masked_value)
                    top = jnp.max(scores, axis=-1, keepdims=True)
                    powers = jnp.exp(scores - top)
                    mass = jnp.sum(powers, axis=-1, keepdims=True)
                    chances = (powers * (1.0 / mass)).astype(BF)
                    gathered = gathered + nn(chances, v) * masks[h]
                    totals = jnp.where(lane == 2 * slab + h, top + jnp.log(mass), totals)
                keep[f"ctx{l}"][at_rows, at] = gathered.astype(BF)
            keep[f"lse{l}"][:, at_rows] = totals.T[:8]
            part = nn(keep[f"ctx{l}"][at_rows], hbuf[l, 3].reshape(heads, width))
            keep[f"own_t{l}{half}"][...] = part.astype(BF)
            exchange(f"t{l}{half}")

        def do_feed(l, half):
            at_rows = slice(half * rows, half * rows + rows)
            x = keep["low0"][at_rows].astype(F32) if l == 0 else keep["x1"][at_rows]
            summed = x + taken(f"t{l}{half}")
            keep[f"pre1{l}"][at_rows] = summed
            middle = row_norm(summed)[0] * part_of(0, l) + part_of(1, l)
            keep["mid"][at_rows] = middle
            low = middle.astype(BF)
            keep[f"spread{l}"][at_rows] = low
            for share in range(2):
                at = slice(share * step, share * step + step)
                gate = nt(low, ubuf[l, 0, share].reshape(step, width))
                up = nt(low, ubuf[l, 1, share].reshape(step, width))
                keep[f"feed{l}"][0, at_rows, at] = gate.astype(BF)
                keep[f"feed{l}"][1, at_rows, at] = up.astype(BF)
                hidden = (gate * jax.nn.sigmoid(gate) * up).astype(BF)
                keep[f"feed{l}"][2, at_rows, at] = hidden
                fed = nn(hidden, ubuf[l, 2, share].reshape(step, width))
                if share == 0:
                    acc_ref[...] = fed
                else:
                    keep[f"own_f{l}{half}"][...] = (acc_ref[...] + fed).astype(BF)
            exchange(f"f{l}{half}")

        hop(0, 1)

        def input_rows(k):
            return keep["low0"].at[pl.ds(pl.multiple_of(peer(k) * own_rows, 16), own_rows)]

        for d in range(2, ring):
            if d == 3:
                arrived(input_rows(2), i_s.at[2], i_r.at[2], tensor=peer(2))
                send(input_rows(2), input_rows(2), i_s.at[3], i_r.at[3], tensor=peer(1))
                own_along(1)
                own_across(1)
            hop(0, d)
        if ring < 4:
            own_along(1)
            own_across(1)
        pass_second(0)
        for k in (1, 3):
            arrived(input_rows(k), i_s.at[k], i_r.at[k], tensor=peer(1))
        local[2].wait()
        local[3].wait()
        arrived(nbuf.at[other], e_s.at[2], e_r.at[2], pipe=other)
        complete(0)
        do_project(0, 0)
        do_project(0, 1)
        hop(1, 1)
        own_along(2)
        do_attend(0, 0)
        do_attend(0, 1)
        hop(1, 2)
        own_across(2)
        hop(2, 1)
        own_along(3)
        for d in range(3, ring):
            hop(1, d)
        for d in range(2, ring):
            hop(2, d)
        own_across(3)
        pass_second(1)
        complete(1)
        do_feed(0, 0)
        hop(3, 1)
        do_feed(0, 1)
        hop(3, 2)
        pass_second(2)
        complete(2)
        do_project(1, 0)
        do_project(1, 1)
        for d in range(3, ring):
            hop(3, d)
        do_attend(1, 0)
        do_attend(1, 1)
        for k in range(1, count):
            send(cot_ref.at[(peer(k) // 2) * 2 + core],
                 keep["cot"].at[pl.ds(pl.multiple_of(place * own_rows, 16), own_rows)],
                 i_s.at[count + k], i_r.at[count + k], tensor=peer(k))
        pass_second(3)
        complete(3)
        do_feed(1, 0)
        do_feed(1, 1)
        flush(nbuf, "norms")
        local[4].wait()
        for k in range(1, count):
            arrived(keep["cot"].at[pl.ds(pl.multiple_of(peer(k) * own_rows, 16), own_rows)],
                    i_s.at[count + k], i_r.at[count + k], tensor=peer(k))
        for half in range(2):
            at_rows = slice(half * rows, half * rows + rows)
            summed = keep["mid"][at_rows] + taken(f"f1{half}")
            keep["pre21"][at_rows] = summed
            keep["acts"][1, at_rows] = (
                row_norm(summed)[0] * part_of(2, 1) + part_of(3, 1)).astype(BF)
        for name in saved:
            if name not in done:
                flush(keep[name], name)
        for copy in sent:
            copy.wait_send()
        for condition, action in conditional:
            @pl.when(condition)
            def _():
                action().wait_send()

        for copy in flushes:
            copy.wait()

    anywhere = pl.BlockSpec(memory_space=pl.ANY)
    inside = pl.BlockSpec(memory_space=pltpu.VMEM)
    dma = pltpu.SemaphoreType.DMA
    scratch = [pltpu.VMEM(shape, kind) for shape, kind in held.values()]
    scratch += [
        pltpu.VMEM((2, 4, 2, ring * head_rows, width), BF),
        pltpu.VMEM((2, 3, 2, 2, ring * half_units, width), BF),
        pltpu.VMEM((2, 4, width), F32),
        pltpu.VMEM((rows, width), F32),
        dma((4, 2 * ring)), dma((4, 2 * ring)), dma((4, 2 * ring)), dma((4, 2 * ring)),
        dma((4, 2, 2 * ring)), dma((4, 2, 2 * ring)), dma((3,)), dma((3,)),
        dma((len(stages),)), dma((len(stages),)), dma((2 * count,)), dma((2 * count,)),
        dma((5,)), dma((len(outs),)),
    ]
    results = pl.pallas_call(
        forward_kernel,
        in_specs=[anywhere] * 4 + [inside] * 5,
        out_specs=[anywhere] * len(outs),
        out_shape=[jax.ShapeDtypeStruct(shape, kind) for shape, kind in outs.values()],
        scratch_shapes=scratch,
        compiler_params=pltpu.CompilerParams(
            collective_id=0, has_side_effects=True, vmem_limit_bytes=62 << 20),
        name="forward_kernel",
    )(layer_inputs, cotangent, heads_in, units_in, norm_in, segment_column, segment_row, cosine, sines)
    return dict(zip(outs, results))


def backward_all(saved, count, tables):
    segment_column, segment_row, cosine, sines = tables
    ring = lax.axis_size(FSDP)
    total, width = saved["cot"].shape
    own_rows = total // count
    rows = total // 2
    heads = saved["q0"].shape[1]
    step = saved["feed0"].shape[2] // 2
    head_rows = heads // (2 * ring)
    half_units = step // (2 * ring)
    order = sorted(range(1, ring), key=lambda k: min(k, ring - k))
    loaded = ("q", "k", "v", "lse", "pre1", "pre2", "spread", "feed", "heads", "units")
    arrays = [saved[f"{name}{l}"] for l in range(2) for name in loaded]
    arrays += [saved["ctx0"], saved["ctx1"], saved["low0"], saved["acts"], saved["cot"]]
    stages = [f"{stage}{l}{h}" for l in range(2) for stage in "gi" for h in range(2)]
    pieces = "dguhe"
    scaling = HEAD_DIM ** (-0.5)

    def backward_kernel(norm_ref, col_ref, row_ref, cos_ref, sin_ref, *refs):
        n = len(arrays)
        from_hbm = {}
        for l in range(2):
            for i, name in enumerate(loaded):
                from_hbm[f"{name}{l}"] = refs[l * len(loaded) + i]
        from_hbm["ctx0"], from_hbm["ctx1"], from_hbm["low0"], acts_ref, cot_ref = refs[n - 5:n]
        from_hbm["low1"] = acts_ref.at[0]
        (act_out, grad_out, units_out, heads_out, norm_out) = refs[n:n + 5]
        rest = refs[n + 5:]
        buffers = [name for name in loaded if name != "spread"]
        here = dict(zip(buffers, rest[:len(buffers)]))
        (lefts, rights, dpre, wide_rights, dctx, grads, own, got, nsum, nred, nget,
         acc, keep_u, keep_h, give_u, give_h, core_u, core_h, side_u, side_h, line_u, line_h,
         fin_u, fin_h, x_s, x_r, a_s, a_r, b_s, b_r, c_s, c_r, y_s, y_r, z_s, z_r,
         n_s, n_r, j_s, j_r, l_s, m_s, credit_c, credit_y) = rest[len(buffers):]
        dfeed = wide_rights.at[1]
        cot = grads.at[0]
        core = lax.axis_index(PIPE)
        place = lax.axis_index(TENSOR)
        group = lax.axis_index(FSDP)
        other = 1 - core
        item = (place // 2) * 2 + core

        def peer(k):
            low, high = place % 2, place // 2
            low = 1 - low if k & 1 else low
            high = 1 - high if k & 2 else high
            return high * 2 + low

        def near(k):
            return lax.rem(group + k, ring)

        pending = []

        def send(src, dst, send_sem, recv_sem, **to):
            copy = pltpu.make_async_remote_copy(
                src_ref=src, dst_ref=dst, send_sem=send_sem, recv_sem=recv_sem,
                device_id=to, device_id_type=MESH)
            copy.start()
            pending.append(copy)
            return copy

        def arrived(dst, send_sem, recv_sem, **to):
            pltpu.make_async_remote_copy(
                src_ref=dst, dst_ref=dst, send_sem=send_sem, recv_sem=recv_sem,
                device_id=to, device_id_type=MESH).wait_recv()

        def sent(copy):
            copy.wait_send()
            pending[:] = [held for held in pending if held is not copy]

        names = loaded + ("ctx", "low")
        loads = {}

        def load(l, *which):
            for name in which:
                to = {"ctx": lefts.at[3], "low": rights.at[0],
                      "spread": wide_rights.at[0]}.get(name)
                to = here[name] if to is None else to
                copy = pltpu.make_async_copy(from_hbm[f"{name}{l}"], to,
                                             l_s.at[l * len(names) + names.index(name)])
                copy.start()
                loads[name, l] = copy

        def ready(l, *which):
            for name in which:
                loads.pop((name, l)).wait()

        def rows_at(index):
            return pl.ds(pl.multiple_of(index * own_rows, 16), own_rows)

        barrier = pltpu.get_barrier_semaphore()
        peers = [dict(tensor=peer(k)) for k in (1, 2, 3)]
        peers += [dict(pipe=other), dict(pipe=other, tensor=peer(2))]
        peers += [dict(fsdp=near(k)) for k in range(1, ring)]
        for to in peers:
            pl.semaphore_signal(barrier, inc=1, device_id=to, device_id_type=MESH)
        pl.semaphore_wait(barrier, len(peers))

        own_cot = pltpu.make_async_copy(cot_ref, cot, m_s.at[0])
        own_cot.start()
        load(1, "pre2", "feed", "spread", "units", "pre1", "heads", "q", "k", "v", "lse", "ctx",
             "low")

        def home(source, result, sems, index):
            copy = pltpu.make_async_copy(source.at[core, rows_at(place)], result.at[item],
                                         m_s.at[index])
            copy.start()
            for k in range(1, 4):
                layer = other if k & 1 else core
                to = dict(pipe=layer, tensor=peer(k & 2))
                send(source.at[layer, rows_at(peer(k & 2))], result.at[item],
                     sems[0].at[k], sems[1].at[k], **to)
            return copy

        def home_arrived(result, sems):
            for k in range(1, 4):
                to = dict(pipe=other if k & 1 else core, tensor=peer(k & 2))
                index = (peer(k & 2) // 2) * 2 + (other if k & 1 else core)
                arrived(result.at[index], sems[0].at[k], sems[1].at[k], **to)

        own_act = home(acts_ref, act_out, (a_s, a_r), 1)
        own_cot.wait()
        last_use = {}

        def exchange(tag, value):
            place_of = "gi".index(tag[0]) * 2 + int(tag[2])
            if place_of in last_use:
                sent(last_use[place_of])
            own[place_of] = value
            index = stages.index(tag)
            last_use[place_of] = send(own.at[place_of], got.at[index], x_s.at[index],
                                      x_r.at[index], tensor=peer(1))

        def taken(tag):
            index = stages.index(tag)
            place_of = "gi".index(tag[0]) * 2 + int(tag[2])
            arrived(got.at[index], x_s.at[index], x_r.at[index], tensor=peer(1))
            return own[place_of].astype(F32) + got[index].astype(F32)

        def part_of(name, l):
            return norm_ref[l, name:name + 1, :]

        def note_sums(l, half, first, sums):
            if half == 0:
                nsum[l, first:first + 2] = sums[:2]
            else:
                nsum[l, first:first + 2] = nsum[l, first:first + 2] + sums[:2]

        def do_norm_back(l, half):
            at_rows = slice(half * rows, half * rows + rows)
            if l == 1:
                upstream = cot[at_rows].astype(F32)
            else:
                upstream = dpre[at_rows] + taken(f"i1{half}")
                grads[1, at_rows] = upstream.astype(BF)
            if half == 0:
                ready(l, "pre2")
            normed, inverse = row_norm(here["pre2"][at_rows])
            through, sums = row_norm_back(normed, inverse, part_of(2, l), upstream)
            note_sums(l, half, 2, sums)
            dpre[at_rows] = through
            dfeed[at_rows] = through.astype(BF)

        def do_feed_back(l, half):
            at_rows = slice(half * rows, half * rows + rows)
            low = dfeed[at_rows]
            if half == 0:
                ready(l, "units")
            units, feed_ref = here["units"], here["feed"]
            for share in range(2):
                at = slice(share * step, share * step + step)
                gate = feed_ref[0, at_rows, at].astype(F32)
                up = feed_ref[1, at_rows, at].astype(F32)
                grad_hidden = nt(low, units[2, share].reshape(step, width))
                sigmoid = jax.nn.sigmoid(gate)
                grad_gate = (
                    grad_hidden * up * sigmoid * (1.0 + gate * (1.0 - sigmoid))).astype(BF)
                grad_up = (grad_hidden * gate * sigmoid).astype(BF)
                feed_ref[0, at_rows, at] = grad_gate
                feed_ref[1, at_rows, at] = grad_up
                back = nn(grad_gate, units[0, share].reshape(step, width))
                back = back + nn(grad_up, units[1, share].reshape(step, width))
                if share == 0:
                    acc[...] = back
                else:
                    exchange(f"g{l}{half}", (acc[...] + back).astype(BF))

        def unit_grads(first, end, share, target):
            size = step // 2

            def one(i, _):
                c, col = i // 2, i % 2
                at = pl.ds(pl.multiple_of(share * step + col * size, 128), size)
                target[c, col] = tn(here["feed"][c, :, at], wide_rights[c // 2]).astype(BF)
                return 0

            lax.fori_loop(2 * first, 2 * end, one, 0)

        def head_grad(share, i, target):
            j = 2 * share + i
            full = tn(lefts[j], rights[j // 3]).astype(BF)
            for col in range(2):
                target[i, col] = full[col * (heads // 2):(col + 1) * (heads // 2)]

        def do_attend_back(l, half):
            at_rows = slice(half * rows, half * rows + rows)
            if half == 0:
                ready(l, "pre1", "heads", "q", "k", "v", "lse")
            upstream = dpre[at_rows] + taken(f"g{l}{half}")
            normed, inverse = row_norm(here["pre1"][at_rows])
            through, sums = row_norm_back(normed, inverse, part_of(0, l), upstream)
            note_sums(l, half, 0, sums)
            dpre[at_rows] = through
            low = through.astype(BF)
            rights[1, at_rows] = low
            dctx[...] = nt(low, here["heads"][3].reshape(heads, width)).astype(BF)
            masks = head_masks(rows)
            wide_masks = head_masks(total)
            same = col_ref[:, :1] == row_ref[:1, at_rows]
            for slab in range(heads // 128):
                at = slice(slab * 128, slab * 128 + 128)
                second_at = slice(heads + slab * 128, heads + slab * 128 + 128)
                q, k = here["q"][at_rows, at], here["k"][:, at]
                v, grad_ctx = here["v"][:, at], dctx[:, at]
                dq = jnp.zeros((rows, 128), F32)
                dk = jnp.zeros((total, 128), F32)
                dv = jnp.zeros((total, 128), F32)
                for h in range(2):
                    mask = masks[h].astype(BF)
                    scores = nt(k, q * mask) * scaling
                    scores = jnp.where(same, scores, masked_value)
                    lse = here["lse"][2 * slab + h:2 * slab + h + 1, at_rows]
                    chances = jnp.exp(scores - lse)
                    grad_chances = nt(v, grad_ctx * mask)
                    row_dot = jnp.sum(chances * grad_chances, axis=0, keepdims=True)
                    grad_scores = (chances * (grad_chances - row_dot)).astype(BF)
                    dv = dv + nn(chances.astype(BF), grad_ctx) * wide_masks[h]
                    dk = dk + nn(grad_scores, q) * wide_masks[h]
                    dq = dq + tn(grad_scores, k) * masks[h]
                lefts[0, at_rows, at] = turned(
                    dq * scaling, cos_ref[at_rows], -sin_ref[at_rows]).astype(BF)
                if half == 0:
                    here["pre2"][:, at] = dk
                    here["pre2"][:, second_at] = dv
                else:
                    dk = here["pre2"][:, at] + dk
                    dv = here["pre2"][:, second_at] + dv
                    lefts[1, :, at] = turned(dk * scaling, cos_ref[...], -sin_ref[...]).astype(BF)
                    lefts[2, :, at] = dv.astype(BF)

        def do_inputs_back(l, half):
            at_rows = slice(half * rows, half * rows + rows)
            back = jnp.zeros((rows, width), F32)
            for c in range(3):
                back = back + nn(lefts[c, at_rows], here["heads"][c].reshape(heads, width))
            exchange(f"i{l}{half}", back.astype(BF))

        def parts(piece, units_ref, heads_ref):
            index = pieces.index(piece)
            if index > 2:
                return heads_ref.at[index - 3:index - 2]
            return units_ref.at[(2, 0, 1)[index]:(3, 1, 2)[index]]

        def cell(piece, l):
            return l * 5 + pieces.index(piece)

        gave = {}

        def give(l, piece):
            if l == 0:
                pl.semaphore_wait(credit_c.at[pieces.index(piece)], 1)
            index = cell(piece, l)
            gave[piece] = send(parts(piece, give_u, give_h), parts(piece, core_u, core_h),
                               c_s.at[index], c_r.at[index], pipe=other)

        def add_core(l, piece):
            index = cell(piece, l)
            come = parts(piece, core_u, core_h)
            arrived(come, c_s.at[index], c_r.at[index], pipe=other)
            mine = parts(piece, keep_u.at[l], keep_h.at[l])
            mine[...] = (mine[...].astype(F32) + come[...].astype(F32)).astype(BF)
            if l == 1:
                pl.semaphore_signal(credit_c.at[pieces.index(piece)], inc=1,
                                    device_id=dict(pipe=other), device_id_type=MESH)
            else:
                pl.semaphore_wait(credit_y.at[pieces.index(piece)], 1)
            send(mine.at[:, 1], parts(piece, side_u, side_h), y_s.at[index], y_r.at[index],
                 tensor=peer(2))

        def slot_of(piece, ref, g):
            size = head_rows if piece in "he" else half_units
            return ref.at[:, pl.ds(pl.multiple_of(g * size, 16), size)]

        def add_side(l, piece):
            index = cell(piece, l)
            come = parts(piece, side_u, side_h)
            arrived(come, y_s.at[index], y_r.at[index], tensor=peer(2))
            mine = parts(piece, keep_u.at[l], keep_h.at[l]).at[:, 0]
            mine[...] = (mine[...].astype(F32) + come[...].astype(F32)).astype(BF)
            if l == 1:
                pl.semaphore_signal(credit_y.at[pieces.index(piece)], inc=1,
                                    device_id=dict(tensor=peer(2)), device_id_type=MESH)
            @pl.when(at_end)
            def _():
                to_relay(l, piece).start()

            for sign in (1, -1):
                @pl.when(inner(sign))
                def _():
                    next_one(l, piece, sign).start()

            @pl.when(at_end)
            def _():
                to_far(l, piece).start()

        at_end = jnp.logical_or(group == 0, group == ring - 1)

        def inner(sign):
            return group + 1 < ring if sign > 0 else group >= 1

        def line_send(l, piece, g, kind, to):
            index = cell(piece, l)
            mine = parts(piece, keep_u.at[l], keep_h.at[l]).at[:, 0]
            return pltpu.make_async_remote_copy(
                src_ref=slot_of(piece, mine, g),
                dst_ref=parts(piece, line_u.at[l, kind], line_h.at[l, kind]),
                send_sem=z_s.at[index, kind], recv_sem=z_r.at[index, kind],
                device_id={FSDP: to}, device_id_type=MESH)

        def next_one(l, piece, sign):
            return line_send(l, piece, group + sign, 0 if sign > 0 else 1, group + sign)

        def far():
            return lax.rem(group + 2, 4)

        def to_far(l, piece):
            return line_send(l, piece, far(), 2, far())

        def to_relay(l, piece):
            opposite = ring - 1 - group
            return line_send(l, piece, opposite, 3, jnp.where(group == 0, 1, 2))

        def relay(l, piece):
            @pl.when(jnp.logical_not(at_end))
            def _():
                index = cell(piece, l)
                come = parts(piece, line_u.at[l, 3], line_h.at[l, 3])
                arrived(come, z_s.at[index, 3], z_r.at[index, 3],
                        fsdp=jnp.where(group == 1, 0, 3))
                mine = slot_of(piece, parts(piece, keep_u.at[l], keep_h.at[l]).at[:, 0], far())
                mine[...] = (mine[...].astype(F32) + come[...].astype(F32)).astype(BF)
                to_far(l, piece).start()

        def add_line(l, piece):
            index = cell(piece, l)
            mine = parts(piece, keep_u.at[l], keep_h.at[l]).at[:, 0]
            result = parts(piece, fin_u.at[l], fin_h.at[l])
            come = [parts(piece, line_u.at[l, kind], line_h.at[l, kind]) for kind in range(3)]
            arrived(come[2], z_s.at[index, 2], z_r.at[index, 2], fsdp=far())
            result[...] = (slot_of(piece, mine, group)[...].astype(F32)
                           + come[2][...].astype(F32)).astype(BF)
            for sign in (1, -1):
                kind = 0 if sign > 0 else 1

                @pl.when(inner(-sign))
                def _():
                    arrived(come[kind], z_s.at[index, kind], z_r.at[index, kind],
                            fsdp=group - sign)
                    result[...] = (result[...].astype(F32)
                                   + come[kind][...].astype(F32)).astype(BF)

        def line_sent(l, piece):
            for sign in (1, -1):
                @pl.when(inner(sign))
                def _():
                    next_one(l, piece, sign).wait_send()

            to_far(l, piece).wait_send()

            @pl.when(at_end)
            def _():
                to_relay(l, piece).wait_send()

        do_norm_back(1, 0)
        do_norm_back(1, 1)
        ready(1, "feed", "spread")
        unit_grads(2, 3, other, give_u)
        give(1, "d")
        unit_grads(2, 3, core, keep_u.at[1])
        do_feed_back(1, 0)
        add_core(1, "d")
        do_feed_back(1, 1)
        unit_grads(0, 1, other, give_u)
        give(1, "g")
        unit_grads(1, 2, other, give_u)
        give(1, "u")
        unit_grads(0, 1, core, keep_u.at[1])
        do_attend_back(1, 0)
        add_core(1, "g")
        unit_grads(1, 2, core, keep_u.at[1])
        load(0, "feed", "spread", "units")
        add_side(1, "d")
        add_core(1, "u")
        do_attend_back(1, 1)
        load(0, "pre2")
        for half in range(2):
            do_inputs_back(1, half)
        ready(1, "ctx", "low")
        head_grad(other, 0, give_h)
        give(1, "h")
        head_grad(other, 1, give_h)
        give(1, "e")
        head_grad(core, 0, keep_h.at[1])
        head_grad(core, 1, keep_h.at[1])
        load(0, "pre1", "heads", "q", "k", "v", "lse", "ctx", "low")
        relay(1, "d")
        add_core(1, "h")
        add_core(1, "e")

        do_norm_back(0, 0)
        ready(0, "feed", "spread")
        do_feed_back(0, 0)
        add_side(1, "g")
        do_norm_back(0, 1)
        sent(gave["d"])
        unit_grads(2, 3, other, give_u)
        give(0, "d")
        unit_grads(2, 3, core, keep_u.at[0])
        do_feed_back(0, 1)
        add_core(0, "d")
        relay(1, "g")
        sent(gave["g"])
        unit_grads(0, 1, other, give_u)
        give(0, "g")
        sent(gave["u"])
        unit_grads(1, 2, other, give_u)
        give(0, "u")
        unit_grads(0, 1, core, keep_u.at[0])
        add_side(1, "u")
        add_core(0, "g")
        unit_grads(1, 2, core, keep_u.at[0])
        do_attend_back(0, 0)
        add_core(0, "u")
        relay(1, "u")
        add_side(1, "h")
        add_side(1, "e")
        do_attend_back(0, 1)
        send(nsum.at[other], nget.at[0], n_s.at[0], n_r.at[0], pipe=other)
        ready(0, "ctx", "low")
        sent(gave["h"])
        head_grad(other, 0, give_h)
        give(0, "h")
        sent(gave["e"])
        head_grad(other, 1, give_h)
        give(0, "e")
        head_grad(core, 0, keep_h.at[0])
        do_inputs_back(0, 0)
        add_core(0, "h")
        head_grad(core, 1, keep_h.at[0])
        do_inputs_back(0, 1)
        add_core(0, "e")
        relay(1, "h")
        relay(1, "e")
        add_side(0, "d")
        arrived(nget.at[0], n_s.at[0], n_r.at[0], pipe=other)
        nred[0] = nsum[core] + nget[0]
        send(nred.at[0], nget.at[1], n_s.at[1], n_r.at[1], tensor=peer(2))
        add_side(0, "g")
        relay(0, "d")

        def finish_rows(half):
            at_rows = slice(half * rows, half * rows + rows)
            grads[0, at_rows] = (dpre[at_rows] + taken(f"i0{half}")).astype(BF)

        finish_rows(0)
        relay(0, "g")
        add_side(0, "u")
        finish_rows(1)
        own_grad = home(grads, grad_out, (b_s, b_r), 2)
        arrived(nget.at[1], n_s.at[1], n_r.at[1], tensor=peer(2))
        nred[1] = nred[0] + nget[1]
        for k in order:
            send(nred.at[1], nget.at[1 + (ring - k) % ring], n_s.at[1 + k],
                 n_r.at[1 + (ring - k) % ring], fsdp=near(k))
        for piece in pieces[:3]:
            add_line(1, piece)
        relay(0, "u")
        add_side(0, "h")
        add_line(1, "h")
        add_line(1, "e")
        add_side(0, "e")
        add_line(0, "d")
        relay(0, "h")
        add_line(0, "g")
        relay(0, "e")
        norms = nred[1]
        for k in order:
            arrived(nget.at[1 + k], n_s.at[1 + k], n_r.at[1 + k], fsdp=near(k))
            norms = norms + nget[1 + k]
        norm_out[...] = norms
        add_line(0, "u")
        add_line(0, "h")
        add_line(0, "e")
        joins = []
        for i, (fin, result) in enumerate(((fin_u, units_out), (fin_h, heads_out))):
            send(fin.at[other], result.at[core], j_s.at[i], j_r.at[i], pipe=other)
            copy = pltpu.make_async_copy(fin.at[core], result.at[core], m_s.at[3 + i])
            copy.start()
            joins.append(copy)
        for i, result in enumerate((units_out, heads_out)):
            arrived(result.at[other], j_s.at[i], j_r.at[i], pipe=other)
        home_arrived(act_out, (a_s, a_r))
        home_arrived(grad_out, (b_s, b_r))
        for copy in [own_act, own_grad] + joins:
            copy.wait()
        for copy in pending:
            copy.wait_send()
        for l in range(2):
            for piece in pieces:
                line_sent(l, piece)

    anywhere = pl.BlockSpec(memory_space=pl.ANY)
    inside = pl.BlockSpec(memory_space=pltpu.VMEM)
    dma = pltpu.SemaphoreType.DMA
    scratch = [pltpu.VMEM(saved[f"{name}0"].shape, saved[f"{name}0"].dtype) for name in loaded
               if name != "spread"]
    scratch += [
        pltpu.VMEM((4, total, heads), BF), pltpu.VMEM((2, total, width), BF),
        pltpu.VMEM((total, width), F32), pltpu.VMEM((2, total, width), BF),
        pltpu.VMEM((rows, heads), BF),
        pltpu.VMEM((2, total, width), BF),
        pltpu.VMEM((4, rows, width), BF), pltpu.VMEM((8, rows, width), BF),
        pltpu.VMEM((2, 4, width), F32), pltpu.VMEM((2, 4, width), F32),
        pltpu.VMEM((1 + ring, 4, width), F32), pltpu.VMEM((rows, width), F32),
        pltpu.VMEM((2, 3, 2, ring * half_units, width), BF),
        pltpu.VMEM((2, 2, 2, ring * head_rows, width), BF),
        pltpu.VMEM((3, 2, ring * half_units, width), BF),
        pltpu.VMEM((2, 2, ring * head_rows, width), BF),
        pltpu.VMEM((3, 2, ring * half_units, width), BF),
        pltpu.VMEM((2, 2, ring * head_rows, width), BF),
        pltpu.VMEM((3, ring * half_units, width), BF),
        pltpu.VMEM((2, ring * head_rows, width), BF),
        pltpu.VMEM((2, ring, 3, half_units, width), BF),
        pltpu.VMEM((2, ring, 2, head_rows, width), BF),
        pltpu.VMEM((2, 3, half_units, width), BF),
        pltpu.VMEM((2, 2, head_rows, width), BF),
        dma((8,)), dma((8,)), dma((4,)), dma((4,)), dma((4,)), dma((4,)),
        dma((10,)), dma((10,)), dma((10,)), dma((10,)), dma((10, 4)), dma((10, 4)),
        dma((1 + ring,)), dma((1 + ring,)), dma((2,)), dma((2,)),
        dma((2 * (len(loaded) + 2),)), dma((5,)),
        pltpu.SemaphoreType.REGULAR((5,)), pltpu.SemaphoreType.REGULAR((5,)),
    ]
    return pl.pallas_call(
        backward_kernel,
        in_specs=[inside] * 5 + [anywhere] * len(arrays),
        out_specs=[anywhere] * 4 + [inside],
        out_shape=[
            jax.ShapeDtypeStruct((count, own_rows, width), BF),
            jax.ShapeDtypeStruct((count, own_rows, width), BF),
            jax.ShapeDtypeStruct((2, 3, half_units, width), BF),
            jax.ShapeDtypeStruct((2, 2, head_rows, width), BF),
            jax.ShapeDtypeStruct((4, width), F32),
        ],
        scratch_shapes=scratch,
        compiler_params=pltpu.CompilerParams(
            collective_id=1, has_side_effects=True, vmem_limit_bytes=67043328),
        name="backward_kernel",
    )(saved["norms"], segment_column, segment_row, cosine, sines, *arrays)


def to_item(array, core, place):
    def piece(k):
        return lax.dynamic_index_in_dim(array, ((place ^ k) & 2) | core, 0, keepdims=False)

    parts = [piece(0)] + [flip(piece(k), TENSOR, k) for k in range(1, 4)]
    return jnp.concatenate(unxor(parts, place), axis=0)


def from_item(by_layer, core, place):
    rows = by_layer[0].shape[0] // 4
    mine = jnp.where(core == 0, by_layer[0], by_layer[1])
    other = jnp.where(core == 0, by_layer[1], by_layer[0])

    def piece(k):
        target = place ^ (k & 2)
        return lax.dynamic_slice_in_dim(other if k & 1 else mine, target * rows, rows, 0)

    parts = [piece(0)] + [mixed_flip(piece(k), k & 1, k & 2) for k in range(1, 4)]
    return jnp.stack(unxor(parts, (place & 2) | core)).astype(F32)


def whole_step(
    layer_inputs,
    cotangent,
    input_master,
    output_master,
    gate_master,
    down_master,
    norm_tables,
    document_lengths,
):
    core = lax.axis_index(PIPE)
    place = lax.axis_index(TENSOR)
    group = lax.axis_index(FSDP)
    ring = lax.axis_size(FSDP)
    width = layer_inputs.shape[2]
    head_rows = input_master.shape[2]
    units = down_master.shape[1]
    half = units // 2
    first_core = core == 0

    item = (place & 2) | core
    lengths = lax.dynamic_index_in_dim(document_lengths[:, 0, :], item, 0, keepdims=False)
    segment, position = segment_info(lengths)
    segment_column = jnp.broadcast_to(segment[:, None], (MB_CAP, 128))
    segment_row = jnp.broadcast_to(segment[None, :], (8, MB_CAP))
    tables = (segment_column, segment_row) + rotary_tables(position)

    def split_by_core(for_first, for_second):
        keep = jnp.where(first_core, for_first, for_second)
        got = flip(jnp.where(first_core, for_second, for_first), PIPE, 1)
        return [jnp.where(first_core, keep, got), jnp.where(first_core, got, keep)]

    def joined_by_core(share_zero, share_one):
        keep = jnp.where(first_core, share_zero, share_one)
        got = flip(jnp.where(first_core, share_one, share_zero), PIPE, 1)
        return jnp.where(first_core, keep, got), jnp.where(first_core, got, keep)

    if head_rows % 16 == 0 and half % 16 == 0 and ring == 4:
        heads_in = jnp.concatenate([input_master[0], output_master], axis=0).astype(BF)
        units_in = jnp.concatenate([gate_master[0], down_master], axis=0).astype(BF)
        saved = forward_all(layer_inputs, cotangent, heads_in, units_in.reshape(3, 2, half, width),
                            norm_tables[0], tables)
        results = backward_all(saved, cotangent.shape[0], tables)
        activations, gradients_in, unit_grad, head_grad, norm_sum = results
        head_grad = head_grad.reshape(4, head_rows, width).astype(F32)
        unit_grad = unit_grad.transpose(1, 0, 2, 3).reshape(3, units, width).astype(F32)
        return (
            activations[None].astype(F32),
            gradients_in[None].astype(F32),
            head_grad[None, :3],
            head_grad[None, 3],
            unit_grad[None, :2],
            unit_grad[None, 2],
            norm_sum[None],
        )

    in_low = input_master[0].astype(BF)
    out_low = output_master.astype(BF)
    head_shares = split_by_core(in_low[:2], jnp.concatenate([in_low[2:], out_low], axis=0))
    unit_low = jnp.concatenate([gate_master[0], down_master], axis=0).astype(BF)
    unit_shares = split_by_core(unit_low[:, :half], unit_low[:, half:])

    x = to_item(layer_inputs, core, place)
    norm_own = norm_tables[0]
    norm_other = flip(norm_own, PIPE, 1)
    norms = [
        jnp.where(first_core, norm_own, norm_other),
        jnp.where(first_core, norm_other, norm_own),
    ]

    quarter = half // 2
    rows = ring * head_rows

    def gather_heads(s, *waits):
        slots = ring_gather(tied(head_shares[s], *waits), f"h{s}")
        ascending = jnp.stack(slots[::-1] + slots[::-1])
        column = lax.dynamic_slice_in_dim(ascending, ring - 1 - group, ring, 0)
        return column.transpose(1, 0, 2, 3).reshape(2, rows, width)

    def head_weights(parts):
        mine = jnp.concatenate(parts[:2], axis=1)
        theirs = jnp.concatenate(parts[2:], axis=1)
        low = jnp.where(first_core, mine, theirs)
        high = jnp.where(first_core, theirs, mine)
        return jnp.concatenate([low, high[:1]], axis=0), high[1]

    def gather_units(s, i, *waits):
        piece = unit_shares[s][:, i * quarter:i * quarter + quarter]
        return jnp.concatenate(ring_gather(tied(piece, *waits), f"u{s}{i}"), axis=1)

    def in_order(pieces):
        return [pieces[i][j] for j in range(4) for i in range(2)]

    column = gather_heads(0)
    heads = spread_out(column, "h0")
    unit_a = gather_units(0, 0, column)
    pieces = [spread_out(unit_a, "u00")]
    unit_b = gather_units(0, 1, unit_a, heads[1])
    pieces.append(spread_out(unit_b, "u01"))
    weights = head_weights(heads) + (in_order(pieces),)
    layers = [weights]
    halves = attention_forward("0", [(tied(x, unit_a),), (x,)], weights, None, tables)
    column = gather_heads(1, unit_b, halves[1][1][0], pieces[0][1])
    heads = spread_out(column, "h1")
    next_a = gather_units(1, 0, column)
    next_pieces = [spread_out(next_a, "u10")]
    next_b = gather_units(1, 1, next_a, heads[1])
    next_pieces.append(spread_out(next_b, "u11"))
    layers.append(head_weights(heads) + (in_order(next_pieces),))
    ends, saved = feed_forward("0", halves, weights, norms[0], (column,), ())
    kept = [saved]
    ends[0] = (tied(ends[0][0], next_a),) + ends[0][1:]
    halves = attention_forward("1", ends, layers[1], norms[0], tables, (next_b,))
    ends, saved = feed_forward("1", halves, layers[1], norms[1], (), ())
    kept.append(saved)
    upstream = to_item(cotangent, core, place)

    def pull_units(tag, gate_up, down):
        parts = []
        for name, grad, count in (("u", gate_up, 2), ("d", down, 1)):
            own = grad[0].reshape(count, 2, ring * half, width)
            got = cross(grad[1], PIPE, 1, f"c_g{name}{tag}").reshape(count, 2, ring * half, width)
            parts.append([added(own[:, 1], got[:, 1]), (own[:, 0], got[:, 0])])
        return parts[0][0], parts[1][0], parts[0][1], parts[1][1]

    def cross_units(tag, units):
        columns = []
        for name, neighbour, (own, got) in (("u", units[0], units[2]), ("d", units[1], units[3])):
            other = cross(neighbour, TENSOR, 2, f"y_g{name}{tag}")
            column = own.astype(F32) + got.astype(F32) + other.astype(F32)
            columns.append(column.astype(BF))
        return columns

    def ring_units(tag, columns):
        totals = []
        for name, column in zip("ud", columns):
            count = column.shape[0]
            column = column.reshape(count, 2, ring, quarter, width)
            total = ring_reduce([column[:, :, k] for k in range(ring)], f"g{name}{tag}")
            totals.append(total.reshape(count, half, width).astype(BF))
        return jnp.concatenate(totals, axis=0)

    def pull_heads(tag, grad_in, grad_out):
        low = jnp.stack(grad_in[:2])
        high = jnp.stack([grad_in[2], grad_out])
        mine = jnp.where(first_core, low, high)
        theirs = cross(jnp.where(first_core, high, low), PIPE, 1, "c_gh" + tag)
        return added(mine[:, rows:], theirs[:, rows:]), mine[:, :rows], theirs[:, :rows]

    def cross_heads(tag, heads):
        neighbour, own, got = heads
        column = own.astype(F32) + got.astype(F32)
        column = column + cross(neighbour, TENSOR, 2, "y_gh" + tag).astype(F32)
        return column.astype(BF)

    def ring_heads(tag, column):
        column = column.reshape(2, ring, head_rows, width).transpose(1, 0, 2, 3)
        ascending = jnp.concatenate([column, column], axis=0)
        rolled = lax.dynamic_slice_in_dim(ascending, (group + 1) % ring, ring, 0)
        return ring_reduce([rolled[ring - 1 - k] for k in range(ring)], "gh" + tag).astype(BF)

    head_totals = [None, None]
    unit_totals = [None, None]
    edges = [None, None]
    norm_grads = [None, None]
    ends = [(upstream,), (upstream,)]
    waits = ()
    for s in (1, 0):
        tag = str(s)
        ends, edges[s], units, heads, norm_grads[s] = layer_backward(
            tag, ends, layers[s], norms[s], tables, kept[s], pull_units, pull_heads, waits
        )
        crossed = cross_units(tag, units)
        unit_totals[s] = ring_units(tag, crossed)
        head_columns = cross_heads(tag, heads)
        head_totals[s] = ring_heads(tag, head_columns)
        waits = crossed
    first_grad = jnp.concatenate(
        [
            (grad[half * MB_CAP // 2:(half + 1) * MB_CAP // 2] + own.astype(F32) + got.astype(F32))
            for half, (grad, own, got) in enumerate(ends)
        ],
        axis=0,
    ).astype(BF)
    activations = from_item([kept[1][1], edges[1]], core, place)
    gradients_in = from_item([first_grad, edges[0]], core, place)

    low, high = joined_by_core(head_totals[0], head_totals[1])
    unit_low, unit_high = joined_by_core(unit_totals[0], unit_totals[1])
    unit_grad = jnp.concatenate([unit_low, unit_high], axis=1).astype(F32)
    head_grad = jnp.concatenate([low, high], axis=0).astype(F32)
    norm_grads[0] = tied(norm_grads[0], heads[0])
    norm_own = jnp.where(first_core, norm_grads[0], norm_grads[1])
    norm_other = jnp.where(first_core, norm_grads[1], norm_grads[0])
    norm_sum = norm_own + flip(norm_other, PIPE, 1)
    norm_sum = norm_sum + flip(norm_sum, TENSOR, 2)
    bit = 1
    while bit < ring:
        norm_sum = norm_sum + flip(norm_sum, FSDP, bit)
        bit = bit * 2
    return (
        activations[None],
        gradients_in[None],
        head_grad[None, :3],
        head_grad[None, 3],
        unit_grad[None, :2],
        unit_grad[None, 2],
        norm_sum[None],
    )


def solution(mesh):
    placed = (
        P(None, (FSDP, TENSOR), None),
        P(None, (FSDP, TENSOR), None),
        P(PIPE, None, (TENSOR, FSDP), None),
        P(PIPE, (TENSOR, FSDP), None),
        P(PIPE, None, (TENSOR, FSDP), None),
        P(PIPE, (TENSOR, FSDP), None),
        P(PIPE, None, None),
        P(None, FSDP, None),
    )
    return jax.shard_map(
        whole_step,
        mesh=mesh,
        in_specs=placed,
        out_specs=(
            P(PIPE, None, (FSDP, TENSOR), None),
            P(PIPE, None, (FSDP, TENSOR), None),
            P(PIPE, None, (TENSOR, FSDP), None),
            P(PIPE, (TENSOR, FSDP), None),
            P(PIPE, None, (TENSOR, FSDP), None),
            P(PIPE, (TENSOR, FSDP), None),
            P(PIPE, None, None),
        ),
        check_vma=False,
    )
```

```python
import jax
import jax.numpy as jnp
from jax import lax
from jax.experimental import pallas as pl
from jax.experimental.pallas import tpu as pltpu
from jax.sharding import PartitionSpec as P

HEAD_DIM = 64
MB_CAP = 512
DOCS = 3

epsilon = 1e-05
rope_base = 1000.0
masked_value = -1e30

BF = jnp.bfloat16
PIPE, FSDP, TENSOR = "pipe", "fsdp", "tensor"
F32 = jnp.float32


def segment_info(lengths):
    doc_ends = jnp.cumsum(lengths)
    starts = doc_ends - lengths
    places = jnp.arange(MB_CAP, dtype=jnp.int32)
    segment = jnp.sum((places[:, None] >= doc_ends[None, :]).astype(jnp.int32), axis=1)
    choose = segment[:, None] == jnp.arange(DOCS, dtype=jnp.int32)[None, :]
    offset = jnp.sum(jnp.where(choose, starts[None, :], 0), axis=1)
    return (segment, places - offset)


def rotary_tables(position):
    half_dim = HEAD_DIM // 2
    lane = jnp.arange(2 * HEAD_DIM, dtype=jnp.int32)
    frequency = rope_base ** (-2.0 * (lane % half_dim).astype(F32) / HEAD_DIM)
    angles = position.astype(F32)[:, None] * frequency[None, :]
    sines = jnp.sin(angles)
    return jnp.cos(angles), jnp.where(lane[None, :] % HEAD_DIM < half_dim, -sines, sines)


def flip(array, axis, bit):
    count = lax.axis_size(axis)
    return lax.ppermute(array, axis, [(i, i ^ bit) for i in range(count)])


def shifted(array, axis, by):
    count = lax.axis_size(axis)
    return lax.ppermute(array, axis, [(i, (i + by) % count) for i in range(count)])


def unxor(parts, index):
    parts = [jnp.where(index & 1, parts[m ^ 1], parts[m]) for m in range(4)]
    return [jnp.where(index & 2, parts[m ^ 2], parts[m]) for m in range(4)]


def mixed_flip(array, core_bit, place_bits):
    count = lax.axis_size(TENSOR)
    pairs = [
        (c * count + t, (c ^ core_bit) * count + (t ^ place_bits))
        for c in range(2)
        for t in range(count)
    ]
    return lax.ppermute(array, (PIPE, TENSOR), pairs)


def ring_gather(shard, tag):
    count = lax.axis_size(FSDP)
    slots = [shard]
    for k in range(1, count):
        with jax.named_scope(f"z{k}_{tag}"):
            slots.append(shifted(shard, FSDP, k))
    return slots


def ring_reduce(parts, tag):
    count = len(parts)
    total = parts[0].astype(F32)
    for k in range(1, count):
        with jax.named_scope(f"z{k}_{tag}"):
            part = shifted(parts[k].astype(BF), FSDP, -k)
        total = total + part.astype(F32)
    return total


def cross(array, axis, bit, tag):
    with jax.named_scope(tag):
        return flip(array, axis, bit)


def spread_out(column, tag):
    neighbour = cross(column, TENSOR, 2, "y_" + tag)
    return [
        column,
        neighbour,
        cross(column, PIPE, 1, "c_" + tag),
        cross(neighbour, PIPE, 1, "n_" + tag),
    ]


def added(a, b):
    return (a.astype(F32) + b.astype(F32)).astype(BF)


def row_norm(summed):
    centered = summed - jnp.mean(summed, axis=-1, keepdims=True)
    inverse = lax.rsqrt(jnp.mean(centered * centered, axis=-1, keepdims=True) + epsilon)
    return centered * inverse, inverse


def row_norm_back(normed, inverse, gain_row, upstream):
    scaled = upstream * gain_row
    through = inverse * (
        scaled
        - jnp.mean(scaled, axis=-1, keepdims=True)
        - normed * jnp.mean(scaled * normed, axis=-1, keepdims=True)
    )
    sums = [
        jnp.sum(upstream * normed, axis=0, keepdims=True),
        jnp.sum(upstream, axis=0, keepdims=True),
    ]
    return through, jnp.concatenate(sums + [jnp.zeros((6, sums[0].shape[1]), F32)], axis=0)


def nn(a, b):
    return lax.dot_general(a, b, (((1,), (0,)), ((), ())), preferred_element_type=F32)


def nt(a, b):
    return lax.dot_general(a, b, (((1,), (1,)), ((), ())), preferred_element_type=F32)


def tn(a, b):
    return lax.dot_general(a, b, (((0,), (0,)), ((), ())), preferred_element_type=F32)


def turned(slab, cosine, sines):
    lane = lax.broadcasted_iota(jnp.int32, slab.shape, 1)
    swapped = jnp.where(
        lane % HEAD_DIM < HEAD_DIM // 2, pltpu.roll(slab, 96, 1), pltpu.roll(slab, 32, 1)
    )
    return slab * cosine + swapped * sines


def head_masks(rows):
    lane = lax.broadcasted_iota(jnp.int32, (rows, 128), 1)
    low = (lane < HEAD_DIM).astype(F32)
    return low, 1.0 - low


def rows_of(half, columns, rows):
    return pl.BlockSpec((rows, columns), lambda i: (half, 0))


def whole(array):
    zeros = (0,) * array.ndim
    return pl.BlockSpec(array.shape, lambda i: zeros)


ANYWHERE = pl.BlockSpec(memory_space=pl.ANY)


def staged(tag, kernel, ins, outs, before, scratch=()):
    before = list(before or [])
    arrays = [array for array, _ in ins] + before
    specs = [spec for _, spec in ins] + [ANYWHERE] * len(before)
    first_out = len(outs) - len(before)
    first_in = len(ins)
    count = len(before)

    def run(*refs):
        kernel(*refs[:first_in], *refs[first_in + count:])

    call = pl.pallas_call(
        run,
        grid=(1,),
        in_specs=specs,
        out_specs=[spec for _, _, spec in outs],
        out_shape=[jax.ShapeDtypeStruct(shape, kind) for shape, kind, _ in outs],
        scratch_shapes=list(scratch),
        input_output_aliases={first_in + i: first_out + i for i in range(count)},
        compiler_params=pltpu.CompilerParams(vmem_limit_bytes=40 << 20),
        cost_estimate=pl.CostEstimate(flops=1024, bytes_accessed=1024, transcendentals=0),
        name=kernel.__name__,
    )
    with jax.named_scope("k_" + tag):
        return call(*arrays)


def project(tag, half, sources, norm_rows, weight, cosine, sines, before):
    given = len(sources) == 1
    total, width = sources[0].shape
    heads = weight.shape[1]
    rows = total // 2

    def project_kernel(*refs):
        if given:
            x_ref, w_ref, cos_ref, sin_ref, q_ref, k_ref, v_ref = refs
            low = x_ref[...]
        else:
            (mid_ref, own_ref, got_ref, norm_ref, w_ref, cos_ref, sin_ref,
             q_ref, k_ref, v_ref, x_ref, low_ref) = refs
            summed = mid_ref[...] + own_ref[...].astype(F32) + got_ref[...].astype(F32)
            x = row_norm(summed)[0] * norm_ref[2:3] + norm_ref[3:4]
            x_ref[...] = x
            low = x.astype(BF)
            low_ref[...] = low
        cosine, sines = cos_ref[...], sin_ref[...]
        for c, out in ((0, q_ref), (1, k_ref)):
            turning = nt(low, w_ref[c])
            for slab in range(heads // 128):
                at = slice(128 * slab, 128 * slab + 128)
                out[:, at] = turned(turning[:, at], cosine, sines).astype(BF)
        v_ref[...] = nt(low, w_ref[2]).astype(BF)

    here = rows_of(half, width, rows)
    ins = [(sources[0], here)]
    outs = [((total, heads), BF, rows_of(half, heads, rows)) for _ in range(3)]
    if not given:
        plain = pl.BlockSpec((rows, width), lambda i: (0, 0))
        ins += [(sources[1], plain), (sources[2], plain), (norm_rows, whole(norm_rows))]
        outs += [((total, width), F32, here), ((total, width), BF, here)]
    ins += [(weight, whole(weight))]
    ins += [(table, rows_of(half, 128, rows)) for table in (cosine, sines)]
    return staged(tag, project_kernel, ins, outs, before)


def attend(tag, half, queries, key_vecs, values, segment_column, segment_row, out_weight, before):
    total, heads = queries.shape
    width = out_weight.shape[1]
    rows = total // 2

    def attend_kernel(q_ref, k_ref, v_ref, col_ref, row_ref, w_ref, part_ref, ctx_ref, lse_ref):
        masks = head_masks(rows)
        lane = lax.broadcasted_iota(jnp.int32, (rows, 128), 1)
        same = col_ref[:, :1] == row_ref[:1, :]
        totals = jnp.zeros((rows, 128), F32)
        for slab in range(heads // 128):
            at = slice(128 * slab, 128 * slab + 128)
            q, k, v = q_ref[:, at], k_ref[:, at], v_ref[:, at]
            gathered = jnp.zeros((rows, 128), F32)
            for h in range(2):
                scores = nt(q * masks[h].astype(BF), k) * HEAD_DIM ** (-0.5)
                scores = jnp.where(same, scores, masked_value)
                top = jnp.max(scores, axis=-1, keepdims=True)
                powers = jnp.exp(scores - top)
                mass = jnp.sum(powers, axis=-1, keepdims=True)
                chances = (powers * (1.0 / mass)).astype(BF)
                gathered = gathered + nn(chances, v) * masks[h]
                totals = jnp.where(lane == 2 * slab + h, top + jnp.log(mass), totals)
            ctx_ref[:, at] = gathered.astype(BF)
        lse_ref[...] = totals.T[:8]
        part_ref[...] = nn(ctx_ref[...], w_ref[...]).astype(BF)

    ins = [
        (queries, rows_of(half, heads, rows)),
        (key_vecs, whole(key_vecs)),
        (values, whole(values)),
        (segment_column, rows_of(half, 128, rows)),
        (segment_row, whole(segment_row)),
        (out_weight, whole(out_weight)),
    ]
    outs = [
        ((rows, width), BF, pl.BlockSpec((rows, width), lambda i: (0, 0))),
        ((total, heads), BF, rows_of(half, heads, rows)),
        ((8, total), F32, pl.BlockSpec((8, rows), lambda i: (0, half))),
    ]
    return staged(tag, attend_kernel, ins, outs, before)


def feed_scratch(blocks, rows, width):
    return [
        pltpu.VMEM((len(blocks),) + blocks[0].shape, BF),
        pltpu.VMEM((rows, width), F32),
        pltpu.SemaphoreType.DMA((len(blocks),)),
    ]


def fetch_blocks(block_refs, buffer, sems):
    for j, ref in enumerate(block_refs):
        pltpu.make_async_copy(ref, buffer.at[j], sems.at[j]).start()


def share_blocks(p, block_refs, buffer, sems):
    each = len(block_refs) // 2
    for j in range(p * each, p * each + each):
        pltpu.make_async_copy(block_refs[j], buffer.at[j], sems.at[j]).wait()

    def joined(c):
        return jnp.concatenate([buffer[p * each + j, c] for j in range(each)], axis=0)

    return joined(0), joined(1), joined(2)


def feed(tag, half, x, own, got, norm_rows, blocks, before):
    total, width = x.shape
    rows = total // 2
    step = len(blocks) // 2 * blocks[0].shape[1]
    units = len(blocks) * blocks[0].shape[1]
    count = len(blocks)

    def feed_kernel(*refs):
        x_ref, own_ref, got_ref, norm_ref = refs[:4]
        block_refs = refs[4:4 + count]
        (part_ref, mid_ref, low_ref, gate_ref, up_ref, own_hid, other_hid,
         buffer, acc_ref, sems) = refs[4 + count:]
        fetch_blocks(block_refs, buffer, sems)
        summed = x_ref[...] + own_ref[...].astype(F32) + got_ref[...].astype(F32)
        middle = row_norm(summed)[0] * norm_ref[0:1] + norm_ref[1:2]
        mid_ref[...] = middle
        low = middle.astype(BF)
        low_ref[...] = low
        for p in range(2):
            gate_w, up_w, down_w = share_blocks(p, block_refs, buffer, sems)
            at = slice(p * step, p * step + step)
            gate = nt(low, gate_w)
            up = nt(low, up_w)
            gate_ref[:, at] = gate.astype(BF)
            up_ref[:, at] = up.astype(BF)
            hidden = (gate * jax.nn.sigmoid(gate) * up).astype(BF)
            (own_hid, other_hid)[p][...] = hidden
            fed = nn(hidden, down_w)
            acc_ref[...] = fed if p == 0 else acc_ref[...] + fed
        part_ref[...] = acc_ref[...].astype(BF)

    plain = pl.BlockSpec((rows, width), lambda i: (0, 0))
    here = rows_of(half, width, rows)
    wide = rows_of(half, units, rows)
    ins = [(x, here), (own, plain), (got, plain), (norm_rows, whole(norm_rows))]
    ins += [(block, ANYWHERE) for block in blocks]
    outs = [((rows, width), BF, plain), ((total, width), F32, here), ((total, width), BF, here)]
    outs += [((total, units), BF, wide) for _ in range(2)]
    outs += [((total, step), BF, rows_of(half, step, rows)) for _ in range(2)]
    return staged(tag, feed_kernel, ins, outs, before, feed_scratch(blocks, rows, width))


def feed_back(tag, half, sources, middle, own, got, norm_rows, gate, up, blocks, before):
    top = len(sources) == 1
    total, width = middle.shape
    rows = total // 2
    step = len(blocks) // 2 * blocks[0].shape[1]
    units = len(blocks) * blocks[0].shape[1]
    count = len(blocks)

    def feed_back_kernel(*refs):
        taken = len(sources)
        mid_ref, own_ref, got_ref, norm_ref, gate_ref, up_ref = refs[taken:taken + 6]
        block_refs = refs[taken + 6:taken + 6 + count]
        (part_ref, sums_ref, edge_ref, pre_ref, feed_ref, own_grads, other_grads,
         buffer, acc_ref, sems) = refs[taken + 6 + count:]
        fetch_blocks(block_refs, buffer, sems)
        summed = mid_ref[...] + own_ref[...].astype(F32) + got_ref[...].astype(F32)
        normed, inverse = row_norm(summed)
        if top:
            upstream = refs[0][...].astype(F32)
            edge_ref[...] = (normed * norm_ref[2:3] + norm_ref[3:4]).astype(BF)
        else:
            upstream = refs[0][...] + refs[1][...].astype(F32) + refs[2][...].astype(F32)
            edge_ref[...] = upstream.astype(BF)
        through, sums_ref[...] = row_norm_back(normed, inverse, norm_ref[2:3], upstream)
        pre_ref[...] = through
        low = through.astype(BF)
        feed_ref[...] = low
        for p in range(2):
            gate_w, up_w, down_w = share_blocks(p, block_refs, buffer, sems)
            at = slice(p * step, p * step + step)
            gate, up = gate_ref[:, at].astype(F32), up_ref[:, at].astype(F32)
            grad_hidden = nt(low, down_w)
            sigmoid = jax.nn.sigmoid(gate)
            grad_gate = (grad_hidden * up * sigmoid * (1.0 + gate * (1.0 - sigmoid))).astype(BF)
            grad_up = (grad_hidden * gate * sigmoid).astype(BF)
            share_ref = (own_grads, other_grads)[p]
            share_ref[:, :step] = grad_gate
            share_ref[:, step:] = grad_up
            back_through = nn(grad_gate, gate_w) + nn(grad_up, up_w)
            acc_ref[...] = back_through if p == 0 else acc_ref[...] + back_through
        part_ref[...] = acc_ref[...].astype(BF)

    plain = pl.BlockSpec((rows, width), lambda i: (0, 0))
    here = rows_of(half, width, rows)
    wide = rows_of(half, units, rows)
    ins = [(sources[0], here)] + [(source, plain) for source in sources[1:]]
    ins += [(middle, here), (own, plain), (got, plain), (norm_rows, whole(norm_rows))]
    ins += [(gate, wide), (up, wide)] + [(block, ANYWHERE) for block in blocks]
    outs = [((rows, width), BF, plain), ((8, width), F32, pl.BlockSpec((8, width), lambda i: (0, 0)))]
    outs += [((total, width), BF, here), ((total, width), F32, here), ((total, width), BF, here)]
    outs += [((total, units), BF, wide) for _ in range(2)]
    return staged(tag, feed_back_kernel, ins, outs, before, feed_scratch(blocks, rows, width))


def attend_back(tag, half, grad_middle, x, own, got, norm_rows, queries, key_vecs, values, totals,
                segment_column, segment_row, out_weight, cosine, sines, partial, before):
    total, heads = queries.shape
    width = out_weight.shape[1]
    rows = total // 2
    last = partial is not None

    def attend_back_kernel(*refs):
        (pre_ref, fed_ref, fed_got_ref, x_ref, own_ref, got_ref, norm_ref, q_ref, k_ref, v_ref,
         lse_ref, col_ref, row_ref, w_ref, cos_ref, sin_ref) = refs[:16]
        if last:
            dk_in, dv_in = refs[16:18]
        sums_ref, dk_ref, dv_ref, mid_ref, att_ref, dq_ref, dctx_ref = refs[18 if last else 16:]
        upstream = pre_ref[...] + fed_ref[...].astype(F32) + fed_got_ref[...].astype(F32)
        summed = x_ref[...] + own_ref[...].astype(F32) + got_ref[...].astype(F32)
        normed, inverse = row_norm(summed)
        through, sums_ref[...] = row_norm_back(normed, inverse, norm_ref[0:1], upstream)
        mid_ref[...] = through
        low = through.astype(BF)
        att_ref[...] = low
        dctx_ref[...] = nt(low, w_ref[...]).astype(BF)
        masks = head_masks(rows)
        wide_masks = head_masks(total)
        same = col_ref[:, :1] == row_ref[:1, :]
        scaling = HEAD_DIM ** (-0.5)
        here = pl.ds(half * rows, rows)
        cosine, sines = cos_ref[...], sin_ref[...]
        for slab in range(heads // 128):
            at = slice(128 * slab, 128 * slab + 128)
            q, k, v, grad_ctx = q_ref[:, at], k_ref[:, at], v_ref[:, at], dctx_ref[:, at]
            dq = jnp.zeros((rows, 128), F32)
            dk = jnp.zeros((total, 128), F32)
            dv = jnp.zeros((total, 128), F32)
            for h in range(2):
                mask = masks[h].astype(BF)
                scores = nt(k, q * mask) * scaling
                scores = jnp.where(same, scores, masked_value)
                chances = jnp.exp(scores - lse_ref[2 * slab + h:2 * slab + h + 1, :])
                grad_chances = nt(v, grad_ctx * mask)
                row_dot = jnp.sum(chances * grad_chances, axis=0, keepdims=True)
                grad_scores = (chances * (grad_chances - row_dot)).astype(BF)
                dv = dv + nn(chances.astype(BF), grad_ctx) * wide_masks[h]
                dk = dk + nn(grad_scores, q) * wide_masks[h]
                dq = dq + tn(grad_scores, k) * masks[h]
            dq_ref[:, at] = turned(dq * scaling, cos_ref[here, :], -sin_ref[here, :]).astype(BF)
            if last:
                dk = dk_in[:, at] + dk
                dv = dv_in[:, at] + dv
                dk_ref[:, at] = turned(dk * scaling, cosine, -sines).astype(BF)
                dv_ref[:, at] = dv.astype(BF)
            else:
                dk_ref[:, at] = dk
                dv_ref[:, at] = dv

    plain = pl.BlockSpec((rows, width), lambda i: (0, 0))
    here = rows_of(half, width, rows)
    ins = [(grad_middle[0], here), (grad_middle[1], plain), (grad_middle[2], plain)]
    ins += [(x, here), (own, plain), (got, plain), (norm_rows, whole(norm_rows))]
    ins += [(queries, rows_of(half, heads, rows)), (key_vecs, whole(key_vecs)),
            (values, whole(values)), (totals, pl.BlockSpec((8, rows), lambda i: (0, half))),
            (segment_column, whole(segment_column)),
            (segment_row, pl.BlockSpec((8, rows), lambda i: (0, half))),
            (out_weight, whole(out_weight)), (cosine, whole(cosine)), (sines, whole(sines))]
    if last:
        ins += [(part, whole(part)) for part in partial]
    kind = BF if last else F32
    all_rows = pl.BlockSpec((total, heads), lambda i: (0, 0))
    outs = [((8, width), F32, pl.BlockSpec((8, width), lambda i: (0, 0))),
            ((total, heads), kind, all_rows), ((total, heads), kind, all_rows),
            ((total, width), F32, here), ((total, width), BF, here),
            ((total, heads), BF, rows_of(half, heads, rows))]
    return staged(tag, attend_back_kernel, ins, outs, before, [pltpu.VMEM((rows, heads), BF)])


def inputs_back(tag, half, grads, weight):
    total, heads = grads[0].shape
    width = weight.shape[2]
    rows = total // 2

    def inputs_back_kernel(dq_ref, dk_ref, dv_ref, w_ref, part_ref):
        acc = nn(dq_ref[...], w_ref[0]) + nn(dk_ref[...], w_ref[1]) + nn(dv_ref[...], w_ref[2])
        part_ref[...] = acc.astype(BF)

    ins = [(grad, rows_of(half, heads, rows)) for grad in grads] + [(weight, whole(weight))]
    outs = [((rows, width), BF, pl.BlockSpec((rows, width), lambda i: (0, 0)))]
    return staged(tag, inputs_back_kernel, ins, outs, None)[0]


def across(part, tag):
    with jax.named_scope("x_" + tag):
        return flip(part, TENSOR, 1)


def tied(value, *others):
    return lax.optimization_barrier((value, *others))[0]


def weight_grad(left, right, tag):
    with jax.named_scope("w_" + tag):
        return jnp.einsum("th,td->hd", left, right, preferred_element_type=F32).astype(BF)


def attention_forward(tag, sources, weights, norm_before, tables, wait=()):
    in_weight, out_weight = weights[:2]
    segment_column, segment_row, cosine, sines = tables
    projected = None
    for half in range(2):
        projected = project(f"p{tag}{half}", half, sources[half], norm_before, in_weight, cosine, sines, projected)
    queries, key_vecs, values = projected[:3]
    if len(projected) == 5:
        x, low = projected[3:]
    else:
        low = sources[0][0]
        x = low.astype(F32)
    kept = None
    attended = []
    for half in range(2):
        taken = tied(queries, *wait) if half == 1 else queries
        part, *kept = attend(f"t{tag}{half}", half, taken, key_vecs, values, segment_column, segment_row,
                             out_weight, kept)
        attended.append((part, across(part, f"t{tag}{half}")))
    context, totals = kept
    return (x, low, queries, key_vecs, values, context, totals), attended


def feed_forward(tag, halves, weights, norm_rows, first_wait, second_wait):
    before, attended = halves
    blocks = weights[2]
    x = before[0]
    saved = None
    fed = []
    for half in range(2):
        taken = tied(x, *(second_wait if half else first_wait))
        part, *saved = feed(f"f{tag}{half}", half, taken, *attended[half], norm_rows, blocks, saved)
        fed.append((part, across(part, f"f{tag}{half}")))
    middle, spread, gate, up, *hidden = saved
    ends = [(middle, *fed[half]) for half in range(2)]
    return ends, (*before, attended, middle, spread, gate, up, hidden, fed)


def layer_backward(tag, sources, weights, norm_rows, tables, kept, pull_units, pull_heads, waits):
    in_weight, out_weight, blocks = weights
    segment_column, segment_row, cosine, sines = tables
    (x, low, queries, key_vecs, values, context, totals, attended, middle, spread,
     gate, up, hidden, fed) = kept
    saved = None
    through = []
    sums = []
    for half in range(2):
        part, total, *saved = feed_back(f"g{tag}{half}", half, sources[half], middle, *fed[half], norm_rows,
                                        gate, up, blocks, saved)
        through.append((part, across(part, f"g{tag}{half}")))
        sums.append(total)
    edge, grad_pre_output, grad_feed, *grad_shares = saved
    down = [weight_grad(hidden[i], grad_feed, f"d{tag}{i}") for i in (1, 0)]
    gate_up = [weight_grad(grad_shares[i], spread, f"u{tag}{i}") for i in (1, 0)]
    down, gate_up = down[::-1], gate_up[::-1]
    units = pull_units(tag, gate_up, down)
    partial = None
    saved = None
    first_sums = []
    for half in range(2):
        wait = waits if half == 0 else units[:2]
        total, dk, dv, *saved = attend_back(
            f"h{tag}{half}", half, (tied(grad_pre_output, *wait), *through[half]), x, *attended[half], norm_rows,
            queries, key_vecs, values, totals, segment_column, segment_row,
            out_weight, cosine, sines, partial, saved)
        partial = (dk, dv)
        first_sums.append(total)
    grad_pre_middle, grad_attended, dq = saved
    ends = []
    for half in range(2):
        part = inputs_back(f"i{tag}{half}", half, (dq, dk, dv), in_weight)
        ends.append((grad_pre_middle, part, across(part, f"i{tag}{half}")))
    grad_in = [weight_grad(grad, low, f"n{tag}") for grad in (dq, dk, dv)]
    grad_out = weight_grad(context, grad_attended, f"o{tag}")
    heads = pull_heads(tag, grad_in, grad_out)
    first = first_sums[0] + first_sums[1]
    second = sums[0] + sums[1]
    norm_grad = jnp.concatenate([first[:2], second[:2]], axis=0)
    return ends, edge, units, heads, norm_grad


MESH = pl.DeviceIdType.MESH


def forward_all(layer_inputs, cotangent, heads_in, units_in, norm_in, tables):
    segment_column, segment_row, cosine, sines = tables
    ring = lax.axis_size(FSDP)
    count, own_rows, width = layer_inputs.shape
    total = count * own_rows
    rows = total // 2
    head_rows = heads_in.shape[1]
    half_units = units_in.shape[2]
    heads = 2 * ring * head_rows
    step = 2 * ring * half_units
    order = sorted(range(1, ring), key=lambda k: min(k, ring - k))

    saved = {}
    for l in range(2):
        saved.update({
            f"q{l}": ((total, heads), BF), f"k{l}": ((total, heads), BF),
            f"v{l}": ((total, heads), BF), f"ctx{l}": ((total, heads), BF),
            f"lse{l}": ((8, total), F32), f"pre1{l}": ((total, width), F32),
            f"pre2{l}": ((total, width), F32),
            f"spread{l}": ((total, width), BF), f"feed{l}": ((3, total, 2 * step), BF),
        })
    saved.update({"low0": ((total, width), BF), "acts": ((2, total, width), BF),
                  "cot": ((total, width), BF)})
    inner = {"x1": ((total, width), F32), "mid": ((total, width), F32)}
    for l in range(2):
        for h in range(2):
            for stage in "tf":
                inner[f"own_{stage}{l}{h}"] = ((rows, width), BF)
                inner[f"got_{stage}{l}{h}"] = ((rows, width), BF)
    weights = {}
    for l in range(2):
        weights[f"heads{l}"] = ((4, 2, ring * head_rows, width), BF)
        weights[f"units{l}"] = ((3, 2, 2, ring * half_units, width), BF)
    outs = {**saved, **weights, "norms": ((2, 4, width), F32)}
    held = {**saved, **inner}
    stages = [f"{stage}{l}{h}" for l in range(2) for stage in "tf" for h in range(2)]

    def forward_kernel(inp, cot_ref, heads_ref, units_ref, norm_ref, col_ref, row_ref, cos_ref, sin_ref,
                       *refs):
        out = dict(zip(outs, refs[:len(outs)]))
        rest = refs[len(outs):]
        keep = dict(zip(held, rest[:len(held)]))
        (hbuf, ubuf, nbuf, acc_ref, z_s, z_r, y_s, y_r, k_s, k_r, e_s, e_r, x_s, x_r, i_s, i_r,
         l_s, f_s) = rest[len(held):]
        core = lax.axis_index(PIPE)
        place = lax.axis_index(TENSOR)
        group = lax.axis_index(FSDP)
        other = 1 - core
        item = (place // 2) * 2 + core

        def peer(k):
            low, high = place % 2, place // 2
            low = 1 - low if k & 1 else low
            high = 1 - high if k & 2 else high
            return high * 2 + low

        def near(k):
            return lax.rem(group + k, ring)

        sent = []
        conditional = []

        def send(src, dst, send_sem, recv_sem, **to):
            copy = pltpu.make_async_remote_copy(
                src_ref=src, dst_ref=dst, send_sem=send_sem, recv_sem=recv_sem,
                device_id=to, device_id_type=MESH)
            copy.start()
            sent.append(copy)

        def arrived(dst, send_sem, recv_sem, **to):
            pltpu.make_async_remote_copy(
                src_ref=dst, dst_ref=dst, send_sem=send_sem, recv_sem=recv_sem,
                device_id=to, device_id_type=MESH).wait_recv()

        flushes = []
        done = set()

        def flush(src, name):
            done.add(name)
            copy = pltpu.make_async_copy(src, out[name], f_s.at[len(flushes)])
            copy.start()
            flushes.append(copy)

        def slot(piece, share, col, g):
            l, kind = piece // 2, piece % 2
            if kind == 0:
                at = pl.ds(pl.multiple_of(g * head_rows, 16), head_rows)
                return hbuf.at[l, pl.ds(2 * share, 2), col, at]
            at = pl.ds(pl.multiple_of(g * half_units, 16), half_units)
            return ubuf.at[l, :, share, col, at]

        barrier = pltpu.get_barrier_semaphore()
        peers = [dict(tensor=peer(k)) for k in (1, 2, 3)] + [dict(pipe=other)]
        peers += [dict(fsdp=near(k)) for k in range(1, ring)]
        for to in peers:
            pl.semaphore_signal(barrier, inc=1, device_id=to, device_id_type=MESH)
        pl.semaphore_wait(barrier, len(peers))

        mine = pl.ds(pl.multiple_of(group * head_rows, 16), head_rows)
        mine_units = pl.ds(pl.multiple_of(group * half_units, 16), half_units)
        local = [
            pltpu.make_async_copy(heads_ref.at[pl.ds(2 * core, 2)],
                                  hbuf.at[core, pl.ds(2 * core, 2), 0, mine], l_s.at[0]),
            pltpu.make_async_copy(units_ref.at[:, core],
                                  ubuf.at[core, :, core, 0, mine_units], l_s.at[1]),
            pltpu.make_async_copy(inp.at[item],
                                  keep["low0"].at[pl.ds(pl.multiple_of(place * own_rows, 16),
                                                        own_rows)], l_s.at[2]),
            pltpu.make_async_copy(norm_ref, nbuf.at[core], l_s.at[3]),
            pltpu.make_async_copy(cot_ref.at[item],
                                  keep["cot"].at[pl.ds(pl.multiple_of(place * own_rows, 16),
                                                       own_rows)], l_s.at[4]),
        ]
        send(heads_ref.at[pl.ds(2 * other, 2)], hbuf.at[core, pl.ds(2 * other, 2), 0, mine],
             e_s.at[0], e_r.at[0], pipe=other)
        for copy in local:
            copy.start()
        send(units_ref.at[:, other], ubuf.at[core, :, other, 0, mine_units],
             e_s.at[1], e_r.at[1], pipe=other)
        send(norm_ref, nbuf.at[core], e_s.at[2], e_r.at[2], pipe=other)
        for k in (1, 2):
            send(inp.at[(peer(k) // 2) * 2 + core],
                 keep["low0"].at[pl.ds(pl.multiple_of(place * own_rows, 16), own_rows)],
                 i_s.at[k], i_r.at[k], tensor=peer(k))

        reach = [(sign, d) for d in range(1, ring) for sign in (1, -1)]

        def number(sign, d):
            return d if sign > 0 else ring - 1 + d

        def exists(sign, d):
            return group + d < ring if sign > 0 else group >= d

        def when(condition, action):
            @pl.when(condition)
            def _():
                action().start()

            conditional.append((condition, action))

        def hop_on(piece, sign, d):
            here = slot(piece, core, 0, group + sign * d)
            onward = group >= 1 if sign > 0 else group + 1 < ring
            index = number(sign, d)

            def action():
                return pltpu.make_async_remote_copy(
                    src_ref=here, dst_ref=here, send_sem=z_s.at[piece, index],
                    recv_sem=z_r.at[piece, number(sign, d + 1)],
                    device_id={FSDP: group - sign}, device_id_type=MESH)

            return onward, action

        def own_along(piece):
            for sign in (1, -1):
                here = slot(piece, core, 0, group)
                onward = group >= 1 if sign > 0 else group + 1 < ring

                def action(sign=sign):
                    return pltpu.make_async_remote_copy(
                        src_ref=here, dst_ref=here,
                        send_sem=z_s.at[piece, 0 if sign > 0 else 2 * ring - 1],
                        recv_sem=z_r.at[piece, number(sign, 1)],
                        device_id={FSDP: group - sign}, device_id_type=MESH)

                when(onward, action)

        def across(piece, g, index):
            here = slot(piece, core, 0, g)
            to_side = pltpu.make_async_remote_copy(
                src_ref=here, dst_ref=slot(piece, core, 1, g), send_sem=y_s.at[piece, index],
                recv_sem=y_r.at[piece, index], device_id={TENSOR: peer(2)}, device_id_type=MESH)
            to_core = pltpu.make_async_remote_copy(
                src_ref=here, dst_ref=here, send_sem=k_s.at[piece, 0, index],
                recv_sem=k_r.at[piece, 0, index], device_id={PIPE: other}, device_id_type=MESH)
            return to_side, to_core

        def own_across(piece):
            for copy in across(piece, group, 0):
                copy.start()
                sent.append(copy)

        def hop(piece, d):
            for sign in (1, -1):
                index = number(sign, d)
                g = group + sign * d
                condition = exists(sign, d)

                @pl.when(condition)
                def _():
                    arrived(slot(piece, core, 0, g), z_s.at[piece, index], z_r.at[piece, index],
                            fsdp=group + sign)
                    for copy in across(piece, g, index):
                        copy.start()

                if d + 1 < ring:
                    onward, action = hop_on(piece, sign, d)
                    when(jnp.logical_and(condition, onward), action)
                for i in range(2):
                    conditional.append(
                        (condition, lambda i=i, g=g, index=index: across(piece, g, index)[i]))

        def own_second(piece):
            here = slot(piece, core, 1, group)
            arrived(here, y_s.at[piece, 0], y_r.at[piece, 0], tensor=peer(2))
            send(here, here, k_s.at[piece, 1, 0], k_r.at[piece, 1, 0], pipe=other)

        def second(piece, d):
            for sign in (1, -1):
                index = number(sign, d)
                here = slot(piece, core, 1, group + sign * d)
                condition = exists(sign, d)

                def action(here=here, index=index):
                    return pltpu.make_async_remote_copy(
                        src_ref=here, dst_ref=here, send_sem=k_s.at[piece, 1, index],
                        recv_sem=k_r.at[piece, 1, index], device_id={PIPE: other},
                        device_id_type=MESH)

                @pl.when(condition)
                def _():
                    arrived(here, y_s.at[piece, index], y_r.at[piece, index], tensor=peer(2))

                when(condition, action)

        def pass_second(piece):
            own_second(piece)
            for d in range(1, ring):
                second(piece, d)

        def complete(piece):
            for col in range(2):
                arrived(slot(piece, other, col, group), k_s.at[piece, col, 0],
                        k_r.at[piece, col, 0], pipe=other)
                for sign, d in reach:
                    index = number(sign, d)

                    @pl.when(exists(sign, d))
                    def _():
                        arrived(slot(piece, other, col, group + sign * d),
                                k_s.at[piece, col, index], k_r.at[piece, col, index], pipe=other)
            l = piece // 2
            if piece % 2 == 0:
                flush(hbuf.at[l], f"heads{l}")
            else:
                flush(ubuf.at[l], f"units{l}")

        local[0].wait()
        arrived(hbuf.at[other, pl.ds(2 * core, 2), 0, mine],
                e_s.at[0], e_r.at[0], pipe=other)
        own_along(0)
        own_across(0)
        local[1].wait()
        arrived(ubuf.at[other, :, core, 0, mine_units], e_s.at[1], e_r.at[1], pipe=other)

        def part_of(name, l):
            return nbuf[l, name:name + 1, :]

        def exchange(tag):
            index = stages.index(tag)
            send(keep["own_" + tag], keep["got_" + tag], x_s.at[index], x_r.at[index],
                 tensor=peer(1))

        def taken(tag):
            index = stages.index(tag)
            arrived(keep["got_" + tag], x_s.at[index], x_r.at[index], tensor=peer(1))
            return keep["own_" + tag][...].astype(F32) + keep["got_" + tag][...].astype(F32)

        def do_project(l, half):
            at_rows = slice(half * rows, half * rows + rows)
            if l == 0:
                low = keep["low0"][at_rows]
            else:
                summed = keep["mid"][at_rows] + taken(f"f0{half}")
                keep["pre20"][at_rows] = summed
                x = row_norm(summed)[0] * part_of(2, 0) + part_of(3, 0)
                keep["x1"][at_rows] = x
                low = x.astype(BF)
                keep["acts"][0, at_rows] = low
            cosine, sines = cos_ref[at_rows], sin_ref[at_rows]
            for c, name in ((0, "q"), (1, "k")):
                turning = nt(low, hbuf[l, c].reshape(heads, width))
                for slab in range(heads // 128):
                    at = slice(128 * slab, 128 * slab + 128)
                    keep[f"{name}{l}"][at_rows, at] = turned(
                        turning[:, at], cosine, sines).astype(BF)
            keep[f"v{l}"][at_rows] = nt(low, hbuf[l, 2].reshape(heads, width)).astype(BF)

        def do_attend(l, half):
            at_rows = slice(half * rows, half * rows + rows)
            masks = head_masks(rows)
            lane = lax.broadcasted_iota(jnp.int32, (rows, 128), 1)
            same = col_ref[at_rows, :1] == row_ref[:1, :]
            totals = jnp.zeros((rows, 128), F32)
            for slab in range(heads // 128):
                at = slice(128 * slab, 128 * slab + 128)
                q, k, v = keep[f"q{l}"][at_rows, at], keep[f"k{l}"][:, at], keep[f"v{l}"][:, at]
                gathered = jnp.zeros((rows, 128), F32)
                for h in range(2):
                    scores = nt(q * masks[h].astype(BF), k) * HEAD_DIM ** (-0.5)
                    scores = jnp.where(same, scores, masked_value)
                    top = jnp.max(scores, axis=-1, keepdims=True)
                    powers = jnp.exp(scores - top)
                    mass = jnp.sum(powers, axis=-1, keepdims=True)
                    chances = (powers * (1.0 / mass)).astype(BF)
                    gathered = gathered + nn(chances, v) * masks[h]
                    totals = jnp.where(lane == 2 * slab + h, top + jnp.log(mass), totals)
                keep[f"ctx{l}"][at_rows, at] = gathered.astype(BF)
            keep[f"lse{l}"][:, at_rows] = totals.T[:8]
            part = nn(keep[f"ctx{l}"][at_rows], hbuf[l, 3].reshape(heads, width))
            keep[f"own_t{l}{half}"][...] = part.astype(BF)
            exchange(f"t{l}{half}")

        def do_feed(l, half):
            at_rows = slice(half * rows, half * rows + rows)
            x = keep["low0"][at_rows].astype(F32) if l == 0 else keep["x1"][at_rows]
            summed = x + taken(f"t{l}{half}")
            keep[f"pre1{l}"][at_rows] = summed
            middle = row_norm(summed)[0] * part_of(0, l) + part_of(1, l)
            keep["mid"][at_rows] = middle
            low = middle.astype(BF)
            keep[f"spread{l}"][at_rows] = low
            for turn, share in enumerate((core, other)):
                if turn == 1 and half == 0:
                    complete(2 * l + 1)
                at = pl.ds(pl.multiple_of(share * step, 128), step)
                gate = nt(low, ubuf[l, 0, share].reshape(step, width))
                up = nt(low, ubuf[l, 1, share].reshape(step, width))
                keep[f"feed{l}"][0, at_rows, at] = gate.astype(BF)
                keep[f"feed{l}"][1, at_rows, at] = up.astype(BF)
                hidden = (gate * jax.nn.sigmoid(gate) * up).astype(BF)
                keep[f"feed{l}"][2, at_rows, at] = hidden
                fed = nn(hidden, ubuf[l, 2, share].reshape(step, width))
                if turn == 0:
                    acc_ref[...] = fed
                else:
                    keep[f"own_f{l}{half}"][...] = (acc_ref[...] + fed).astype(BF)
            exchange(f"f{l}{half}")

        hop(0, 1)

        def input_rows(k):
            return keep["low0"].at[pl.ds(pl.multiple_of(peer(k) * own_rows, 16), own_rows)]

        for d in range(2, ring):
            if d == 3:
                arrived(input_rows(2), i_s.at[2], i_r.at[2], tensor=peer(2))
                send(input_rows(2), input_rows(2), i_s.at[3], i_r.at[3], tensor=peer(1))
                own_along(1)
                own_across(1)
            hop(0, d)
        if ring < 4:
            own_along(1)
            own_across(1)
        pass_second(0)
        for k in (1, 3):
            arrived(input_rows(k), i_s.at[k], i_r.at[k], tensor=peer(1))
        local[2].wait()
        local[3].wait()
        arrived(nbuf.at[other], e_s.at[2], e_r.at[2], pipe=other)
        complete(0)
        do_project(0, 0)
        do_project(0, 1)
        hop(1, 1)
        own_along(2)
        do_attend(0, 0)
        do_attend(0, 1)
        hop(1, 2)
        own_across(2)
        hop(2, 1)
        own_along(3)
        for d in range(3, ring):
            hop(1, d)
        for d in range(2, ring):
            hop(2, d)
        own_across(3)
        pass_second(1)
        do_feed(0, 0)
        hop(3, 1)
        do_feed(0, 1)
        hop(3, 2)
        pass_second(2)
        complete(2)
        do_project(1, 0)
        do_project(1, 1)
        for d in range(3, ring):
            hop(3, d)
        do_attend(1, 0)
        do_attend(1, 1)
        for k in range(1, count):
            send(cot_ref.at[(peer(k) // 2) * 2 + core],
                 keep["cot"].at[pl.ds(pl.multiple_of(place * own_rows, 16), own_rows)],
                 i_s.at[count + k], i_r.at[count + k], tensor=peer(k))
        pass_second(3)
        do_feed(1, 0)
        do_feed(1, 1)
        flush(nbuf, "norms")
        for name in saved:
            if name not in done and name not in ("pre21", "acts", "cot"):
                flush(keep[name], name)
        local[4].wait()
        for k in range(1, count):
            arrived(keep["cot"].at[pl.ds(pl.multiple_of(peer(k) * own_rows, 16), own_rows)],
                    i_s.at[count + k], i_r.at[count + k], tensor=peer(k))
        for half in range(2):
            at_rows = slice(half * rows, half * rows + rows)
            summed = keep["mid"][at_rows] + taken(f"f1{half}")
            keep["pre21"][at_rows] = summed
            keep["acts"][1, at_rows] = (
                row_norm(summed)[0] * part_of(2, 1) + part_of(3, 1)).astype(BF)
        for name in saved:
            if name not in done:
                flush(keep[name], name)
        for copy in sent:
            copy.wait_send()
        for condition, action in conditional:
            @pl.when(condition)
            def _():
                action().wait_send()

        for copy in flushes:
            copy.wait()

    anywhere = pl.BlockSpec(memory_space=pl.ANY)
    inside = pl.BlockSpec(memory_space=pltpu.VMEM)
    dma = pltpu.SemaphoreType.DMA
    scratch = [pltpu.VMEM(shape, kind) for shape, kind in held.values()]
    scratch += [
        pltpu.VMEM((2, 4, 2, ring * head_rows, width), BF),
        pltpu.VMEM((2, 3, 2, 2, ring * half_units, width), BF),
        pltpu.VMEM((2, 4, width), F32),
        pltpu.VMEM((rows, width), F32),
        dma((4, 2 * ring)), dma((4, 2 * ring)), dma((4, 2 * ring)), dma((4, 2 * ring)),
        dma((4, 2, 2 * ring)), dma((4, 2, 2 * ring)), dma((3,)), dma((3,)),
        dma((len(stages),)), dma((len(stages),)), dma((2 * count,)), dma((2 * count,)),
        dma((5,)), dma((len(outs),)),
    ]
    results = pl.pallas_call(
        forward_kernel,
        in_specs=[anywhere] * 4 + [inside] * 5,
        out_specs=[anywhere] * len(outs),
        out_shape=[jax.ShapeDtypeStruct(shape, kind) for shape, kind in outs.values()],
        scratch_shapes=scratch,
        compiler_params=pltpu.CompilerParams(
            collective_id=0, has_side_effects=True, vmem_limit_bytes=62 << 20),
        name="forward_kernel",
    )(layer_inputs, cotangent, heads_in, units_in, norm_in, segment_column, segment_row, cosine, sines)
    return dict(zip(outs, results))


def backward_all(saved, count, tables):
    segment_column, segment_row, cosine, sines = tables
    ring = lax.axis_size(FSDP)
    total, width = saved["cot"].shape
    own_rows = total // count
    rows = total // 2
    heads = saved["q0"].shape[1]
    step = saved["feed0"].shape[2] // 2
    head_rows = heads // (2 * ring)
    half_units = step // (2 * ring)
    order = sorted(range(1, ring), key=lambda k: min(k, ring - k))
    loaded = ("q", "k", "v", "lse", "pre1", "pre2", "spread", "feed", "heads", "units")
    arrays = [saved[f"{name}{l}"] for l in range(2) for name in loaded]
    arrays += [saved["ctx0"], saved["ctx1"], saved["low0"], saved["acts"], saved["cot"]]
    stages = [f"{stage}{l}{h}" for l in range(2) for stage in "gi" for h in range(2)]
    pieces = "dguhe"
    scaling = HEAD_DIM ** (-0.5)

    def backward_kernel(norm_ref, col_ref, row_ref, cos_ref, sin_ref, *refs):
        n = len(arrays)
        from_hbm = {}
        for l in range(2):
            for i, name in enumerate(loaded):
                from_hbm[f"{name}{l}"] = refs[l * len(loaded) + i]
        from_hbm["ctx0"], from_hbm["ctx1"], from_hbm["low0"], acts_ref, cot_ref = refs[n - 5:n]
        from_hbm["low1"] = acts_ref.at[0]
        (act_out, grad_out, units_out, heads_out, norm_out) = refs[n:n + 5]
        rest = refs[n + 5:]
        buffers = [name for name in loaded if name != "spread"]
        here = dict(zip(buffers, rest[:len(buffers)]))
        (lefts, rights, dpre, wide_rights, dctx, grads, own, got, nsum, nred, nget,
         acc, keep_u, keep_h, give_u, give_h, core_u, core_h, side_u, side_h, line_u, line_h,
         fin_u, fin_h, x_s, x_r, a_s, a_r, b_s, b_r, c_s, c_r, y_s, y_r, z_s, z_r,
         n_s, n_r, j_s, j_r, l_s, m_s, credit_c, credit_y) = rest[len(buffers):]
        dfeed = wide_rights.at[1]
        cot = grads.at[0]
        core = lax.axis_index(PIPE)
        place = lax.axis_index(TENSOR)
        group = lax.axis_index(FSDP)
        other = 1 - core
        item = (place // 2) * 2 + core

        def peer(k):
            low, high = place % 2, place // 2
            low = 1 - low if k & 1 else low
            high = 1 - high if k & 2 else high
            return high * 2 + low

        def near(k):
            return lax.rem(group + k, ring)

        pending = []

        def send(src, dst, send_sem, recv_sem, **to):
            copy = pltpu.make_async_remote_copy(
                src_ref=src, dst_ref=dst, send_sem=send_sem, recv_sem=recv_sem,
                device_id=to, device_id_type=MESH)
            copy.start()
            pending.append(copy)
            return copy

        def arrived(dst, send_sem, recv_sem, **to):
            pltpu.make_async_remote_copy(
                src_ref=dst, dst_ref=dst, send_sem=send_sem, recv_sem=recv_sem,
                device_id=to, device_id_type=MESH).wait_recv()

        def sent(copy):
            copy.wait_send()
            pending[:] = [held for held in pending if held is not copy]

        names = loaded + ("ctx", "low")
        loads = {}

        def load(l, *which):
            for name in which:
                to = {"ctx": lefts.at[3], "low": rights.at[0],
                      "spread": wide_rights.at[0]}.get(name)
                to = here[name] if to is None else to
                copy = pltpu.make_async_copy(from_hbm[f"{name}{l}"], to,
                                             l_s.at[l * len(names) + names.index(name)])
                copy.start()
                loads[name, l] = copy

        def ready(l, *which):
            for name in which:
                loads.pop((name, l)).wait()

        def rows_at(index):
            return pl.ds(pl.multiple_of(index * own_rows, 16), own_rows)

        barrier = pltpu.get_barrier_semaphore()
        peers = [dict(tensor=peer(k)) for k in (1, 2, 3)]
        peers += [dict(pipe=other), dict(pipe=other, tensor=peer(2))]
        peers += [dict(fsdp=near(k)) for k in range(1, ring)]
        for to in peers:
            pl.semaphore_signal(barrier, inc=1, device_id=to, device_id_type=MESH)
        pl.semaphore_wait(barrier, len(peers))

        own_cot = pltpu.make_async_copy(cot_ref, cot, m_s.at[0])
        own_cot.start()
        load(1, "pre2", "feed", "spread", "units", "pre1", "heads", "q", "k", "v", "lse", "ctx",
             "low")

        def home(source, result, sems, index):
            copy = pltpu.make_async_copy(source.at[core, rows_at(place)], result.at[item],
                                         m_s.at[index])
            copy.start()
            for k in range(1, 4):
                layer = other if k & 1 else core
                to = dict(pipe=layer, tensor=peer(k & 2))
                send(source.at[layer, rows_at(peer(k & 2))], result.at[item],
                     sems[0].at[k], sems[1].at[k], **to)
            return copy

        def home_arrived(result, sems):
            for k in range(1, 4):
                to = dict(pipe=other if k & 1 else core, tensor=peer(k & 2))
                index = (peer(k & 2) // 2) * 2 + (other if k & 1 else core)
                arrived(result.at[index], sems[0].at[k], sems[1].at[k], **to)

        own_act = home(acts_ref, act_out, (a_s, a_r), 1)
        own_cot.wait()
        last_use = {}

        def exchange(tag, value):
            place_of = "gi".index(tag[0]) * 2 + int(tag[2])
            if place_of in last_use:
                sent(last_use[place_of])
            own[place_of] = value
            index = stages.index(tag)
            last_use[place_of] = send(own.at[place_of], got.at[index], x_s.at[index],
                                      x_r.at[index], tensor=peer(1))

        def taken(tag):
            index = stages.index(tag)
            place_of = "gi".index(tag[0]) * 2 + int(tag[2])
            arrived(got.at[index], x_s.at[index], x_r.at[index], tensor=peer(1))
            return own[place_of].astype(F32) + got[index].astype(F32)

        def part_of(name, l):
            return norm_ref[l, name:name + 1, :]

        def note_sums(l, half, first, sums):
            if half == 0:
                nsum[l, first:first + 2] = sums[:2]
            else:
                nsum[l, first:first + 2] = nsum[l, first:first + 2] + sums[:2]

        def do_norm_back(l, half):
            at_rows = slice(half * rows, half * rows + rows)
            if l == 1:
                upstream = cot[at_rows].astype(F32)
            else:
                upstream = dpre[at_rows] + taken(f"i1{half}")
                grads[1, at_rows] = upstream.astype(BF)
            if half == 0:
                ready(l, "pre2")
            normed, inverse = row_norm(here["pre2"][at_rows])
            through, sums = row_norm_back(normed, inverse, part_of(2, l), upstream)
            note_sums(l, half, 2, sums)
            dpre[at_rows] = through
            dfeed[at_rows] = through.astype(BF)

        def do_feed_back(l, half):
            at_rows = slice(half * rows, half * rows + rows)
            low = dfeed[at_rows]
            if half == 0:
                ready(l, "units")
            units, feed_ref = here["units"], here["feed"]
            for share in range(2):
                at = slice(share * step, share * step + step)
                gate = feed_ref[0, at_rows, at].astype(F32)
                up = feed_ref[1, at_rows, at].astype(F32)
                grad_hidden = nt(low, units[2, share].reshape(step, width))
                sigmoid = jax.nn.sigmoid(gate)
                grad_gate = (
                    grad_hidden * up * sigmoid * (1.0 + gate * (1.0 - sigmoid))).astype(BF)
                grad_up = (grad_hidden * gate * sigmoid).astype(BF)
                feed_ref[0, at_rows, at] = grad_gate
                feed_ref[1, at_rows, at] = grad_up
                back = nn(grad_gate, units[0, share].reshape(step, width))
                back = back + nn(grad_up, units[1, share].reshape(step, width))
                if share == 0:
                    acc[...] = back
                else:
                    exchange(f"g{l}{half}", (acc[...] + back).astype(BF))

        def unit_grads(first, end, share, target):
            size = step // 2

            def one(i, _):
                c, col = i // 2, i % 2
                at = pl.ds(pl.multiple_of(share * step + col * size, 128), size)
                target[c, col] = tn(here["feed"][c, :, at], wide_rights[c // 2]).astype(BF)
                return 0

            lax.fori_loop(2 * first, 2 * end, one, 0)

        def head_grad(share, i, target):
            j = 2 * share + i
            full = tn(lefts[j], rights[j // 3]).astype(BF)
            for col in range(2):
                target[i, col] = full[col * (heads // 2):(col + 1) * (heads // 2)]

        def do_attend_back(l, half):
            at_rows = slice(half * rows, half * rows + rows)
            if half == 0:
                ready(l, "pre1", "heads", "q", "k", "v", "lse")
            upstream = dpre[at_rows] + taken(f"g{l}{half}")
            normed, inverse = row_norm(here["pre1"][at_rows])
            through, sums = row_norm_back(normed, inverse, part_of(0, l), upstream)
            note_sums(l, half, 0, sums)
            dpre[at_rows] = through
            low = through.astype(BF)
            rights[1, at_rows] = low
            dctx[...] = nt(low, here["heads"][3].reshape(heads, width)).astype(BF)
            masks = head_masks(rows)
            wide_masks = head_masks(total)
            same = col_ref[:, :1] == row_ref[:1, at_rows]
            for slab in range(heads // 128):
                at = slice(slab * 128, slab * 128 + 128)
                second_at = slice(heads + slab * 128, heads + slab * 128 + 128)
                q, k = here["q"][at_rows, at], here["k"][:, at]
                v, grad_ctx = here["v"][:, at], dctx[:, at]
                dq = jnp.zeros((rows, 128), F32)
                dk = jnp.zeros((total, 128), F32)
                dv = jnp.zeros((total, 128), F32)
                for h in range(2):
                    mask = masks[h].astype(BF)
                    scores = nt(k, q * mask) * scaling
                    scores = jnp.where(same, scores, masked_value)
                    lse = here["lse"][2 * slab + h:2 * slab + h + 1, at_rows]
                    chances = jnp.exp(scores - lse)
                    grad_chances = nt(v, grad_ctx * mask)
                    row_dot = jnp.sum(chances * grad_chances, axis=0, keepdims=True)
                    grad_scores = (chances * (grad_chances - row_dot)).astype(BF)
                    dv = dv + nn(chances.astype(BF), grad_ctx) * wide_masks[h]
                    dk = dk + nn(grad_scores, q) * wide_masks[h]
                    dq = dq + tn(grad_scores, k) * masks[h]
                lefts[0, at_rows, at] = turned(
                    dq * scaling, cos_ref[at_rows], -sin_ref[at_rows]).astype(BF)
                if half == 0:
                    here["pre2"][:, at] = dk
                    here["pre2"][:, second_at] = dv
                else:
                    dk = here["pre2"][:, at] + dk
                    dv = here["pre2"][:, second_at] + dv
                    lefts[1, :, at] = turned(dk * scaling, cos_ref[...], -sin_ref[...]).astype(BF)
                    lefts[2, :, at] = dv.astype(BF)

        def do_inputs_back(l, half):
            at_rows = slice(half * rows, half * rows + rows)
            back = jnp.zeros((rows, width), F32)
            for c in range(3):
                back = back + nn(lefts[c, at_rows], here["heads"][c].reshape(heads, width))
            exchange(f"i{l}{half}", back.astype(BF))

        def parts(piece, units_ref, heads_ref):
            index = pieces.index(piece)
            if index > 2:
                return heads_ref.at[index - 3:index - 2]
            return units_ref.at[(2, 0, 1)[index]:(3, 1, 2)[index]]

        def cell(piece, l):
            return l * 5 + pieces.index(piece)

        gave = {}

        def give(l, piece):
            if l == 0:
                pl.semaphore_wait(credit_c.at[pieces.index(piece)], 1)
            index = cell(piece, l)
            gave[piece] = send(parts(piece, give_u, give_h), parts(piece, core_u, core_h),
                               c_s.at[index], c_r.at[index], pipe=other)

        def add_core(l, piece):
            index = cell(piece, l)
            come = parts(piece, core_u, core_h)
            arrived(come, c_s.at[index], c_r.at[index], pipe=other)
            mine = parts(piece, keep_u.at[l], keep_h.at[l])
            mine[...] = (mine[...].astype(F32) + come[...].astype(F32)).astype(BF)
            if l == 1:
                pl.semaphore_signal(credit_c.at[pieces.index(piece)], inc=1,
                                    device_id=dict(pipe=other), device_id_type=MESH)
            else:
                pl.semaphore_wait(credit_y.at[pieces.index(piece)], 1)
            send(mine.at[:, 1], parts(piece, side_u, side_h), y_s.at[index], y_r.at[index],
                 tensor=peer(2))

        def slot_of(piece, ref, g):
            size = head_rows if piece in "he" else half_units
            return ref.at[:, pl.ds(pl.multiple_of(g * size, 16), size)]

        def add_side(l, piece):
            index = cell(piece, l)
            come = parts(piece, side_u, side_h)
            arrived(come, y_s.at[index], y_r.at[index], tensor=peer(2))
            mine = parts(piece, keep_u.at[l], keep_h.at[l]).at[:, 0]
            mine[...] = (mine[...].astype(F32) + come[...].astype(F32)).astype(BF)
            if l == 1:
                pl.semaphore_signal(credit_y.at[pieces.index(piece)], inc=1,
                                    device_id=dict(tensor=peer(2)), device_id_type=MESH)
            @pl.when(at_end)
            def _():
                to_relay(l, piece).start()

            for sign in (1, -1):
                @pl.when(inner(sign))
                def _():
                    next_one(l, piece, sign).start()

            @pl.when(at_end)
            def _():
                to_far(l, piece).start()

        at_end = jnp.logical_or(group == 0, group == ring - 1)

        def inner(sign):
            return group + 1 < ring if sign > 0 else group >= 1

        def line_send(l, piece, g, kind, to):
            index = cell(piece, l)
            mine = parts(piece, keep_u.at[l], keep_h.at[l]).at[:, 0]
            return pltpu.make_async_remote_copy(
                src_ref=slot_of(piece, mine, g),
                dst_ref=parts(piece, line_u.at[l, kind], line_h.at[l, kind]),
                send_sem=z_s.at[index, kind], recv_sem=z_r.at[index, kind],
                device_id={FSDP: to}, device_id_type=MESH)

        def next_one(l, piece, sign):
            return line_send(l, piece, group + sign, 0 if sign > 0 else 1, group + sign)

        def far():
            return lax.rem(group + 2, 4)

        def to_far(l, piece):
            return line_send(l, piece, far(), 2, far())

        def to_relay(l, piece):
            opposite = ring - 1 - group
            return line_send(l, piece, opposite, 3, jnp.where(group == 0, 1, 2))

        def relay(l, piece):
            @pl.when(jnp.logical_not(at_end))
            def _():
                index = cell(piece, l)
                come = parts(piece, line_u.at[l, 3], line_h.at[l, 3])
                arrived(come, z_s.at[index, 3], z_r.at[index, 3],
                        fsdp=jnp.where(group == 1, 0, 3))
                mine = slot_of(piece, parts(piece, keep_u.at[l], keep_h.at[l]).at[:, 0], far())
                mine[...] = (mine[...].astype(F32) + come[...].astype(F32)).astype(BF)
                to_far(l, piece).start()

        def add_line(l, piece):
            index = cell(piece, l)
            mine = parts(piece, keep_u.at[l], keep_h.at[l]).at[:, 0]
            result = parts(piece, fin_u.at[l], fin_h.at[l])
            come = [parts(piece, line_u.at[l, kind], line_h.at[l, kind]) for kind in range(3)]
            arrived(come[2], z_s.at[index, 2], z_r.at[index, 2], fsdp=far())
            result[...] = (slot_of(piece, mine, group)[...].astype(F32)
                           + come[2][...].astype(F32)).astype(BF)
            for sign in (1, -1):
                kind = 0 if sign > 0 else 1

                @pl.when(inner(-sign))
                def _():
                    arrived(come[kind], z_s.at[index, kind], z_r.at[index, kind],
                            fsdp=group - sign)
                    result[...] = (result[...].astype(F32)
                                   + come[kind][...].astype(F32)).astype(BF)

        def line_sent(l, piece):
            for sign in (1, -1):
                @pl.when(inner(sign))
                def _():
                    next_one(l, piece, sign).wait_send()

            to_far(l, piece).wait_send()

            @pl.when(at_end)
            def _():
                to_relay(l, piece).wait_send()

        do_norm_back(1, 0)
        do_norm_back(1, 1)
        ready(1, "feed", "spread")
        unit_grads(2, 3, other, give_u)
        give(1, "d")
        unit_grads(2, 3, core, keep_u.at[1])
        do_feed_back(1, 0)
        add_core(1, "d")
        do_feed_back(1, 1)
        unit_grads(0, 1, other, give_u)
        give(1, "g")
        unit_grads(1, 2, other, give_u)
        give(1, "u")
        unit_grads(0, 1, core, keep_u.at[1])
        do_attend_back(1, 0)
        add_core(1, "g")
        unit_grads(1, 2, core, keep_u.at[1])
        load(0, "feed", "spread", "units")
        add_side(1, "d")
        add_core(1, "u")
        do_attend_back(1, 1)
        load(0, "pre2")
        for half in range(2):
            do_inputs_back(1, half)
        ready(1, "ctx", "low")
        head_grad(other, 0, give_h)
        give(1, "h")
        head_grad(other, 1, give_h)
        give(1, "e")
        head_grad(core, 0, keep_h.at[1])
        head_grad(core, 1, keep_h.at[1])
        load(0, "pre1", "heads", "q", "k", "v", "lse", "ctx", "low")
        relay(1, "d")
        add_core(1, "h")
        add_core(1, "e")

        do_norm_back(0, 0)
        ready(0, "feed", "spread")
        do_feed_back(0, 0)
        add_side(1, "g")
        do_norm_back(0, 1)
        sent(gave["d"])
        unit_grads(2, 3, other, give_u)
        give(0, "d")
        unit_grads(2, 3, core, keep_u.at[0])
        do_feed_back(0, 1)
        add_core(0, "d")
        relay(1, "g")
        sent(gave["g"])
        unit_grads(0, 1, other, give_u)
        give(0, "g")
        sent(gave["u"])
        unit_grads(1, 2, other, give_u)
        give(0, "u")
        unit_grads(0, 1, core, keep_u.at[0])
        add_side(1, "u")
        add_core(0, "g")
        unit_grads(1, 2, core, keep_u.at[0])
        do_attend_back(0, 0)
        add_core(0, "u")
        relay(1, "u")
        add_side(1, "h")
        add_side(1, "e")
        do_attend_back(0, 1)
        send(nsum.at[other], nget.at[0], n_s.at[0], n_r.at[0], pipe=other)
        ready(0, "ctx", "low")
        sent(gave["h"])
        head_grad(other, 0, give_h)
        give(0, "h")
        sent(gave["e"])
        head_grad(other, 1, give_h)
        give(0, "e")
        head_grad(core, 0, keep_h.at[0])
        do_inputs_back(0, 0)
        add_core(0, "h")
        head_grad(core, 1, keep_h.at[0])
        do_inputs_back(0, 1)
        add_core(0, "e")
        relay(1, "h")
        relay(1, "e")
        add_side(0, "d")
        arrived(nget.at[0], n_s.at[0], n_r.at[0], pipe=other)
        nred[0] = nsum[core] + nget[0]
        send(nred.at[0], nget.at[1], n_s.at[1], n_r.at[1], tensor=peer(2))
        add_side(0, "g")
        relay(0, "d")

        def finish_rows(half):
            at_rows = slice(half * rows, half * rows + rows)
            grads[0, at_rows] = (dpre[at_rows] + taken(f"i0{half}")).astype(BF)

        finish_rows(0)
        relay(0, "g")
        add_side(0, "u")
        finish_rows(1)
        own_grad = home(grads, grad_out, (b_s, b_r), 2)
        arrived(nget.at[1], n_s.at[1], n_r.at[1], tensor=peer(2))
        nred[1] = nred[0] + nget[1]
        for k in order:
            send(nred.at[1], nget.at[1 + (ring - k) % ring], n_s.at[1 + k],
                 n_r.at[1 + (ring - k) % ring], fsdp=near(k))
        for piece in pieces[:3]:
            add_line(1, piece)
        relay(0, "u")
        add_side(0, "h")
        add_line(1, "h")
        add_line(1, "e")
        add_side(0, "e")
        add_line(0, "d")
        relay(0, "h")
        add_line(0, "g")
        relay(0, "e")
        norms = nred[1]
        for k in order:
            arrived(nget.at[1 + k], n_s.at[1 + k], n_r.at[1 + k], fsdp=near(k))
            norms = norms + nget[1 + k]
        norm_out[...] = norms
        add_line(0, "u")
        add_line(0, "h")
        add_line(0, "e")
        joins = []
        for i, (fin, result) in enumerate(((fin_u, units_out), (fin_h, heads_out))):
            send(fin.at[other], result.at[core], j_s.at[i], j_r.at[i], pipe=other)
            copy = pltpu.make_async_copy(fin.at[core], result.at[core], m_s.at[3 + i])
            copy.start()
            joins.append(copy)
        for i, result in enumerate((units_out, heads_out)):
            arrived(result.at[other], j_s.at[i], j_r.at[i], pipe=other)
        home_arrived(act_out, (a_s, a_r))
        home_arrived(grad_out, (b_s, b_r))
        for copy in [own_act, own_grad] + joins:
            copy.wait()
        for copy in pending:
            copy.wait_send()
        for l in range(2):
            for piece in pieces:
                line_sent(l, piece)

    anywhere = pl.BlockSpec(memory_space=pl.ANY)
    inside = pl.BlockSpec(memory_space=pltpu.VMEM)
    dma = pltpu.SemaphoreType.DMA
    scratch = [pltpu.VMEM(saved[f"{name}0"].shape, saved[f"{name}0"].dtype) for name in loaded
               if name != "spread"]
    scratch += [
        pltpu.VMEM((4, total, heads), BF), pltpu.VMEM((2, total, width), BF),
        pltpu.VMEM((total, width), F32), pltpu.VMEM((2, total, width), BF),
        pltpu.VMEM((rows, heads), BF),
        pltpu.VMEM((2, total, width), BF),
        pltpu.VMEM((4, rows, width), BF), pltpu.VMEM((8, rows, width), BF),
        pltpu.VMEM((2, 4, width), F32), pltpu.VMEM((2, 4, width), F32),
        pltpu.VMEM((1 + ring, 4, width), F32), pltpu.VMEM((rows, width), F32),
        pltpu.VMEM((2, 3, 2, ring * half_units, width), BF),
        pltpu.VMEM((2, 2, 2, ring * head_rows, width), BF),
        pltpu.VMEM((3, 2, ring * half_units, width), BF),
        pltpu.VMEM((2, 2, ring * head_rows, width), BF),
        pltpu.VMEM((3, 2, ring * half_units, width), BF),
        pltpu.VMEM((2, 2, ring * head_rows, width), BF),
        pltpu.VMEM((3, ring * half_units, width), BF),
        pltpu.VMEM((2, ring * head_rows, width), BF),
        pltpu.VMEM((2, ring, 3, half_units, width), BF),
        pltpu.VMEM((2, ring, 2, head_rows, width), BF),
        pltpu.VMEM((2, 3, half_units, width), BF),
        pltpu.VMEM((2, 2, head_rows, width), BF),
        dma((8,)), dma((8,)), dma((4,)), dma((4,)), dma((4,)), dma((4,)),
        dma((10,)), dma((10,)), dma((10,)), dma((10,)), dma((10, 4)), dma((10, 4)),
        dma((1 + ring,)), dma((1 + ring,)), dma((2,)), dma((2,)),
        dma((2 * (len(loaded) + 2),)), dma((5,)),
        pltpu.SemaphoreType.REGULAR((5,)), pltpu.SemaphoreType.REGULAR((5,)),
    ]
    return pl.pallas_call(
        backward_kernel,
        in_specs=[inside] * 5 + [anywhere] * len(arrays),
        out_specs=[anywhere] * 4 + [inside],
        out_shape=[
            jax.ShapeDtypeStruct((count, own_rows, width), BF),
            jax.ShapeDtypeStruct((count, own_rows, width), BF),
            jax.ShapeDtypeStruct((2, 3, half_units, width), BF),
            jax.ShapeDtypeStruct((2, 2, head_rows, width), BF),
            jax.ShapeDtypeStruct((4, width), F32),
        ],
        scratch_shapes=scratch,
        compiler_params=pltpu.CompilerParams(
            collective_id=1, has_side_effects=True, vmem_limit_bytes=67043328),
        name="backward_kernel",
    )(saved["norms"], segment_column, segment_row, cosine, sines, *arrays)


def to_item(array, core, place):
    def piece(k):
        return lax.dynamic_index_in_dim(array, ((place ^ k) & 2) | core, 0, keepdims=False)

    parts = [piece(0)] + [flip(piece(k), TENSOR, k) for k in range(1, 4)]
    return jnp.concatenate(unxor(parts, place), axis=0)


def from_item(by_layer, core, place):
    rows = by_layer[0].shape[0] // 4
    mine = jnp.where(core == 0, by_layer[0], by_layer[1])
    other = jnp.where(core == 0, by_layer[1], by_layer[0])

    def piece(k):
        target = place ^ (k & 2)
        return lax.dynamic_slice_in_dim(other if k & 1 else mine, target * rows, rows, 0)

    parts = [piece(0)] + [mixed_flip(piece(k), k & 1, k & 2) for k in range(1, 4)]
    return jnp.stack(unxor(parts, (place & 2) | core)).astype(F32)


def whole_step(
    layer_inputs,
    cotangent,
    input_master,
    output_master,
    gate_master,
    down_master,
    norm_tables,
    document_lengths,
):
    core = lax.axis_index(PIPE)
    place = lax.axis_index(TENSOR)
    group = lax.axis_index(FSDP)
    ring = lax.axis_size(FSDP)
    width = layer_inputs.shape[2]
    head_rows = input_master.shape[2]
    units = down_master.shape[1]
    half = units // 2
    first_core = core == 0

    item = (place & 2) | core
    lengths = lax.dynamic_index_in_dim(document_lengths[:, 0, :], item, 0, keepdims=False)
    segment, position = segment_info(lengths)
    segment_column = jnp.broadcast_to(segment[:, None], (MB_CAP, 128))
    segment_row = jnp.broadcast_to(segment[None, :], (8, MB_CAP))
    tables = (segment_column, segment_row) + rotary_tables(position)

    def split_by_core(for_first, for_second):
        keep = jnp.where(first_core, for_first, for_second)
        got = flip(jnp.where(first_core, for_second, for_first), PIPE, 1)
        return [jnp.where(first_core, keep, got), jnp.where(first_core, got, keep)]

    def joined_by_core(share_zero, share_one):
        keep = jnp.where(first_core, share_zero, share_one)
        got = flip(jnp.where(first_core, share_one, share_zero), PIPE, 1)
        return jnp.where(first_core, keep, got), jnp.where(first_core, got, keep)

    if head_rows % 16 == 0 and half % 16 == 0 and ring == 4:
        heads_in = jnp.concatenate([input_master[0], output_master], axis=0).astype(BF)
        units_in = jnp.concatenate([gate_master[0], down_master], axis=0).astype(BF)
        saved = forward_all(layer_inputs, cotangent, heads_in, units_in.reshape(3, 2, half, width),
                            norm_tables[0], tables)
        results = backward_all(saved, cotangent.shape[0], tables)
        activations, gradients_in, unit_grad, head_grad, norm_sum = results
        head_grad = head_grad.reshape(4, head_rows, width).astype(F32)
        unit_grad = unit_grad.transpose(1, 0, 2, 3).reshape(3, units, width).astype(F32)
        return (
            activations[None].astype(F32),
            gradients_in[None].astype(F32),
            head_grad[None, :3],
            head_grad[None, 3],
            unit_grad[None, :2],
            unit_grad[None, 2],
            norm_sum[None],
        )

    in_low = input_master[0].astype(BF)
    out_low = output_master.astype(BF)
    head_shares = split_by_core(in_low[:2], jnp.concatenate([in_low[2:], out_low], axis=0))
    unit_low = jnp.concatenate([gate_master[0], down_master], axis=0).astype(BF)
    unit_shares = split_by_core(unit_low[:, :half], unit_low[:, half:])

    x = to_item(layer_inputs, core, place)
    norm_own = norm_tables[0]
    norm_other = flip(norm_own, PIPE, 1)
    norms = [
        jnp.where(first_core, norm_own, norm_other),
        jnp.where(first_core, norm_other, norm_own),
    ]

    quarter = half // 2
    rows = ring * head_rows

    def gather_heads(s, *waits):
        slots = ring_gather(tied(head_shares[s], *waits), f"h{s}")
        ascending = jnp.stack(slots[::-1] + slots[::-1])
        column = lax.dynamic_slice_in_dim(ascending, ring - 1 - group, ring, 0)
        return column.transpose(1, 0, 2, 3).reshape(2, rows, width)

    def head_weights(parts):
        mine = jnp.concatenate(parts[:2], axis=1)
        theirs = jnp.concatenate(parts[2:], axis=1)
        low = jnp.where(first_core, mine, theirs)
        high = jnp.where(first_core, theirs, mine)
        return jnp.concatenate([low, high[:1]], axis=0), high[1]

    def gather_units(s, i, *waits):
        piece = unit_shares[s][:, i * quarter:i * quarter + quarter]
        return jnp.concatenate(ring_gather(tied(piece, *waits), f"u{s}{i}"), axis=1)

    def in_order(pieces):
        return [pieces[i][j] for j in range(4) for i in range(2)]

    column = gather_heads(0)
    heads = spread_out(column, "h0")
    unit_a = gather_units(0, 0, column)
    pieces = [spread_out(unit_a, "u00")]
    unit_b = gather_units(0, 1, unit_a, heads[1])
    pieces.append(spread_out(unit_b, "u01"))
    weights = head_weights(heads) + (in_order(pieces),)
    layers = [weights]
    halves = attention_forward("0", [(tied(x, unit_a),), (x,)], weights, None, tables)
    column = gather_heads(1, unit_b, halves[1][1][0], pieces[0][1])
    heads = spread_out(column, "h1")
    next_a = gather_units(1, 0, column)
    next_pieces = [spread_out(next_a, "u10")]
    next_b = gather_units(1, 1, next_a, heads[1])
    next_pieces.append(spread_out(next_b, "u11"))
    layers.append(head_weights(heads) + (in_order(next_pieces),))
    ends, saved = feed_forward("0", halves, weights, norms[0], (column,), ())
    kept = [saved]
    ends[0] = (tied(ends[0][0], next_a),) + ends[0][1:]
    halves = attention_forward("1", ends, layers[1], norms[0], tables, (next_b,))
    ends, saved = feed_forward("1", halves, layers[1], norms[1], (), ())
    kept.append(saved)
    upstream = to_item(cotangent, core, place)

    def pull_units(tag, gate_up, down):
        parts = []
        for name, grad, count in (("u", gate_up, 2), ("d", down, 1)):
            own = grad[0].reshape(count, 2, ring * half, width)
            got = cross(grad[1], PIPE, 1, f"c_g{name}{tag}").reshape(count, 2, ring * half, width)
            parts.append([added(own[:, 1], got[:, 1]), (own[:, 0], got[:, 0])])
        return parts[0][0], parts[1][0], parts[0][1], parts[1][1]

    def cross_units(tag, units):
        columns = []
        for name, neighbour, (own, got) in (("u", units[0], units[2]), ("d", units[1], units[3])):
            other = cross(neighbour, TENSOR, 2, f"y_g{name}{tag}")
            column = own.astype(F32) + got.astype(F32) + other.astype(F32)
            columns.append(column.astype(BF))
        return columns

    def ring_units(tag, columns):
        totals = []
        for name, column in zip("ud", columns):
            count = column.shape[0]
            column = column.reshape(count, 2, ring, quarter, width)
            total = ring_reduce([column[:, :, k] for k in range(ring)], f"g{name}{tag}")
            totals.append(total.reshape(count, half, width).astype(BF))
        return jnp.concatenate(totals, axis=0)

    def pull_heads(tag, grad_in, grad_out):
        low = jnp.stack(grad_in[:2])
        high = jnp.stack([grad_in[2], grad_out])
        mine = jnp.where(first_core, low, high)
        theirs = cross(jnp.where(first_core, high, low), PIPE, 1, "c_gh" + tag)
        return added(mine[:, rows:], theirs[:, rows:]), mine[:, :rows], theirs[:, :rows]

    def cross_heads(tag, heads):
        neighbour, own, got = heads
        column = own.astype(F32) + got.astype(F32)
        column = column + cross(neighbour, TENSOR, 2, "y_gh" + tag).astype(F32)
        return column.astype(BF)

    def ring_heads(tag, column):
        column = column.reshape(2, ring, head_rows, width).transpose(1, 0, 2, 3)
        ascending = jnp.concatenate([column, column], axis=0)
        rolled = lax.dynamic_slice_in_dim(ascending, (group + 1) % ring, ring, 0)
        return ring_reduce([rolled[ring - 1 - k] for k in range(ring)], "gh" + tag).astype(BF)

    head_totals = [None, None]
    unit_totals = [None, None]
    edges = [None, None]
    norm_grads = [None, None]
    ends = [(upstream,), (upstream,)]
    waits = ()
    for s in (1, 0):
        tag = str(s)
        ends, edges[s], units, heads, norm_grads[s] = layer_backward(
            tag, ends, layers[s], norms[s], tables, kept[s], pull_units, pull_heads, waits
        )
        crossed = cross_units(tag, units)
        unit_totals[s] = ring_units(tag, crossed)
        head_columns = cross_heads(tag, heads)
        head_totals[s] = ring_heads(tag, head_columns)
        waits = crossed
    first_grad = jnp.concatenate(
        [
            (grad[half * MB_CAP // 2:(half + 1) * MB_CAP // 2] + own.astype(F32) + got.astype(F32))
            for half, (grad, own, got) in enumerate(ends)
        ],
        axis=0,
    ).astype(BF)
    activations = from_item([kept[1][1], edges[1]], core, place)
    gradients_in = from_item([first_grad, edges[0]], core, place)

    low, high = joined_by_core(head_totals[0], head_totals[1])
    unit_low, unit_high = joined_by_core(unit_totals[0], unit_totals[1])
    unit_grad = jnp.concatenate([unit_low, unit_high], axis=1).astype(F32)
    head_grad = jnp.concatenate([low, high], axis=0).astype(F32)
    norm_grads[0] = tied(norm_grads[0], heads[0])
    norm_own = jnp.where(first_core, norm_grads[0], norm_grads[1])
    norm_other = jnp.where(first_core, norm_grads[1], norm_grads[0])
    norm_sum = norm_own + flip(norm_other, PIPE, 1)
    norm_sum = norm_sum + flip(norm_sum, TENSOR, 2)
    bit = 1
    while bit < ring:
        norm_sum = norm_sum + flip(norm_sum, FSDP, bit)
        bit = bit * 2
    return (
        activations[None],
        gradients_in[None],
        head_grad[None, :3],
        head_grad[None, 3],
        unit_grad[None, :2],
        unit_grad[None, 2],
        norm_sum[None],
    )


def solution(mesh):
    placed = (
        P(None, (FSDP, TENSOR), None),
        P(None, (FSDP, TENSOR), None),
        P(PIPE, None, (TENSOR, FSDP), None),
        P(PIPE, (TENSOR, FSDP), None),
        P(PIPE, None, (TENSOR, FSDP), None),
        P(PIPE, (TENSOR, FSDP), None),
        P(PIPE, None, None),
        P(None, FSDP, None),
    )
    return jax.shard_map(
        whole_step,
        mesh=mesh,
        in_specs=placed,
        out_specs=(
            P(PIPE, None, (FSDP, TENSOR), None),
            P(PIPE, None, (FSDP, TENSOR), None),
            P(PIPE, None, (TENSOR, FSDP), None),
            P(PIPE, (TENSOR, FSDP), None),
            P(PIPE, None, (TENSOR, FSDP), None),
            P(PIPE, (TENSOR, FSDP), None),
            P(PIPE, None, None),
        ),
        check_vma=False,
    )
```

```python
import jax
import jax.numpy as jnp
from jax import lax
from jax.experimental import pallas as pl
from jax.experimental.pallas import tpu as pltpu
from jax.sharding import PartitionSpec as P

HEAD_DIM = 64
MB_CAP = 512
DOCS = 3

epsilon = 1e-05
rope_base = 1000.0
masked_value = -1e30

BF = jnp.bfloat16
PIPE, FSDP, TENSOR = "pipe", "fsdp", "tensor"
F32 = jnp.float32


def segment_info(lengths):
    doc_ends = jnp.cumsum(lengths)
    starts = doc_ends - lengths
    places = jnp.arange(MB_CAP, dtype=jnp.int32)
    segment = jnp.sum((places[:, None] >= doc_ends[None, :]).astype(jnp.int32), axis=1)
    choose = segment[:, None] == jnp.arange(DOCS, dtype=jnp.int32)[None, :]
    offset = jnp.sum(jnp.where(choose, starts[None, :], 0), axis=1)
    return (segment, places - offset)


def rotary_tables(position):
    half_dim = HEAD_DIM // 2
    lane = jnp.arange(2 * HEAD_DIM, dtype=jnp.int32)
    frequency = rope_base ** (-2.0 * (lane % half_dim).astype(F32) / HEAD_DIM)
    angles = position.astype(F32)[:, None] * frequency[None, :]
    sines = jnp.sin(angles)
    return jnp.cos(angles), jnp.where(lane[None, :] % HEAD_DIM < half_dim, -sines, sines)


def flip(array, axis, bit):
    count = lax.axis_size(axis)
    return lax.ppermute(array, axis, [(i, i ^ bit) for i in range(count)])


def shifted(array, axis, by):
    count = lax.axis_size(axis)
    return lax.ppermute(array, axis, [(i, (i + by) % count) for i in range(count)])


def unxor(parts, index):
    parts = [jnp.where(index & 1, parts[m ^ 1], parts[m]) for m in range(4)]
    return [jnp.where(index & 2, parts[m ^ 2], parts[m]) for m in range(4)]


def mixed_flip(array, core_bit, place_bits):
    count = lax.axis_size(TENSOR)
    pairs = [
        (c * count + t, (c ^ core_bit) * count + (t ^ place_bits))
        for c in range(2)
        for t in range(count)
    ]
    return lax.ppermute(array, (PIPE, TENSOR), pairs)


def ring_gather(shard, tag):
    count = lax.axis_size(FSDP)
    slots = [shard]
    for k in range(1, count):
        with jax.named_scope(f"z{k}_{tag}"):
            slots.append(shifted(shard, FSDP, k))
    return slots


def ring_reduce(parts, tag):
    count = len(parts)
    total = parts[0].astype(F32)
    for k in range(1, count):
        with jax.named_scope(f"z{k}_{tag}"):
            part = shifted(parts[k].astype(BF), FSDP, -k)
        total = total + part.astype(F32)
    return total


def cross(array, axis, bit, tag):
    with jax.named_scope(tag):
        return flip(array, axis, bit)


def spread_out(column, tag):
    neighbour = cross(column, TENSOR, 2, "y_" + tag)
    return [
        column,
        neighbour,
        cross(column, PIPE, 1, "c_" + tag),
        cross(neighbour, PIPE, 1, "n_" + tag),
    ]


def added(a, b):
    return (a.astype(F32) + b.astype(F32)).astype(BF)


def row_norm(summed):
    centered = summed - jnp.mean(summed, axis=-1, keepdims=True)
    inverse = lax.rsqrt(jnp.mean(centered * centered, axis=-1, keepdims=True) + epsilon)
    return centered * inverse, inverse


def row_norm_back(normed, inverse, gain_row, upstream):
    scaled = upstream * gain_row
    through = inverse * (
        scaled
        - jnp.mean(scaled, axis=-1, keepdims=True)
        - normed * jnp.mean(scaled * normed, axis=-1, keepdims=True)
    )
    sums = [
        jnp.sum(upstream * normed, axis=0, keepdims=True),
        jnp.sum(upstream, axis=0, keepdims=True),
    ]
    return through, jnp.concatenate(sums + [jnp.zeros((6, sums[0].shape[1]), F32)], axis=0)


def nn(a, b):
    return lax.dot_general(a, b, (((1,), (0,)), ((), ())), preferred_element_type=F32)


def nt(a, b):
    return lax.dot_general(a, b, (((1,), (1,)), ((), ())), preferred_element_type=F32)


def tn(a, b):
    return lax.dot_general(a, b, (((0,), (0,)), ((), ())), preferred_element_type=F32)


def turned(slab, cosine, sines):
    lane = lax.broadcasted_iota(jnp.int32, slab.shape, 1)
    swapped = jnp.where(
        lane % HEAD_DIM < HEAD_DIM // 2, pltpu.roll(slab, 96, 1), pltpu.roll(slab, 32, 1)
    )
    return slab * cosine + swapped * sines


def head_masks(rows):
    lane = lax.broadcasted_iota(jnp.int32, (rows, 128), 1)
    low = (lane < HEAD_DIM).astype(F32)
    return low, 1.0 - low


def rows_of(half, columns, rows):
    return pl.BlockSpec((rows, columns), lambda i: (half, 0))


def whole(array):
    zeros = (0,) * array.ndim
    return pl.BlockSpec(array.shape, lambda i: zeros)


ANYWHERE = pl.BlockSpec(memory_space=pl.ANY)


def staged(tag, kernel, ins, outs, before, scratch=()):
    before = list(before or [])
    arrays = [array for array, _ in ins] + before
    specs = [spec for _, spec in ins] + [ANYWHERE] * len(before)
    first_out = len(outs) - len(before)
    first_in = len(ins)
    count = len(before)

    def run(*refs):
        kernel(*refs[:first_in], *refs[first_in + count:])

    call = pl.pallas_call(
        run,
        grid=(1,),
        in_specs=specs,
        out_specs=[spec for _, _, spec in outs],
        out_shape=[jax.ShapeDtypeStruct(shape, kind) for shape, kind, _ in outs],
        scratch_shapes=list(scratch),
        input_output_aliases={first_in + i: first_out + i for i in range(count)},
        compiler_params=pltpu.CompilerParams(vmem_limit_bytes=40 << 20),
        cost_estimate=pl.CostEstimate(flops=1024, bytes_accessed=1024, transcendentals=0),
        name=kernel.__name__,
    )
    with jax.named_scope("k_" + tag):
        return call(*arrays)


def project(tag, half, sources, norm_rows, weight, cosine, sines, before):
    given = len(sources) == 1
    total, width = sources[0].shape
    heads = weight.shape[1]
    rows = total // 2

    def project_kernel(*refs):
        if given:
            x_ref, w_ref, cos_ref, sin_ref, q_ref, k_ref, v_ref = refs
            low = x_ref[...]
        else:
            (mid_ref, own_ref, got_ref, norm_ref, w_ref, cos_ref, sin_ref,
             q_ref, k_ref, v_ref, x_ref, low_ref) = refs
            summed = mid_ref[...] + own_ref[...].astype(F32) + got_ref[...].astype(F32)
            x = row_norm(summed)[0] * norm_ref[2:3] + norm_ref[3:4]
            x_ref[...] = x
            low = x.astype(BF)
            low_ref[...] = low
        cosine, sines = cos_ref[...], sin_ref[...]
        for c, out in ((0, q_ref), (1, k_ref)):
            turning = nt(low, w_ref[c])
            for slab in range(heads // 128):
                at = slice(128 * slab, 128 * slab + 128)
                out[:, at] = turned(turning[:, at], cosine, sines).astype(BF)
        v_ref[...] = nt(low, w_ref[2]).astype(BF)

    here = rows_of(half, width, rows)
    ins = [(sources[0], here)]
    outs = [((total, heads), BF, rows_of(half, heads, rows)) for _ in range(3)]
    if not given:
        plain = pl.BlockSpec((rows, width), lambda i: (0, 0))
        ins += [(sources[1], plain), (sources[2], plain), (norm_rows, whole(norm_rows))]
        outs += [((total, width), F32, here), ((total, width), BF, here)]
    ins += [(weight, whole(weight))]
    ins += [(table, rows_of(half, 128, rows)) for table in (cosine, sines)]
    return staged(tag, project_kernel, ins, outs, before)


def attend(tag, half, queries, key_vecs, values, segment_column, segment_row, out_weight, before):
    total, heads = queries.shape
    width = out_weight.shape[1]
    rows = total // 2

    def attend_kernel(q_ref, k_ref, v_ref, col_ref, row_ref, w_ref, part_ref, ctx_ref, lse_ref):
        masks = head_masks(rows)
        lane = lax.broadcasted_iota(jnp.int32, (rows, 128), 1)
        same = col_ref[:, :1] == row_ref[:1, :]
        totals = jnp.zeros((rows, 128), F32)
        for slab in range(heads // 128):
            at = slice(128 * slab, 128 * slab + 128)
            q, k, v = q_ref[:, at], k_ref[:, at], v_ref[:, at]
            gathered = jnp.zeros((rows, 128), F32)
            for h in range(2):
                scores = nt(q * masks[h].astype(BF), k) * HEAD_DIM ** (-0.5)
                scores = jnp.where(same, scores, masked_value)
                top = jnp.max(scores, axis=-1, keepdims=True)
                powers = jnp.exp(scores - top)
                mass = jnp.sum(powers, axis=-1, keepdims=True)
                chances = (powers * (1.0 / mass)).astype(BF)
                gathered = gathered + nn(chances, v) * masks[h]
                totals = jnp.where(lane == 2 * slab + h, top + jnp.log(mass), totals)
            ctx_ref[:, at] = gathered.astype(BF)
        lse_ref[...] = totals.T[:8]
        part_ref[...] = nn(ctx_ref[...], w_ref[...]).astype(BF)

    ins = [
        (queries, rows_of(half, heads, rows)),
        (key_vecs, whole(key_vecs)),
        (values, whole(values)),
        (segment_column, rows_of(half, 128, rows)),
        (segment_row, whole(segment_row)),
        (out_weight, whole(out_weight)),
    ]
    outs = [
        ((rows, width), BF, pl.BlockSpec((rows, width), lambda i: (0, 0))),
        ((total, heads), BF, rows_of(half, heads, rows)),
        ((8, total), F32, pl.BlockSpec((8, rows), lambda i: (0, half))),
    ]
    return staged(tag, attend_kernel, ins, outs, before)


def feed_scratch(blocks, rows, width):
    return [
        pltpu.VMEM((len(blocks),) + blocks[0].shape, BF),
        pltpu.VMEM((rows, width), F32),
        pltpu.SemaphoreType.DMA((len(blocks),)),
    ]


def fetch_blocks(block_refs, buffer, sems):
    for j, ref in enumerate(block_refs):
        pltpu.make_async_copy(ref, buffer.at[j], sems.at[j]).start()


def share_blocks(p, block_refs, buffer, sems):
    each = len(block_refs) // 2
    for j in range(p * each, p * each + each):
        pltpu.make_async_copy(block_refs[j], buffer.at[j], sems.at[j]).wait()

    def joined(c):
        return jnp.concatenate([buffer[p * each + j, c] for j in range(each)], axis=0)

    return joined(0), joined(1), joined(2)


def feed(tag, half, x, own, got, norm_rows, blocks, before):
    total, width = x.shape
    rows = total // 2
    step = len(blocks) // 2 * blocks[0].shape[1]
    units = len(blocks) * blocks[0].shape[1]
    count = len(blocks)

    def feed_kernel(*refs):
        x_ref, own_ref, got_ref, norm_ref = refs[:4]
        block_refs = refs[4:4 + count]
        (part_ref, mid_ref, low_ref, gate_ref, up_ref, own_hid, other_hid,
         buffer, acc_ref, sems) = refs[4 + count:]
        fetch_blocks(block_refs, buffer, sems)
        summed = x_ref[...] + own_ref[...].astype(F32) + got_ref[...].astype(F32)
        middle = row_norm(summed)[0] * norm_ref[0:1] + norm_ref[1:2]
        mid_ref[...] = middle
        low = middle.astype(BF)
        low_ref[...] = low
        for p in range(2):
            gate_w, up_w, down_w = share_blocks(p, block_refs, buffer, sems)
            at = slice(p * step, p * step + step)
            gate = nt(low, gate_w)
            up = nt(low, up_w)
            gate_ref[:, at] = gate.astype(BF)
            up_ref[:, at] = up.astype(BF)
            hidden = (gate * jax.nn.sigmoid(gate) * up).astype(BF)
            (own_hid, other_hid)[p][...] = hidden
            fed = nn(hidden, down_w)
            acc_ref[...] = fed if p == 0 else acc_ref[...] + fed
        part_ref[...] = acc_ref[...].astype(BF)

    plain = pl.BlockSpec((rows, width), lambda i: (0, 0))
    here = rows_of(half, width, rows)
    wide = rows_of(half, units, rows)
    ins = [(x, here), (own, plain), (got, plain), (norm_rows, whole(norm_rows))]
    ins += [(block, ANYWHERE) for block in blocks]
    outs = [((rows, width), BF, plain), ((total, width), F32, here), ((total, width), BF, here)]
    outs += [((total, units), BF, wide) for _ in range(2)]
    outs += [((total, step), BF, rows_of(half, step, rows)) for _ in range(2)]
    return staged(tag, feed_kernel, ins, outs, before, feed_scratch(blocks, rows, width))


def feed_back(tag, half, sources, middle, own, got, norm_rows, gate, up, blocks, before):
    top = len(sources) == 1
    total, width = middle.shape
    rows = total // 2
    step = len(blocks) // 2 * blocks[0].shape[1]
    units = len(blocks) * blocks[0].shape[1]
    count = len(blocks)

    def feed_back_kernel(*refs):
        taken = len(sources)
        mid_ref, own_ref, got_ref, norm_ref, gate_ref, up_ref = refs[taken:taken + 6]
        block_refs = refs[taken + 6:taken + 6 + count]
        (part_ref, sums_ref, edge_ref, pre_ref, feed_ref, own_grads, other_grads,
         buffer, acc_ref, sems) = refs[taken + 6 + count:]
        fetch_blocks(block_refs, buffer, sems)
        summed = mid_ref[...] + own_ref[...].astype(F32) + got_ref[...].astype(F32)
        normed, inverse = row_norm(summed)
        if top:
            upstream = refs[0][...].astype(F32)
            edge_ref[...] = (normed * norm_ref[2:3] + norm_ref[3:4]).astype(BF)
        else:
            upstream = refs[0][...] + refs[1][...].astype(F32) + refs[2][...].astype(F32)
            edge_ref[...] = upstream.astype(BF)
        through, sums_ref[...] = row_norm_back(normed, inverse, norm_ref[2:3], upstream)
        pre_ref[...] = through
        low = through.astype(BF)
        feed_ref[...] = low
        for p in range(2):
            gate_w, up_w, down_w = share_blocks(p, block_refs, buffer, sems)
            at = slice(p * step, p * step + step)
            gate, up = gate_ref[:, at].astype(F32), up_ref[:, at].astype(F32)
            grad_hidden = nt(low, down_w)
            sigmoid = jax.nn.sigmoid(gate)
            grad_gate = (grad_hidden * up * sigmoid * (1.0 + gate * (1.0 - sigmoid))).astype(BF)
            grad_up = (grad_hidden * gate * sigmoid).astype(BF)
            share_ref = (own_grads, other_grads)[p]
            share_ref[:, :step] = grad_gate
            share_ref[:, step:] = grad_up
            back_through = nn(grad_gate, gate_w) + nn(grad_up, up_w)
            acc_ref[...] = back_through if p == 0 else acc_ref[...] + back_through
        part_ref[...] = acc_ref[...].astype(BF)

    plain = pl.BlockSpec((rows, width), lambda i: (0, 0))
    here = rows_of(half, width, rows)
    wide = rows_of(half, units, rows)
    ins = [(sources[0], here)] + [(source, plain) for source in sources[1:]]
    ins += [(middle, here), (own, plain), (got, plain), (norm_rows, whole(norm_rows))]
    ins += [(gate, wide), (up, wide)] + [(block, ANYWHERE) for block in blocks]
    outs = [((rows, width), BF, plain), ((8, width), F32, pl.BlockSpec((8, width), lambda i: (0, 0)))]
    outs += [((total, width), BF, here), ((total, width), F32, here), ((total, width), BF, here)]
    outs += [((total, units), BF, wide) for _ in range(2)]
    return staged(tag, feed_back_kernel, ins, outs, before, feed_scratch(blocks, rows, width))


def attend_back(tag, half, grad_middle, x, own, got, norm_rows, queries, key_vecs, values, totals,
                segment_column, segment_row, out_weight, cosine, sines, partial, before):
    total, heads = queries.shape
    width = out_weight.shape[1]
    rows = total // 2
    last = partial is not None

    def attend_back_kernel(*refs):
        (pre_ref, fed_ref, fed_got_ref, x_ref, own_ref, got_ref, norm_ref, q_ref, k_ref, v_ref,
         lse_ref, col_ref, row_ref, w_ref, cos_ref, sin_ref) = refs[:16]
        if last:
            dk_in, dv_in = refs[16:18]
        sums_ref, dk_ref, dv_ref, mid_ref, att_ref, dq_ref, dctx_ref = refs[18 if last else 16:]
        upstream = pre_ref[...] + fed_ref[...].astype(F32) + fed_got_ref[...].astype(F32)
        summed = x_ref[...] + own_ref[...].astype(F32) + got_ref[...].astype(F32)
        normed, inverse = row_norm(summed)
        through, sums_ref[...] = row_norm_back(normed, inverse, norm_ref[0:1], upstream)
        mid_ref[...] = through
        low = through.astype(BF)
        att_ref[...] = low
        dctx_ref[...] = nt(low, w_ref[...]).astype(BF)
        masks = head_masks(rows)
        wide_masks = head_masks(total)
        same = col_ref[:, :1] == row_ref[:1, :]
        scaling = HEAD_DIM ** (-0.5)
        here = pl.ds(half * rows, rows)
        cosine, sines = cos_ref[...], sin_ref[...]
        for slab in range(heads // 128):
            at = slice(128 * slab, 128 * slab + 128)
            q, k, v, grad_ctx = q_ref[:, at], k_ref[:, at], v_ref[:, at], dctx_ref[:, at]
            dq = jnp.zeros((rows, 128), F32)
            dk = jnp.zeros((total, 128), F32)
            dv = jnp.zeros((total, 128), F32)
            for h in range(2):
                mask = masks[h].astype(BF)
                scores = nt(k, q * mask) * scaling
                scores = jnp.where(same, scores, masked_value)
                chances = jnp.exp(scores - lse_ref[2 * slab + h:2 * slab + h + 1, :])
                grad_chances = nt(v, grad_ctx * mask)
                row_dot = jnp.sum(chances * grad_chances, axis=0, keepdims=True)
                grad_scores = (chances * (grad_chances - row_dot)).astype(BF)
                dv = dv + nn(chances.astype(BF), grad_ctx) * wide_masks[h]
                dk = dk + nn(grad_scores, q) * wide_masks[h]
                dq = dq + tn(grad_scores, k) * masks[h]
            dq_ref[:, at] = turned(dq * scaling, cos_ref[here, :], -sin_ref[here, :]).astype(BF)
            if last:
                dk = dk_in[:, at] + dk
                dv = dv_in[:, at] + dv
                dk_ref[:, at] = turned(dk * scaling, cosine, -sines).astype(BF)
                dv_ref[:, at] = dv.astype(BF)
            else:
                dk_ref[:, at] = dk
                dv_ref[:, at] = dv

    plain = pl.BlockSpec((rows, width), lambda i: (0, 0))
    here = rows_of(half, width, rows)
    ins = [(grad_middle[0], here), (grad_middle[1], plain), (grad_middle[2], plain)]
    ins += [(x, here), (own, plain), (got, plain), (norm_rows, whole(norm_rows))]
    ins += [(queries, rows_of(half, heads, rows)), (key_vecs, whole(key_vecs)),
            (values, whole(values)), (totals, pl.BlockSpec((8, rows), lambda i: (0, half))),
            (segment_column, whole(segment_column)),
            (segment_row, pl.BlockSpec((8, rows), lambda i: (0, half))),
            (out_weight, whole(out_weight)), (cosine, whole(cosine)), (sines, whole(sines))]
    if last:
        ins += [(part, whole(part)) for part in partial]
    kind = BF if last else F32
    all_rows = pl.BlockSpec((total, heads), lambda i: (0, 0))
    outs = [((8, width), F32, pl.BlockSpec((8, width), lambda i: (0, 0))),
            ((total, heads), kind, all_rows), ((total, heads), kind, all_rows),
            ((total, width), F32, here), ((total, width), BF, here),
            ((total, heads), BF, rows_of(half, heads, rows))]
    return staged(tag, attend_back_kernel, ins, outs, before, [pltpu.VMEM((rows, heads), BF)])


def inputs_back(tag, half, grads, weight):
    total, heads = grads[0].shape
    width = weight.shape[2]
    rows = total // 2

    def inputs_back_kernel(dq_ref, dk_ref, dv_ref, w_ref, part_ref):
        acc = nn(dq_ref[...], w_ref[0]) + nn(dk_ref[...], w_ref[1]) + nn(dv_ref[...], w_ref[2])
        part_ref[...] = acc.astype(BF)

    ins = [(grad, rows_of(half, heads, rows)) for grad in grads] + [(weight, whole(weight))]
    outs = [((rows, width), BF, pl.BlockSpec((rows, width), lambda i: (0, 0)))]
    return staged(tag, inputs_back_kernel, ins, outs, None)[0]


def across(part, tag):
    with jax.named_scope("x_" + tag):
        return flip(part, TENSOR, 1)


def tied(value, *others):
    return lax.optimization_barrier((value, *others))[0]


def weight_grad(left, right, tag):
    with jax.named_scope("w_" + tag):
        return jnp.einsum("th,td->hd", left, right, preferred_element_type=F32).astype(BF)


def attention_forward(tag, sources, weights, norm_before, tables, wait=()):
    in_weight, out_weight = weights[:2]
    segment_column, segment_row, cosine, sines = tables
    projected = None
    for half in range(2):
        projected = project(f"p{tag}{half}", half, sources[half], norm_before, in_weight, cosine, sines, projected)
    queries, key_vecs, values = projected[:3]
    if len(projected) == 5:
        x, low = projected[3:]
    else:
        low = sources[0][0]
        x = low.astype(F32)
    kept = None
    attended = []
    for half in range(2):
        taken = tied(queries, *wait) if half == 1 else queries
        part, *kept = attend(f"t{tag}{half}", half, taken, key_vecs, values, segment_column, segment_row,
                             out_weight, kept)
        attended.append((part, across(part, f"t{tag}{half}")))
    context, totals = kept
    return (x, low, queries, key_vecs, values, context, totals), attended


def feed_forward(tag, halves, weights, norm_rows, first_wait, second_wait):
    before, attended = halves
    blocks = weights[2]
    x = before[0]
    saved = None
    fed = []
    for half in range(2):
        taken = tied(x, *(second_wait if half else first_wait))
        part, *saved = feed(f"f{tag}{half}", half, taken, *attended[half], norm_rows, blocks, saved)
        fed.append((part, across(part, f"f{tag}{half}")))
    middle, spread, gate, up, *hidden = saved
    ends = [(middle, *fed[half]) for half in range(2)]
    return ends, (*before, attended, middle, spread, gate, up, hidden, fed)


def layer_backward(tag, sources, weights, norm_rows, tables, kept, pull_units, pull_heads, waits):
    in_weight, out_weight, blocks = weights
    segment_column, segment_row, cosine, sines = tables
    (x, low, queries, key_vecs, values, context, totals, attended, middle, spread,
     gate, up, hidden, fed) = kept
    saved = None
    through = []
    sums = []
    for half in range(2):
        part, total, *saved = feed_back(f"g{tag}{half}", half, sources[half], middle, *fed[half], norm_rows,
                                        gate, up, blocks, saved)
        through.append((part, across(part, f"g{tag}{half}")))
        sums.append(total)
    edge, grad_pre_output, grad_feed, *grad_shares = saved
    down = [weight_grad(hidden[i], grad_feed, f"d{tag}{i}") for i in (1, 0)]
    gate_up = [weight_grad(grad_shares[i], spread, f"u{tag}{i}") for i in (1, 0)]
    down, gate_up = down[::-1], gate_up[::-1]
    units = pull_units(tag, gate_up, down)
    partial = None
    saved = None
    first_sums = []
    for half in range(2):
        wait = waits if half == 0 else units[:2]
        total, dk, dv, *saved = attend_back(
            f"h{tag}{half}", half, (tied(grad_pre_output, *wait), *through[half]), x, *attended[half], norm_rows,
            queries, key_vecs, values, totals, segment_column, segment_row,
            out_weight, cosine, sines, partial, saved)
        partial = (dk, dv)
        first_sums.append(total)
    grad_pre_middle, grad_attended, dq = saved
    ends = []
    for half in range(2):
        part = inputs_back(f"i{tag}{half}", half, (dq, dk, dv), in_weight)
        ends.append((grad_pre_middle, part, across(part, f"i{tag}{half}")))
    grad_in = [weight_grad(grad, low, f"n{tag}") for grad in (dq, dk, dv)]
    grad_out = weight_grad(context, grad_attended, f"o{tag}")
    heads = pull_heads(tag, grad_in, grad_out)
    first = first_sums[0] + first_sums[1]
    second = sums[0] + sums[1]
    norm_grad = jnp.concatenate([first[:2], second[:2]], axis=0)
    return ends, edge, units, heads, norm_grad


MESH = pl.DeviceIdType.MESH


def forward_all(layer_inputs, cotangent, heads_in, units_in, norm_in, tables):
    segment_column, segment_row, cosine, sines = tables
    ring = lax.axis_size(FSDP)
    count, own_rows, width = layer_inputs.shape
    total = count * own_rows
    rows = total // 2
    head_rows = heads_in.shape[1]
    half_units = units_in.shape[2]
    heads = 2 * ring * head_rows
    step = 2 * ring * half_units
    order = sorted(range(1, ring), key=lambda k: min(k, ring - k))

    saved = {}
    for l in range(2):
        saved.update({
            f"q{l}": ((total, heads), BF), f"k{l}": ((total, heads), BF),
            f"v{l}": ((total, heads), BF), f"ctx{l}": ((total, heads), BF),
            f"lse{l}": ((8, total), F32), f"pre1{l}": ((total, width), F32),
            f"pre2{l}": ((total, width), F32),
            f"spread{l}": ((total, width), BF), f"feed{l}": ((3, total, 2 * step), BF),
        })
    saved.update({"low0": ((total, width), BF), "acts": ((2, total, width), BF),
                  "cot": ((total, width), BF)})
    inner = {"x1": ((total, width), F32), "mid": ((total, width), F32)}
    for l in range(2):
        for h in range(2):
            for stage in "tf":
                inner[f"own_{stage}{l}{h}"] = ((rows, width), BF)
                inner[f"got_{stage}{l}{h}"] = ((rows, width), BF)
    weights = {}
    for l in range(2):
        weights[f"heads{l}"] = ((4, 2, ring * head_rows, width), BF)
        weights[f"units{l}"] = ((3, 2, 2, ring * half_units, width), BF)
    outs = {**saved, **weights, "norms": ((2, 4, width), F32)}
    held = {**saved, **inner}
    stages = [f"{stage}{l}{h}" for l in range(2) for stage in "tf" for h in range(2)]

    def forward_kernel(inp, cot_ref, heads_ref, units_ref, norm_ref, col_ref, row_ref, cos_ref, sin_ref,
                       *refs):
        out = dict(zip(outs, refs[:len(outs)]))
        rest = refs[len(outs):]
        keep = dict(zip(held, rest[:len(held)]))
        (hbuf, ubuf, nbuf, acc_ref, z_s, z_r, y_s, y_r, k_s, k_r, e_s, e_r, x_s, x_r, i_s, i_r,
         l_s, f_s) = rest[len(held):]
        core = lax.axis_index(PIPE)
        place = lax.axis_index(TENSOR)
        group = lax.axis_index(FSDP)
        other = 1 - core
        item = (place // 2) * 2 + core

        def peer(k):
            low, high = place % 2, place // 2
            low = 1 - low if k & 1 else low
            high = 1 - high if k & 2 else high
            return high * 2 + low

        def near(k):
            return lax.rem(group + k, ring)

        sent = []
        conditional = []

        def send(src, dst, send_sem, recv_sem, **to):
            copy = pltpu.make_async_remote_copy(
                src_ref=src, dst_ref=dst, send_sem=send_sem, recv_sem=recv_sem,
                device_id=to, device_id_type=MESH)
            copy.start()
            sent.append(copy)

        def arrived(dst, send_sem, recv_sem, **to):
            pltpu.make_async_remote_copy(
                src_ref=dst, dst_ref=dst, send_sem=send_sem, recv_sem=recv_sem,
                device_id=to, device_id_type=MESH).wait_recv()

        flushes = []
        done = set()

        def flush(src, name):
            done.add(name)
            copy = pltpu.make_async_copy(src, out[name], f_s.at[len(flushes)])
            copy.start()
            flushes.append(copy)

        def slot(piece, share, col, g):
            l, kind = piece // 2, piece % 2
            if kind == 0:
                at = pl.ds(pl.multiple_of(g * head_rows, 16), head_rows)
                return hbuf.at[l, pl.ds(2 * share, 2), col, at]
            at = pl.ds(pl.multiple_of(g * half_units, 16), half_units)
            return ubuf.at[l, :, share, col, at]

        barrier = pltpu.get_barrier_semaphore()
        peers = [dict(tensor=peer(k)) for k in (1, 2, 3)] + [dict(pipe=other)]
        peers += [dict(fsdp=near(k)) for k in range(1, ring)]
        for to in peers:
            pl.semaphore_signal(barrier, inc=1, device_id=to, device_id_type=MESH)
        pl.semaphore_wait(barrier, len(peers))

        mine = pl.ds(pl.multiple_of(group * head_rows, 16), head_rows)
        mine_units = pl.ds(pl.multiple_of(group * half_units, 16), half_units)
        local = [
            pltpu.make_async_copy(heads_ref.at[pl.ds(2 * core, 2)],
                                  hbuf.at[core, pl.ds(2 * core, 2), 0, mine], l_s.at[0]),
            pltpu.make_async_copy(units_ref.at[:, core],
                                  ubuf.at[core, :, core, 0, mine_units], l_s.at[1]),
            pltpu.make_async_copy(inp.at[item],
                                  keep["low0"].at[pl.ds(pl.multiple_of(place * own_rows, 16),
                                                        own_rows)], l_s.at[2]),
            pltpu.make_async_copy(norm_ref, nbuf.at[core], l_s.at[3]),
            pltpu.make_async_copy(cot_ref.at[item],
                                  keep["cot"].at[pl.ds(pl.multiple_of(place * own_rows, 16),
                                                       own_rows)], l_s.at[4]),
        ]
        send(heads_ref.at[pl.ds(2 * other, 2)], hbuf.at[core, pl.ds(2 * other, 2), 0, mine],
             e_s.at[0], e_r.at[0], pipe=other)
        for copy in local:
            copy.start()
        send(units_ref.at[:, other], ubuf.at[core, :, other, 0, mine_units],
             e_s.at[1], e_r.at[1], pipe=other)
        send(norm_ref, nbuf.at[core], e_s.at[2], e_r.at[2], pipe=other)
        for k in (1, 2):
            send(inp.at[(peer(k) // 2) * 2 + core],
                 keep["low0"].at[pl.ds(pl.multiple_of(place * own_rows, 16), own_rows)],
                 i_s.at[k], i_r.at[k], tensor=peer(k))

        reach = [(sign, d) for d in range(1, ring) for sign in (1, -1)]

        def number(sign, d):
            return d if sign > 0 else ring - 1 + d

        def exists(sign, d):
            return group + d < ring if sign > 0 else group >= d

        def when(condition, action):
            @pl.when(condition)
            def _():
                action().start()

            conditional.append((condition, action))

        def hop_on(piece, sign, d):
            here = slot(piece, core, 0, group + sign * d)
            onward = group >= 1 if sign > 0 else group + 1 < ring
            index = number(sign, d)

            def action():
                return pltpu.make_async_remote_copy(
                    src_ref=here, dst_ref=here, send_sem=z_s.at[piece, index],
                    recv_sem=z_r.at[piece, number(sign, d + 1)],
                    device_id={FSDP: group - sign}, device_id_type=MESH)

            return onward, action

        def own_along(piece):
            for sign in (1, -1):
                here = slot(piece, core, 0, group)
                onward = group >= 1 if sign > 0 else group + 1 < ring

                def action(sign=sign):
                    return pltpu.make_async_remote_copy(
                        src_ref=here, dst_ref=here,
                        send_sem=z_s.at[piece, 0 if sign > 0 else 2 * ring - 1],
                        recv_sem=z_r.at[piece, number(sign, 1)],
                        device_id={FSDP: group - sign}, device_id_type=MESH)

                when(onward, action)

        def across(piece, g, index):
            here = slot(piece, core, 0, g)
            to_side = pltpu.make_async_remote_copy(
                src_ref=here, dst_ref=slot(piece, core, 1, g), send_sem=y_s.at[piece, index],
                recv_sem=y_r.at[piece, index], device_id={TENSOR: peer(2)}, device_id_type=MESH)
            to_core = pltpu.make_async_remote_copy(
                src_ref=here, dst_ref=here, send_sem=k_s.at[piece, 0, index],
                recv_sem=k_r.at[piece, 0, index], device_id={PIPE: other}, device_id_type=MESH)
            return to_side, to_core

        def own_across(piece):
            for copy in across(piece, group, 0):
                copy.start()
                sent.append(copy)

        def hop(piece, d):
            for sign in (1, -1):
                index = number(sign, d)
                g = group + sign * d
                condition = exists(sign, d)

                @pl.when(condition)
                def _():
                    arrived(slot(piece, core, 0, g), z_s.at[piece, index], z_r.at[piece, index],
                            fsdp=group + sign)
                    for copy in across(piece, g, index):
                        copy.start()

                if d + 1 < ring:
                    onward, action = hop_on(piece, sign, d)
                    when(jnp.logical_and(condition, onward), action)
                for i in range(2):
                    conditional.append(
                        (condition, lambda i=i, g=g, index=index: across(piece, g, index)[i]))

        def own_second(piece):
            here = slot(piece, core, 1, group)
            arrived(here, y_s.at[piece, 0], y_r.at[piece, 0], tensor=peer(2))
            send(here, here, k_s.at[piece, 1, 0], k_r.at[piece, 1, 0], pipe=other)

        def second(piece, d):
            for sign in (1, -1):
                index = number(sign, d)
                here = slot(piece, core, 1, group + sign * d)
                condition = exists(sign, d)

                def action(here=here, index=index):
                    return pltpu.make_async_remote_copy(
                        src_ref=here, dst_ref=here, send_sem=k_s.at[piece, 1, index],
                        recv_sem=k_r.at[piece, 1, index], device_id={PIPE: other},
                        device_id_type=MESH)

                @pl.when(condition)
                def _():
                    arrived(here, y_s.at[piece, index], y_r.at[piece, index], tensor=peer(2))

                when(condition, action)

        def pass_second(piece):
            own_second(piece)
            for d in range(1, ring):
                second(piece, d)

        def complete(piece):
            for col in range(2):
                arrived(slot(piece, other, col, group), k_s.at[piece, col, 0],
                        k_r.at[piece, col, 0], pipe=other)
                for sign, d in reach:
                    index = number(sign, d)

                    @pl.when(exists(sign, d))
                    def _():
                        arrived(slot(piece, other, col, group + sign * d),
                                k_s.at[piece, col, index], k_r.at[piece, col, index], pipe=other)
            l = piece // 2
            if piece % 2 == 0:
                flush(hbuf.at[l], f"heads{l}")
            else:
                flush(ubuf.at[l], f"units{l}")

        local[0].wait()
        arrived(hbuf.at[other, pl.ds(2 * core, 2), 0, mine],
                e_s.at[0], e_r.at[0], pipe=other)
        own_along(0)
        own_across(0)
        local[1].wait()
        arrived(ubuf.at[other, :, core, 0, mine_units], e_s.at[1], e_r.at[1], pipe=other)

        def part_of(name, l):
            return nbuf[l, name:name + 1, :]

        def exchange(tag):
            index = stages.index(tag)
            send(keep["own_" + tag], keep["got_" + tag], x_s.at[index], x_r.at[index],
                 tensor=peer(1))

        def taken(tag):
            index = stages.index(tag)
            arrived(keep["got_" + tag], x_s.at[index], x_r.at[index], tensor=peer(1))
            return keep["own_" + tag][...].astype(F32) + keep["got_" + tag][...].astype(F32)

        def do_project(l, half):
            at_rows = slice(half * rows, half * rows + rows)
            if l == 0:
                low = keep["low0"][at_rows]
            else:
                summed = keep["mid"][at_rows] + taken(f"f0{half}")
                keep["pre20"][at_rows] = summed
                x = row_norm(summed)[0] * part_of(2, 0) + part_of(3, 0)
                keep["x1"][at_rows] = x
                low = x.astype(BF)
                keep["acts"][0, at_rows] = low
            cosine, sines = cos_ref[at_rows], sin_ref[at_rows]
            for c, name in ((0, "q"), (1, "k")):
                turning = nt(low, hbuf[l, c].reshape(heads, width))
                for slab in range(heads // 128):
                    at = slice(128 * slab, 128 * slab + 128)
                    keep[f"{name}{l}"][at_rows, at] = turned(
                        turning[:, at], cosine, sines).astype(BF)
            keep[f"v{l}"][at_rows] = nt(low, hbuf[l, 2].reshape(heads, width)).astype(BF)

        def do_attend(l, half):
            at_rows = slice(half * rows, half * rows + rows)
            masks = head_masks(rows)
            lane = lax.broadcasted_iota(jnp.int32, (rows, 128), 1)
            same = col_ref[at_rows, :1] == row_ref[:1, :]
            totals = jnp.zeros((rows, 128), F32)
            for slab in range(heads // 128):
                at = slice(128 * slab, 128 * slab + 128)
                q, k, v = keep[f"q{l}"][at_rows, at], keep[f"k{l}"][:, at], keep[f"v{l}"][:, at]
                gathered = jnp.zeros((rows, 128), F32)
                for h in range(2):
                    scores = nt(q * masks[h].astype(BF), k) * HEAD_DIM ** (-0.5)
                    scores = jnp.where(same, scores, masked_value)
                    top = jnp.max(scores, axis=-1, keepdims=True)
                    powers = jnp.exp(scores - top)
                    mass = jnp.sum(powers, axis=-1, keepdims=True)
                    chances = (powers * (1.0 / mass)).astype(BF)
                    gathered = gathered + nn(chances, v) * masks[h]
                    totals = jnp.where(lane == 2 * slab + h, top + jnp.log(mass), totals)
                keep[f"ctx{l}"][at_rows, at] = gathered.astype(BF)
            keep[f"lse{l}"][:, at_rows] = totals.T[:8]
            part = nn(keep[f"ctx{l}"][at_rows], hbuf[l, 3].reshape(heads, width))
            keep[f"own_t{l}{half}"][...] = part.astype(BF)
            exchange(f"t{l}{half}")

        def do_feed(l, half):
            at_rows = slice(half * rows, half * rows + rows)
            x = keep["low0"][at_rows].astype(F32) if l == 0 else keep["x1"][at_rows]
            summed = x + taken(f"t{l}{half}")
            keep[f"pre1{l}"][at_rows] = summed
            middle = row_norm(summed)[0] * part_of(0, l) + part_of(1, l)
            keep["mid"][at_rows] = middle
            low = middle.astype(BF)
            keep[f"spread{l}"][at_rows] = low
            for turn, share in enumerate((core, other)):
                if turn == 1 and half == 0:
                    complete(2 * l + 1)
                at = pl.ds(pl.multiple_of(share * step, 128), step)
                gate = nt(low, ubuf[l, 0, share].reshape(step, width))
                up = nt(low, ubuf[l, 1, share].reshape(step, width))
                keep[f"feed{l}"][0, at_rows, at] = gate.astype(BF)
                keep[f"feed{l}"][1, at_rows, at] = up.astype(BF)
                hidden = (gate * jax.nn.sigmoid(gate) * up).astype(BF)
                keep[f"feed{l}"][2, at_rows, at] = hidden
                fed = nn(hidden, ubuf[l, 2, share].reshape(step, width))
                if turn == 0:
                    acc_ref[...] = fed
                else:
                    keep[f"own_f{l}{half}"][...] = (acc_ref[...] + fed).astype(BF)
            exchange(f"f{l}{half}")

        hop(0, 1)

        def input_rows(k):
            return keep["low0"].at[pl.ds(pl.multiple_of(peer(k) * own_rows, 16), own_rows)]

        for d in range(2, ring):
            if d == 3:
                arrived(input_rows(2), i_s.at[2], i_r.at[2], tensor=peer(2))
                send(input_rows(2), input_rows(2), i_s.at[3], i_r.at[3], tensor=peer(1))
                own_along(1)
                own_across(1)
            hop(0, d)
        if ring < 4:
            own_along(1)
            own_across(1)
        pass_second(0)
        for k in (1, 3):
            arrived(input_rows(k), i_s.at[k], i_r.at[k], tensor=peer(1))
        local[2].wait()
        local[3].wait()
        arrived(nbuf.at[other], e_s.at[2], e_r.at[2], pipe=other)
        complete(0)
        do_project(0, 0)
        do_project(0, 1)
        hop(1, 1)
        own_along(2)
        do_attend(0, 0)
        do_attend(0, 1)
        hop(1, 2)
        own_across(2)
        hop(2, 1)
        own_along(3)
        for d in range(3, ring):
            hop(1, d)
        for d in range(2, ring):
            hop(2, d)
        own_across(3)
        pass_second(1)
        do_feed(0, 0)
        hop(3, 1)
        do_feed(0, 1)
        hop(3, 2)
        pass_second(2)
        complete(2)
        do_project(1, 0)
        for d in range(3, ring):
            hop(3, d)
        do_project(1, 1)
        do_attend(1, 0)
        do_attend(1, 1)
        for k in range(1, count):
            send(cot_ref.at[(peer(k) // 2) * 2 + core],
                 keep["cot"].at[pl.ds(pl.multiple_of(place * own_rows, 16), own_rows)],
                 i_s.at[count + k], i_r.at[count + k], tensor=peer(k))
        pass_second(3)
        do_feed(1, 0)
        do_feed(1, 1)
        flush(nbuf, "norms")
        for name in saved:
            if name not in done and name not in ("pre21", "acts", "cot"):
                flush(keep[name], name)
        local[4].wait()
        for k in range(1, count):
            arrived(keep["cot"].at[pl.ds(pl.multiple_of(peer(k) * own_rows, 16), own_rows)],
                    i_s.at[count + k], i_r.at[count + k], tensor=peer(k))
        for half in range(2):
            at_rows = slice(half * rows, half * rows + rows)
            summed = keep["mid"][at_rows] + taken(f"f1{half}")
            keep["pre21"][at_rows] = summed
            keep["acts"][1, at_rows] = (
                row_norm(summed)[0] * part_of(2, 1) + part_of(3, 1)).astype(BF)
        for name in saved:
            if name not in done:
                flush(keep[name], name)
        for copy in sent:
            copy.wait_send()
        for condition, action in conditional:
            @pl.when(condition)
            def _():
                action().wait_send()

        for copy in flushes:
            copy.wait()

    anywhere = pl.BlockSpec(memory_space=pl.ANY)
    inside = pl.BlockSpec(memory_space=pltpu.VMEM)
    dma = pltpu.SemaphoreType.DMA
    scratch = [pltpu.VMEM(shape, kind) for shape, kind in held.values()]
    scratch += [
        pltpu.VMEM((2, 4, 2, ring * head_rows, width), BF),
        pltpu.VMEM((2, 3, 2, 2, ring * half_units, width), BF),
        pltpu.VMEM((2, 4, width), F32),
        pltpu.VMEM((rows, width), F32),
        dma((4, 2 * ring)), dma((4, 2 * ring)), dma((4, 2 * ring)), dma((4, 2 * ring)),
        dma((4, 2, 2 * ring)), dma((4, 2, 2 * ring)), dma((3,)), dma((3,)),
        dma((len(stages),)), dma((len(stages),)), dma((2 * count,)), dma((2 * count,)),
        dma((5,)), dma((len(outs),)),
    ]
    results = pl.pallas_call(
        forward_kernel,
        in_specs=[anywhere] * 4 + [inside] * 5,
        out_specs=[anywhere] * len(outs),
        out_shape=[jax.ShapeDtypeStruct(shape, kind) for shape, kind in outs.values()],
        scratch_shapes=scratch,
        compiler_params=pltpu.CompilerParams(
            collective_id=0, has_side_effects=True, vmem_limit_bytes=62 << 20),
        name="forward_kernel",
    )(layer_inputs, cotangent, heads_in, units_in, norm_in, segment_column, segment_row, cosine, sines)
    return dict(zip(outs, results))


def backward_all(saved, count, tables):
    segment_column, segment_row, cosine, sines = tables
    ring = lax.axis_size(FSDP)
    total, width = saved["cot"].shape
    own_rows = total // count
    rows = total // 2
    heads = saved["q0"].shape[1]
    step = saved["feed0"].shape[2] // 2
    head_rows = heads // (2 * ring)
    half_units = step // (2 * ring)
    order = sorted(range(1, ring), key=lambda k: min(k, ring - k))
    loaded = ("q", "k", "v", "lse", "pre1", "pre2", "spread", "feed", "heads", "units")
    arrays = [saved[f"{name}{l}"] for l in range(2) for name in loaded]
    arrays += [saved["ctx0"], saved["ctx1"], saved["low0"], saved["acts"], saved["cot"]]
    stages = [f"{stage}{l}{h}" for l in range(2) for stage in "gi" for h in range(2)]
    pieces = "dguhe"
    scaling = HEAD_DIM ** (-0.5)

    def backward_kernel(norm_ref, col_ref, row_ref, cos_ref, sin_ref, *refs):
        n = len(arrays)
        from_hbm = {}
        for l in range(2):
            for i, name in enumerate(loaded):
                from_hbm[f"{name}{l}"] = refs[l * len(loaded) + i]
        from_hbm["ctx0"], from_hbm["ctx1"], from_hbm["low0"], acts_ref, cot_ref = refs[n - 5:n]
        from_hbm["low1"] = acts_ref.at[0]
        (act_out, grad_out, units_out, heads_out, norm_out) = refs[n:n + 5]
        rest = refs[n + 5:]
        buffers = [name for name in loaded if name != "spread"]
        here = dict(zip(buffers, rest[:len(buffers)]))
        (lefts, rights, dpre, wide_rights, dctx, grads, own, got, nsum, nred, nget,
         acc, keep_u, keep_h, give_u, give_h, core_u, core_h, side_u, side_h, line_u, line_h,
         fin_u, fin_h, x_s, x_r, a_s, a_r, b_s, b_r, c_s, c_r, y_s, y_r, z_s, z_r,
         n_s, n_r, j_s, j_r, l_s, m_s, credit_c, credit_y) = rest[len(buffers):]
        dfeed = wide_rights.at[1]
        cot = grads.at[0]
        core = lax.axis_index(PIPE)
        place = lax.axis_index(TENSOR)
        group = lax.axis_index(FSDP)
        other = 1 - core
        item = (place // 2) * 2 + core

        def peer(k):
            low, high = place % 2, place // 2
            low = 1 - low if k & 1 else low
            high = 1 - high if k & 2 else high
            return high * 2 + low

        def near(k):
            return lax.rem(group + k, ring)

        pending = []

        def send(src, dst, send_sem, recv_sem, **to):
            copy = pltpu.make_async_remote_copy(
                src_ref=src, dst_ref=dst, send_sem=send_sem, recv_sem=recv_sem,
                device_id=to, device_id_type=MESH)
            copy.start()
            pending.append(copy)
            return copy

        def arrived(dst, send_sem, recv_sem, **to):
            pltpu.make_async_remote_copy(
                src_ref=dst, dst_ref=dst, send_sem=send_sem, recv_sem=recv_sem,
                device_id=to, device_id_type=MESH).wait_recv()

        def sent(copy):
            copy.wait_send()
            pending[:] = [held for held in pending if held is not copy]

        names = loaded + ("ctx", "low")
        loads = {}

        def load(l, *which):
            for name in which:
                to = {"ctx": lefts.at[3], "low": rights.at[0],
                      "spread": wide_rights.at[0]}.get(name)
                to = here[name] if to is None else to
                copy = pltpu.make_async_copy(from_hbm[f"{name}{l}"], to,
                                             l_s.at[l * len(names) + names.index(name)])
                copy.start()
                loads[name, l] = copy

        def ready(l, *which):
            for name in which:
                loads.pop((name, l)).wait()

        def rows_at(index):
            return pl.ds(pl.multiple_of(index * own_rows, 16), own_rows)

        barrier = pltpu.get_barrier_semaphore()
        peers = [dict(tensor=peer(k)) for k in (1, 2, 3)]
        peers += [dict(pipe=other), dict(pipe=other, tensor=peer(2))]
        peers += [dict(fsdp=near(k)) for k in range(1, ring)]
        for to in peers:
            pl.semaphore_signal(barrier, inc=1, device_id=to, device_id_type=MESH)
        pl.semaphore_wait(barrier, len(peers))

        own_cot = pltpu.make_async_copy(cot_ref, cot, m_s.at[0])
        own_cot.start()
        load(1, "pre2", "feed", "spread", "units", "pre1", "heads", "q", "k", "v", "lse", "ctx",
             "low")

        def home(source, result, sems, index):
            copy = pltpu.make_async_copy(source.at[core, rows_at(place)], result.at[item],
                                         m_s.at[index])
            copy.start()
            for k in range(1, 4):
                layer = other if k & 1 else core
                to = dict(pipe=layer, tensor=peer(k & 2))
                send(source.at[layer, rows_at(peer(k & 2))], result.at[item],
                     sems[0].at[k], sems[1].at[k], **to)
            return copy

        def home_arrived(result, sems):
            for k in range(1, 4):
                to = dict(pipe=other if k & 1 else core, tensor=peer(k & 2))
                index = (peer(k & 2) // 2) * 2 + (other if k & 1 else core)
                arrived(result.at[index], sems[0].at[k], sems[1].at[k], **to)

        own_act = home(acts_ref, act_out, (a_s, a_r), 1)
        own_cot.wait()
        last_use = {}

        def exchange(tag, value):
            place_of = "gi".index(tag[0]) * 2 + int(tag[2])
            if place_of in last_use:
                sent(last_use[place_of])
            own[place_of] = value
            index = stages.index(tag)
            last_use[place_of] = send(own.at[place_of], got.at[index], x_s.at[index],
                                      x_r.at[index], tensor=peer(1))

        def taken(tag):
            index = stages.index(tag)
            place_of = "gi".index(tag[0]) * 2 + int(tag[2])
            arrived(got.at[index], x_s.at[index], x_r.at[index], tensor=peer(1))
            return own[place_of].astype(F32) + got[index].astype(F32)

        def part_of(name, l):
            return norm_ref[l, name:name + 1, :]

        def note_sums(l, half, first, sums):
            if half == 0:
                nsum[l, first:first + 2] = sums[:2]
            else:
                nsum[l, first:first + 2] = nsum[l, first:first + 2] + sums[:2]

        def do_norm_back(l, half):
            at_rows = slice(half * rows, half * rows + rows)
            if l == 1:
                upstream = cot[at_rows].astype(F32)
            else:
                upstream = dpre[at_rows] + taken(f"i1{half}")
                grads[1, at_rows] = upstream.astype(BF)
            if half == 0:
                ready(l, "pre2")
            normed, inverse = row_norm(here["pre2"][at_rows])
            through, sums = row_norm_back(normed, inverse, part_of(2, l), upstream)
            note_sums(l, half, 2, sums)
            dpre[at_rows] = through
            dfeed[at_rows] = through.astype(BF)

        def do_feed_back(l, half):
            at_rows = slice(half * rows, half * rows + rows)
            low = dfeed[at_rows]
            if half == 0:
                ready(l, "units")
            units, feed_ref = here["units"], here["feed"]
            for share in range(2):
                at = slice(share * step, share * step + step)
                gate = feed_ref[0, at_rows, at].astype(F32)
                up = feed_ref[1, at_rows, at].astype(F32)
                grad_hidden = nt(low, units[2, share].reshape(step, width))
                sigmoid = jax.nn.sigmoid(gate)
                grad_gate = (
                    grad_hidden * up * sigmoid * (1.0 + gate * (1.0 - sigmoid))).astype(BF)
                grad_up = (grad_hidden * gate * sigmoid).astype(BF)
                feed_ref[0, at_rows, at] = grad_gate
                feed_ref[1, at_rows, at] = grad_up
                back = nn(grad_gate, units[0, share].reshape(step, width))
                back = back + nn(grad_up, units[1, share].reshape(step, width))
                if share == 0:
                    acc[...] = back
                else:
                    exchange(f"g{l}{half}", (acc[...] + back).astype(BF))

        def unit_grads(first, end, share, target):
            size = step // 2

            def one(i, _):
                c, col = i // 2, i % 2
                at = pl.ds(pl.multiple_of(share * step + col * size, 128), size)
                target[c, col] = tn(here["feed"][c, :, at], wide_rights[c // 2]).astype(BF)
                return 0

            lax.fori_loop(2 * first, 2 * end, one, 0)

        def head_grad(share, i, target):
            j = 2 * share + i
            full = tn(lefts[j], rights[j // 3]).astype(BF)
            for col in range(2):
                target[i, col] = full[col * (heads // 2):(col + 1) * (heads // 2)]

        def do_attend_back(l, half):
            at_rows = slice(half * rows, half * rows + rows)
            if half == 0:
                ready(l, "pre1", "heads", "q", "k", "v", "lse")
            upstream = dpre[at_rows] + taken(f"g{l}{half}")
            normed, inverse = row_norm(here["pre1"][at_rows])
            through, sums = row_norm_back(normed, inverse, part_of(0, l), upstream)
            note_sums(l, half, 0, sums)
            dpre[at_rows] = through
            low = through.astype(BF)
            rights[1, at_rows] = low
            dctx[...] = nt(low, here["heads"][3].reshape(heads, width)).astype(BF)
            masks = head_masks(rows)
            wide_masks = head_masks(total)
            same = col_ref[:, :1] == row_ref[:1, at_rows]
            for slab in range(heads // 128):
                at = slice(slab * 128, slab * 128 + 128)
                second_at = slice(heads + slab * 128, heads + slab * 128 + 128)
                q, k = here["q"][at_rows, at], here["k"][:, at]
                v, grad_ctx = here["v"][:, at], dctx[:, at]
                dq = jnp.zeros((rows, 128), F32)
                dk = jnp.zeros((total, 128), F32)
                dv = jnp.zeros((total, 128), F32)
                for h in range(2):
                    mask = masks[h].astype(BF)
                    scores = nt(k, q * mask) * scaling
                    scores = jnp.where(same, scores, masked_value)
                    lse = here["lse"][2 * slab + h:2 * slab + h + 1, at_rows]
                    chances = jnp.exp(scores - lse)
                    grad_chances = nt(v, grad_ctx * mask)
                    row_dot = jnp.sum(chances * grad_chances, axis=0, keepdims=True)
                    grad_scores = (chances * (grad_chances - row_dot)).astype(BF)
                    dv = dv + nn(chances.astype(BF), grad_ctx) * wide_masks[h]
                    dk = dk + nn(grad_scores, q) * wide_masks[h]
                    dq = dq + tn(grad_scores, k) * masks[h]
                lefts[0, at_rows, at] = turned(
                    dq * scaling, cos_ref[at_rows], -sin_ref[at_rows]).astype(BF)
                if half == 0:
                    here["pre2"][:, at] = dk
                    here["pre2"][:, second_at] = dv
                else:
                    dk = here["pre2"][:, at] + dk
                    dv = here["pre2"][:, second_at] + dv
                    lefts[1, :, at] = turned(dk * scaling, cos_ref[...], -sin_ref[...]).astype(BF)
                    lefts[2, :, at] = dv.astype(BF)

        def do_inputs_back(l, half):
            at_rows = slice(half * rows, half * rows + rows)
            back = jnp.zeros((rows, width), F32)
            for c in range(3):
                back = back + nn(lefts[c, at_rows], here["heads"][c].reshape(heads, width))
            exchange(f"i{l}{half}", back.astype(BF))

        def parts(piece, units_ref, heads_ref):
            index = pieces.index(piece)
            if index > 2:
                return heads_ref.at[index - 3:index - 2]
            return units_ref.at[(2, 0, 1)[index]:(3, 1, 2)[index]]

        def cell(piece, l):
            return l * 5 + pieces.index(piece)

        gave = {}

        def give(l, piece):
            if l == 0:
                pl.semaphore_wait(credit_c.at[pieces.index(piece)], 1)
            index = cell(piece, l)
            gave[piece] = send(parts(piece, give_u, give_h), parts(piece, core_u, core_h),
                               c_s.at[index], c_r.at[index], pipe=other)

        def add_core(l, piece):
            index = cell(piece, l)
            come = parts(piece, core_u, core_h)
            arrived(come, c_s.at[index], c_r.at[index], pipe=other)
            mine = parts(piece, keep_u.at[l], keep_h.at[l])
            mine[...] = (mine[...].astype(F32) + come[...].astype(F32)).astype(BF)
            if l == 1:
                pl.semaphore_signal(credit_c.at[pieces.index(piece)], inc=1,
                                    device_id=dict(pipe=other), device_id_type=MESH)
            else:
                pl.semaphore_wait(credit_y.at[pieces.index(piece)], 1)
            send(mine.at[:, 1], parts(piece, side_u, side_h), y_s.at[index], y_r.at[index],
                 tensor=peer(2))

        def slot_of(piece, ref, g):
            size = head_rows if piece in "he" else half_units
            return ref.at[:, pl.ds(pl.multiple_of(g * size, 16), size)]

        def add_side(l, piece):
            index = cell(piece, l)
            come = parts(piece, side_u, side_h)
            arrived(come, y_s.at[index], y_r.at[index], tensor=peer(2))
            mine = parts(piece, keep_u.at[l], keep_h.at[l]).at[:, 0]
            mine[...] = (mine[...].astype(F32) + come[...].astype(F32)).astype(BF)
            if l == 1:
                pl.semaphore_signal(credit_y.at[pieces.index(piece)], inc=1,
                                    device_id=dict(tensor=peer(2)), device_id_type=MESH)
            @pl.when(at_end)
            def _():
                to_relay(l, piece).start()

            for sign in (1, -1):
                @pl.when(inner(sign))
                def _():
                    next_one(l, piece, sign).start()

            @pl.when(at_end)
            def _():
                to_far(l, piece).start()

        at_end = jnp.logical_or(group == 0, group == ring - 1)

        def inner(sign):
            return group + 1 < ring if sign > 0 else group >= 1

        def line_send(l, piece, g, kind, to):
            index = cell(piece, l)
            mine = parts(piece, keep_u.at[l], keep_h.at[l]).at[:, 0]
            return pltpu.make_async_remote_copy(
                src_ref=slot_of(piece, mine, g),
                dst_ref=parts(piece, line_u.at[l, kind], line_h.at[l, kind]),
                send_sem=z_s.at[index, kind], recv_sem=z_r.at[index, kind],
                device_id={FSDP: to}, device_id_type=MESH)

        def next_one(l, piece, sign):
            return line_send(l, piece, group + sign, 0 if sign > 0 else 1, group + sign)

        def far():
            return lax.rem(group + 2, 4)

        def to_far(l, piece):
            return line_send(l, piece, far(), 2, far())

        def to_relay(l, piece):
            opposite = ring - 1 - group
            return line_send(l, piece, opposite, 3, jnp.where(group == 0, 1, 2))

        def relay(l, piece):
            @pl.when(jnp.logical_not(at_end))
            def _():
                index = cell(piece, l)
                come = parts(piece, line_u.at[l, 3], line_h.at[l, 3])
                arrived(come, z_s.at[index, 3], z_r.at[index, 3],
                        fsdp=jnp.where(group == 1, 0, 3))
                mine = slot_of(piece, parts(piece, keep_u.at[l], keep_h.at[l]).at[:, 0], far())
                mine[...] = (mine[...].astype(F32) + come[...].astype(F32)).astype(BF)
                to_far(l, piece).start()

        def add_line(l, piece):
            index = cell(piece, l)
            mine = parts(piece, keep_u.at[l], keep_h.at[l]).at[:, 0]
            result = parts(piece, fin_u.at[l], fin_h.at[l])
            come = [parts(piece, line_u.at[l, kind], line_h.at[l, kind]) for kind in range(3)]
            arrived(come[2], z_s.at[index, 2], z_r.at[index, 2], fsdp=far())
            result[...] = (slot_of(piece, mine, group)[...].astype(F32)
                           + come[2][...].astype(F32)).astype(BF)
            for sign in (1, -1):
                kind = 0 if sign > 0 else 1

                @pl.when(inner(-sign))
                def _():
                    arrived(come[kind], z_s.at[index, kind], z_r.at[index, kind],
                            fsdp=group - sign)
                    result[...] = (result[...].astype(F32)
                                   + come[kind][...].astype(F32)).astype(BF)

        def line_sent(l, piece):
            for sign in (1, -1):
                @pl.when(inner(sign))
                def _():
                    next_one(l, piece, sign).wait_send()

            to_far(l, piece).wait_send()

            @pl.when(at_end)
            def _():
                to_relay(l, piece).wait_send()

        do_norm_back(1, 0)
        do_norm_back(1, 1)
        ready(1, "feed", "spread")
        unit_grads(2, 3, other, give_u)
        give(1, "d")
        unit_grads(2, 3, core, keep_u.at[1])
        do_feed_back(1, 0)
        add_core(1, "d")
        do_feed_back(1, 1)
        unit_grads(0, 1, other, give_u)
        give(1, "g")
        unit_grads(1, 2, other, give_u)
        give(1, "u")
        unit_grads(0, 1, core, keep_u.at[1])
        do_attend_back(1, 0)
        add_core(1, "g")
        unit_grads(1, 2, core, keep_u.at[1])
        load(0, "feed", "spread", "units")
        add_side(1, "d")
        add_core(1, "u")
        do_attend_back(1, 1)
        load(0, "pre2")
        for half in range(2):
            do_inputs_back(1, half)
        ready(1, "ctx", "low")
        head_grad(other, 0, give_h)
        give(1, "h")
        head_grad(other, 1, give_h)
        give(1, "e")
        head_grad(core, 0, keep_h.at[1])
        head_grad(core, 1, keep_h.at[1])
        load(0, "pre1", "heads", "q", "k", "v", "lse", "ctx", "low")
        relay(1, "d")
        add_core(1, "h")
        add_core(1, "e")

        do_norm_back(0, 0)
        ready(0, "feed", "spread")
        do_feed_back(0, 0)
        add_side(1, "g")
        do_norm_back(0, 1)
        sent(gave["d"])
        unit_grads(2, 3, other, give_u)
        give(0, "d")
        unit_grads(2, 3, core, keep_u.at[0])
        do_feed_back(0, 1)
        add_core(0, "d")
        relay(1, "g")
        sent(gave["g"])
        unit_grads(0, 1, other, give_u)
        give(0, "g")
        sent(gave["u"])
        unit_grads(1, 2, other, give_u)
        give(0, "u")
        unit_grads(0, 1, core, keep_u.at[0])
        add_side(1, "u")
        add_core(0, "g")
        unit_grads(1, 2, core, keep_u.at[0])
        do_attend_back(0, 0)
        add_core(0, "u")
        relay(1, "u")
        add_side(1, "h")
        add_side(1, "e")
        do_attend_back(0, 1)
        send(nsum.at[other], nget.at[0], n_s.at[0], n_r.at[0], pipe=other)
        ready(0, "ctx", "low")
        sent(gave["h"])
        head_grad(other, 0, give_h)
        give(0, "h")
        sent(gave["e"])
        head_grad(other, 1, give_h)
        give(0, "e")
        head_grad(core, 0, keep_h.at[0])
        do_inputs_back(0, 0)
        add_core(0, "h")
        head_grad(core, 1, keep_h.at[0])
        do_inputs_back(0, 1)
        add_core(0, "e")
        relay(1, "h")
        relay(1, "e")
        add_side(0, "d")
        arrived(nget.at[0], n_s.at[0], n_r.at[0], pipe=other)
        nred[0] = nsum[core] + nget[0]
        send(nred.at[0], nget.at[1], n_s.at[1], n_r.at[1], tensor=peer(2))
        add_side(0, "g")
        relay(0, "d")

        def finish_rows(half):
            at_rows = slice(half * rows, half * rows + rows)
            grads[0, at_rows] = (dpre[at_rows] + taken(f"i0{half}")).astype(BF)

        finish_rows(0)
        relay(0, "g")
        add_side(0, "u")
        finish_rows(1)
        own_grad = home(grads, grad_out, (b_s, b_r), 2)
        arrived(nget.at[1], n_s.at[1], n_r.at[1], tensor=peer(2))
        nred[1] = nred[0] + nget[1]
        for k in order:
            send(nred.at[1], nget.at[1 + (ring - k) % ring], n_s.at[1 + k],
                 n_r.at[1 + (ring - k) % ring], fsdp=near(k))
        for piece in pieces[:3]:
            add_line(1, piece)
        relay(0, "u")
        add_side(0, "h")
        add_line(1, "h")
        add_line(1, "e")
        add_side(0, "e")
        add_line(0, "d")
        relay(0, "h")
        add_line(0, "g")
        relay(0, "e")
        norms = nred[1]
        for k in order:
            arrived(nget.at[1 + k], n_s.at[1 + k], n_r.at[1 + k], fsdp=near(k))
            norms = norms + nget[1 + k]
        norm_out[...] = norms
        add_line(0, "u")
        add_line(0, "h")
        add_line(0, "e")
        joins = []
        for i, (fin, result) in enumerate(((fin_u, units_out), (fin_h, heads_out))):
            send(fin.at[other], result.at[core], j_s.at[i], j_r.at[i], pipe=other)
            copy = pltpu.make_async_copy(fin.at[core], result.at[core], m_s.at[3 + i])
            copy.start()
            joins.append(copy)
        for i, result in enumerate((units_out, heads_out)):
            arrived(result.at[other], j_s.at[i], j_r.at[i], pipe=other)
        home_arrived(act_out, (a_s, a_r))
        home_arrived(grad_out, (b_s, b_r))
        for copy in [own_act, own_grad] + joins:
            copy.wait()
        for copy in pending:
            copy.wait_send()
        for l in range(2):
            for piece in pieces:
                line_sent(l, piece)

    anywhere = pl.BlockSpec(memory_space=pl.ANY)
    inside = pl.BlockSpec(memory_space=pltpu.VMEM)
    dma = pltpu.SemaphoreType.DMA
    scratch = [pltpu.VMEM(saved[f"{name}0"].shape, saved[f"{name}0"].dtype) for name in loaded
               if name != "spread"]
    scratch += [
        pltpu.VMEM((4, total, heads), BF), pltpu.VMEM((2, total, width), BF),
        pltpu.VMEM((total, width), F32), pltpu.VMEM((2, total, width), BF),
        pltpu.VMEM((rows, heads), BF),
        pltpu.VMEM((2, total, width), BF),
        pltpu.VMEM((4, rows, width), BF), pltpu.VMEM((8, rows, width), BF),
        pltpu.VMEM((2, 4, width), F32), pltpu.VMEM((2, 4, width), F32),
        pltpu.VMEM((1 + ring, 4, width), F32), pltpu.VMEM((rows, width), F32),
        pltpu.VMEM((2, 3, 2, ring * half_units, width), BF),
        pltpu.VMEM((2, 2, 2, ring * head_rows, width), BF),
        pltpu.VMEM((3, 2, ring * half_units, width), BF),
        pltpu.VMEM((2, 2, ring * head_rows, width), BF),
        pltpu.VMEM((3, 2, ring * half_units, width), BF),
        pltpu.VMEM((2, 2, ring * head_rows, width), BF),
        pltpu.VMEM((3, ring * half_units, width), BF),
        pltpu.VMEM((2, ring * head_rows, width), BF),
        pltpu.VMEM((2, ring, 3, half_units, width), BF),
        pltpu.VMEM((2, ring, 2, head_rows, width), BF),
        pltpu.VMEM((2, 3, half_units, width), BF),
        pltpu.VMEM((2, 2, head_rows, width), BF),
        dma((8,)), dma((8,)), dma((4,)), dma((4,)), dma((4,)), dma((4,)),
        dma((10,)), dma((10,)), dma((10,)), dma((10,)), dma((10, 4)), dma((10, 4)),
        dma((1 + ring,)), dma((1 + ring,)), dma((2,)), dma((2,)),
        dma((2 * (len(loaded) + 2),)), dma((5,)),
        pltpu.SemaphoreType.REGULAR((5,)), pltpu.SemaphoreType.REGULAR((5,)),
    ]
    return pl.pallas_call(
        backward_kernel,
        in_specs=[inside] * 5 + [anywhere] * len(arrays),
        out_specs=[anywhere] * 4 + [inside],
        out_shape=[
            jax.ShapeDtypeStruct((count, own_rows, width), BF),
            jax.ShapeDtypeStruct((count, own_rows, width), BF),
            jax.ShapeDtypeStruct((2, 3, half_units, width), BF),
            jax.ShapeDtypeStruct((2, 2, head_rows, width), BF),
            jax.ShapeDtypeStruct((4, width), F32),
        ],
        scratch_shapes=scratch,
        compiler_params=pltpu.CompilerParams(
            collective_id=1, has_side_effects=True, vmem_limit_bytes=67043328),
        name="backward_kernel",
    )(saved["norms"], segment_column, segment_row, cosine, sines, *arrays)


def to_item(array, core, place):
    def piece(k):
        return lax.dynamic_index_in_dim(array, ((place ^ k) & 2) | core, 0, keepdims=False)

    parts = [piece(0)] + [flip(piece(k), TENSOR, k) for k in range(1, 4)]
    return jnp.concatenate(unxor(parts, place), axis=0)


def from_item(by_layer, core, place):
    rows = by_layer[0].shape[0] // 4
    mine = jnp.where(core == 0, by_layer[0], by_layer[1])
    other = jnp.where(core == 0, by_layer[1], by_layer[0])

    def piece(k):
        target = place ^ (k & 2)
        return lax.dynamic_slice_in_dim(other if k & 1 else mine, target * rows, rows, 0)

    parts = [piece(0)] + [mixed_flip(piece(k), k & 1, k & 2) for k in range(1, 4)]
    return jnp.stack(unxor(parts, (place & 2) | core)).astype(F32)


def whole_step(
    layer_inputs,
    cotangent,
    input_master,
    output_master,
    gate_master,
    down_master,
    norm_tables,
    document_lengths,
):
    core = lax.axis_index(PIPE)
    place = lax.axis_index(TENSOR)
    group = lax.axis_index(FSDP)
    ring = lax.axis_size(FSDP)
    width = layer_inputs.shape[2]
    head_rows = input_master.shape[2]
    units = down_master.shape[1]
    half = units // 2
    first_core = core == 0

    item = (place & 2) | core
    lengths = lax.dynamic_index_in_dim(document_lengths[:, 0, :], item, 0, keepdims=False)
    segment, position = segment_info(lengths)
    segment_column = jnp.broadcast_to(segment[:, None], (MB_CAP, 128))
    segment_row = jnp.broadcast_to(segment[None, :], (8, MB_CAP))
    tables = (segment_column, segment_row) + rotary_tables(position)

    def split_by_core(for_first, for_second):
        keep = jnp.where(first_core, for_first, for_second)
        got = flip(jnp.where(first_core, for_second, for_first), PIPE, 1)
        return [jnp.where(first_core, keep, got), jnp.where(first_core, got, keep)]

    def joined_by_core(share_zero, share_one):
        keep = jnp.where(first_core, share_zero, share_one)
        got = flip(jnp.where(first_core, share_one, share_zero), PIPE, 1)
        return jnp.where(first_core, keep, got), jnp.where(first_core, got, keep)

    if head_rows % 16 == 0 and half % 16 == 0 and ring == 4:
        heads_in = jnp.concatenate([input_master[0], output_master], axis=0).astype(BF)
        units_in = jnp.concatenate([gate_master[0], down_master], axis=0).astype(BF)
        saved = forward_all(layer_inputs, cotangent, heads_in, units_in.reshape(3, 2, half, width),
                            norm_tables[0], tables)
        results = backward_all(saved, cotangent.shape[0], tables)
        activations, gradients_in, unit_grad, head_grad, norm_sum = results
        head_grad = head_grad.reshape(4, head_rows, width).astype(F32)
        unit_grad = unit_grad.transpose(1, 0, 2, 3).reshape(3, units, width).astype(F32)
        return (
            activations[None].astype(F32),
            gradients_in[None].astype(F32),
            head_grad[None, :3],
            head_grad[None, 3],
            unit_grad[None, :2],
            unit_grad[None, 2],
            norm_sum[None],
        )

    in_low = input_master[0].astype(BF)
    out_low = output_master.astype(BF)
    head_shares = split_by_core(in_low[:2], jnp.concatenate([in_low[2:], out_low], axis=0))
    unit_low = jnp.concatenate([gate_master[0], down_master], axis=0).astype(BF)
    unit_shares = split_by_core(unit_low[:, :half], unit_low[:, half:])

    x = to_item(layer_inputs, core, place)
    norm_own = norm_tables[0]
    norm_other = flip(norm_own, PIPE, 1)
    norms = [
        jnp.where(first_core, norm_own, norm_other),
        jnp.where(first_core, norm_other, norm_own),
    ]

    quarter = half // 2
    rows = ring * head_rows

    def gather_heads(s, *waits):
        slots = ring_gather(tied(head_shares[s], *waits), f"h{s}")
        ascending = jnp.stack(slots[::-1] + slots[::-1])
        column = lax.dynamic_slice_in_dim(ascending, ring - 1 - group, ring, 0)
        return column.transpose(1, 0, 2, 3).reshape(2, rows, width)

    def head_weights(parts):
        mine = jnp.concatenate(parts[:2], axis=1)
        theirs = jnp.concatenate(parts[2:], axis=1)
        low = jnp.where(first_core, mine, theirs)
        high = jnp.where(first_core, theirs, mine)
        return jnp.concatenate([low, high[:1]], axis=0), high[1]

    def gather_units(s, i, *waits):
        piece = unit_shares[s][:, i * quarter:i * quarter + quarter]
        return jnp.concatenate(ring_gather(tied(piece, *waits), f"u{s}{i}"), axis=1)

    def in_order(pieces):
        return [pieces[i][j] for j in range(4) for i in range(2)]

    column = gather_heads(0)
    heads = spread_out(column, "h0")
    unit_a = gather_units(0, 0, column)
    pieces = [spread_out(unit_a, "u00")]
    unit_b = gather_units(0, 1, unit_a, heads[1])
    pieces.append(spread_out(unit_b, "u01"))
    weights = head_weights(heads) + (in_order(pieces),)
    layers = [weights]
    halves = attention_forward("0", [(tied(x, unit_a),), (x,)], weights, None, tables)
    column = gather_heads(1, unit_b, halves[1][1][0], pieces[0][1])
    heads = spread_out(column, "h1")
    next_a = gather_units(1, 0, column)
    next_pieces = [spread_out(next_a, "u10")]
    next_b = gather_units(1, 1, next_a, heads[1])
    next_pieces.append(spread_out(next_b, "u11"))
    layers.append(head_weights(heads) + (in_order(next_pieces),))
    ends, saved = feed_forward("0", halves, weights, norms[0], (column,), ())
    kept = [saved]
    ends[0] = (tied(ends[0][0], next_a),) + ends[0][1:]
    halves = attention_forward("1", ends, layers[1], norms[0], tables, (next_b,))
    ends, saved = feed_forward("1", halves, layers[1], norms[1], (), ())
    kept.append(saved)
    upstream = to_item(cotangent, core, place)

    def pull_units(tag, gate_up, down):
        parts = []
        for name, grad, count in (("u", gate_up, 2), ("d", down, 1)):
            own = grad[0].reshape(count, 2, ring * half, width)
            got = cross(grad[1], PIPE, 1, f"c_g{name}{tag}").reshape(count, 2, ring * half, width)
            parts.append([added(own[:, 1], got[:, 1]), (own[:, 0], got[:, 0])])
        return parts[0][0], parts[1][0], parts[0][1], parts[1][1]

    def cross_units(tag, units):
        columns = []
        for name, neighbour, (own, got) in (("u", units[0], units[2]), ("d", units[1], units[3])):
            other = cross(neighbour, TENSOR, 2, f"y_g{name}{tag}")
            column = own.astype(F32) + got.astype(F32) + other.astype(F32)
            columns.append(column.astype(BF))
        return columns

    def ring_units(tag, columns):
        totals = []
        for name, column in zip("ud", columns):
            count = column.shape[0]
            column = column.reshape(count, 2, ring, quarter, width)
            total = ring_reduce([column[:, :, k] for k in range(ring)], f"g{name}{tag}")
            totals.append(total.reshape(count, half, width).astype(BF))
        return jnp.concatenate(totals, axis=0)

    def pull_heads(tag, grad_in, grad_out):
        low = jnp.stack(grad_in[:2])
        high = jnp.stack([grad_in[2], grad_out])
        mine = jnp.where(first_core, low, high)
        theirs = cross(jnp.where(first_core, high, low), PIPE, 1, "c_gh" + tag)
        return added(mine[:, rows:], theirs[:, rows:]), mine[:, :rows], theirs[:, :rows]

    def cross_heads(tag, heads):
        neighbour, own, got = heads
        column = own.astype(F32) + got.astype(F32)
        column = column + cross(neighbour, TENSOR, 2, "y_gh" + tag).astype(F32)
        return column.astype(BF)

    def ring_heads(tag, column):
        column = column.reshape(2, ring, head_rows, width).transpose(1, 0, 2, 3)
        ascending = jnp.concatenate([column, column], axis=0)
        rolled = lax.dynamic_slice_in_dim(ascending, (group + 1) % ring, ring, 0)
        return ring_reduce([rolled[ring - 1 - k] for k in range(ring)], "gh" + tag).astype(BF)

    head_totals = [None, None]
    unit_totals = [None, None]
    edges = [None, None]
    norm_grads = [None, None]
    ends = [(upstream,), (upstream,)]
    waits = ()
    for s in (1, 0):
        tag = str(s)
        ends, edges[s], units, heads, norm_grads[s] = layer_backward(
            tag, ends, layers[s], norms[s], tables, kept[s], pull_units, pull_heads, waits
        )
        crossed = cross_units(tag, units)
        unit_totals[s] = ring_units(tag, crossed)
        head_columns = cross_heads(tag, heads)
        head_totals[s] = ring_heads(tag, head_columns)
        waits = crossed
    first_grad = jnp.concatenate(
        [
            (grad[half * MB_CAP // 2:(half + 1) * MB_CAP // 2] + own.astype(F32) + got.astype(F32))
            for half, (grad, own, got) in enumerate(ends)
        ],
        axis=0,
    ).astype(BF)
    activations = from_item([kept[1][1], edges[1]], core, place)
    gradients_in = from_item([first_grad, edges[0]], core, place)

    low, high = joined_by_core(head_totals[0], head_totals[1])
    unit_low, unit_high = joined_by_core(unit_totals[0], unit_totals[1])
    unit_grad = jnp.concatenate([unit_low, unit_high], axis=1).astype(F32)
    head_grad = jnp.concatenate([low, high], axis=0).astype(F32)
    norm_grads[0] = tied(norm_grads[0], heads[0])
    norm_own = jnp.where(first_core, norm_grads[0], norm_grads[1])
    norm_other = jnp.where(first_core, norm_grads[1], norm_grads[0])
    norm_sum = norm_own + flip(norm_other, PIPE, 1)
    norm_sum = norm_sum + flip(norm_sum, TENSOR, 2)
    bit = 1
    while bit < ring:
        norm_sum = norm_sum + flip(norm_sum, FSDP, bit)
        bit = bit * 2
    return (
        activations[None],
        gradients_in[None],
        head_grad[None, :3],
        head_grad[None, 3],
        unit_grad[None, :2],
        unit_grad[None, 2],
        norm_sum[None],
    )


def solution(mesh):
    placed = (
        P(None, (FSDP, TENSOR), None),
        P(None, (FSDP, TENSOR), None),
        P(PIPE, None, (TENSOR, FSDP), None),
        P(PIPE, (TENSOR, FSDP), None),
        P(PIPE, None, (TENSOR, FSDP), None),
        P(PIPE, (TENSOR, FSDP), None),
        P(PIPE, None, None),
        P(None, FSDP, None),
    )
    return jax.shard_map(
        whole_step,
        mesh=mesh,
        in_specs=placed,
        out_specs=(
            P(PIPE, None, (FSDP, TENSOR), None),
            P(PIPE, None, (FSDP, TENSOR), None),
            P(PIPE, None, (TENSOR, FSDP), None),
            P(PIPE, (TENSOR, FSDP), None),
            P(PIPE, None, (TENSOR, FSDP), None),
            P(PIPE, (TENSOR, FSDP), None),
            P(PIPE, None, None),
        ),
        check_vma=False,
    )
```
